32 devices in a mesh: fsdp: 8 (over y, x, core), ctx: 4 (over z).
Axes of the slice: x: 2, y: 2, z: 4, core: 2. Of those that a mesh axis runs over, the one named last changes fastest.
Arguments:
- hidden_in: bfloat16 [8, 512, 1024], P('fsdp', 'ctx'), may hold values from -24 to 24
- block_order: int32 [8, 8], P('fsdp'), may hold values from 0 to 7, each once within a row
- cotangent: bfloat16 [8, 512, 1024], P('fsdp', 'ctx'), may hold values from -6 to 6
- q_weight: bfloat16 [1024, 2048], P(('fsdp', 'ctx')), may hold values from -0.1875 to 0.1875
- k_weight: bfloat16 [1024, 1024], P(('fsdp', 'ctx')), may hold values from -0.1875 to 0.1875
- v_weight: bfloat16 [1024, 1024], P(('fsdp', 'ctx')), may hold values from -0.1875 to 0.1875
- o_weight: bfloat16 [1024, 2048], P(('fsdp', 'ctx')), may hold values from -1.5 to 1.5
- attn_gain: bfloat16 [1024], P(('fsdp', 'ctx')), may hold values from 0.5 to 1.5
- query_gain: bfloat16 [128], P(('fsdp', 'ctx')), may hold values from 0.5 to 1.5
- key_gain: bfloat16 [128], P(('fsdp', 'ctx')), may hold values from 0.5 to 1.5
- mlp_gain: bfloat16 [1024], P(('fsdp', 'ctx')), may hold values from 0.5 to 1.5
- gate_weight: bfloat16 [1024, 3072], P(('fsdp', 'ctx')), may hold values from -0.1875 to 0.1875
- up_weight: bfloat16 [1024, 3072], P(('fsdp', 'ctx')), may hold values from -0.1875 to 0.1875
- down_weight: bfloat16 [1024, 3072], P(('fsdp', 'ctx')), may hold values from -0.109375 to 0.109375
Outputs:
- hidden_out: bfloat16 [8, 512, 1024], P('fsdp', 'ctx')
- input_grad: float32 [8, 512, 1024], P('fsdp', 'ctx')
- q_grad: float32 [1024, 2048], P(('fsdp', 'ctx'))
- k_grad: float32 [1024, 1024], P(('fsdp', 'ctx'))
- v_grad: float32 [1024, 1024], P(('fsdp', 'ctx'))
- o_grad: float32 [1024, 2048], P(('fsdp', 'ctx'))
- attn_gain_grad: float32 [1024], P(('fsdp', 'ctx'))
- query_gain_grad: float32 [128], P(('fsdp', 'ctx'))
- key_gain_grad: float32 [128], P(('fsdp', 'ctx'))
- mlp_gain_grad: float32 [1024], P(('fsdp', 'ctx'))
- gate_grad: float32 [1024, 3072], P(('fsdp', 'ctx'))
- up_grad: float32 [1024, 3072], P(('fsdp', 'ctx'))
- down_grad: float32 [1024, 3072], P(('fsdp', 'ctx'))
The draws below stay inside these ranges and needn't reach their ends.
Inputs may be any that keep to these rules, and one draw needn't show every extreme that they name: `block_order`: each row is a permutation: every position block of a sequence sits in exactly one slot.
All inputs are finite; a program needn't handle non-finite values.
Results may differ from the reference program's by a relative error of at most 0.023.
Values may be sent and summed in bfloat16 or wider, within the bound.
A program may use at most 256 MiB of HBM per device.

```python
import math
import jax
import jax.numpy as jnp
from jax import lax

D = 1024
HEADS = 16
KV_HEADS = 8
HEAD_DIM = 128
FF = 3072
SEQS = 8
LEN = 512
SLOTS = 8
BLOCK = 64


def draw_hidden_in(key, part):
    base_key = jax.random.fold_in(key, 11)
    keys_list = jax.random.split(base_key, 3)
    row_scale = jnp.exp(jax.random.uniform(keys_list[1], (SEQS, LEN, 1), jnp.float32, -1.15, 1.15))
    column_scale = jnp.exp(jax.random.uniform(keys_list[2], (1, 1, D), jnp.float32, -1.15, 1.15))
    signal = jax.random.normal(keys_list[0], (SEQS, LEN, D), jnp.float32)
    return jnp.clip(0.5 * signal * row_scale * column_scale, -24.0, 24.0).astype(jnp.bfloat16)


def block_levels(own_key, shape, shards, low, high):
    def one(position, parts):
        steps = jax.random.uniform(jax.random.fold_in(jax.random.fold_in(own_key, 6), position), (parts,), jnp.float32, low / len(shards), high / len(shards))
        return jnp.repeat(jnp.exp(steps), shape[position] // parts).reshape((-1,) + (1,) * (len(shape) - position - 1))

    factor_of = one(*shards[0])
    for cut in shards[1:]:
        factor_of = factor_of * one(*cut)
    return factor_of


def normal_values(rng, shape, spread, most, cuts=(), held_as=jnp.bfloat16):
    entries = jax.random.normal(rng, shape, jnp.float32) * spread
    if len(cuts) > 0:
        entries = block_levels(rng, shape, cuts, -0.22, 0.18) * entries
    return jnp.clip(entries, min=-most, max=most).astype(held_as)


def setup_inputs(seed: int = 0) -> dict:
    seeds = jax.random.split(jax.random.key(seed), 15)
    hidden_in = draw_hidden_in(jax.random.fold_in(seeds[14], 71), 0)
    block_order = jax.vmap(lambda own: jax.random.permutation(own, SLOTS))(jax.random.split(seeds[1], SEQS)).reshape((SEQS, SLOTS)).astype(jnp.int32)
    cotangent = normal_values(seeds[2], (SEQS, LEN, D), 1.0, 6.0, ((0, 8), (1, 4)))
    q_weight = normal_values(seeds[3], (D, HEADS * HEAD_DIM), D ** -0.5, 0.1875, ((0, 32),))
    k_weight = normal_values(seeds[4], (D, KV_HEADS * HEAD_DIM), D ** -0.5, 0.1875, ((0, 32),))
    v_weight = normal_values(seeds[5], (D, KV_HEADS * HEAD_DIM), D ** -0.5, 0.1875, ((0, 32),))
    o_weight = normal_values(seeds[6], (D, HEADS * HEAD_DIM), (HEADS * HEAD_DIM // 128) ** -0.5, 1.5, ((0, 32),))
    attn_gain = jnp.clip(1.0 + 0.1 * jax.random.normal(seeds[7], (D,), jnp.float32), 0.5, 1.5).astype(jnp.bfloat16)
    query_gain = jnp.clip(1.0 + 0.1 * jax.random.normal(seeds[8], (HEAD_DIM,), jnp.float32), 0.5, 1.5).astype(jnp.bfloat16)
    key_gain = jnp.clip(1.0 + 0.1 * jax.random.normal(seeds[9], (HEAD_DIM,), jnp.float32), 0.5, 1.5).astype(jnp.bfloat16)
    mlp_gain = jnp.clip(1.0 + 0.1 * jax.random.normal(seeds[10], (D,), jnp.float32), 0.5, 1.5).astype(jnp.bfloat16)
    gate_weight = normal_values(seeds[11], (D, FF), D ** -0.5, 0.1875, ((0, 32),))
    up_weight = normal_values(seeds[12], (D, FF), D ** -0.5, 0.1875, ((0, 32),))
    down_weight = normal_values(seeds[13], (D, FF), FF ** -0.5, 0.109375, ((0, 32),))
    return dict(hidden_in=hidden_in, block_order=block_order, cotangent=cotangent, q_weight=q_weight, k_weight=k_weight, v_weight=v_weight, o_weight=o_weight, attn_gain=attn_gain, query_gain=query_gain, key_gain=key_gain, mlp_gain=mlp_gain, gate_weight=gate_weight, up_weight=up_weight, down_weight=down_weight)


@jax.custom_vjp
def low(v):
    return lax.optimization_barrier(v.astype(jnp.bfloat16)).astype(jnp.float32)

@jax.custom_vjp
def low_back(v):
    return v

def low_keep(v):
    return (low(v), None)

def low_pass(kept, grad):
    return (grad,)

def back_keep(v):
    return (v, None)

def back_low(kept, grad):
    return (low(grad),)
low.defvjp(low_keep, low_pass)
low_back.defvjp(back_keep, back_low)

def matmul(left, right):
    return jnp.dot(left, right, precision=lax.Precision.HIGHEST, preferred_element_type=jnp.float32)

def rms_norm(signal, gain_vec):
    inverse_rms = lax.rsqrt(lax.optimization_barrier(jnp.mean(signal * signal, axis=-1, keepdims=True)) + 1e-06)
    return signal * inverse_rms * gain_vec

def rope_tables(positions, head_width):
    exponent = jnp.arange(head_width // 2, dtype=jnp.float32) * (2.0 / head_width)
    inverse = jnp.exp(-exponent * math.log(1000000.0))
    angles = positions.astype(jnp.float32)[:, None] * inverse[None, :]
    angles = jnp.concatenate([angles, angles], axis=-1)
    return (jnp.cos(angles)[:, None, :], jnp.sin(angles)[:, None, :])

def rotate(signal, cosine, sine):
    half_dim = signal.shape[-1] // 2
    turned = jnp.concatenate([-signal[..., half_dim:], signal[..., :half_dim]], axis=-1)
    return signal * cosine + turned * sine

def sequence_forward(inputs, order_row, params):
    q_mat, k_mat, v_mat, o_mat, norm_gain, qgain, kgain, mlp_norm_gain, gate_mat, up_mat, down_mat = params
    group_size = HEADS // KV_HEADS
    factor = 1.0 / math.sqrt(HEAD_DIM)
    positions = (order_row[:, None] * BLOCK + jnp.arange(BLOCK, dtype=jnp.int32)[None, :]).reshape(-1)
    normed = low(rms_norm(inputs, norm_gain))
    query_proj = low_back(matmul(normed, q_mat)).reshape(LEN, HEADS, HEAD_DIM)
    key_proj = low_back(matmul(normed, k_mat)).reshape(LEN, KV_HEADS, HEAD_DIM)
    values = low(low_back(matmul(normed, v_mat))).reshape(LEN, KV_HEADS, HEAD_DIM)
    cosine, sine = rope_tables(positions, HEAD_DIM)
    queries = low(rotate(rms_norm(query_proj, qgain), cosine, sine)).reshape(LEN, KV_HEADS, group_size, HEAD_DIM)
    keys_rot = low(rotate(rms_norm(key_proj, kgain), cosine, sine))
    scores = low_back(jnp.einsum('qkgd,nkd->kgqn', queries, keys_rot, precision=lax.Precision.HIGHEST) * factor)
    allowed = positions[None, :] <= positions[:, None]
    weights_exp = jnp.where(allowed, jnp.exp(scores), 0.0)
    totals = lax.optimization_barrier(jnp.sum(weights_exp, axis=-1))
    numerator = low_back(jnp.einsum('kgqn,nkd->qkgd', low(weights_exp), values, precision=lax.Precision.HIGHEST))
    attn_full = numerator / jnp.transpose(totals, (2, 0, 1))[..., None]
    attn_low = low(attn_full).reshape(LEN, HEADS * HEAD_DIM)
    residual = inputs + low_back(matmul(attn_low, o_mat.T))
    mixed = low(rms_norm(residual, mlp_norm_gain))
    gate_val = low_back(matmul(mixed, gate_mat))
    up_val = low_back(matmul(mixed, up_mat))
    hidden_low = low(jax.nn.silu(gate_val) * up_val)
    return residual + low_back(matmul(hidden_low, down_mat.T))

def reference(hidden_in, block_order, cotangent, q_weight, k_weight, v_weight, o_weight, attn_gain, query_gain, key_gain, mlp_gain, gate_weight, up_weight, down_weight):
    params = tuple((matrix.astype(jnp.float32) for matrix in (q_weight, k_weight, v_weight, o_weight, attn_gain, query_gain, key_gain, mlp_gain, gate_weight, up_weight, down_weight)))
    inputs = hidden_in.astype(jnp.float32)

    def forward(all_inputs, all_params):

        def one_sequence(paired):
            return sequence_forward(paired[0], paired[1], all_params)
        return lax.map(jax.checkpoint(one_sequence), (all_inputs, block_order))
    result, pullback = jax.vjp(forward, inputs, params)
    input_grad, param_grads = pullback(cotangent.astype(jnp.float32))
    return (result.astype(jnp.bfloat16), input_grad, param_grads[0], param_grads[1], param_grads[2], param_grads[3], param_grads[4], param_grads[5], param_grads[6], param_grads[7], param_grads[8], param_grads[9], param_grads[10])
```

```python
import functools
import math

import jax
import jax.numpy as jnp
from jax import lax
from jax.sharding import PartitionSpec as P

HEADS = 16
KV_HEADS = 8
HEAD_DIM = 128
EPSILON = 1e-06
FIRST_AXIS = (((0,), (0,)), ((), ()))
LAST_AXIS = (((1,), (1,)), ((), ()))
BF16 = jnp.bfloat16
F32 = jnp.float32


def mm(left, right, dims=(((1,), (0,)), ((), ()))):
    return lax.dot_general(left, right, dims, preferred_element_type=F32)


def rms(signal):
    return lax.rsqrt(jnp.mean(signal * signal, axis=-1, keepdims=True) + EPSILON)


def norm_back(signal, inverse_rms, gain_vec, upstream):
    unit_values = signal * inverse_rms
    scaled_up = upstream * gain_vec
    inner = scaled_up - unit_values * jnp.mean(scaled_up * unit_values, axis=-1, keepdims=True)
    return (inverse_rms * inner, upstream * unit_values)


def rope_tables(positions, head_width):
    exponent = jnp.arange(head_width // 2, dtype=F32) * (2.0 / head_width)
    inverse = jnp.exp(-exponent * math.log(1000000.0))
    angles = positions.astype(F32)[:, None] * inverse[None, :]
    angles = jnp.concatenate([angles, angles], axis=-1)
    return (jnp.cos(angles), jnp.sin(angles))


def rotate(signal, cosine, sine):
    half = signal.shape[-1] // 2
    turned = jnp.concatenate([-signal[..., half:], signal[..., :half]], axis=-1)
    return signal * cosine + turned * sine


def rotate_back(upstream, cosine, sine):
    half = upstream.shape[-1] // 2
    scaled_up = upstream * sine
    return upstream * cosine + jnp.concatenate(
        [scaled_up[..., half:], -scaled_up[..., :half]], axis=-1
    )


def gather_columns(ctx, shards):
    rows = shards[0].shape[0]
    cut = [s.reshape(rows, ctx, s.shape[1] // ctx).transpose(1, 0, 2) for s in shards]
    widths = [c.shape[2] for c in cut]
    both = jnp.concatenate(cut, axis=2)
    both = lax.all_to_all(both, "ctx", 0, 0, tiled=True)
    both = both.reshape(ctx * rows, -1)
    whole = lax.all_gather(both, "fsdp", axis=0, tiled=True)
    out, at = [], 0
    for width in widths:
        out.append(whole[:, at : at + width])
        at += width
    return out


def scatter_grads(ctx, fsdp, grads):
    rows = grads[0].shape[0] // (ctx * fsdp)
    widths = [g.shape[1] for g in grads]
    both = jnp.concatenate([g.astype(BF16) for g in grads], axis=1)
    both = lax.psum_scatter(both, "fsdp", scatter_dimension=0, tiled=True)
    both = lax.all_to_all(both.reshape(ctx, rows, -1), "ctx", 0, 0, tiled=True)
    out, at = [], 0
    for width in widths:
        piece = both[:, :, at : at + width]
        out.append(piece.transpose(1, 0, 2).reshape(rows, ctx * width).astype(F32))
        at += width
    return out


def ctx_gather(rows):
    return lax.all_gather(rows, "ctx", axis=0, tiled=True)


def ctx_scatter(partial):
    return lax.psum_scatter(partial.astype(BF16), "ctx", scatter_dimension=0, tiled=True).astype(
        F32
    )


def local(
    ctx,
    fsdp,
    hidden_in,
    block_order,
    cotangent,
    q_weight,
    k_weight,
    v_weight,
    o_weight,
    attn_gain,
    query_gain,
    key_gain,
    mlp_gain,
    gate_weight,
    up_weight,
    down_weight,
):
    inputs = hidden_in[0].astype(F32)
    row_count = inputs.shape[0]
    tokens = row_count * ctx
    slots = block_order.shape[1]
    block_len = tokens // slots
    heads, kv_heads = HEADS // ctx, KV_HEADS // ctx
    group = heads // kv_heads
    factor = 1.0 / math.sqrt(HEAD_DIM)
    positions = (
        block_order[0][:, None] * block_len + jnp.arange(block_len, dtype=jnp.int32)[None, :]
    ).reshape(-1)
    cosine, sine = rope_tables(positions, HEAD_DIM)
    cosine, sine = cosine[:, None, :], sine[:, None, :]

    both = ("fsdp", "ctx")
    norm_gain, qgain, kgain, mlp_norm_gain = (
        lax.all_gather(g, both, axis=0, tiled=True).astype(F32)
        for g in (attn_gain, query_gain, key_gain, mlp_gain)
    )
    norm_scale = rms(inputs)
    normed = ctx_gather((inputs * norm_scale * norm_gain).astype(BF16))
    upstream = ctx_gather(cotangent[0])
    q_full, k_full, v_full, o_full = gather_columns(ctx, (q_weight, k_weight, v_weight, o_weight))
    gate_full, up_full, down_full = gather_columns(ctx, (gate_weight, up_weight, down_weight))

    query_proj = mm(normed, q_full).reshape(tokens, heads, HEAD_DIM)
    key_proj = mm(normed, k_full).reshape(tokens, kv_heads, HEAD_DIM)
    value_low = mm(normed, v_full).astype(BF16).reshape(tokens, kv_heads, HEAD_DIM)
    query_scale, key_scale = rms(query_proj), rms(key_proj)
    query_low = (
        rotate(query_proj * query_scale * qgain, cosine, sine)
        .astype(BF16)
        .reshape(tokens, kv_heads, group, HEAD_DIM)
    )
    key_low = rotate(key_proj * key_scale * kgain, cosine, sine).astype(BF16)
    scores = jnp.einsum("rkgd,nkd->kgrn", query_low, key_low, preferred_element_type=F32) * factor
    allowed = positions[None, :] <= positions[:, None]
    weights_exp = jnp.where(allowed, jnp.exp(scores), 0.0)
    denominator = jnp.sum(weights_exp, axis=-1)
    weights_low = weights_exp.astype(BF16)
    numerator = jnp.einsum("kgrn,nkd->rkgd", weights_low, value_low, preferred_element_type=F32)
    denom_rows = jnp.transpose(denominator, (2, 0, 1))[..., None]
    attn_full = numerator / denom_rows
    attn_low = attn_full.astype(BF16).reshape(tokens, heads * HEAD_DIM)
    residual = inputs + ctx_scatter(mm(attn_low, o_full, LAST_AXIS))

    mix_scale = rms(residual)
    mixed = ctx_gather((residual * mix_scale * mlp_norm_gain).astype(BF16))
    gate_val = mm(mixed, gate_full)
    up_val = mm(mixed, up_full)
    sigmoid_gate = jax.nn.sigmoid(gate_val)
    swish_gate = gate_val * sigmoid_gate
    hidden_low = (swish_gate * up_val).astype(BF16)
    result = residual + ctx_scatter(mm(hidden_low, down_full, LAST_AXIS))
    hidden_grad = mm(upstream, down_full)
    gate_back = (
        hidden_grad * up_val * sigmoid_gate * (1.0 + gate_val * (1.0 - sigmoid_gate))
    ).astype(BF16)
    up_back = (hidden_grad * swish_gate).astype(BF16)
    mixed_grad = ctx_scatter(mm(gate_back, gate_full, LAST_AXIS) + mm(up_back, up_full, LAST_AXIS))
    resid_from_norm, mlp_gain_term = norm_back(residual, mix_scale, mlp_norm_gain, mixed_grad)
    residual_grad = cotangent[0].astype(F32) + resid_from_norm
    mlp_grads = scatter_grads(
        ctx,
        fsdp,
        (
            mm(mixed, gate_back, FIRST_AXIS),
            mm(mixed, up_back, FIRST_AXIS),
            mm(upstream, hidden_low, FIRST_AXIS),
        ),
    )
    resid_low = ctx_gather(residual_grad.astype(BF16))

    attn_grad = mm(resid_low, o_full).reshape(tokens, kv_heads, group, HEAD_DIM)
    share_low = (attn_grad / denom_rows).astype(BF16)
    denom_grad = jnp.transpose(jnp.sum(attn_grad * attn_full, axis=-1), (1, 2, 0)) / denominator
    weight_grad = jnp.einsum("rkgd,nkd->kgrn", share_low, value_low, preferred_element_type=F32)
    score_low = (weights_exp * (weight_grad - denom_grad[..., None])).astype(BF16)
    query_rot = (
        jnp.einsum("kgrn,nkd->rkgd", score_low, key_low, preferred_element_type=F32) * factor
    ).reshape(tokens, heads, HEAD_DIM)
    key_rot = (
        jnp.einsum("kgrn,rkgd->nkd", score_low, query_low, preferred_element_type=F32) * factor
    )
    value_back = (
        jnp.einsum("kgrn,rkgd->nkd", weights_low, share_low, preferred_element_type=F32)
        .reshape(tokens, kv_heads * HEAD_DIM)
        .astype(BF16)
    )
    query_grad, query_term = norm_back(
        query_proj, query_scale, qgain, rotate_back(query_rot, cosine, sine)
    )
    key_grad, key_term = norm_back(key_proj, key_scale, kgain, rotate_back(key_rot, cosine, sine))
    query_back = query_grad.reshape(tokens, heads * HEAD_DIM).astype(BF16)
    key_back = key_grad.reshape(tokens, kv_heads * HEAD_DIM).astype(BF16)
    normed_grad = ctx_scatter(
        mm(query_back, q_full, LAST_AXIS)
        + mm(key_back, k_full, LAST_AXIS)
        + mm(value_back, v_full, LAST_AXIS)
    )
    input_from_norm, attn_gain_term = norm_back(inputs, norm_scale, norm_gain, normed_grad)
    input_grad = residual_grad + input_from_norm
    attn_grads = scatter_grads(
        ctx,
        fsdp,
        (
            mm(normed, query_back, FIRST_AXIS),
            mm(normed, key_back, FIRST_AXIS),
            mm(normed, value_back, FIRST_AXIS),
            mm(resid_low, attn_low, FIRST_AXIS),
        ),
    )
    gains = (
        jnp.sum(attn_gain_term, axis=0),
        jnp.sum(query_term, axis=(0, 1)),
        jnp.sum(key_term, axis=(0, 1)),
        jnp.sum(mlp_gain_term, axis=0),
    )
    gains = [lax.psum_scatter(g, both, scatter_dimension=0, tiled=True) for g in gains]
    return (
        result.astype(BF16)[None],
        input_grad[None],
        *attn_grads,
        *gains,
        *mlp_grads,
    )


def solution(mesh):
    ctx, fsdp = mesh.shape["ctx"], mesh.shape["fsdp"]
    tokens = P("fsdp", "ctx", None)
    matrix = P(("fsdp", "ctx"), None)
    vector = P(("fsdp", "ctx"))
    return jax.shard_map(
        functools.partial(local, ctx, fsdp),
        mesh=mesh,
        in_specs=(tokens, P("fsdp", None), tokens)
        + (matrix,) * 4
        + (vector,) * 4
        + (matrix,) * 3,
        out_specs=(tokens,) * 2 + (matrix,) * 4 + (vector,) * 4 + (matrix,) * 3,
        check_vma=False,
    )
```

```python
import functools
import math
import types

import jax
import jax.numpy as jnp
from jax import lax
from jax.experimental import pallas as pl
from jax.experimental.pallas import tpu as pltpu
from jax.sharding import PartitionSpec as P

HEADS = 16
KV_HEADS = 8
HEAD_DIM = 128
EPSILON = 1e-06
FIRST_AXIS = (((0,), (0,)), ((), ()))
LAST_AXIS = (((1,), (1,)), ((), ()))
BF16 = jnp.bfloat16
F32 = jnp.float32
VMEM_LIMIT = 67043328


def mm(left, right, dims=(((1,), (0,)), ((), ()))):
    return lax.dot_general(left, right, dims, preferred_element_type=F32)


def rms(signal):
    return lax.rsqrt(jnp.mean(signal * signal, axis=-1, keepdims=True) + EPSILON)


def norm_back(signal, inverse_rms, gain_vec, upstream):
    unit_values = signal * inverse_rms
    scaled_up = upstream * gain_vec
    inner = scaled_up - unit_values * jnp.mean(scaled_up * unit_values, axis=-1, keepdims=True)
    return (inverse_rms * inner, upstream * unit_values)


def rope_tables(positions, head_width):
    exponent = jnp.arange(head_width // 2, dtype=F32) * (2.0 / head_width)
    inverse = jnp.exp(-exponent * math.log(1000000.0))
    angles = positions.astype(F32)[:, None] * inverse[None, :]
    angles = jnp.concatenate([angles, angles], axis=-1)
    return (jnp.cos(angles), jnp.sin(angles))


def rotate(signal, cosine, sine):
    half = signal.shape[-1] // 2
    turned = jnp.concatenate([-signal[..., half:], signal[..., :half]], axis=-1)
    return signal * cosine + turned * sine


def rotate_back(upstream, cosine, sine):
    half = upstream.shape[-1] // 2
    scaled_up = upstream * sine
    return upstream * cosine + jnp.concatenate(
        [scaled_up[..., half:], -scaled_up[..., :half]], axis=-1
    )


def gather_columns(ctx, shards):
    rows = shards[0].shape[0]
    cut = [s.reshape(rows, ctx, s.shape[1] // ctx).transpose(1, 0, 2) for s in shards]
    widths = [c.shape[2] for c in cut]
    both = jnp.concatenate(cut, axis=2)
    both = lax.all_to_all(both, "ctx", 0, 0, tiled=True)
    both = both.reshape(ctx * rows, -1)
    whole = lax.all_gather(both, "fsdp", axis=0, tiled=True)
    out, at = [], 0
    for width in widths:
        out.append(whole[:, at : at + width])
        at += width
    return out


def scatter_grads(ctx, fsdp, grads):
    rows = grads[0].shape[0] // (ctx * fsdp)
    widths = [g.shape[1] for g in grads]
    both = jnp.concatenate([g.astype(BF16) for g in grads], axis=1)
    both = lax.psum_scatter(both, "fsdp", scatter_dimension=0, tiled=True)
    both = lax.all_to_all(both.reshape(ctx, rows, -1), "ctx", 0, 0, tiled=True)
    out, at = [], 0
    for width in widths:
        piece = both[:, :, at : at + width]
        out.append(piece.transpose(1, 0, 2).reshape(rows, ctx * width).astype(F32))
        at += width
    return out


def ctx_gather(rows):
    return lax.all_gather(rows, "ctx", axis=0, tiled=True)


def ctx_scatter(partial):
    return lax.psum_scatter(partial.astype(BF16), "ctx", scatter_dimension=0, tiled=True).astype(
        F32
    )


def local(
    ctx,
    fsdp,
    hidden_in,
    block_order,
    cotangent,
    q_weight,
    k_weight,
    v_weight,
    o_weight,
    attn_gain,
    query_gain,
    key_gain,
    mlp_gain,
    gate_weight,
    up_weight,
    down_weight,
):
    inputs = hidden_in[0].astype(F32)
    row_count = inputs.shape[0]
    tokens = row_count * ctx
    slots = block_order.shape[1]
    block_len = tokens // slots
    heads, kv_heads = HEADS // ctx, KV_HEADS // ctx
    group = heads // kv_heads
    factor = 1.0 / math.sqrt(HEAD_DIM)
    positions = (
        block_order[0][:, None] * block_len + jnp.arange(block_len, dtype=jnp.int32)[None, :]
    ).reshape(-1)
    cosine, sine = rope_tables(positions, HEAD_DIM)
    cosine, sine = cosine[:, None, :], sine[:, None, :]

    both = ("fsdp", "ctx")
    norm_gain, qgain, kgain, mlp_norm_gain = (
        lax.all_gather(g, both, axis=0, tiled=True).astype(F32)
        for g in (attn_gain, query_gain, key_gain, mlp_gain)
    )
    norm_scale = rms(inputs)
    normed = ctx_gather((inputs * norm_scale * norm_gain).astype(BF16))
    upstream = ctx_gather(cotangent[0])
    q_full, k_full, v_full, o_full = gather_columns(ctx, (q_weight, k_weight, v_weight, o_weight))
    gate_full, up_full, down_full = gather_columns(ctx, (gate_weight, up_weight, down_weight))

    query_proj = mm(normed, q_full).reshape(tokens, heads, HEAD_DIM)
    key_proj = mm(normed, k_full).reshape(tokens, kv_heads, HEAD_DIM)
    value_low = mm(normed, v_full).astype(BF16).reshape(tokens, kv_heads, HEAD_DIM)
    query_scale, key_scale = rms(query_proj), rms(key_proj)
    query_low = (
        rotate(query_proj * query_scale * qgain, cosine, sine)
        .astype(BF16)
        .reshape(tokens, kv_heads, group, HEAD_DIM)
    )
    key_low = rotate(key_proj * key_scale * kgain, cosine, sine).astype(BF16)
    scores = jnp.einsum("rkgd,nkd->kgrn", query_low, key_low, preferred_element_type=F32) * factor
    allowed = positions[None, :] <= positions[:, None]
    weights_exp = jnp.where(allowed, jnp.exp(scores), 0.0)
    denominator = jnp.sum(weights_exp, axis=-1)
    weights_low = weights_exp.astype(BF16)
    numerator = jnp.einsum("kgrn,nkd->rkgd", weights_low, value_low, preferred_element_type=F32)
    denom_rows = jnp.transpose(denominator, (2, 0, 1))[..., None]
    attn_full = numerator / denom_rows
    attn_low = attn_full.astype(BF16).reshape(tokens, heads * HEAD_DIM)
    residual = inputs + ctx_scatter(mm(attn_low, o_full, LAST_AXIS))

    mix_scale = rms(residual)
    mixed = ctx_gather((residual * mix_scale * mlp_norm_gain).astype(BF16))
    gate_val = mm(mixed, gate_full)
    up_val = mm(mixed, up_full)
    sigmoid_gate = jax.nn.sigmoid(gate_val)
    swish_gate = gate_val * sigmoid_gate
    hidden_low = (swish_gate * up_val).astype(BF16)
    result = residual + ctx_scatter(mm(hidden_low, down_full, LAST_AXIS))
    hidden_grad = mm(upstream, down_full)
    gate_back = (
        hidden_grad * up_val * sigmoid_gate * (1.0 + gate_val * (1.0 - sigmoid_gate))
    ).astype(BF16)
    up_back = (hidden_grad * swish_gate).astype(BF16)
    mixed_grad = ctx_scatter(mm(gate_back, gate_full, LAST_AXIS) + mm(up_back, up_full, LAST_AXIS))
    resid_from_norm, mlp_gain_term = norm_back(residual, mix_scale, mlp_norm_gain, mixed_grad)
    residual_grad = cotangent[0].astype(F32) + resid_from_norm
    mlp_grads = scatter_grads(
        ctx,
        fsdp,
        (
            mm(mixed, gate_back, FIRST_AXIS),
            mm(mixed, up_back, FIRST_AXIS),
            mm(upstream, hidden_low, FIRST_AXIS),
        ),
    )
    resid_low = ctx_gather(residual_grad.astype(BF16))

    attn_grad = mm(resid_low, o_full).reshape(tokens, kv_heads, group, HEAD_DIM)
    share_low = (attn_grad / denom_rows).astype(BF16)
    denom_grad = jnp.transpose(jnp.sum(attn_grad * attn_full, axis=-1), (1, 2, 0)) / denominator
    weight_grad = jnp.einsum("rkgd,nkd->kgrn", share_low, value_low, preferred_element_type=F32)
    score_low = (weights_exp * (weight_grad - denom_grad[..., None])).astype(BF16)
    query_rot = (
        jnp.einsum("kgrn,nkd->rkgd", score_low, key_low, preferred_element_type=F32) * factor
    ).reshape(tokens, heads, HEAD_DIM)
    key_rot = (
        jnp.einsum("kgrn,rkgd->nkd", score_low, query_low, preferred_element_type=F32) * factor
    )
    value_back = (
        jnp.einsum("kgrn,rkgd->nkd", weights_low, share_low, preferred_element_type=F32)
        .reshape(tokens, kv_heads * HEAD_DIM)
        .astype(BF16)
    )
    query_grad, query_term = norm_back(
        query_proj, query_scale, qgain, rotate_back(query_rot, cosine, sine)
    )
    key_grad, key_term = norm_back(key_proj, key_scale, kgain, rotate_back(key_rot, cosine, sine))
    query_back = query_grad.reshape(tokens, heads * HEAD_DIM).astype(BF16)
    key_back = key_grad.reshape(tokens, kv_heads * HEAD_DIM).astype(BF16)
    normed_grad = ctx_scatter(
        mm(query_back, q_full, LAST_AXIS)
        + mm(key_back, k_full, LAST_AXIS)
        + mm(value_back, v_full, LAST_AXIS)
    )
    input_from_norm, attn_gain_term = norm_back(inputs, norm_scale, norm_gain, normed_grad)
    input_grad = residual_grad + input_from_norm
    attn_grads = scatter_grads(
        ctx,
        fsdp,
        (
            mm(normed, query_back, FIRST_AXIS),
            mm(normed, key_back, FIRST_AXIS),
            mm(normed, value_back, FIRST_AXIS),
            mm(resid_low, attn_low, FIRST_AXIS),
        ),
    )
    gains = (
        jnp.sum(attn_gain_term, axis=0),
        jnp.sum(query_term, axis=(0, 1)),
        jnp.sum(key_term, axis=(0, 1)),
        jnp.sum(mlp_gain_term, axis=0),
    )
    gains = [lax.psum_scatter(g, both, scatter_dimension=0, tiled=True) for g in gains]
    return (
        result.astype(BF16)[None],
        input_grad[None],
        *attn_grads,
        *gains,
        *mlp_grads,
    )


def rope_fwd(u, cosine, sine):
    return u * cosine + pltpu.roll(u, HEAD_DIM // 2, u.ndim - 1) * sine


def rope_bwd(du, cosine, sine):
    return du * cosine - pltpu.roll(du, HEAD_DIM // 2, du.ndim - 1) * sine


class Sizes:
    def __init__(self, ctx, fsdp, rows, shards):
        self.ctx, self.fsdp, self.rows = ctx, fsdp, rows
        self.chips = fsdp // 2
        self.shard = shards[0].shape[0]
        self.block = self.shard * ctx
        self.width = self.block * fsdp
        self.tokens = rows * ctx
        self.heads, self.kv = HEADS // ctx, KV_HEADS // ctx
        self.cols = [s.shape[1] // ctx for s in shards]
        self.attn_cols = sum(self.cols[:4])
        self.mlp_cols = sum(self.cols[4:])
        self.lines = self.width // HEAD_DIM
        self.gain_rows = 8 * ((2 * self.lines + 2 + 7) // 8)


def scratch_of(n):
    bf, f32 = (lambda *s: pltpu.VMEM(s, BF16)), (lambda *s: pltpu.VMEM(s, F32))
    sem = lambda *s: pltpu.SemaphoreType.DMA(s)
    c, d, s, h, kv = n.ctx, n.width, n.tokens, n.heads, n.kv
    ff = n.cols[4]
    out = dict(
        wa=bf(d, n.attn_cols),
        wm=bf(d, n.mlp_cols),
        xb=bf(c, n.rows, d),
        gb=bf(c, n.rows, d),
        mb=bf(c, n.rows, d),
        rb=bf(c, n.rows, d),
        xn=bf(s, d),
        qp=f32(h, s, HEAD_DIM),
        kp=f32(kv, s, HEAD_DIM),
        qr=bf(h, s, HEAD_DIM),
        kr=bf(kv, s, HEAD_DIM),
        vv=bf(kv, s, HEAD_DIM),
        es=f32(h, s, s),
        af=f32(h, s, HEAD_DIM),
        at=bf(s, h * HEAD_DIM),
        da=f32(h, s, HEAD_DIM),
        dk=f32(kv, s, HEAD_DIM),
        dv=f32(kv, s, HEAD_DIM),
        ds=bf(s, s),
        eb=bf(s, s),
        wb=bf(s, HEAD_DIM),
        dqkv=bf(s, (h + 2 * kv) * HEAD_DIM),
        hid=bf(s, ff),
        dgu=bf(s, 2 * ff),
        ho=f32(n.rows, d),
        dh=f32(n.rows, d),
        gv=f32(2, 1, d),
        ga=bf(d, n.attn_cols),
        gm=bf(d, n.mlp_cols),
        ga_sib=bf(n.chips, n.block, n.attn_cols),
        gm_sib=bf(n.chips, n.block, n.mlp_cols),
        ga_in=bf(n.chips - 1, n.block, n.attn_cols),
        gm_in=bf(n.chips - 1, n.block, n.mlp_cols),
        ga_z=bf(n.block, n.attn_cols),
        gm_z=bf(n.block, n.mlp_cols),
        ga_land=bf(c, n.shard, n.attn_cols),
        gm_land=bf(c, n.shard, n.mlp_cols),
        local_sem=sem(9),
    )
    for name in ("o", "x2", "x1"):
        out["p_" + name] = bf(c, n.rows, d)
        out["l_" + name] = bf(c, n.rows, d)
        out["r_" + name] = bf(c, n.rows, d)
        out["sem_" + name] = sem(4, c)
    out["p_y"] = bf(c, n.rows, d)
    out["i_y"] = bf(c - 1, n.rows, d)
    out["sem_y"] = sem(2, c)
    out["sem_g"] = sem(2, c)
    for name in ("xb", "mb", "rb"):
        out["sem_" + name] = sem(3, c)
    out["sem_wa"] = sem(2, c - 1, 4)
    out["sem_wm"] = sem(2, c - 1, 3)
    for name in ("wa", "wm"):
        out["sem_p" + name] = sem(2, n.chips)
        out["sem_s" + name] = sem(2, n.chips)
    for name in ("ga", "gm"):
        out["sem_s" + name] = sem(2, n.chips)
        out["sem_p" + name] = sem(2, n.chips)
        out["sem_z" + name] = sem(2, c)
    for name in ("g0", "g1"):
        out[name + "_in"] = f32(n.chips + c, n.gain_rows, HEAD_DIM)
        out[name + "_acc"] = f32(4, n.gain_rows, HEAD_DIM)
        out["sem_" + name] = sem(2, n.chips + c)
    return out


def layer_kernel(n, names, *refs):
    r = types.SimpleNamespace(**dict(zip(names, refs)))
    c, f = lax.axis_index("ctx"), lax.axis_index("fsdp")
    chip, core = f // 2, f % 2
    sibling = chip * 2 + 1 - core
    rows, d, block, shard = n.rows, n.width, n.block, n.shard
    sends = []

    def ahead(by):
        return lax.rem(c + by, n.ctx)

    def behind(by):
        return lax.rem(c + n.ctx - by, n.ctx)

    def chip_ahead(by):
        return lax.rem(chip + by, n.chips)

    def chip_behind(by):
        return lax.rem(chip + n.chips - by, n.chips)

    def remote(src, dst, send_sem, recv_sem, to_f=None, to_c=None):
        return pltpu.make_async_remote_copy(
            src_ref=src,
            dst_ref=dst,
            send_sem=send_sem,
            recv_sem=recv_sem,
            device_id={"fsdp": f if to_f is None else to_f, "ctx": c if to_c is None else to_c},
            device_id_type=pl.DeviceIdType.MESH,
        )

    def send(src, dst, send_sem, recv_sem, to_f=None, to_c=None):
        copy = remote(src, dst, send_sem, recv_sem, to_f, to_c)
        copy.start()
        sends.append(copy.wait_send)

    def arrived(dst, recv_sem):
        remote(dst, dst, recv_sem, recv_sem).wait_recv()

    def send_if(cond, src, dst, send_sem, recv_sem, to_c):
        copy = remote(src, dst, send_sem, recv_sem, None, to_c)
        pl.when(cond)(copy.start)
        sends.append(lambda: pl.when(cond)(copy.wait_send))

    barrier = pltpu.get_barrier_semaphore()

    def greet(to_f, to_c):
        pl.semaphore_signal(
            barrier,
            inc=1,
            device_id={"fsdp": to_f, "ctx": to_c},
            device_id_type=pl.DeviceIdType.MESH,
        )

    for by in range(1, n.ctx):
        greet(f, ahead(by))
    for by in range(1, n.chips):
        greet(chip_ahead(by) * 2 + core, c)
    greet(sibling, c)
    pl.semaphore_wait(barrier, n.ctx - 1 + n.chips)

    right, left = jnp.minimum(c + 1, n.ctx - 1), jnp.maximum(c - 1, 0)

    def gather_start(src, buf, sem):
        send_if(c + 1 < n.ctx, src, buf.at[c], sem.at[0, 0], sem.at[2, c], right)
        send_if(c > 0, src, buf.at[c], sem.at[1, 0], sem.at[2, c], left)

    def gather_relay(buf, sem):
        for by in range(1, n.ctx):
            low = jnp.maximum(c - by, 0)
            pl.when(c - by >= 0)(lambda: arrived(buf.at[low], sem.at[2, low]))
            send_if(
                (c - by >= 0) & (c + 1 < n.ctx),
                buf.at[low],
                buf.at[low],
                sem.at[0, by],
                sem.at[2, low],
                right,
            )
            high = jnp.minimum(c + by, n.ctx - 1)
            pl.when(c + by < n.ctx)(lambda: arrived(buf.at[high], sem.at[2, high]))
            send_if(
                (c + by < n.ctx) & (c > 0),
                buf.at[high],
                buf.at[high],
                sem.at[1, by],
                sem.at[2, high],
                left,
            )

    def scatter(part, from_left, from_right, sem, fill=None):
        for step in range(n.ctx - 1):
            target = step
            down = c > target

            @pl.when(down & (c + 1 < n.ctx))
            def _():
                arrived(from_right.at[target], sem.at[3, target])
                part[target] = (part[target].astype(F32) + from_right[target].astype(F32)).astype(
                    BF16
                )

            send_if(
                down,
                part.at[target],
                from_right.at[target],
                sem.at[1, target],
                sem.at[3, target],
                left,
            )
            target = n.ctx - 1 - step
            up = c < target

            @pl.when(up & (c > 0))
            def _():
                arrived(from_left.at[target], sem.at[2, target])
                part[target] = (part[target].astype(F32) + from_left[target].astype(F32)).astype(
                    BF16
                )

            send_if(
                up, part.at[target], from_left.at[target], sem.at[0, target], sem.at[2, target], right
            )
            if fill:
                fill(step)

    def scatter_total(part, from_left, from_right, sem, out):
        out[...] = out[...] + part[c].astype(F32)

        @pl.when(c > 0)
        def _():
            arrived(from_left.at[c], sem.at[2, c])
            out[...] = out[...] + from_left[c].astype(F32)

        @pl.when(c + 1 < n.ctx)
        def _():
            arrived(from_right.at[c], sem.at[3, c])
            out[...] = out[...] + from_right[c].astype(F32)

    def block_of(buf, index):
        return buf.at[pl.ds(pl.multiple_of(index * block, block), block), :]

    def piece_of(buf, line, at, width):
        start = pl.multiple_of(f * block + line * shard, shard)
        return buf.at[pl.ds(start, shard), pl.ds(at, width)]

    def weights_send(shards, cols, buf, sem):
        for by in range(1, n.ctx):
            at = 0
            for i, (src, width) in enumerate(zip(shards, cols)):
                column = pl.multiple_of(ahead(by) * width, HEAD_DIM)
                send(
                    src.at[:, pl.ds(column, width)],
                    piece_of(buf, c, at, width),
                    sem.at[0, by - 1, i],
                    sem.at[1, by - 1, i],
                    None,
                    ahead(by),
                )
                at += width

    def weights_own(shards, cols, buf, first):
        at, out = 0, []
        for i, (src, width) in enumerate(zip(shards, cols)):
            column = pl.multiple_of(c * width, HEAD_DIM)
            copy = pltpu.make_async_copy(
                src.at[:, pl.ds(column, width)],
                piece_of(buf, c, at, width),
                r.local_sem.at[first + i],
            )
            copy.start()
            out.append(copy)
            at += width
        return out

    def weights_spread(own, cols, buf, sem, plane_sem, sib_sem):
        for copy in own:
            copy.wait()
        for by in range(1, n.ctx):
            at = 0
            for i, width in enumerate(cols):
                arrived(piece_of(buf, behind(by), at, width), sem.at[1, by - 1, i])
                at += width
        mine = block_of(buf, f)
        for by in range(1, n.chips):
            send(
                mine, mine, plane_sem.at[0, by], plane_sem.at[1, by], chip_ahead(by) * 2 + core
            )
        send(mine, mine, sib_sem.at[0, 0], sib_sem.at[1, 0], sibling)

    def weights_forward(buf, plane_sem, sib_sem):
        for by in range(1, n.chips):
            piece = block_of(buf, chip_behind(by) * 2 + core)
            arrived(piece, plane_sem.at[1, by])
            send(piece, piece, sib_sem.at[0, by], sib_sem.at[1, by], sibling)

    def weights_wait(buf, sib_sem):
        for by in range(n.chips):
            arrived(block_of(buf, chip_behind(by) * 2 + 1 - core), sib_sem.at[1, by])

    def grads_pair(buf, sib_in, sib_sem):
        for by in range(n.chips):
            send(
                block_of(buf, chip_ahead(by) * 2 + 1 - core),
                sib_in.at[by],
                sib_sem.at[0, by],
                sib_sem.at[1, by],
                sibling,
            )

    def grads_plane(buf, sib_in, sib_sem, plane_in, plane_sem):
        for by in range(1, n.chips):
            arrived(sib_in.at[by], sib_sem.at[1, by])
            piece = block_of(buf, chip_ahead(by) * 2 + core)
            piece[...] = (piece[...].astype(F32) + sib_in[by].astype(F32)).astype(BF16)
            send(
                piece,
                plane_in.at[by - 1],
                plane_sem.at[0, by],
                plane_sem.at[1, by],
                chip_ahead(by) * 2 + core,
            )

    def grads_line(buf, sib_in, sib_sem, plane_in, plane_sem, total, land, line_sem):
        arrived(sib_in.at[0], sib_sem.at[1, 0])
        for by in range(1, n.chips):
            arrived(plane_in.at[by - 1], plane_sem.at[1, by])
        acc = block_of(buf, f)[...].astype(F32) + sib_in[0].astype(F32)
        for by in range(1, n.chips):
            acc = acc + plane_in[by - 1].astype(F32)
        total[...] = acc.astype(BF16)
        for by in range(1, n.ctx):
            start = pl.multiple_of(ahead(by) * shard, shard)
            send(
                total.at[pl.ds(start, shard), :],
                land.at[c],
                line_sem.at[0, by],
                line_sem.at[1, by],
                None,
                ahead(by),
            )
        land[c] = total[pl.ds(pl.multiple_of(c * shard, shard), shard), :]

    def grads_out(land, line_sem, outs, cols):
        for by in range(1, n.ctx):
            arrived(land.at[behind(by)], line_sem.at[1, by])
        at = 0
        for out, width in zip(outs, cols):
            for j in range(n.ctx):
                out[:, j * width : (j + 1) * width] = land[j, :, at : at + width].astype(F32)
            at += width

    def save_lines(first, line):
        for j in range(n.lines):
            r.g1_acc[3, first + j : first + j + 1, :] = line[:, j * HEAD_DIM : (j + 1) * HEAD_DIM]

    def small_start(src, incoming, sem):
        send(src, incoming.at[0], sem.at[0, 0], sem.at[1, 0], sibling)

    def small_plane(src, incoming, acc, sem):
        arrived(incoming.at[0], sem.at[1, 0])
        acc[0] = src[...] + incoming[0]
        for by in range(1, n.chips):
            send(
                acc.at[0],
                incoming.at[by],
                sem.at[0, by],
                sem.at[1, by],
                chip_ahead(by) * 2 + core,
            )

    def small_line(incoming, acc, sem):
        total = acc[0]
        for by in range(1, n.chips):
            arrived(incoming.at[by], sem.at[1, by])
            total = total + incoming[by]
        acc[1] = total
        for by in range(1, n.ctx):
            slot = n.chips + by
            send(acc.at[1], incoming.at[slot], sem.at[0, slot], sem.at[1, slot], None, ahead(by))

    def small_end(incoming, acc, sem):
        total = acc[1]
        for by in range(1, n.ctx):
            slot = n.chips + by
            arrived(incoming.at[slot], sem.at[1, slot])
            total = total + incoming[slot]
        return total

    attn_shards, mlp_shards = (r.wq, r.wk, r.wv, r.wo), (r.wg, r.wu, r.wd)
    attn_cols, mlp_cols = n.cols[:4], n.cols[4:]
    q_cols, k_cols, _, o_cols = attn_cols
    ff = mlp_cols[0]
    group = n.heads // n.kv
    factor = 1.0 / math.sqrt(HEAD_DIM)

    small_start(r.gains, r.g0_in, r.sem_g0)
    weights_send(attn_shards, attn_cols, r.wa, r.sem_wa)
    gather_start(r.hidden, r.xb, r.sem_xb)
    own_x = pltpu.make_async_copy(r.hidden, r.xb.at[c], r.local_sem.at[7])
    own_x.start()
    own_g = pltpu.make_async_copy(r.cot, r.gb.at[c], r.local_sem.at[8])
    own_g.start()
    own_attn = weights_own(attn_shards, attn_cols, r.wa, 0)
    own_mlp = weights_own(mlp_shards, mlp_cols, r.wm, 4)
    small_plane(r.gains, r.g0_in, r.g0_acc, r.sem_g0)
    small_line(r.g0_in, r.g0_acc, r.sem_g0)
    gains = small_end(r.g0_in, r.g0_acc, r.sem_g0)
    r.g0_acc[2] = gains
    for j in range(n.lines):
        r.gv[0, :, j * HEAD_DIM : (j + 1) * HEAD_DIM] = r.g0_acc[2, j : j + 1, :]
        r.gv[1, :, j * HEAD_DIM : (j + 1) * HEAD_DIM] = r.g0_acc[
            2, n.lines + j : n.lines + j + 1, :
        ]
    qgain = r.g0_acc[2, 2 * n.lines : 2 * n.lines + 1, :]
    kgain = r.g0_acc[2, 2 * n.lines + 1 : 2 * n.lines + 2, :]
    attn_gain, mlp_gain = r.gv[0], r.gv[1]

    weights_spread(own_attn, attn_cols, r.wa, r.sem_wa, r.sem_pwa, r.sem_swa)
    gather_relay(r.xb, r.sem_xb)
    weights_send(mlp_shards, mlp_cols, r.wm, r.sem_wm)
    for by in range(1, n.ctx):
        send(r.cot, r.gb.at[c], r.sem_g.at[0, by], r.sem_g.at[1, by], None, ahead(by))
    own_x.wait()
    own_g.wait()

    def norm_rows(j, carry):
        x = r.xb[j].astype(F32)
        start = pl.multiple_of(j * rows, rows)
        r.xn[pl.ds(start, rows), :] = (x * rms(x) * attn_gain).astype(BF16)
        return carry

    lax.fori_loop(0, n.ctx, norm_rows, 0)
    weights_forward(r.wa, r.sem_pwa, r.sem_swa)
    weights_wait(r.wa, r.sem_swa)

    cosine, sine = r.cos, r.sin
    tile = 2 * HEAD_DIM if n.kv % 2 == 0 else HEAD_DIM
    for at in range(0, q_cols + 2 * k_cols, tile):
        product = mm(r.xn[...], r.wa[:, at : at + tile])
        for part in range(tile // HEAD_DIM):
            head = at // HEAD_DIM + part
            u = product[:, part * HEAD_DIM : (part + 1) * HEAD_DIM]
            if head < n.heads:
                r.qp[head] = u
                r.qr[head] = rope_fwd(u * rms(u) * qgain, cosine[...], sine[...]).astype(BF16)
            elif head < n.heads + n.kv:
                r.kp[head - n.heads] = u
                r.kr[head - n.heads] = rope_fwd(u * rms(u) * kgain, cosine[...], sine[...]).astype(
                    BF16
                )
            else:
                r.vv[head - n.heads - n.kv] = u.astype(BF16)
    half = n.tokens // 2

    def head_forward(h, carry):
        kv = h // group
        for q0 in (0, half):
            s = mm(r.qr[h, q0 : q0 + half, :], r.kr[kv], LAST_AXIS)
            allowed = r.posk[...] <= r.posq[q0 : q0 + half, :]
            e = jnp.where(allowed, jnp.exp(s * factor), 0.0)
            r.es[h, q0 : q0 + half, :] = e
            total = jnp.sum(e, axis=-1, keepdims=True)
            a = mm(e.astype(BF16), r.vv[kv]) / total
            r.af[h, q0 : q0 + half, :] = a
            lane = pl.multiple_of(h * HEAD_DIM, HEAD_DIM)
            r.at[q0 : q0 + half, pl.ds(lane, HEAD_DIM)] = a.astype(BF16)
        return carry

    lax.fori_loop(0, n.heads, head_forward, 0)
    o_at = q_cols + 2 * k_cols

    def by_rows(left, right, out):
        def step(j, carry):
            start = pl.multiple_of(j * rows, rows)
            out[j] = mm(left[pl.ds(start, rows), :], right(), LAST_AXIS).astype(BF16)
            return carry

        lax.fori_loop(0, n.ctx, step, 0)

    by_rows(r.at, lambda: r.wa[:, o_at:], r.p_o)
    scatter(r.p_o, r.l_o, r.r_o, r.sem_o)
    weights_spread(own_mlp, mlp_cols, r.wm, r.sem_wm, r.sem_pwm, r.sem_swm)
    r.ho[...] = r.xb[c].astype(F32)
    scatter_total(r.p_o, r.l_o, r.r_o, r.sem_o, r.ho)
    h_own = r.ho[...]
    r.mb[c] = (h_own * rms(h_own) * mlp_gain).astype(BF16)
    gather_start(r.mb.at[c], r.mb, r.sem_mb)
    gather_relay(r.mb, r.sem_mb)
    weights_forward(r.wm, r.sem_pwm, r.sem_swm)
    for by in range(1, n.ctx):
        arrived(r.gb.at[behind(by)], r.sem_g.at[1, by])
    weights_wait(r.wm, r.sem_swm)

    mixed = r.mb[...].reshape(n.tokens, d)
    upstream = r.gb[...].reshape(n.tokens, d)
    tile = 2 * HEAD_DIM if ff % (2 * HEAD_DIM) == 0 else HEAD_DIM
    for at in range(0, ff, tile):
        gate = mm(mixed, r.wm[:, at : at + tile])
        up = mm(mixed, r.wm[:, ff + at : ff + at + tile])
        back = mm(upstream, r.wm[:, 2 * ff + at : 2 * ff + at + tile])
        sig = jax.nn.sigmoid(gate)
        swish = gate * sig
        r.hid[:, at : at + tile] = (swish * up).astype(BF16)
        r.dgu[:, at : at + tile] = (back * up * sig * (1.0 + gate * (1.0 - sig))).astype(BF16)
        r.dgu[:, ff + at : ff + at + tile] = (back * swish).astype(BF16)

    by_rows(r.dgu, lambda: r.wm[:, : 2 * ff], r.p_x2)
    scatter(r.p_x2, r.l_x2, r.r_x2, r.sem_x2)
    by_rows(r.hid, lambda: r.wm[:, 2 * ff :], r.p_y)
    r.dh[...] = jnp.zeros_like(r.dh)
    scatter_total(r.p_x2, r.l_x2, r.r_x2, r.sem_x2, r.dh)
    h_own = r.ho[...]
    from_norm, term = norm_back(h_own, rms(h_own), mlp_gain, r.dh[...])
    r.g1_acc[3] = jnp.zeros_like(r.g1_acc[3])
    save_lines(n.lines, jnp.sum(term, axis=0, keepdims=True))
    r.dh[...] = r.gb[c].astype(F32) + from_norm
    r.rb[c] = r.dh[...].astype(BF16)
    gather_start(r.rb.at[c], r.rb, r.sem_rb)
    gather_relay(r.rb, r.sem_rb)
    for by in range(1, n.ctx):
        send(
            r.p_y.at[ahead(by)], r.i_y.at[by - 1], r.sem_y.at[0, by], r.sem_y.at[1, by], None, ahead(by)
        )
    for at in range(0, 2 * ff, tile):
        r.gm[:, at : at + tile] = mm(mixed, r.dgu[:, at : at + tile], FIRST_AXIS).astype(BF16)
    for at in range(0, ff, tile):
        r.gm[:, 2 * ff + at : 2 * ff + at + tile] = mm(
            upstream, r.hid[:, at : at + tile], FIRST_AXIS
        ).astype(BF16)
    grads_pair(r.gm, r.gm_sib, r.sem_sgm)

    upstream = r.rb[...].reshape(n.tokens, d)
    for at in range(0, o_cols, HEAD_DIM):
        r.da[at // HEAD_DIM] = mm(upstream, r.wa[:, o_at + at : o_at + at + HEAD_DIM])
    grads_plane(r.gm, r.gm_sib, r.sem_sgm, r.gm_in, r.sem_pgm)
    r.dk[...] = jnp.zeros_like(r.dk)
    r.dv[...] = jnp.zeros_like(r.dv)

    def head_backward(h, carry):
        kv = h // group
        for q0 in (0, half):
            span = slice(q0, q0 + half)
            e = r.es[h, span, :]
            total = jnp.sum(e, axis=-1, keepdims=True)
            da = r.da[h, span, :]
            w = (da / total).astype(BF16)
            dl = jnp.sum(da * r.af[h, span, :], axis=-1, keepdims=True) / total
            ds = (e * (mm(w, r.vv[kv], LAST_AXIS) - dl)).astype(BF16)
            r.ds[span, :] = ds
            r.eb[span, :] = e.astype(BF16)
            r.wb[span, :] = w
            r.da[h, span, :] = mm(ds, r.kr[kv])
        r.dk[kv] = r.dk[kv] + mm(r.ds[...], r.qr[h], FIRST_AXIS)
        r.dv[kv] = r.dv[kv] + mm(r.eb[...], r.wb[...], FIRST_AXIS)
        return carry

    lax.fori_loop(0, n.heads, head_backward, 0)

    def query_backward(h, term):
        u = r.qp[h]
        du, gain_term = norm_back(
            u, rms(u), qgain, rope_bwd(r.da[h] * factor, cosine[...], sine[...])
        )
        lane = pl.multiple_of(h * HEAD_DIM, HEAD_DIM)
        r.dqkv[:, pl.ds(lane, HEAD_DIM)] = du.astype(BF16)
        return term + jnp.sum(gain_term, axis=0, keepdims=True)

    q_term = lax.fori_loop(0, n.heads, query_backward, jnp.zeros((1, HEAD_DIM), F32))
    k_term = jnp.zeros((1, HEAD_DIM), F32)
    for kv in range(n.kv):
        u = r.kp[kv]
        du, gain_term = norm_back(
            u, rms(u), kgain, rope_bwd(r.dk[kv] * factor, cosine[...], sine[...])
        )
        at = q_cols + kv * HEAD_DIM
        r.dqkv[:, at : at + HEAD_DIM] = du.astype(BF16)
        at += k_cols
        r.dqkv[:, at : at + HEAD_DIM] = r.dv[kv].astype(BF16)
        k_term = k_term + jnp.sum(gain_term, axis=0, keepdims=True)
    by_rows(r.dqkv, lambda: r.wa[:, :o_at], r.p_x1)
    scatter(r.p_x1, r.l_x1, r.r_x1, r.sem_x1)
    for at in range(0, o_at, 2 * HEAD_DIM):
        r.ga[:, at : at + 2 * HEAD_DIM] = mm(
            r.xn[...], r.dqkv[:, at : at + 2 * HEAD_DIM], FIRST_AXIS
        ).astype(BF16)
    r.ga[:, o_at:] = mm(upstream, r.at[...], FIRST_AXIS).astype(BF16)
    grads_pair(r.ga, r.ga_sib, r.sem_sga)
    grads_line(
        r.gm, r.gm_sib, r.sem_sgm, r.gm_in, r.sem_pgm, r.gm_z, r.gm_land, r.sem_zgm
    )
    grads_plane(r.ga, r.ga_sib, r.sem_sga, r.ga_in, r.sem_pga)

    r.out_input[...] = jnp.zeros_like(r.out_input)
    scatter_total(r.p_x1, r.l_x1, r.r_x1, r.sem_x1, r.out_input)
    x = r.xb[c].astype(F32)
    from_norm, term = norm_back(x, rms(x), attn_gain, r.out_input[...])
    save_lines(0, jnp.sum(term, axis=0, keepdims=True))
    r.out_input[...] = r.dh[...] + from_norm
    r.g1_acc[3, 2 * n.lines : 2 * n.lines + 1, :] = q_term
    r.g1_acc[3, 2 * n.lines + 1 : 2 * n.lines + 2, :] = k_term
    small_start(r.g1_acc.at[3], r.g1_in, r.sem_g1)
    small_plane(r.g1_acc.at[3], r.g1_in, r.g1_acc, r.sem_g1)
    out = r.ho[...] + r.p_y[c].astype(F32)
    for by in range(1, n.ctx):
        arrived(r.i_y.at[by - 1], r.sem_y.at[1, by])
        out = out + r.i_y[by - 1].astype(F32)
    r.out_hidden[...] = out.astype(BF16)
    small_line(r.g1_in, r.g1_acc, r.sem_g1)
    grads_line(
        r.ga, r.ga_sib, r.sem_sga, r.ga_in, r.sem_pga, r.ga_z, r.ga_land, r.sem_zga
    )
    grads_out(r.gm_land, r.sem_zgm, (r.og, r.ou, r.od), mlp_cols)
    r.out_gains[...] = small_end(r.g1_in, r.g1_acc, r.sem_g1)
    grads_out(r.ga_land, r.sem_zga, (r.oq, r.ok, r.ov, r.oo), attn_cols)
    for wait in sends:
        wait()


def fused(
    ctx,
    fsdp,
    hidden_in,
    block_order,
    cotangent,
    q_weight,
    k_weight,
    v_weight,
    o_weight,
    attn_gain,
    query_gain,
    key_gain,
    mlp_gain,
    gate_weight,
    up_weight,
    down_weight,
):
    shards = (q_weight, k_weight, v_weight, o_weight, gate_weight, up_weight, down_weight)
    n = Sizes(ctx, fsdp, hidden_in.shape[1], shards)
    me = lax.axis_index("fsdp") * ctx + lax.axis_index("ctx")
    count = ctx * fsdp
    slots = block_order.shape[1]
    block_len = n.tokens // slots
    positions = (
        block_order[0][:, None] * block_len + jnp.arange(block_len, dtype=jnp.int32)[None, :]
    ).reshape(-1)
    cosine, sine = rope_tables(positions, HEAD_DIM)
    sign = jnp.where(jnp.arange(HEAD_DIM) < HEAD_DIM // 2, -1.0, 1.0)
    sine = sine * sign

    def placed(gain):
        own = jnp.arange(count, dtype=jnp.int32)[:, None] == me
        whole = jnp.where(own, gain.astype(F32)[None, :], 0.0)
        return whole.reshape(-1, HEAD_DIM)

    gains = jnp.concatenate([placed(g) for g in (attn_gain, mlp_gain, query_gain, key_gain)])
    gains = jnp.pad(gains, ((0, n.gain_rows - gains.shape[0]), (0, 0)))
    hbm, vmem = pl.BlockSpec(memory_space=pl.ANY), pl.BlockSpec(memory_space=pltpu.VMEM)
    inputs = dict(
        hidden=(hidden_in[0], hbm),
        cot=(cotangent[0], hbm),
        wq=(q_weight, hbm),
        wk=(k_weight, hbm),
        wv=(v_weight, hbm),
        wo=(o_weight, hbm),
        wg=(gate_weight, hbm),
        wu=(up_weight, hbm),
        wd=(down_weight, hbm),
        gains=(gains, vmem),
        cos=(cosine, vmem),
        sin=(sine, vmem),
        posq=(positions[:, None], vmem),
        posk=(positions[None, :], vmem),
    )
    outputs = dict(
        out_hidden=jax.ShapeDtypeStruct((n.rows, n.width), BF16),
        out_input=jax.ShapeDtypeStruct((n.rows, n.width), F32),
        oq=jax.ShapeDtypeStruct(q_weight.shape, F32),
        ok=jax.ShapeDtypeStruct(k_weight.shape, F32),
        ov=jax.ShapeDtypeStruct(v_weight.shape, F32),
        oo=jax.ShapeDtypeStruct(o_weight.shape, F32),
        og=jax.ShapeDtypeStruct(gate_weight.shape, F32),
        ou=jax.ShapeDtypeStruct(up_weight.shape, F32),
        od=jax.ShapeDtypeStruct(down_weight.shape, F32),
        out_gains=jax.ShapeDtypeStruct((n.gain_rows, HEAD_DIM), F32),
    )
    scratch = scratch_of(n)
    result, input_grad, oq, ok, ov, oo, og, ou, od, sums = pl.pallas_call(
        functools.partial(layer_kernel, n, [*inputs, *outputs, *scratch]),
        out_shape=tuple(outputs.values()),
        in_specs=[spec for _, spec in inputs.values()],
        out_specs=tuple(vmem for _ in outputs),
        scratch_shapes=list(scratch.values()),
        compiler_params=pltpu.CompilerParams(
            collective_id=0, has_side_effects=True, vmem_limit_bytes=VMEM_LIMIT
        ),
        name="layer",
    )(*[value for value, _ in inputs.values()])

    def own(first, size):
        flat = sums[first : first + size // HEAD_DIM].reshape(-1)
        return lax.dynamic_slice_in_dim(flat, me * (size // count), size // count)

    lines = n.lines
    return (
        result[None],
        input_grad[None],
        oq,
        ok,
        ov,
        oo,
        own(0, n.width),
        own(2 * lines, HEAD_DIM),
        own(2 * lines + 1, HEAD_DIM),
        own(lines, n.width),
        og,
        ou,
        od,
    )


def fits(ctx, fsdp, shard_rows):
    return shard_rows % 16 == 0 and fsdp % 2 == 0 and KV_HEADS % ctx == 0


def solution(mesh):
    ctx, fsdp = mesh.shape["ctx"], mesh.shape["fsdp"]
    tokens = P("fsdp", "ctx", None)
    matrix = P(("fsdp", "ctx"), None)
    vector = P(("fsdp", "ctx"))
    def step(hidden_in, block_order, cotangent, q_weight, *rest):
        whole = fused if fits(ctx, fsdp, q_weight.shape[0]) else local
        return whole(ctx, fsdp, hidden_in, block_order, cotangent, q_weight, *rest)

    return jax.shard_map(
        step,
        mesh=mesh,
        in_specs=(tokens, P("fsdp", None), tokens)
        + (matrix,) * 4
        + (vector,) * 4
        + (matrix,) * 3,
        out_specs=(tokens,) * 2 + (matrix,) * 4 + (vector,) * 4 + (matrix,) * 3,
        check_vma=False,
    )
```

```python
import functools
import math
import types

import jax
import jax.numpy as jnp
from jax import lax
from jax.experimental import pallas as pl
from jax.experimental.pallas import tpu as pltpu
from jax.sharding import PartitionSpec as P

HEADS = 16
KV_HEADS = 8
HEAD_DIM = 128
EPSILON = 1e-06
FIRST_AXIS = (((0,), (0,)), ((), ()))
LAST_AXIS = (((1,), (1,)), ((), ()))
BF16 = jnp.bfloat16
F32 = jnp.float32
VMEM_LIMIT = 67043328
PARTS = 2


def mm(left, right, dims=(((1,), (0,)), ((), ()))):
    return lax.dot_general(left, right, dims, preferred_element_type=F32)


def rms(signal):
    return lax.rsqrt(jnp.mean(signal * signal, axis=-1, keepdims=True) + EPSILON)


def norm_back(signal, inverse_rms, gain_vec, upstream):
    unit_values = signal * inverse_rms
    scaled_up = upstream * gain_vec
    inner = scaled_up - unit_values * jnp.mean(scaled_up * unit_values, axis=-1, keepdims=True)
    return (inverse_rms * inner, upstream * unit_values)


def rope_tables(positions, head_width):
    exponent = jnp.arange(head_width // 2, dtype=F32) * (2.0 / head_width)
    inverse = jnp.exp(-exponent * math.log(1000000.0))
    angles = positions.astype(F32)[:, None] * inverse[None, :]
    angles = jnp.concatenate([angles, angles], axis=-1)
    return (jnp.cos(angles), jnp.sin(angles))


def rotate(signal, cosine, sine):
    half = signal.shape[-1] // 2
    turned = jnp.concatenate([-signal[..., half:], signal[..., :half]], axis=-1)
    return signal * cosine + turned * sine


def rotate_back(upstream, cosine, sine):
    half = upstream.shape[-1] // 2
    scaled_up = upstream * sine
    return upstream * cosine + jnp.concatenate(
        [scaled_up[..., half:], -scaled_up[..., :half]], axis=-1
    )


def gather_columns(ctx, shards):
    rows = shards[0].shape[0]
    cut = [s.reshape(rows, ctx, s.shape[1] // ctx).transpose(1, 0, 2) for s in shards]
    widths = [c.shape[2] for c in cut]
    both = jnp.concatenate(cut, axis=2)
    both = lax.all_to_all(both, "ctx", 0, 0, tiled=True)
    both = both.reshape(ctx * rows, -1)
    whole = lax.all_gather(both, "fsdp", axis=0, tiled=True)
    out, at = [], 0
    for width in widths:
        out.append(whole[:, at : at + width])
        at += width
    return out


def scatter_grads(ctx, fsdp, grads):
    rows = grads[0].shape[0] // (ctx * fsdp)
    widths = [g.shape[1] for g in grads]
    both = jnp.concatenate([g.astype(BF16) for g in grads], axis=1)
    both = lax.psum_scatter(both, "fsdp", scatter_dimension=0, tiled=True)
    both = lax.all_to_all(both.reshape(ctx, rows, -1), "ctx", 0, 0, tiled=True)
    out, at = [], 0
    for width in widths:
        piece = both[:, :, at : at + width]
        out.append(piece.transpose(1, 0, 2).reshape(rows, ctx * width).astype(F32))
        at += width
    return out


def ctx_gather(rows):
    return lax.all_gather(rows, "ctx", axis=0, tiled=True)


def ctx_scatter(partial):
    return lax.psum_scatter(partial.astype(BF16), "ctx", scatter_dimension=0, tiled=True).astype(
        F32
    )


def local(
    ctx,
    fsdp,
    hidden_in,
    block_order,
    cotangent,
    q_weight,
    k_weight,
    v_weight,
    o_weight,
    attn_gain,
    query_gain,
    key_gain,
    mlp_gain,
    gate_weight,
    up_weight,
    down_weight,
):
    inputs = hidden_in[0].astype(F32)
    row_count = inputs.shape[0]
    tokens = row_count * ctx
    slots = block_order.shape[1]
    block_len = tokens // slots
    heads, kv_heads = HEADS // ctx, KV_HEADS // ctx
    group = heads // kv_heads
    factor = 1.0 / math.sqrt(HEAD_DIM)
    positions = (
        block_order[0][:, None] * block_len + jnp.arange(block_len, dtype=jnp.int32)[None, :]
    ).reshape(-1)
    cosine, sine = rope_tables(positions, HEAD_DIM)
    cosine, sine = cosine[:, None, :], sine[:, None, :]

    both = ("fsdp", "ctx")
    norm_gain, qgain, kgain, mlp_norm_gain = (
        lax.all_gather(g, both, axis=0, tiled=True).astype(F32)
        for g in (attn_gain, query_gain, key_gain, mlp_gain)
    )
    norm_scale = rms(inputs)
    normed = ctx_gather((inputs * norm_scale * norm_gain).astype(BF16))
    upstream = ctx_gather(cotangent[0])
    q_full, k_full, v_full, o_full = gather_columns(ctx, (q_weight, k_weight, v_weight, o_weight))
    gate_full, up_full, down_full = gather_columns(ctx, (gate_weight, up_weight, down_weight))

    query_proj = mm(normed, q_full).reshape(tokens, heads, HEAD_DIM)
    key_proj = mm(normed, k_full).reshape(tokens, kv_heads, HEAD_DIM)
    value_low = mm(normed, v_full).astype(BF16).reshape(tokens, kv_heads, HEAD_DIM)
    query_scale, key_scale = rms(query_proj), rms(key_proj)
    query_low = (
        rotate(query_proj * query_scale * qgain, cosine, sine)
        .astype(BF16)
        .reshape(tokens, kv_heads, group, HEAD_DIM)
    )
    key_low = rotate(key_proj * key_scale * kgain, cosine, sine).astype(BF16)
    scores = jnp.einsum("rkgd,nkd->kgrn", query_low, key_low, preferred_element_type=F32) * factor
    allowed = positions[None, :] <= positions[:, None]
    weights_exp = jnp.where(allowed, jnp.exp(scores), 0.0)
    denominator = jnp.sum(weights_exp, axis=-1)
    weights_low = weights_exp.astype(BF16)
    numerator = jnp.einsum("kgrn,nkd->rkgd", weights_low, value_low, preferred_element_type=F32)
    denom_rows = jnp.transpose(denominator, (2, 0, 1))[..., None]
    attn_full = numerator / denom_rows
    attn_low = attn_full.astype(BF16).reshape(tokens, heads * HEAD_DIM)
    residual = inputs + ctx_scatter(mm(attn_low, o_full, LAST_AXIS))

    mix_scale = rms(residual)
    mixed = ctx_gather((residual * mix_scale * mlp_norm_gain).astype(BF16))
    gate_val = mm(mixed, gate_full)
    up_val = mm(mixed, up_full)
    sigmoid_gate = jax.nn.sigmoid(gate_val)
    swish_gate = gate_val * sigmoid_gate
    hidden_low = (swish_gate * up_val).astype(BF16)
    result = residual + ctx_scatter(mm(hidden_low, down_full, LAST_AXIS))
    hidden_grad = mm(upstream, down_full)
    gate_back = (
        hidden_grad * up_val * sigmoid_gate * (1.0 + gate_val * (1.0 - sigmoid_gate))
    ).astype(BF16)
    up_back = (hidden_grad * swish_gate).astype(BF16)
    mixed_grad = ctx_scatter(mm(gate_back, gate_full, LAST_AXIS) + mm(up_back, up_full, LAST_AXIS))
    resid_from_norm, mlp_gain_term = norm_back(residual, mix_scale, mlp_norm_gain, mixed_grad)
    residual_grad = cotangent[0].astype(F32) + resid_from_norm
    mlp_grads = scatter_grads(
        ctx,
        fsdp,
        (
            mm(mixed, gate_back, FIRST_AXIS),
            mm(mixed, up_back, FIRST_AXIS),
            mm(upstream, hidden_low, FIRST_AXIS),
        ),
    )
    resid_low = ctx_gather(residual_grad.astype(BF16))

    attn_grad = mm(resid_low, o_full).reshape(tokens, kv_heads, group, HEAD_DIM)
    share_low = (attn_grad / denom_rows).astype(BF16)
    denom_grad = jnp.transpose(jnp.sum(attn_grad * attn_full, axis=-1), (1, 2, 0)) / denominator
    weight_grad = jnp.einsum("rkgd,nkd->kgrn", share_low, value_low, preferred_element_type=F32)
    score_low = (weights_exp * (weight_grad - denom_grad[..., None])).astype(BF16)
    query_rot = (
        jnp.einsum("kgrn,nkd->rkgd", score_low, key_low, preferred_element_type=F32) * factor
    ).reshape(tokens, heads, HEAD_DIM)
    key_rot = (
        jnp.einsum("kgrn,rkgd->nkd", score_low, query_low, preferred_element_type=F32) * factor
    )
    value_back = (
        jnp.einsum("kgrn,rkgd->nkd", weights_low, share_low, preferred_element_type=F32)
        .reshape(tokens, kv_heads * HEAD_DIM)
        .astype(BF16)
    )
    query_grad, query_term = norm_back(
        query_proj, query_scale, qgain, rotate_back(query_rot, cosine, sine)
    )
    key_grad, key_term = norm_back(key_proj, key_scale, kgain, rotate_back(key_rot, cosine, sine))
    query_back = query_grad.reshape(tokens, heads * HEAD_DIM).astype(BF16)
    key_back = key_grad.reshape(tokens, kv_heads * HEAD_DIM).astype(BF16)
    normed_grad = ctx_scatter(
        mm(query_back, q_full, LAST_AXIS)
        + mm(key_back, k_full, LAST_AXIS)
        + mm(value_back, v_full, LAST_AXIS)
    )
    input_from_norm, attn_gain_term = norm_back(inputs, norm_scale, norm_gain, normed_grad)
    input_grad = residual_grad + input_from_norm
    attn_grads = scatter_grads(
        ctx,
        fsdp,
        (
            mm(normed, query_back, FIRST_AXIS),
            mm(normed, key_back, FIRST_AXIS),
            mm(normed, value_back, FIRST_AXIS),
            mm(resid_low, attn_low, FIRST_AXIS),
        ),
    )
    gains = (
        jnp.sum(attn_gain_term, axis=0),
        jnp.sum(query_term, axis=(0, 1)),
        jnp.sum(key_term, axis=(0, 1)),
        jnp.sum(mlp_gain_term, axis=0),
    )
    gains = [lax.psum_scatter(g, both, scatter_dimension=0, tiled=True) for g in gains]
    return (
        result.astype(BF16)[None],
        input_grad[None],
        *attn_grads,
        *gains,
        *mlp_grads,
    )


def rope_fwd(u, cosine, sine):
    return u * cosine + pltpu.roll(u, HEAD_DIM // 2, u.ndim - 1) * sine


def rope_bwd(du, cosine, sine):
    return du * cosine - pltpu.roll(du, HEAD_DIM // 2, du.ndim - 1) * sine


class Sizes:
    def __init__(self, ctx, fsdp, rows, shards):
        self.ctx, self.fsdp, self.rows = ctx, fsdp, rows
        self.chips = fsdp // 2
        self.shard = shards[0].shape[0]
        self.block = self.shard * ctx
        self.width = self.block * fsdp
        self.tokens = rows * ctx
        self.heads, self.kv = HEADS // ctx, KV_HEADS // ctx
        self.cols = [s.shape[1] // ctx for s in shards]
        self.attn_cols = sum(self.cols[:4])
        self.mlp_cols = sum(self.cols[4:])
        self.lines = self.width // HEAD_DIM
        self.gain_rows = 8 * ((2 * self.lines + 2 + 7) // 8)
        self.each, self.few = self.width // (ctx * fsdp), HEAD_DIM // (ctx * fsdp)


def scratch_of(n):
    bf, f32 = (lambda *s: pltpu.VMEM(s, BF16)), (lambda *s: pltpu.VMEM(s, F32))
    sem = lambda *s: pltpu.SemaphoreType.DMA(s)
    c, d, s, h, kv = n.ctx, n.width, n.tokens, n.heads, n.kv
    ff = n.cols[4]
    out = dict(
        wa=bf(d, n.attn_cols),
        wm=bf(d, n.mlp_cols),
        xb=bf(c, n.rows, d),
        gb=bf(c, n.rows, d),
        mb=bf(c, n.rows, d),
        rb=bf(c, n.rows, d),
        xn=bf(s, d),
        qp=f32(h, s, HEAD_DIM),
        kp=f32(kv, s, HEAD_DIM),
        qr=bf(h, s, HEAD_DIM),
        kr=bf(kv, s, HEAD_DIM),
        vv=bf(kv, s, HEAD_DIM),
        es=f32(h, s, s),
        af=f32(h, s, HEAD_DIM),
        at=bf(s, h * HEAD_DIM),
        da=f32(h, s, HEAD_DIM),
        dk=f32(kv, s, HEAD_DIM),
        dv=f32(kv, s, HEAD_DIM),
        ds=bf(s, s),
        eb=bf(s, s),
        wb=bf(s, HEAD_DIM),
        dqkv=bf(s, (h + 2 * kv) * HEAD_DIM),
        hid=bf(c, n.rows, ff),
        dgu=bf(c, n.rows, 2 * ff),
        ho=f32(n.rows, d),
        dh=f32(n.rows, d),
        gv=f32(2, 1, d),
        gp=f32(n.gain_rows, HEAD_DIM),
        cos=f32(s, HEAD_DIM),
        sin=f32(s, HEAD_DIM),
        posq=pltpu.VMEM((s, HEAD_DIM), jnp.int32),
        posk=pltpu.VMEM((1, s), jnp.int32),
        ga=bf(d, n.attn_cols),
        gm=bf(d, n.mlp_cols),
        ga_sib=bf(n.chips, n.block, n.attn_cols),
        gm_sib=bf(n.chips, n.block, n.mlp_cols),
        ga_in=bf(n.chips - 1, n.block, n.attn_cols),
        gm_in=bf(n.chips - 1, n.block, n.mlp_cols),
        ga_z=bf(n.block, n.attn_cols),
        gm_z=bf(n.block, n.mlp_cols),
        local_sem=sem(9),
    )
    for name in ("o", "y", "x2", "x1"):
        out["p_" + name] = bf(c, n.rows, d)
        out["l_" + name] = bf(c, n.rows, d)
        out["r_" + name] = bf(c, n.rows, d)
        out["sem_" + name] = sem(4, c, PARTS)
    for name in ("xb", "gb", "mb", "rb"):
        out["sem_" + name] = sem(3, c, PARTS)
    out["sem_wa"] = sem(2, c - 1, 4)
    out["sem_wm"] = sem(2, c - 1, 3)
    for name in ("pq", "po", "pm"):
        out["sem_" + name] = sem(4, n.chips)
    for name in ("gm", "go", "gq"):
        out["sem_" + name] = sem(4, n.chips)
        out["sem_z" + name] = sem(2, c)
    for name in ("g0", "g1"):
        out[name + "_in"] = f32(n.chips + c, n.gain_rows, HEAD_DIM)
        out[name + "_acc"] = f32(4, n.gain_rows, HEAD_DIM)
        out["sem_" + name] = sem(2, n.chips + c)
    return out


def layer_kernel(n, names, *refs):
    r = types.SimpleNamespace(**dict(zip(names, refs)))
    c, f = lax.axis_index("ctx"), lax.axis_index("fsdp")
    chip, core = f // 2, f % 2
    sibling = chip * 2 + 1 - core
    rows, d, block, shard = n.rows, n.width, n.block, n.shard
    sends = []

    def ahead(by):
        return lax.rem(c + by, n.ctx)

    def behind(by):
        return lax.rem(c + n.ctx - by, n.ctx)

    def chip_ahead(by):
        return lax.rem(chip + by, n.chips)

    def chip_behind(by):
        return lax.rem(chip + n.chips - by, n.chips)

    def remote(src, dst, send_sem, recv_sem, to_f=None, to_c=None):
        return pltpu.make_async_remote_copy(
            src_ref=src,
            dst_ref=dst,
            send_sem=send_sem,
            recv_sem=recv_sem,
            device_id={"fsdp": f if to_f is None else to_f, "ctx": c if to_c is None else to_c},
            device_id_type=pl.DeviceIdType.MESH,
        )

    def send(src, dst, send_sem, recv_sem, to_f=None, to_c=None):
        copy = remote(src, dst, send_sem, recv_sem, to_f, to_c)
        copy.start()
        sends.append(copy.wait_send)

    def arrived(dst, recv_sem):
        remote(dst, dst, recv_sem, recv_sem).wait_recv()

    def send_if(cond, src, dst, send_sem, recv_sem, to_c):
        copy = remote(src, dst, send_sem, recv_sem, None, to_c)
        pl.when(cond)(copy.start)
        sends.append(lambda: pl.when(cond)(copy.wait_send))

    barrier = pltpu.get_barrier_semaphore()

    def greet(to_f, to_c):
        pl.semaphore_signal(
            barrier,
            inc=1,
            device_id={"fsdp": to_f, "ctx": to_c},
            device_id_type=pl.DeviceIdType.MESH,
        )

    for by in range(1, n.ctx):
        greet(f, ahead(by))
    for by in range(1, n.chips):
        greet(chip_ahead(by) * 2 + core, c)
    greet(sibling, c)
    pl.semaphore_wait(barrier, n.ctx - 1 + n.chips)

    right, left = jnp.minimum(c + 1, n.ctx - 1), jnp.maximum(c - 1, 0)
    part_rows = rows // PARTS

    def part_of(buf, j, k):
        return buf.at[j, pl.ds(k * part_rows, part_rows), :]

    def gather_start(src, buf, sem, k, to=None):
        piece = src.at[pl.ds(k * part_rows, part_rows), :]
        here = part_of(buf, c, k)
        up, down = c + 1 < n.ctx, c > 0
        if to == "between":
            up, down = c + 1 < n.ctx - 1, c > 1
        elif to == "ends":
            up, down = c + 1 == n.ctx - 1, c == 1
        send_if(up, piece, here, sem.at[0, 0, k], sem.at[2, c, k], right)
        send_if(down, piece, here, sem.at[1, 0, k], sem.at[2, c, k], left)

    def gather_relay(buf, sem, by, k):
        low, high = jnp.maximum(c - by, 0), jnp.minimum(c + by, n.ctx - 1)
        piece, here = part_of(buf, low, k), sem.at[2, low, k]
        pl.when(c - by >= 0)(functools.partial(arrived, piece, here))
        cond = (c - by >= 0) & (c + 1 < n.ctx)
        send_if(cond, piece, piece, sem.at[0, by, k], here, right)
        piece, here = part_of(buf, high, k), sem.at[2, high, k]
        pl.when(c + by < n.ctx)(functools.partial(arrived, piece, here))
        cond = (c + by < n.ctx) & (c > 0)
        send_if(cond, piece, piece, sem.at[1, by, k], here, left)

    def rows_of(k):
        return slice(k * part_rows, (k + 1) * part_rows)

    def scatter_send(cond, part, there, sem, target, k, way, to_c):
        send_if(
            cond,
            part_of(part, target, k),
            part_of(there, target, k),
            sem.at[way, target, k],
            sem.at[2 + way, target, k],
            to_c,
        )

    def scatter_add(part, there, sem, target, k, way):
        arrived(part_of(there, target, k), sem.at[2 + way, target, k])
        span = rows_of(k)
        part[target, span, :] = (
            part[target, span, :].astype(F32) + there[target, span, :].astype(F32)
        ).astype(BF16)

    def scatter_start(g, k):
        for step in range(n.ctx - 1):
            scatter_send(c == n.ctx - 1, g.part, g.high, g.sem, step, k, 1, left)
            scatter_send(c == 0, g.part, g.low, g.sem, n.ctx - 1 - step, k, 0, right)

    def scatter_relay(g, step, k):
        target = step
        down = (c > target) & (c + 1 < n.ctx)
        pl.when(down)(functools.partial(scatter_add, g.part, g.high, g.sem, target, k, 1))
        scatter_send(down, g.part, g.high, g.sem, target, k, 1, left)
        target = n.ctx - 1 - step
        up = (c < target) & (c > 0)
        pl.when(up)(functools.partial(scatter_add, g.part, g.low, g.sem, target, k, 0))
        scatter_send(up, g.part, g.low, g.sem, target, k, 0, right)

    def scatter_total(g, out, k):
        span = rows_of(k)
        out[span, :] = out[span, :] + g.part[c, span, :].astype(F32)

        @pl.when(c > 0)
        def _():
            arrived(part_of(g.low, c, k), g.sem.at[2, c, k])
            out[span, :] = out[span, :] + g.low[c, span, :].astype(F32)

        @pl.when(c + 1 < n.ctx)
        def _():
            arrived(part_of(g.high, c, k), g.sem.at[3, c, k])
            out[span, :] = out[span, :] + g.high[c, span, :].astype(F32)

    def block_of(buf, index, span):
        return buf.at[pl.ds(pl.multiple_of(index * block, block), block), pl.ds(*span)]

    def piece_of(buf, line, at, width):
        start = pl.multiple_of(f * block + line * shard, shard)
        return buf.at[pl.ds(start, shard), pl.ds(at, width)]

    def weights_send(shards, cols, buf, sem, now=None):
        for by in range(1, n.ctx):
            at = 0
            for i, (src, width) in enumerate(zip(shards, cols)):
                column = pl.multiple_of(ahead(by) * width, HEAD_DIM)
                copy = remote(
                    src.at[:, pl.ds(column, width)],
                    piece_of(buf, c, at, width),
                    sem.at[0, by - 1, i],
                    sem.at[1, by - 1, i],
                    None,
                    ahead(by),
                )
                at_end = (ahead(by) == 0) | (ahead(by) == n.ctx - 1)
                if now is None:
                    copy.start()
                else:
                    pl.when(at_end if now == "ends" else ~at_end)(copy.start)
                if now != "ends":
                    sends.append(copy.wait_send)
                at += width

    def weights_own(shards, cols, buf, first):
        at, out = 0, []
        for i, (src, width) in enumerate(zip(shards, cols)):
            column = pl.multiple_of(c * width, HEAD_DIM)
            copy = pltpu.make_async_copy(
                src.at[:, pl.ds(column, width)],
                piece_of(buf, c, at, width),
                r.local_sem.at[first + i],
            )
            copy.start()
            out.append(copy)
            at += width
        return out

    def weights_spread(own, cols, sem, g):
        for copy in own:
            copy.wait()
        for by in range(1, n.ctx):
            at = g.span[0]
            for i, width in enumerate(cols):
                arrived(piece_of(g.buf, behind(by), at, width), sem.at[1, by - 1, g.first + i])
                at += width
        mine = block_of(g.buf, f, g.span)
        for by in range(1, n.chips):
            send(mine, mine, g.sem.at[0, by], g.sem.at[1, by], chip_ahead(by) * 2 + core)
        send(mine, mine, g.sem.at[2, 0], g.sem.at[3, 0], sibling)

    def weights_forward(g):
        for by in range(1, n.chips):
            piece = block_of(g.buf, chip_behind(by) * 2 + core, g.span)
            arrived(piece, g.sem.at[1, by])
            send(piece, piece, g.sem.at[2, by], g.sem.at[3, by], sibling)

    def weights_wait(g):
        for by in range(n.chips):
            arrived(block_of(g.buf, chip_behind(by) * 2 + 1 - core, g.span), g.sem.at[3, by])

    def share_of(buf, index, span):
        return buf.at[pl.ds(pl.multiple_of(index * block, block), block), pl.ds(*span)]

    def grads_pair(g):
        for by in (*range(1, n.chips), 0):
            send(
                share_of(g.whole, chip_ahead(by) * 2 + 1 - core, g.span),
                g.pair.at[by, :, pl.ds(*g.span)],
                g.sem.at[0, by],
                g.sem.at[1, by],
                sibling,
            )

    def grads_plane(g):
        for by in range(1, n.chips):
            theirs = g.pair.at[by, :, pl.ds(*g.span)]
            arrived(theirs, g.sem.at[1, by])
            piece = share_of(g.whole, chip_ahead(by) * 2 + core, g.span)
            piece[...] = (piece[...].astype(F32) + theirs[...].astype(F32)).astype(BF16)
            send(
                piece,
                g.plane.at[by - 1, :, pl.ds(*g.span)],
                g.sem.at[2, by],
                g.sem.at[3, by],
                chip_ahead(by) * 2 + core,
            )

    def grads_line(g):
        theirs = g.pair.at[0, :, pl.ds(*g.span)]
        arrived(theirs, g.sem.at[1, 0])
        acc = share_of(g.whole, f, g.span)[...].astype(F32) + theirs[...].astype(F32)
        for by in range(1, n.chips):
            theirs = g.plane.at[by - 1, :, pl.ds(*g.span)]
            arrived(theirs, g.sem.at[3, by])
            acc = acc + theirs[...].astype(F32)
        g.total[:, pl.ds(*g.span)] = acc.astype(BF16)
        for by in range(1, n.ctx):
            start = pl.multiple_of(ahead(by) * shard, shard)
            send(
                g.total.at[pl.ds(start, shard), pl.ds(*g.span)],
                g.land.at[c, :, pl.ds(*g.span)],
                g.line_sem.at[0, by],
                g.line_sem.at[1, by],
                None,
                ahead(by),
            )
        start = pl.multiple_of(c * shard, shard)
        g.land[c, :, pl.ds(*g.span)] = g.total[pl.ds(start, shard), pl.ds(*g.span)]

    def grads_wait(g):
        for by in range(1, n.ctx):
            arrived(g.land.at[behind(by), :, pl.ds(*g.span)], g.line_sem.at[1, by])

    def small_peers(way):
        if way == "line":
            return [(n.chips + by, f, ahead(by)) for by in range(1, n.ctx)]
        if way == "plane":
            return [(by, chip_ahead(by) * 2 + core, c) for by in range(1, n.chips)]
        return [(0, sibling, c)]

    def small_send(src, incoming, sem, way):
        for slot, to_f, to_c in small_peers(way):
            send(src, incoming.at[slot], sem.at[0, slot], sem.at[1, slot], to_f, to_c)

    def small_sum(own, incoming, sem, way):
        total = own[...]
        for slot, _, _ in small_peers(way):
            arrived(incoming.at[slot], sem.at[1, slot])
            total = total + incoming[slot]
        return total

    def save_lines(first, line):
        for j in range(n.lines):
            row = slice(first + j, first + j + 1)
            r.g1_acc[3, row, :] += line[:, j * HEAD_DIM : (j + 1) * HEAD_DIM]

    attn_shards, mlp_shards = (r.wq, r.wk, r.wv, r.wo), (r.wg, r.wu, r.wd)
    attn_cols, mlp_cols = n.cols[:4], n.cols[4:]
    q_cols, k_cols, _, o_cols = attn_cols
    ff = mlp_cols[0]
    group = n.heads // n.kv
    factor = 1.0 / math.sqrt(HEAD_DIM)

    o_at = q_cols + 2 * k_cols
    attn_bufs = dict(whole=r.ga, pair=r.ga_sib, plane=r.ga_in, total=r.ga_z, land=r.ga_land)
    mlp_bufs = dict(whole=r.gm, pair=r.gm_sib, plane=r.gm_in, total=r.gm_z, land=r.gm_land)
    plane_q = types.SimpleNamespace(buf=r.wa, span=(0, o_at), first=0, sem=r.sem_pq)
    plane_o = types.SimpleNamespace(buf=r.wa, span=(o_at, o_cols), first=3, sem=r.sem_po)
    plane_m = types.SimpleNamespace(buf=r.wm, span=(0, n.mlp_cols), first=0, sem=r.sem_pm)
    group_m = types.SimpleNamespace(
        **mlp_bufs, span=(0, n.mlp_cols), sem=r.sem_gm, line_sem=r.sem_zgm
    )
    group_o = types.SimpleNamespace(
        **attn_bufs, span=(o_at, o_cols), sem=r.sem_go, line_sem=r.sem_zgo
    )
    group_q = types.SimpleNamespace(**attn_bufs, span=(0, o_at), sem=r.sem_gq, line_sem=r.sem_zgq)

    sum_o, sum_y, sum_x2, sum_x1 = (
        types.SimpleNamespace(part=part, low=low, high=high, sem=sem)
        for part, low, high, sem in (
            (r.p_o, r.l_o, r.r_o, r.sem_o),
            (r.p_y, r.l_y, r.r_y, r.sem_y),
            (r.p_x2, r.l_x2, r.r_x2, r.sem_x2),
            (r.p_x1, r.l_x1, r.r_x1, r.sem_x1),
        )
    )
    r.g1_acc[3] = jnp.zeros_like(r.g1_acc[3])

    me = f * n.ctx + c
    lane = lax.broadcasted_iota(jnp.int32, (1, HEAD_DIM), 1)

    def place(row, at, size, first):
        moved = pltpu.roll(r.gains[...], lax.rem(at + HEAD_DIM - first, HEAD_DIM), 1)
        r.gp[pl.ds(row, 1), :] = jnp.where((lane >= at) & (lane < at + size), moved, 0.0)

    r.gp[...] = jnp.zeros_like(r.gp)
    row, at = me * n.each // HEAD_DIM, lax.rem(me * n.each, HEAD_DIM)
    place(row, at, n.each, 0)
    place(n.lines + row, at, n.each, n.each)
    place(2 * n.lines, me * n.few, n.few, 2 * n.each)
    place(2 * n.lines + 1, me * n.few, n.few, 2 * n.each + n.few)
    small_send(r.gp, r.g0_in, r.sem_g0, "line")
    weights_send(attn_shards, attn_cols, r.wa, r.sem_wa)
    for k in range(PARTS):
        gather_start(r.hidden, r.xb, r.sem_xb, k)
    own_x = pltpu.make_async_copy(r.hidden, r.xb.at[c], r.local_sem.at[7])
    own_x.start()
    own_g = pltpu.make_async_copy(r.cot, r.gb.at[c], r.local_sem.at[8])
    own_g.start()
    own_attn = weights_own(attn_shards, attn_cols, r.wa, 0)
    own_mlp = weights_own(mlp_shards, mlp_cols, r.wm, 4)
    r.g0_acc[0] = small_sum(r.gp, r.g0_in, r.sem_g0, "line")
    small_send(r.g0_acc.at[0], r.g0_in, r.sem_g0, "pair")
    slots = r.order.shape[1]
    slot_len = n.tokens // slots
    exponent = (lane % (HEAD_DIM // 2)).astype(F32) * (2.0 / HEAD_DIM)
    inverse = jnp.exp(-exponent * math.log(1000000.0))
    sign = jnp.where(lane < HEAD_DIM // 2, -1.0, 1.0)
    for j in range(slots):
        first = r.order[0, j] * slot_len
        span = slice(j * slot_len, (j + 1) * slot_len)
        position = first + lax.broadcasted_iota(jnp.int32, (slot_len, HEAD_DIM), 0)
        r.posq[span, :] = position
        angle = position.astype(F32) * inverse
        r.cos[span, :] = jnp.cos(angle)
        r.sin[span, :] = jnp.sin(angle) * sign
    token = lax.broadcasted_iota(jnp.int32, (1, n.tokens), 1)
    posk = token % slot_len
    for j in range(slots):
        posk = posk + jnp.where(token // slot_len == j, r.order[0, j] * slot_len, 0)
    r.posk[...] = posk
    r.g0_acc[1] = small_sum(r.g0_acc.at[0], r.g0_in, r.sem_g0, "pair")
    small_send(r.g0_acc.at[1], r.g0_in, r.sem_g0, "plane")
    weights_spread(own_attn[:3], attn_cols[:3], r.sem_wa, plane_q)
    weights_spread(own_attn[3:], attn_cols[3:], r.sem_wa, plane_o)
    r.g0_acc[2] = small_sum(r.g0_acc.at[1], r.g0_in, r.sem_g0, "plane")
    for j in range(n.lines):
        r.gv[0, :, j * HEAD_DIM : (j + 1) * HEAD_DIM] = r.g0_acc[2, j : j + 1, :]
        r.gv[1, :, j * HEAD_DIM : (j + 1) * HEAD_DIM] = r.g0_acc[
            2, n.lines + j : n.lines + j + 1, :
        ]
    qgain = r.g0_acc[2, 2 * n.lines : 2 * n.lines + 1, :]
    kgain = r.g0_acc[2, 2 * n.lines + 1 : 2 * n.lines + 2, :]
    attn_gain, mlp_gain = r.gv[0], r.gv[1]
    for by in range(1, n.ctx):
        if by == n.ctx - 1:
            weights_send(mlp_shards, mlp_cols, r.wm, r.sem_wm, "between")
            for k in range(PARTS):
                gather_start(r.cot, r.gb, r.sem_gb, k, "between")
        for k in range(PARTS):
            gather_relay(r.xb, r.sem_xb, by, k)
    own_x.wait()
    own_g.wait()

    def norm_rows(j, carry):
        x = r.xb[j].astype(F32)
        start = pl.multiple_of(j * rows, rows)
        r.xn[pl.ds(start, rows), :] = (x * rms(x) * attn_gain).astype(BF16)
        return carry

    lax.fori_loop(0, n.ctx, norm_rows, 0)
    weights_forward(plane_q)
    weights_wait(plane_q)
    weights_send(mlp_shards, mlp_cols, r.wm, r.sem_wm, "ends")
    for k in range(PARTS):
        gather_start(r.cot, r.gb, r.sem_gb, k, "ends")

    cosine, sine = r.cos, r.sin
    tile = 2 * HEAD_DIM if n.kv % 2 == 0 else HEAD_DIM
    for at in range(0, q_cols + 2 * k_cols, tile):
        product = mm(r.xn[...], r.wa[:, at : at + tile])
        for part in range(tile // HEAD_DIM):
            head = at // HEAD_DIM + part
            u = product[:, part * HEAD_DIM : (part + 1) * HEAD_DIM]
            if head < n.heads:
                r.qp[head] = u
                r.qr[head] = rope_fwd(u * rms(u) * qgain, cosine[...], sine[...]).astype(BF16)
            elif head < n.heads + n.kv:
                r.kp[head - n.heads] = u
                r.kr[head - n.heads] = rope_fwd(u * rms(u) * kgain, cosine[...], sine[...]).astype(
                    BF16
                )
            else:
                r.vv[head - n.heads - n.kv] = u.astype(BF16)
    half = n.tokens // 2

    def head_forward(h, carry):
        kv = h // group
        for q0 in (0, half):
            s = mm(r.qr[h, q0 : q0 + half, :], r.kr[kv], LAST_AXIS)
            allowed = r.posk[...] <= r.posq[q0 : q0 + half, 0:1]
            e = jnp.where(allowed, jnp.exp(s * factor), 0.0)
            r.es[h, q0 : q0 + half, :] = e
            total = jnp.sum(e, axis=-1, keepdims=True)
            a = mm(e.astype(BF16), r.vv[kv]) / total
            r.af[h, q0 : q0 + half, :] = a
            lane = pl.multiple_of(h * HEAD_DIM, HEAD_DIM)
            r.at[q0 : q0 + half, pl.ds(lane, HEAD_DIM)] = a.astype(BF16)
        return carry

    lax.fori_loop(0, n.heads, head_forward, 0)
    weights_forward(plane_o)
    weights_wait(plane_o)

    def by_rows(left, right, out):
        step = 2 * HEAD_DIM
        for at in range(0, d, step):
            product = mm(left[...], right(slice(at, at + step)), LAST_AXIS)
            out[:, :, at : at + step] = product.astype(BF16).reshape(n.ctx, rows, step)

    by_rows(r.at, lambda span: r.wa[span, o_at:], r.p_o)
    steps = range(n.ctx - 1)
    for k in range(PARTS):
        scatter_start(sum_o, k)
    weights_spread(own_mlp, mlp_cols, r.sem_wm, plane_m)

    def residual(k):
        span = rows_of(k)
        r.ho[span, :] = r.xb[c, span, :].astype(F32)
        scatter_total(sum_o, r.ho, k)
        own = r.ho[span, :]
        r.mb[c, span, :] = (own * rms(own) * mlp_gain).astype(BF16)
        gather_start(r.mb.at[c], r.mb, r.sem_mb, k)

    for by in range(1, n.ctx - 1):
        for k in range(PARTS):
            gather_relay(r.gb, r.sem_gb, by, k)
    for step in steps:
        scatter_relay(sum_o, step, 0)
    residual(0)
    for k in range(1, PARTS):
        for step in steps:
            scatter_relay(sum_o, step, k)
        gather_relay(r.mb, r.sem_mb, 1, k - 1)
        residual(k)
    weights_forward(plane_m)
    for by in range(2, n.ctx):
        gather_relay(r.mb, r.sem_mb, by, 0)
    for k in range(PARTS):
        gather_relay(r.gb, r.sem_gb, n.ctx - 1, k)
    weights_wait(plane_m)

    tile = 2 * HEAD_DIM if ff % (2 * HEAD_DIM) == 0 else HEAD_DIM
    span_rows = n.ctx * part_rows

    def mlp_part(k):
        span = rows_of(k)
        mixed = r.mb[:, span, :].reshape(span_rows, d)
        upstream = r.gb[:, span, :].reshape(span_rows, d)
        for at in range(0, ff, tile):
            gate = mm(mixed, r.wm[:, at : at + tile])
            up = mm(mixed, r.wm[:, ff + at : ff + at + tile])
            back = mm(upstream, r.wm[:, 2 * ff + at : 2 * ff + at + tile])
            sig = jax.nn.sigmoid(gate)
            swish = gate * sig
            shape = (n.ctx, part_rows, tile)
            r.hid[:, span, at : at + tile] = (swish * up).astype(BF16).reshape(shape)
            r.dgu[:, span, at : at + tile] = (
                (back * up * sig * (1.0 + gate * (1.0 - sig))).astype(BF16).reshape(shape)
            )
            r.dgu[:, span, ff + at : ff + at + tile] = (
                (back * swish).astype(BF16).reshape(shape)
            )
        both = r.dgu[:, span, :].reshape(span_rows, 2 * ff)
        for at in range(0, d, 2 * HEAD_DIM):
            product = mm(both, r.wm[at : at + 2 * HEAD_DIM, : 2 * ff], LAST_AXIS).astype(BF16)
            r.p_x2[:, span, at : at + 2 * HEAD_DIM] = product.reshape(
                n.ctx, part_rows, 2 * HEAD_DIM
            )
        scatter_start(sum_x2, k)

    def residual_back(k):
        span = rows_of(k)
        r.dh[span, :] = jnp.zeros((part_rows, d), F32)
        scatter_total(sum_x2, r.dh, k)
        own = r.ho[span, :]
        from_norm, term = norm_back(own, rms(own), mlp_gain, r.dh[span, :])
        save_lines(n.lines, jnp.sum(term, axis=0, keepdims=True))
        r.dh[span, :] = r.gb[c, span, :].astype(F32) + from_norm
        r.rb[c, span, :] = r.dh[span, :].astype(BF16)
        gather_start(r.rb.at[c], r.rb, r.sem_rb, k)

    mlp_part(0)
    for k in range(1, PARTS):
        for step in steps:
            gather_relay(r.mb, r.sem_mb, step + 1, k)
            scatter_relay(sum_x2, step, k - 1)
        mlp_part(k)
        residual_back(k - 1)
    hidden = r.hid[...].reshape(n.tokens, ff)
    by_rows(hidden, lambda span: r.wm[span, 2 * ff :], r.p_y)
    scatter_start(sum_y, 0)
    mixed = r.mb[...].reshape(n.tokens, d)
    upstream = r.gb[...].reshape(n.tokens, d)
    for at in range(0, 2 * ff, tile):
        part = r.dgu[:, :, at : at + tile].reshape(n.tokens, tile)
        r.gm[:, at : at + tile] = mm(mixed, part, FIRST_AXIS).astype(BF16)
    for at in range(0, ff, tile):
        part = r.hid[:, :, at : at + tile].reshape(n.tokens, tile)
        r.gm[:, 2 * ff + at : 2 * ff + at + tile] = mm(upstream, part, FIRST_AXIS).astype(BF16)
    grads_pair(group_m)
    for step in steps:
        scatter_relay(sum_x2, step, PARTS - 1)
        if step == 0:
            grads_plane(group_m)
    for k in range(PARTS - 1):
        gather_relay(r.rb, r.sem_rb, 1, k)
    residual_back(PARTS - 1)
    for k in range(1, PARTS):
        scatter_start(sum_y, k)
    for k in range(PARTS - 1):
        gather_relay(r.rb, r.sem_rb, 2, k)
    gather_relay(r.rb, r.sem_rb, 1, PARTS - 1)
    gather_relay(r.rb, r.sem_rb, 2, PARTS - 1)
    for step in steps:
        scatter_relay(sum_y, step, 0)
    for by in range(3, n.ctx):
        for k in range(PARTS):
            gather_relay(r.rb, r.sem_rb, by, k)

    upstream = r.rb[...].reshape(n.tokens, d)
    for at in range(0, o_cols, HEAD_DIM):
        r.da[at // HEAD_DIM] = mm(upstream, r.wa[:, o_at + at : o_at + at + HEAD_DIM])
    r.ga[:, o_at:] = mm(upstream, r.at[...], FIRST_AXIS).astype(BF16)
    grads_pair(group_o)
    grads_line(group_m)
    r.dk[...] = jnp.zeros_like(r.dk)
    r.dv[...] = jnp.zeros_like(r.dv)

    def head_backward(h, carry):
        kv = h // group
        for q0 in (0, half):
            span = slice(q0, q0 + half)
            e = r.es[h, span, :]
            total = jnp.sum(e, axis=-1, keepdims=True)
            da = r.da[h, span, :]
            w = (da / total).astype(BF16)
            dl = jnp.sum(da * r.af[h, span, :], axis=-1, keepdims=True) / total
            ds = (e * (mm(w, r.vv[kv], LAST_AXIS) - dl)).astype(BF16)
            r.ds[span, :] = ds
            r.eb[span, :] = e.astype(BF16)
            r.wb[span, :] = w
            r.da[h, span, :] = mm(ds, r.kr[kv])
        r.dk[kv] = r.dk[kv] + mm(r.ds[...], r.qr[h], FIRST_AXIS)
        r.dv[kv] = r.dv[kv] + mm(r.eb[...], r.wb[...], FIRST_AXIS)
        return carry

    lax.fori_loop(0, n.heads, head_backward, 0)

    def query_backward(h, term):
        u = r.qp[h]
        du, gain_term = norm_back(
            u, rms(u), qgain, rope_bwd(r.da[h] * factor, cosine[...], sine[...])
        )
        lane = pl.multiple_of(h * HEAD_DIM, HEAD_DIM)
        r.dqkv[:, pl.ds(lane, HEAD_DIM)] = du.astype(BF16)
        return term + jnp.sum(gain_term, axis=0, keepdims=True)

    q_term = lax.fori_loop(0, n.heads, query_backward, jnp.zeros((1, HEAD_DIM), F32))
    for k in range(1, PARTS):
        for step in steps:
            scatter_relay(sum_y, step, k)
    grads_plane(group_o)
    k_term = jnp.zeros((1, HEAD_DIM), F32)
    for kv in range(n.kv):
        u = r.kp[kv]
        du, gain_term = norm_back(
            u, rms(u), kgain, rope_bwd(r.dk[kv] * factor, cosine[...], sine[...])
        )
        at = q_cols + kv * HEAD_DIM
        r.dqkv[:, at : at + HEAD_DIM] = du.astype(BF16)
        at += k_cols
        r.dqkv[:, at : at + HEAD_DIM] = r.dv[kv].astype(BF16)
        k_term = k_term + jnp.sum(gain_term, axis=0, keepdims=True)
    for at in range(0, o_at, 2 * HEAD_DIM):
        r.ga[:, at : at + 2 * HEAD_DIM] = mm(
            r.xn[...], r.dqkv[:, at : at + 2 * HEAD_DIM], FIRST_AXIS
        ).astype(BF16)
    grads_pair(group_q)
    by_rows(r.dqkv, lambda span: r.wa[span, :o_at], r.p_x1)
    for k in range(PARTS):
        scatter_start(sum_x1, k)
    grads_plane(group_q)
    grads_line(group_o)
    for k in range(PARTS):
        for step in steps:
            scatter_relay(sum_x1, step, k)
        if k == 0:
            grads_line(group_q)
    for k in range(PARTS):
        scatter_total(sum_y, r.ho, k)
    r.out_hidden[...] = r.ho[...].astype(BF16)
    r.out_input[...] = jnp.zeros_like(r.out_input)
    for k in range(PARTS):
        scatter_total(sum_x1, r.out_input, k)
    x = r.xb[c].astype(F32)
    from_norm, term = norm_back(x, rms(x), attn_gain, r.out_input[...])
    save_lines(0, jnp.sum(term, axis=0, keepdims=True))
    r.out_input[...] = r.dh[...] + from_norm
    r.g1_acc[3, 2 * n.lines : 2 * n.lines + 1, :] = q_term
    r.g1_acc[3, 2 * n.lines + 1 : 2 * n.lines + 2, :] = k_term
    small_send(r.g1_acc.at[3], r.g1_in, r.sem_g1, "pair")
    r.g1_acc[0] = small_sum(r.g1_acc.at[3], r.g1_in, r.sem_g1, "pair")
    small_send(r.g1_acc.at[0], r.g1_in, r.sem_g1, "plane")
    r.g1_acc[1] = small_sum(r.g1_acc.at[0], r.g1_in, r.sem_g1, "plane")
    small_send(r.g1_acc.at[1], r.g1_in, r.sem_g1, "line")
    grads_wait(group_m)
    grads_wait(group_o)
    grads_wait(group_q)
    r.out_gains[...] = small_sum(r.g1_acc.at[1], r.g1_in, r.sem_g1, "line")
    for wait in sends:
        wait()


def fused(
    ctx,
    fsdp,
    hidden_in,
    block_order,
    cotangent,
    q_weight,
    k_weight,
    v_weight,
    o_weight,
    attn_gain,
    query_gain,
    key_gain,
    mlp_gain,
    gate_weight,
    up_weight,
    down_weight,
):
    shards = (q_weight, k_weight, v_weight, o_weight, gate_weight, up_weight, down_weight)
    n = Sizes(ctx, fsdp, hidden_in.shape[1], shards)
    gains = jnp.concatenate([attn_gain, mlp_gain, query_gain, key_gain]).astype(F32)
    gains = jnp.pad(gains, (0, HEAD_DIM - gains.shape[0])).reshape(1, HEAD_DIM)
    hbm, vmem = pl.BlockSpec(memory_space=pl.ANY), pl.BlockSpec(memory_space=pltpu.VMEM)
    inputs = dict(
        hidden=(hidden_in[0], hbm),
        cot=(cotangent[0], hbm),
        wq=(q_weight, hbm),
        wk=(k_weight, hbm),
        wv=(v_weight, hbm),
        wo=(o_weight, hbm),
        wg=(gate_weight, hbm),
        wu=(up_weight, hbm),
        wd=(down_weight, hbm),
        gains=(gains, vmem),
        order=(block_order, pl.BlockSpec(memory_space=pltpu.SMEM)),
    )
    outputs = dict(
        out_hidden=jax.ShapeDtypeStruct((n.rows, n.width), BF16),
        out_input=jax.ShapeDtypeStruct((n.rows, n.width), F32),
        ga_land=jax.ShapeDtypeStruct((ctx, n.shard, n.attn_cols), BF16),
        gm_land=jax.ShapeDtypeStruct((ctx, n.shard, n.mlp_cols), BF16),
        out_gains=jax.ShapeDtypeStruct((n.gain_rows, HEAD_DIM), F32),
    )
    scratch = scratch_of(n)
    landed = pl.pallas_call(
        functools.partial(layer_kernel, n, [*inputs, *outputs, *scratch]),
        out_shape=tuple(outputs.values()),
        in_specs=[spec for _, spec in inputs.values()],
        out_specs=tuple(vmem for _ in outputs),
        scratch_shapes=list(scratch.values()),
        compiler_params=pltpu.CompilerParams(
            collective_id=0, has_side_effects=True, vmem_limit_bytes=VMEM_LIMIT
        ),
        name="layer",
    )(*[value for value, _ in inputs.values()])

    finals = [(n.rows, n.width, BF16), (n.rows, n.width, F32)]
    finals += [(s.shape[0], s.shape[1], F32) for s in shards] + [(8, HEAD_DIM, F32)]
    result, input_grad, oq, ok, ov, oo, og, ou, od, sums = pl.pallas_call(
        functools.partial(emit_kernel, n),
        out_shape=tuple(jax.ShapeDtypeStruct(f[:2], f[2]) for f in finals),
        in_specs=[vmem] * len(outputs),
        out_specs=tuple(vmem for _ in finals),
        name="emit",
    )(*landed)
    return (
        result[None],
        input_grad[None],
        oq,
        ok,
        ov,
        oo,
        sums[0, : n.each],
        sums[2, : n.few],
        sums[3, : n.few],
        sums[1, : n.each],
        og,
        ou,
        od,
    )


def emit_kernel(n, result, input_grad, attn_land, mlp_land, sums, *outs):
    outs[0][...] = result[...]
    outs[1][...] = input_grad[...]
    which = 2
    for land, widths in ((attn_land, n.cols[:4]), (mlp_land, n.cols[4:])):
        at = 0
        for width in widths:
            for j in range(n.ctx):
                outs[which][:, j * width : (j + 1) * width] = land[j, :, at : at + width].astype(
                    F32
                )
            at += width
            which += 1
    me = lax.axis_index("fsdp") * n.ctx + lax.axis_index("ctx")
    row, at = me * n.each // HEAD_DIM, lax.rem(me * n.each, HEAD_DIM)
    sums_out = outs[which]
    sums_out[...] = jnp.zeros_like(sums_out)
    for i, (line, lane) in enumerate(
        (
            (row, at),
            (n.lines + row, at),
            (2 * n.lines, me * n.few),
            (2 * n.lines + 1, me * n.few),
        )
    ):
        back = lax.rem(HEAD_DIM - lane, HEAD_DIM)
        sums_out[i : i + 1, :] = pltpu.roll(sums[pl.ds(line, 1), :], back, 1)


def fits(ctx, fsdp, shard_rows):
    per_tile = HEAD_DIM % (2 * shard_rows) == 0 and HEAD_DIM % (ctx * fsdp) == 0
    return per_tile and shard_rows % 16 == 0 and fsdp % 2 == 0 and KV_HEADS % ctx == 0


def solution(mesh):
    ctx, fsdp = mesh.shape["ctx"], mesh.shape["fsdp"]
    tokens = P("fsdp", "ctx", None)
    matrix = P(("fsdp", "ctx"), None)
    vector = P(("fsdp", "ctx"))
    def step(hidden_in, block_order, cotangent, q_weight, *rest):
        whole = fused if fits(ctx, fsdp, q_weight.shape[0]) else local
        return whole(ctx, fsdp, hidden_in, block_order, cotangent, q_weight, *rest)

    return jax.shard_map(
        step,
        mesh=mesh,
        in_specs=(tokens, P("fsdp", None), tokens)
        + (matrix,) * 4
        + (vector,) * 4
        + (matrix,) * 3,
        out_specs=(tokens,) * 2 + (matrix,) * 4 + (vector,) * 4 + (matrix,) * 3,
        check_vma=False,
    )
```

```python
import functools
import math
import types

import jax
import jax.numpy as jnp
from jax import lax
from jax.experimental import pallas as pl
from jax.experimental.pallas import tpu as pltpu
from jax.sharding import PartitionSpec as P

HEADS = 16
KV_HEADS = 8
HEAD_DIM = 128
EPSILON = 1e-06
FIRST_AXIS = (((0,), (0,)), ((), ()))
LAST_AXIS = (((1,), (1,)), ((), ()))
BF16 = jnp.bfloat16
F32 = jnp.float32
VMEM_LIMIT = 67043328
PARTS = 2


def mm(left, right, dims=(((1,), (0,)), ((), ()))):
    return lax.dot_general(left, right, dims, preferred_element_type=F32)


def rms(signal):
    return lax.rsqrt(jnp.mean(signal * signal, axis=-1, keepdims=True) + EPSILON)


def norm_back(signal, inverse_rms, gain_vec, upstream):
    unit_values = signal * inverse_rms
    scaled_up = upstream * gain_vec
    inner = scaled_up - unit_values * jnp.mean(scaled_up * unit_values, axis=-1, keepdims=True)
    return (inverse_rms * inner, upstream * unit_values)


def rope_tables(positions, head_width):
    exponent = jnp.arange(head_width // 2, dtype=F32) * (2.0 / head_width)
    inverse = jnp.exp(-exponent * math.log(1000000.0))
    angles = positions.astype(F32)[:, None] * inverse[None, :]
    angles = jnp.concatenate([angles, angles], axis=-1)
    return (jnp.cos(angles), jnp.sin(angles))


def rotate(signal, cosine, sine):
    half = signal.shape[-1] // 2
    turned = jnp.concatenate([-signal[..., half:], signal[..., :half]], axis=-1)
    return signal * cosine + turned * sine


def rotate_back(upstream, cosine, sine):
    half = upstream.shape[-1] // 2
    scaled_up = upstream * sine
    return upstream * cosine + jnp.concatenate(
        [scaled_up[..., half:], -scaled_up[..., :half]], axis=-1
    )


def gather_columns(ctx, shards):
    rows = shards[0].shape[0]
    cut = [s.reshape(rows, ctx, s.shape[1] // ctx).transpose(1, 0, 2) for s in shards]
    widths = [c.shape[2] for c in cut]
    both = jnp.concatenate(cut, axis=2)
    both = lax.all_to_all(both, "ctx", 0, 0, tiled=True)
    both = both.reshape(ctx * rows, -1)
    whole = lax.all_gather(both, "fsdp", axis=0, tiled=True)
    out, at = [], 0
    for width in widths:
        out.append(whole[:, at : at + width])
        at += width
    return out


def scatter_grads(ctx, fsdp, grads):
    rows = grads[0].shape[0] // (ctx * fsdp)
    widths = [g.shape[1] for g in grads]
    both = jnp.concatenate([g.astype(BF16) for g in grads], axis=1)
    both = lax.psum_scatter(both, "fsdp", scatter_dimension=0, tiled=True)
    both = lax.all_to_all(both.reshape(ctx, rows, -1), "ctx", 0, 0, tiled=True)
    out, at = [], 0
    for width in widths:
        piece = both[:, :, at : at + width]
        out.append(piece.transpose(1, 0, 2).reshape(rows, ctx * width).astype(F32))
        at += width
    return out


def ctx_gather(rows):
    return lax.all_gather(rows, "ctx", axis=0, tiled=True)


def ctx_scatter(partial):
    return lax.psum_scatter(partial.astype(BF16), "ctx", scatter_dimension=0, tiled=True).astype(
        F32
    )


def local(
    ctx,
    fsdp,
    hidden_in,
    block_order,
    cotangent,
    q_weight,
    k_weight,
    v_weight,
    o_weight,
    attn_gain,
    query_gain,
    key_gain,
    mlp_gain,
    gate_weight,
    up_weight,
    down_weight,
):
    inputs = hidden_in[0].astype(F32)
    row_count = inputs.shape[0]
    tokens = row_count * ctx
    slots = block_order.shape[1]
    block_len = tokens // slots
    heads, kv_heads = HEADS // ctx, KV_HEADS // ctx
    group = heads // kv_heads
    factor = 1.0 / math.sqrt(HEAD_DIM)
    positions = (
        block_order[0][:, None] * block_len + jnp.arange(block_len, dtype=jnp.int32)[None, :]
    ).reshape(-1)
    cosine, sine = rope_tables(positions, HEAD_DIM)
    cosine, sine = cosine[:, None, :], sine[:, None, :]

    both = ("fsdp", "ctx")
    norm_gain, qgain, kgain, mlp_norm_gain = (
        lax.all_gather(g, both, axis=0, tiled=True).astype(F32)
        for g in (attn_gain, query_gain, key_gain, mlp_gain)
    )
    norm_scale = rms(inputs)
    normed = ctx_gather((inputs * norm_scale * norm_gain).astype(BF16))
    upstream = ctx_gather(cotangent[0])
    q_full, k_full, v_full, o_full = gather_columns(ctx, (q_weight, k_weight, v_weight, o_weight))
    gate_full, up_full, down_full = gather_columns(ctx, (gate_weight, up_weight, down_weight))

    query_proj = mm(normed, q_full).reshape(tokens, heads, HEAD_DIM)
    key_proj = mm(normed, k_full).reshape(tokens, kv_heads, HEAD_DIM)
    value_low = mm(normed, v_full).astype(BF16).reshape(tokens, kv_heads, HEAD_DIM)
    query_scale, key_scale = rms(query_proj), rms(key_proj)
    query_low = (
        rotate(query_proj * query_scale * qgain, cosine, sine)
        .astype(BF16)
        .reshape(tokens, kv_heads, group, HEAD_DIM)
    )
    key_low = rotate(key_proj * key_scale * kgain, cosine, sine).astype(BF16)
    scores = jnp.einsum("rkgd,nkd->kgrn", query_low, key_low, preferred_element_type=F32) * factor
    allowed = positions[None, :] <= positions[:, None]
    weights_exp = jnp.where(allowed, jnp.exp(scores), 0.0)
    denominator = jnp.sum(weights_exp, axis=-1)
    weights_low = weights_exp.astype(BF16)
    numerator = jnp.einsum("kgrn,nkd->rkgd", weights_low, value_low, preferred_element_type=F32)
    denom_rows = jnp.transpose(denominator, (2, 0, 1))[..., None]
    attn_full = numerator / denom_rows
    attn_low = attn_full.astype(BF16).reshape(tokens, heads * HEAD_DIM)
    residual = inputs + ctx_scatter(mm(attn_low, o_full, LAST_AXIS))

    mix_scale = rms(residual)
    mixed = ctx_gather((residual * mix_scale * mlp_norm_gain).astype(BF16))
    gate_val = mm(mixed, gate_full)
    up_val = mm(mixed, up_full)
    sigmoid_gate = jax.nn.sigmoid(gate_val)
    swish_gate = gate_val * sigmoid_gate
    hidden_low = (swish_gate * up_val).astype(BF16)
    result = residual + ctx_scatter(mm(hidden_low, down_full, LAST_AXIS))
    hidden_grad = mm(upstream, down_full)
    gate_back = (
        hidden_grad * up_val * sigmoid_gate * (1.0 + gate_val * (1.0 - sigmoid_gate))
    ).astype(BF16)
    up_back = (hidden_grad * swish_gate).astype(BF16)
    mixed_grad = ctx_scatter(mm(gate_back, gate_full, LAST_AXIS) + mm(up_back, up_full, LAST_AXIS))
    resid_from_norm, mlp_gain_term = norm_back(residual, mix_scale, mlp_norm_gain, mixed_grad)
    residual_grad = cotangent[0].astype(F32) + resid_from_norm
    mlp_grads = scatter_grads(
        ctx,
        fsdp,
        (
            mm(mixed, gate_back, FIRST_AXIS),
            mm(mixed, up_back, FIRST_AXIS),
            mm(upstream, hidden_low, FIRST_AXIS),
        ),
    )
    resid_low = ctx_gather(residual_grad.astype(BF16))

    attn_grad = mm(resid_low, o_full).reshape(tokens, kv_heads, group, HEAD_DIM)
    share_low = (attn_grad / denom_rows).astype(BF16)
    denom_grad = jnp.transpose(jnp.sum(attn_grad * attn_full, axis=-1), (1, 2, 0)) / denominator
    weight_grad = jnp.einsum("rkgd,nkd->kgrn", share_low, value_low, preferred_element_type=F32)
    score_low = (weights_exp * (weight_grad - denom_grad[..., None])).astype(BF16)
    query_rot = (
        jnp.einsum("kgrn,nkd->rkgd", score_low, key_low, preferred_element_type=F32) * factor
    ).reshape(tokens, heads, HEAD_DIM)
    key_rot = (
        jnp.einsum("kgrn,rkgd->nkd", score_low, query_low, preferred_element_type=F32) * factor
    )
    value_back = (
        jnp.einsum("kgrn,rkgd->nkd", weights_low, share_low, preferred_element_type=F32)
        .reshape(tokens, kv_heads * HEAD_DIM)
        .astype(BF16)
    )
    query_grad, query_term = norm_back(
        query_proj, query_scale, qgain, rotate_back(query_rot, cosine, sine)
    )
    key_grad, key_term = norm_back(key_proj, key_scale, kgain, rotate_back(key_rot, cosine, sine))
    query_back = query_grad.reshape(tokens, heads * HEAD_DIM).astype(BF16)
    key_back = key_grad.reshape(tokens, kv_heads * HEAD_DIM).astype(BF16)
    normed_grad = ctx_scatter(
        mm(query_back, q_full, LAST_AXIS)
        + mm(key_back, k_full, LAST_AXIS)
        + mm(value_back, v_full, LAST_AXIS)
    )
    input_from_norm, attn_gain_term = norm_back(inputs, norm_scale, norm_gain, normed_grad)
    input_grad = residual_grad + input_from_norm
    attn_grads = scatter_grads(
        ctx,
        fsdp,
        (
            mm(normed, query_back, FIRST_AXIS),
            mm(normed, key_back, FIRST_AXIS),
            mm(normed, value_back, FIRST_AXIS),
            mm(resid_low, attn_low, FIRST_AXIS),
        ),
    )
    gains = (
        jnp.sum(attn_gain_term, axis=0),
        jnp.sum(query_term, axis=(0, 1)),
        jnp.sum(key_term, axis=(0, 1)),
        jnp.sum(mlp_gain_term, axis=0),
    )
    gains = [lax.psum_scatter(g, both, scatter_dimension=0, tiled=True) for g in gains]
    return (
        result.astype(BF16)[None],
        input_grad[None],
        *attn_grads,
        *gains,
        *mlp_grads,
    )


def rope_fwd(u, cosine, sine):
    return u * cosine + pltpu.roll(u, HEAD_DIM // 2, u.ndim - 1) * sine


def rope_bwd(du, cosine, sine):
    return du * cosine - pltpu.roll(du, HEAD_DIM // 2, du.ndim - 1) * sine


class Sizes:
    def __init__(self, ctx, fsdp, rows, shards):
        self.ctx, self.fsdp, self.rows = ctx, fsdp, rows
        self.chips = fsdp // 2
        self.shard = shards[0].shape[0]
        self.block = self.shard * ctx
        self.width = self.block * fsdp
        self.tokens = rows * ctx
        self.heads, self.kv = HEADS // ctx, KV_HEADS // ctx
        self.cols = [s.shape[1] // ctx for s in shards]
        self.attn_cols = sum(self.cols[:4])
        self.mlp_cols = sum(self.cols[4:])
        self.lines = self.width // HEAD_DIM
        self.gain_rows = 8 * ((2 * self.lines + 2 + 7) // 8)
        self.each, self.few = self.width // (ctx * fsdp), HEAD_DIM // (ctx * fsdp)


def scratch_of(n):
    bf, f32 = (lambda *s: pltpu.VMEM(s, BF16)), (lambda *s: pltpu.VMEM(s, F32))
    sem = lambda *s: pltpu.SemaphoreType.DMA(s)
    c, d, s, h, kv = n.ctx, n.width, n.tokens, n.heads, n.kv
    ff = n.cols[4]
    out = dict(
        wa=bf(d, n.attn_cols),
        wm=bf(d, n.mlp_cols),
        xb=bf(c, n.rows, d),
        gb=bf(c, n.rows, d),
        mb=bf(c, n.rows, d),
        rb=bf(c, n.rows, d),
        xn=bf(s, d),
        qp=f32(h, s, HEAD_DIM),
        kp=f32(kv, s, HEAD_DIM),
        qr=bf(h, s, HEAD_DIM),
        kr=bf(kv, s, HEAD_DIM),
        vv=bf(kv, s, HEAD_DIM),
        es=f32(h, s, s),
        af=f32(h, s, HEAD_DIM),
        at=bf(s, h * HEAD_DIM),
        da=f32(h, s, HEAD_DIM),
        dk=f32(kv, s, HEAD_DIM),
        dv=f32(kv, s, HEAD_DIM),
        ds=bf(s, s),
        eb=bf(s, s),
        wb=bf(s, HEAD_DIM),
        dqkv=bf(s, (h + 2 * kv) * HEAD_DIM),
        hid=bf(c, n.rows, ff),
        dgu=bf(c, n.rows, 2 * ff),
        ho=f32(n.rows, d),
        dh=f32(n.rows, d),
        gv=f32(2, 1, d),
        gp=f32(n.gain_rows, HEAD_DIM),
        cos=f32(s, HEAD_DIM),
        sin=f32(s, HEAD_DIM),
        posq=pltpu.VMEM((s, HEAD_DIM), jnp.int32),
        posk=pltpu.VMEM((1, s), jnp.int32),
        ga=bf(d, n.attn_cols),
        gm=bf(d, n.mlp_cols),
        ga_sib=bf(n.chips, n.block, n.attn_cols),
        gm_sib=bf(n.chips, n.block, n.mlp_cols),
        ga_in=bf(n.chips - 1, n.block, n.attn_cols),
        gm_in=bf(n.chips - 1, n.block, n.mlp_cols),
        ga_z=bf(n.block, n.attn_cols),
        gm_z=bf(n.block, n.mlp_cols),
        local_sem=sem(9),
    )
    for name in ("o", "y", "x2", "x1"):
        out["p_" + name] = bf(c, n.rows, d)
        out["l_" + name] = bf(c, n.rows, d)
        out["r_" + name] = bf(c, n.rows, d)
        out["sem_" + name] = sem(4, c, PARTS)
    for name in ("xb", "gb", "mb", "rb"):
        out["sem_" + name] = sem(3, c, PARTS)
    out["sem_wa"] = sem(2, c - 1, 4)
    out["sem_wm"] = sem(2, c - 1, 3)
    for name in ("pq", "po", "pm"):
        out["sem_" + name] = sem(4, n.chips)
    for name in ("gm", "go", "gq"):
        out["sem_" + name] = sem(4, n.chips)
        out["sem_z" + name] = sem(2, c)
    for name in ("g0", "g1"):
        out[name + "_in"] = f32(n.chips + c, n.gain_rows, HEAD_DIM)
        out[name + "_acc"] = f32(4, n.gain_rows, HEAD_DIM)
        out["sem_" + name] = sem(2, n.chips + c)
    return out


def layer_kernel(n, names, *refs):
    r = types.SimpleNamespace(**dict(zip(names, refs)))
    c, f = lax.axis_index("ctx"), lax.axis_index("fsdp")
    chip, core = f // 2, f % 2
    sibling = chip * 2 + 1 - core
    rows, d, block, shard = n.rows, n.width, n.block, n.shard
    sends = []

    def ahead(by):
        return lax.rem(c + by, n.ctx)

    def behind(by):
        return lax.rem(c + n.ctx - by, n.ctx)

    def chip_ahead(by):
        return lax.rem(chip + by, n.chips)

    def chip_behind(by):
        return lax.rem(chip + n.chips - by, n.chips)

    def remote(src, dst, send_sem, recv_sem, to_f=None, to_c=None):
        return pltpu.make_async_remote_copy(
            src_ref=src,
            dst_ref=dst,
            send_sem=send_sem,
            recv_sem=recv_sem,
            device_id={"fsdp": f if to_f is None else to_f, "ctx": c if to_c is None else to_c},
            device_id_type=pl.DeviceIdType.MESH,
        )

    def send(src, dst, send_sem, recv_sem, to_f=None, to_c=None):
        copy = remote(src, dst, send_sem, recv_sem, to_f, to_c)
        copy.start()
        sends.append(copy.wait_send)

    def arrived(dst, recv_sem):
        remote(dst, dst, recv_sem, recv_sem).wait_recv()

    def send_if(cond, src, dst, send_sem, recv_sem, to_c):
        copy = remote(src, dst, send_sem, recv_sem, None, to_c)
        pl.when(cond)(copy.start)
        sends.append(lambda: pl.when(cond)(copy.wait_send))

    barrier = pltpu.get_barrier_semaphore()

    def greet(to_f, to_c):
        pl.semaphore_signal(
            barrier,
            inc=1,
            device_id={"fsdp": to_f, "ctx": to_c},
            device_id_type=pl.DeviceIdType.MESH,
        )

    for by in range(1, n.ctx):
        greet(f, ahead(by))
    for by in range(1, n.chips):
        greet(chip_ahead(by) * 2 + core, c)
    greet(sibling, c)
    pl.semaphore_wait(barrier, n.ctx - 1 + n.chips)

    right, left = jnp.minimum(c + 1, n.ctx - 1), jnp.maximum(c - 1, 0)
    part_rows = rows // PARTS

    def part_of(buf, j, k):
        return buf.at[j, pl.ds(k * part_rows, part_rows), :]

    def gather_start(src, buf, sem, k, to=None):
        piece = src.at[pl.ds(k * part_rows, part_rows), :]
        here = part_of(buf, c, k)
        up, down = c + 1 < n.ctx, c > 0
        if to == "between":
            up, down = c + 1 < n.ctx - 1, c > 1
        elif to == "ends":
            up, down = c + 1 == n.ctx - 1, c == 1
        send_if(up, piece, here, sem.at[0, 0, k], sem.at[2, c, k], right)
        send_if(down, piece, here, sem.at[1, 0, k], sem.at[2, c, k], left)

    def gather_relay(buf, sem, by, k, source=None):
        low, high = jnp.maximum(c - by, 0), jnp.minimum(c + by, n.ctx - 1)
        from_low, from_high = c - by >= 0, c + by < n.ctx
        if source == "end":
            from_low, from_high = c == by, c + by == n.ctx - 1
        elif source == "between":
            from_low, from_high = c > by, c + by < n.ctx - 1
        piece, here = part_of(buf, low, k), sem.at[2, low, k]
        pl.when(from_low)(functools.partial(arrived, piece, here))
        send_if(from_low & (c + 1 < n.ctx), piece, piece, sem.at[0, by, k], here, right)
        piece, here = part_of(buf, high, k), sem.at[2, high, k]
        pl.when(from_high)(functools.partial(arrived, piece, here))
        send_if(from_high & (c > 0), piece, piece, sem.at[1, by, k], here, left)

    def rows_of(k):
        return slice(k * part_rows, (k + 1) * part_rows)

    def scatter_send(cond, part, there, sem, target, k, way, to_c):
        send_if(
            cond,
            part_of(part, target, k),
            part_of(there, target, k),
            sem.at[way, target, k],
            sem.at[2 + way, target, k],
            to_c,
        )

    def scatter_add(part, there, sem, target, k, way):
        arrived(part_of(there, target, k), sem.at[2 + way, target, k])
        span = rows_of(k)
        part[target, span, :] = (
            part[target, span, :].astype(F32) + there[target, span, :].astype(F32)
        ).astype(BF16)

    def scatter_start(g, k):
        for step in range(n.ctx - 1):
            scatter_send(c == n.ctx - 1, g.part, g.high, g.sem, step, k, 1, left)
            scatter_send(c == 0, g.part, g.low, g.sem, n.ctx - 1 - step, k, 0, right)

    def scatter_relay(g, step, k):
        near = c < n.ctx // 2
        low, high = n.ctx - 1 - step, step
        up, down = (c < low) & (c > 0), (c > high) & (c + 1 < n.ctx)

        def go_up(cond):
            pl.when(cond)(functools.partial(scatter_add, g.part, g.low, g.sem, low, k, 0))
            scatter_send(cond, g.part, g.low, g.sem, low, k, 0, right)

        go_up(up & near)
        pl.when(down)(functools.partial(scatter_add, g.part, g.high, g.sem, high, k, 1))
        scatter_send(down, g.part, g.high, g.sem, high, k, 1, left)
        go_up(up & ~near)

    def scatter_total(g, out, k):
        span = rows_of(k)
        out[span, :] = out[span, :] + g.part[c, span, :].astype(F32)

        @pl.when(c > 0)
        def _():
            arrived(part_of(g.low, c, k), g.sem.at[2, c, k])
            out[span, :] = out[span, :] + g.low[c, span, :].astype(F32)

        @pl.when(c + 1 < n.ctx)
        def _():
            arrived(part_of(g.high, c, k), g.sem.at[3, c, k])
            out[span, :] = out[span, :] + g.high[c, span, :].astype(F32)

    def block_of(buf, index, span):
        return buf.at[pl.ds(pl.multiple_of(index * block, block), block), pl.ds(*span)]

    def piece_of(buf, line, at, width):
        start = pl.multiple_of(f * block + line * shard, shard)
        return buf.at[pl.ds(start, shard), pl.ds(at, width)]

    def weights_send(shards, cols, buf, sem, now=None):
        for by in range(1, n.ctx):
            at = 0
            for i, (src, width) in enumerate(zip(shards, cols)):
                column = pl.multiple_of(ahead(by) * width, HEAD_DIM)
                copy = remote(
                    src.at[:, pl.ds(column, width)],
                    piece_of(buf, c, at, width),
                    sem.at[0, by - 1, i],
                    sem.at[1, by - 1, i],
                    None,
                    ahead(by),
                )
                at_end = (ahead(by) == 0) | (ahead(by) == n.ctx - 1)
                if now is None:
                    copy.start()
                else:
                    pl.when(at_end if now == "ends" else ~at_end)(copy.start)
                if now != "ends":
                    sends.append(copy.wait_send)
                at += width

    def weights_own(shards, cols, buf, first):
        at, out = 0, []
        for i, (src, width) in enumerate(zip(shards, cols)):
            column = pl.multiple_of(c * width, HEAD_DIM)
            copy = pltpu.make_async_copy(
                src.at[:, pl.ds(column, width)],
                piece_of(buf, c, at, width),
                r.local_sem.at[first + i],
            )
            copy.start()
            out.append(copy)
            at += width
        return out

    def weights_spread(own, cols, sem, g):
        for copy in own:
            copy.wait()
        for by in range(1, n.ctx):
            at = g.span[0]
            for i, width in enumerate(cols):
                arrived(piece_of(g.buf, behind(by), at, width), sem.at[1, by - 1, g.first + i])
                at += width
        mine = block_of(g.buf, f, g.span)
        for by in range(1, n.chips):
            send(mine, mine, g.sem.at[0, by], g.sem.at[1, by], chip_ahead(by) * 2 + core)
        send(mine, mine, g.sem.at[2, 0], g.sem.at[3, 0], sibling)

    def weights_forward(g):
        for by in range(1, n.chips):
            piece = block_of(g.buf, chip_behind(by) * 2 + core, g.span)
            arrived(piece, g.sem.at[1, by])
            send(piece, piece, g.sem.at[2, by], g.sem.at[3, by], sibling)

    def weights_wait(g):
        for by in range(n.chips):
            arrived(block_of(g.buf, chip_behind(by) * 2 + 1 - core, g.span), g.sem.at[3, by])

    def share_of(buf, index, span):
        return buf.at[pl.ds(pl.multiple_of(index * block, block), block), pl.ds(*span)]

    def grads_pair(g):
        for by in (*range(1, n.chips), 0):
            send(
                share_of(g.whole, chip_ahead(by) * 2 + 1 - core, g.span),
                g.pair.at[by, :, pl.ds(*g.span)],
                g.sem.at[0, by],
                g.sem.at[1, by],
                sibling,
            )

    def grads_plane(g):
        for by in range(1, n.chips):
            theirs = g.pair.at[by, :, pl.ds(*g.span)]
            arrived(theirs, g.sem.at[1, by])
            piece = share_of(g.whole, chip_ahead(by) * 2 + core, g.span)
            piece[...] = (piece[...].astype(F32) + theirs[...].astype(F32)).astype(BF16)
            send(
                piece,
                g.plane.at[by - 1, :, pl.ds(*g.span)],
                g.sem.at[2, by],
                g.sem.at[3, by],
                chip_ahead(by) * 2 + core,
            )

    def grads_line(g):
        theirs = g.pair.at[0, :, pl.ds(*g.span)]
        arrived(theirs, g.sem.at[1, 0])
        acc = share_of(g.whole, f, g.span)[...].astype(F32) + theirs[...].astype(F32)
        for by in range(1, n.chips):
            theirs = g.plane.at[by - 1, :, pl.ds(*g.span)]
            arrived(theirs, g.sem.at[3, by])
            acc = acc + theirs[...].astype(F32)
        g.total[:, pl.ds(*g.span)] = acc.astype(BF16)
        for by in range(1, n.ctx):
            start = pl.multiple_of(ahead(by) * shard, shard)
            send(
                g.total.at[pl.ds(start, shard), pl.ds(*g.span)],
                g.land.at[c, :, pl.ds(*g.span)],
                g.line_sem.at[0, by],
                g.line_sem.at[1, by],
                None,
                ahead(by),
            )
        start = pl.multiple_of(c * shard, shard)
        g.land[c, :, pl.ds(*g.span)] = g.total[pl.ds(start, shard), pl.ds(*g.span)]

    def grads_wait(g):
        for by in range(1, n.ctx):
            arrived(g.land.at[behind(by), :, pl.ds(*g.span)], g.line_sem.at[1, by])

    def small_peers(way):
        if way == "line":
            return [(n.chips + by, f, ahead(by)) for by in range(1, n.ctx)]
        if way == "plane":
            return [(by, chip_ahead(by) * 2 + core, c) for by in range(1, n.chips)]
        return [(0, sibling, c)]

    def small_send(src, incoming, sem, way):
        for slot, to_f, to_c in small_peers(way):
            send(src, incoming.at[slot], sem.at[0, slot], sem.at[1, slot], to_f, to_c)

    def small_sum(own, incoming, sem, way):
        total = own[...]
        for slot, _, _ in small_peers(way):
            arrived(incoming.at[slot], sem.at[1, slot])
            total = total + incoming[slot]
        return total

    def save_lines(first, line):
        for j in range(n.lines):
            row = slice(first + j, first + j + 1)
            r.g1_acc[3, row, :] += line[:, j * HEAD_DIM : (j + 1) * HEAD_DIM]

    attn_shards, mlp_shards = (r.wq, r.wk, r.wv, r.wo), (r.wg, r.wu, r.wd)
    attn_cols, mlp_cols = n.cols[:4], n.cols[4:]
    q_cols, k_cols, _, o_cols = attn_cols
    ff = mlp_cols[0]
    group = n.heads // n.kv
    factor = 1.0 / math.sqrt(HEAD_DIM)

    o_at = q_cols + 2 * k_cols
    attn_bufs = dict(whole=r.ga, pair=r.ga_sib, plane=r.ga_in, total=r.ga_z, land=r.ga_land)
    mlp_bufs = dict(whole=r.gm, pair=r.gm_sib, plane=r.gm_in, total=r.gm_z, land=r.gm_land)
    plane_q = types.SimpleNamespace(buf=r.wa, span=(0, o_at), first=0, sem=r.sem_pq)
    plane_o = types.SimpleNamespace(buf=r.wa, span=(o_at, o_cols), first=3, sem=r.sem_po)
    plane_m = types.SimpleNamespace(buf=r.wm, span=(0, n.mlp_cols), first=0, sem=r.sem_pm)
    group_m = types.SimpleNamespace(
        **mlp_bufs, span=(0, n.mlp_cols), sem=r.sem_gm, line_sem=r.sem_zgm
    )
    group_o = types.SimpleNamespace(
        **attn_bufs, span=(o_at, o_cols), sem=r.sem_go, line_sem=r.sem_zgo
    )
    group_q = types.SimpleNamespace(**attn_bufs, span=(0, o_at), sem=r.sem_gq, line_sem=r.sem_zgq)

    sum_o, sum_y, sum_x2, sum_x1 = (
        types.SimpleNamespace(part=part, low=low, high=high, sem=sem)
        for part, low, high, sem in (
            (r.p_o, r.l_o, r.r_o, r.sem_o),
            (r.p_y, r.l_y, r.r_y, r.sem_y),
            (r.p_x2, r.l_x2, r.r_x2, r.sem_x2),
            (r.p_x1, r.l_x1, r.r_x1, r.sem_x1),
        )
    )
    r.g1_acc[3] = jnp.zeros_like(r.g1_acc[3])

    me = f * n.ctx + c
    lane = lax.broadcasted_iota(jnp.int32, (1, HEAD_DIM), 1)

    def place(row, at, size, first):
        moved = pltpu.roll(r.gains[...], lax.rem(at + HEAD_DIM - first, HEAD_DIM), 1)
        r.gp[pl.ds(row, 1), :] = jnp.where((lane >= at) & (lane < at + size), moved, 0.0)

    r.gp[...] = jnp.zeros_like(r.gp)
    row, at = me * n.each // HEAD_DIM, lax.rem(me * n.each, HEAD_DIM)
    place(row, at, n.each, 0)
    place(n.lines + row, at, n.each, n.each)
    place(2 * n.lines, me * n.few, n.few, 2 * n.each)
    place(2 * n.lines + 1, me * n.few, n.few, 2 * n.each + n.few)
    small_send(r.gp, r.g0_in, r.sem_g0, "line")
    weights_send(attn_shards, attn_cols, r.wa, r.sem_wa)
    for k in range(PARTS):
        gather_start(r.hidden, r.xb, r.sem_xb, k)
    own_x = pltpu.make_async_copy(r.hidden, r.xb.at[c], r.local_sem.at[7])
    own_x.start()
    own_g = pltpu.make_async_copy(r.cot, r.gb.at[c], r.local_sem.at[8])
    own_g.start()
    own_attn = weights_own(attn_shards, attn_cols, r.wa, 0)
    own_mlp = weights_own(mlp_shards, mlp_cols, r.wm, 4)
    r.g0_acc[0] = small_sum(r.gp, r.g0_in, r.sem_g0, "line")
    small_send(r.g0_acc.at[0], r.g0_in, r.sem_g0, "pair")
    slots = r.order.shape[1]
    slot_len = n.tokens // slots
    exponent = (lane % (HEAD_DIM // 2)).astype(F32) * (2.0 / HEAD_DIM)
    inverse = jnp.exp(-exponent * math.log(1000000.0))
    sign = jnp.where(lane < HEAD_DIM // 2, -1.0, 1.0)
    for j in range(slots):
        first = r.order[0, j] * slot_len
        span = slice(j * slot_len, (j + 1) * slot_len)
        position = first + lax.broadcasted_iota(jnp.int32, (slot_len, HEAD_DIM), 0)
        r.posq[span, :] = position
        angle = position.astype(F32) * inverse
        r.cos[span, :] = jnp.cos(angle)
        r.sin[span, :] = jnp.sin(angle) * sign
    token = lax.broadcasted_iota(jnp.int32, (1, n.tokens), 1)
    posk = token % slot_len
    for j in range(slots):
        posk = posk + jnp.where(token // slot_len == j, r.order[0, j] * slot_len, 0)
    r.posk[...] = posk
    r.g0_acc[1] = small_sum(r.g0_acc.at[0], r.g0_in, r.sem_g0, "pair")
    small_send(r.g0_acc.at[1], r.g0_in, r.sem_g0, "plane")
    weights_spread(own_attn[:3], attn_cols[:3], r.sem_wa, plane_q)
    weights_spread(own_attn[3:], attn_cols[3:], r.sem_wa, plane_o)
    r.g0_acc[2] = small_sum(r.g0_acc.at[1], r.g0_in, r.sem_g0, "plane")
    for j in range(n.lines):
        r.gv[0, :, j * HEAD_DIM : (j + 1) * HEAD_DIM] = r.g0_acc[2, j : j + 1, :]
        r.gv[1, :, j * HEAD_DIM : (j + 1) * HEAD_DIM] = r.g0_acc[
            2, n.lines + j : n.lines + j + 1, :
        ]
    qgain = r.g0_acc[2, 2 * n.lines : 2 * n.lines + 1, :]
    kgain = r.g0_acc[2, 2 * n.lines + 1 : 2 * n.lines + 2, :]
    attn_gain, mlp_gain = r.gv[0], r.gv[1]
    for by in range(1, n.ctx):
        if by == n.ctx - 1:
            weights_send(mlp_shards, mlp_cols, r.wm, r.sem_wm, "between")
            for k in range(PARTS):
                gather_start(r.cot, r.gb, r.sem_gb, k, "between")
        for k in range(PARTS):
            gather_relay(r.xb, r.sem_xb, by, k)
    own_x.wait()
    own_g.wait()

    def norm_rows(j, carry):
        x = r.xb[j].astype(F32)
        start = pl.multiple_of(j * rows, rows)
        r.xn[pl.ds(start, rows), :] = (x * rms(x) * attn_gain).astype(BF16)
        return carry

    lax.fori_loop(0, n.ctx, norm_rows, 0)
    weights_forward(plane_q)
    weights_wait(plane_q)
    weights_send(mlp_shards, mlp_cols, r.wm, r.sem_wm, "ends")
    for k in range(PARTS):
        gather_start(r.cot, r.gb, r.sem_gb, k, "ends")

    cosine, sine = r.cos, r.sin
    tile = 2 * HEAD_DIM if n.kv % 2 == 0 else HEAD_DIM
    for at in range(0, q_cols + 2 * k_cols, tile):
        product = mm(r.xn[...], r.wa[:, at : at + tile])
        for part in range(tile // HEAD_DIM):
            head = at // HEAD_DIM + part
            u = product[:, part * HEAD_DIM : (part + 1) * HEAD_DIM]
            if head < n.heads:
                r.qp[head] = u
                r.qr[head] = rope_fwd(u * rms(u) * qgain, cosine[...], sine[...]).astype(BF16)
            elif head < n.heads + n.kv:
                r.kp[head - n.heads] = u
                r.kr[head - n.heads] = rope_fwd(u * rms(u) * kgain, cosine[...], sine[...]).astype(
                    BF16
                )
            else:
                r.vv[head - n.heads - n.kv] = u.astype(BF16)
    weights_forward(plane_o)
    half = n.tokens // 2

    def head_forward(h, carry):
        kv = h // group
        for q0 in (0, half):
            s = mm(r.qr[h, q0 : q0 + half, :], r.kr[kv], LAST_AXIS)
            allowed = r.posk[...] <= r.posq[q0 : q0 + half, 0:1]
            e = jnp.where(allowed, jnp.exp(s * factor), 0.0)
            r.es[h, q0 : q0 + half, :] = e
            total = jnp.sum(e, axis=-1, keepdims=True)
            a = mm(e.astype(BF16), r.vv[kv]) / total
            r.af[h, q0 : q0 + half, :] = a
            lane = pl.multiple_of(h * HEAD_DIM, HEAD_DIM)
            r.at[q0 : q0 + half, pl.ds(lane, HEAD_DIM)] = a.astype(BF16)
        return carry

    lax.fori_loop(0, n.heads, head_forward, 0)
    weights_wait(plane_o)

    def by_rows(left, right, out):
        step = 2 * HEAD_DIM
        for at in range(0, d, step):
            product = mm(left[...], right(slice(at, at + step)), LAST_AXIS)
            out[:, :, at : at + step] = product.astype(BF16).reshape(n.ctx, rows, step)

    by_rows(r.at, lambda span: r.wa[span, o_at:], r.p_o)
    steps = range(n.ctx - 1)
    for k in range(PARTS):
        scatter_start(sum_o, k)
    weights_spread(own_mlp, mlp_cols, r.sem_wm, plane_m)

    def residual(k):
        span = rows_of(k)
        r.ho[span, :] = r.xb[c, span, :].astype(F32)
        scatter_total(sum_o, r.ho, k)
        own = r.ho[span, :]
        r.mb[c, span, :] = (own * rms(own) * mlp_gain).astype(BF16)
        gather_start(r.mb.at[c], r.mb, r.sem_mb, k)

    gather_relay(r.gb, r.sem_gb, 1, 0)
    for step in steps:
        scatter_relay(sum_o, step, 0)
    for by in range(2, n.ctx - 1):
        gather_relay(r.gb, r.sem_gb, by, 0)
    residual(0)
    for step in steps:
        scatter_relay(sum_o, step, 1)
        if step == 0:
            gather_relay(r.mb, r.sem_mb, 1, 0, "between")
    residual(1)
    gather_relay(r.mb, r.sem_mb, 1, 0, "end")
    gather_relay(r.mb, r.sem_mb, 1, 1, "between")
    for by in range(2, n.ctx - 1):
        gather_relay(r.mb, r.sem_mb, by, 0)
    weights_forward(plane_m)
    gather_relay(r.mb, r.sem_mb, n.ctx - 1, 0)
    gather_relay(r.gb, r.sem_gb, n.ctx - 1, 0)
    weights_wait(plane_m)

    tile = 2 * HEAD_DIM if ff % (2 * HEAD_DIM) == 0 else HEAD_DIM
    span_rows = n.ctx * part_rows

    def mlp_part(k):
        span = rows_of(k)
        mixed = r.mb[:, span, :].reshape(span_rows, d)
        upstream = r.gb[:, span, :].reshape(span_rows, d)
        for at in range(0, ff, tile):
            gate = mm(mixed, r.wm[:, at : at + tile])
            up = mm(mixed, r.wm[:, ff + at : ff + at + tile])
            back = mm(upstream, r.wm[:, 2 * ff + at : 2 * ff + at + tile])
            sig = jax.nn.sigmoid(gate)
            swish = gate * sig
            shape = (n.ctx, part_rows, tile)
            r.hid[:, span, at : at + tile] = (swish * up).astype(BF16).reshape(shape)
            r.dgu[:, span, at : at + tile] = (
                (back * up * sig * (1.0 + gate * (1.0 - sig))).astype(BF16).reshape(shape)
            )
            r.dgu[:, span, ff + at : ff + at + tile] = (
                (back * swish).astype(BF16).reshape(shape)
            )
        both = r.dgu[:, span, :].reshape(span_rows, 2 * ff)
        for at in range(0, d, 2 * HEAD_DIM):
            product = mm(both, r.wm[at : at + 2 * HEAD_DIM, : 2 * ff], LAST_AXIS).astype(BF16)
            r.p_x2[:, span, at : at + 2 * HEAD_DIM] = product.reshape(
                n.ctx, part_rows, 2 * HEAD_DIM
            )
        scatter_start(sum_x2, k)

    def residual_back(k):
        span = rows_of(k)
        r.dh[span, :] = jnp.zeros((part_rows, d), F32)
        scatter_total(sum_x2, r.dh, k)
        own = r.ho[span, :]
        from_norm, term = norm_back(own, rms(own), mlp_gain, r.dh[span, :])
        save_lines(n.lines, jnp.sum(term, axis=0, keepdims=True))
        r.dh[span, :] = r.gb[c, span, :].astype(F32) + from_norm
        r.rb[c, span, :] = r.dh[span, :].astype(BF16)
        gather_start(r.rb.at[c], r.rb, r.sem_rb, k)

    mlp_part(0)
    gather_relay(r.mb, r.sem_mb, 1, 1, "end")
    gather_relay(r.gb, r.sem_gb, 1, 1)
    for step in steps:
        scatter_relay(sum_x2, step, 0)
        if step == 0:
            for by in range(2, n.ctx - 1):
                gather_relay(r.mb, r.sem_mb, by, 1)
                gather_relay(r.gb, r.sem_gb, by, 1)
    gather_relay(r.mb, r.sem_mb, n.ctx - 1, 1)
    gather_relay(r.gb, r.sem_gb, n.ctx - 1, 1)
    mlp_part(1)
    residual_back(0)
    hidden = r.hid[...].reshape(n.tokens, ff)
    by_rows(hidden, lambda span: r.wm[span, 2 * ff :], r.p_y)
    scatter_start(sum_y, 0)
    mixed = r.mb[...].reshape(n.tokens, d)
    upstream = r.gb[...].reshape(n.tokens, d)
    for at in range(0, 2 * ff, tile):
        part = r.dgu[:, :, at : at + tile].reshape(n.tokens, tile)
        r.gm[:, at : at + tile] = mm(mixed, part, FIRST_AXIS).astype(BF16)
    for at in range(0, ff, tile):
        part = r.hid[:, :, at : at + tile].reshape(n.tokens, tile)
        r.gm[:, 2 * ff + at : 2 * ff + at + tile] = mm(upstream, part, FIRST_AXIS).astype(BF16)
    grads_pair(group_m)
    for step in steps:
        scatter_relay(sum_x2, step, 1)
        if step == 0:
            gather_relay(r.rb, r.sem_rb, 1, 0, "between")
            grads_plane(group_m)
        elif step == 1:
            gather_relay(r.rb, r.sem_rb, 1, 0, "end")
    for by in range(2, n.ctx - 1):
        gather_relay(r.rb, r.sem_rb, by, 0)
    residual_back(1)
    scatter_start(sum_y, 1)
    gather_relay(r.rb, r.sem_rb, 1, 1, "between")
    gather_relay(r.rb, r.sem_rb, 1, 1, "end")
    for by in range(2, n.ctx - 1):
        gather_relay(r.rb, r.sem_rb, by, 1)
    for step in steps:
        scatter_relay(sum_y, step, 0)
    for k in range(PARTS):
        gather_relay(r.rb, r.sem_rb, n.ctx - 1, k)

    upstream = r.rb[...].reshape(n.tokens, d)
    for at in range(0, o_cols, HEAD_DIM):
        r.da[at // HEAD_DIM] = mm(upstream, r.wa[:, o_at + at : o_at + at + HEAD_DIM])
    r.ga[:, o_at:] = mm(upstream, r.at[...], FIRST_AXIS).astype(BF16)
    grads_pair(group_o)
    grads_line(group_m)
    r.dk[...] = jnp.zeros_like(r.dk)
    r.dv[...] = jnp.zeros_like(r.dv)

    def head_backward(h, carry):
        kv = h // group
        for q0 in (0, half):
            span = slice(q0, q0 + half)
            e = r.es[h, span, :]
            total = jnp.sum(e, axis=-1, keepdims=True)
            da = r.da[h, span, :]
            w = (da / total).astype(BF16)
            dl = jnp.sum(da * r.af[h, span, :], axis=-1, keepdims=True) / total
            ds = (e * (mm(w, r.vv[kv], LAST_AXIS) - dl)).astype(BF16)
            r.ds[span, :] = ds
            r.eb[span, :] = e.astype(BF16)
            r.wb[span, :] = w
            r.da[h, span, :] = mm(ds, r.kr[kv])
        r.dk[kv] = r.dk[kv] + mm(r.ds[...], r.qr[h], FIRST_AXIS)
        r.dv[kv] = r.dv[kv] + mm(r.eb[...], r.wb[...], FIRST_AXIS)
        return carry

    lax.fori_loop(0, n.heads, head_backward, 0)

    def query_backward(h, term):
        u = r.qp[h]
        du, gain_term = norm_back(
            u, rms(u), qgain, rope_bwd(r.da[h] * factor, cosine[...], sine[...])
        )
        lane = pl.multiple_of(h * HEAD_DIM, HEAD_DIM)
        r.dqkv[:, pl.ds(lane, HEAD_DIM)] = du.astype(BF16)
        return term + jnp.sum(gain_term, axis=0, keepdims=True)

    q_term = lax.fori_loop(0, n.heads, query_backward, jnp.zeros((1, HEAD_DIM), F32))
    grads_plane(group_o)
    k_term = jnp.zeros((1, HEAD_DIM), F32)
    for kv in range(n.kv):
        u = r.kp[kv]
        du, gain_term = norm_back(
            u, rms(u), kgain, rope_bwd(r.dk[kv] * factor, cosine[...], sine[...])
        )
        at = q_cols + kv * HEAD_DIM
        r.dqkv[:, at : at + HEAD_DIM] = du.astype(BF16)
        at += k_cols
        r.dqkv[:, at : at + HEAD_DIM] = r.dv[kv].astype(BF16)
        k_term = k_term + jnp.sum(gain_term, axis=0, keepdims=True)
    for at in range(0, o_at, 2 * HEAD_DIM):
        r.ga[:, at : at + 2 * HEAD_DIM] = mm(
            r.xn[...], r.dqkv[:, at : at + 2 * HEAD_DIM], FIRST_AXIS
        ).astype(BF16)
    grads_pair(group_q)
    by_rows(r.dqkv, lambda span: r.wa[span, :o_at], r.p_x1)
    for k in range(PARTS):
        scatter_start(sum_x1, k)
    for step in steps:
        scatter_relay(sum_y, step, 1)
    grads_plane(group_q)
    grads_line(group_o)
    for k in range(PARTS):
        for step in steps:
            scatter_relay(sum_x1, step, k)
        if k == 0:
            grads_line(group_q)
    for k in range(PARTS):
        scatter_total(sum_y, r.ho, k)
    r.out_hidden[...] = r.ho[...].astype(BF16)
    r.out_input[...] = jnp.zeros_like(r.out_input)
    for k in range(PARTS):
        scatter_total(sum_x1, r.out_input, k)
    x = r.xb[c].astype(F32)
    from_norm, term = norm_back(x, rms(x), attn_gain, r.out_input[...])
    save_lines(0, jnp.sum(term, axis=0, keepdims=True))
    r.out_input[...] = r.dh[...] + from_norm
    r.g1_acc[3, 2 * n.lines : 2 * n.lines + 1, :] = q_term
    r.g1_acc[3, 2 * n.lines + 1 : 2 * n.lines + 2, :] = k_term
    small_send(r.g1_acc.at[3], r.g1_in, r.sem_g1, "pair")
    r.g1_acc[0] = small_sum(r.g1_acc.at[3], r.g1_in, r.sem_g1, "pair")
    small_send(r.g1_acc.at[0], r.g1_in, r.sem_g1, "plane")
    r.g1_acc[1] = small_sum(r.g1_acc.at[0], r.g1_in, r.sem_g1, "plane")
    small_send(r.g1_acc.at[1], r.g1_in, r.sem_g1, "line")
    grads_wait(group_m)
    grads_wait(group_o)
    grads_wait(group_q)
    r.out_gains[...] = small_sum(r.g1_acc.at[1], r.g1_in, r.sem_g1, "line")
    for wait in sends:
        wait()


def fused(
    ctx,
    fsdp,
    hidden_in,
    block_order,
    cotangent,
    q_weight,
    k_weight,
    v_weight,
    o_weight,
    attn_gain,
    query_gain,
    key_gain,
    mlp_gain,
    gate_weight,
    up_weight,
    down_weight,
):
    shards = (q_weight, k_weight, v_weight, o_weight, gate_weight, up_weight, down_weight)
    n = Sizes(ctx, fsdp, hidden_in.shape[1], shards)
    gains = jnp.concatenate([attn_gain, mlp_gain, query_gain, key_gain]).astype(F32)
    gains = jnp.pad(gains, (0, HEAD_DIM - gains.shape[0])).reshape(1, HEAD_DIM)
    hbm, vmem = pl.BlockSpec(memory_space=pl.ANY), pl.BlockSpec(memory_space=pltpu.VMEM)
    inputs = dict(
        hidden=(hidden_in[0], hbm),
        cot=(cotangent[0], hbm),
        wq=(q_weight, hbm),
        wk=(k_weight, hbm),
        wv=(v_weight, hbm),
        wo=(o_weight, hbm),
        wg=(gate_weight, hbm),
        wu=(up_weight, hbm),
        wd=(down_weight, hbm),
        gains=(gains, vmem),
        order=(block_order, pl.BlockSpec(memory_space=pltpu.SMEM)),
    )
    outputs = dict(
        out_hidden=jax.ShapeDtypeStruct((n.rows, n.width), BF16),
        out_input=jax.ShapeDtypeStruct((n.rows, n.width), F32),
        ga_land=jax.ShapeDtypeStruct((ctx, n.shard, n.attn_cols), BF16),
        gm_land=jax.ShapeDtypeStruct((ctx, n.shard, n.mlp_cols), BF16),
        out_gains=jax.ShapeDtypeStruct((n.gain_rows, HEAD_DIM), F32),
    )
    scratch = scratch_of(n)
    landed = pl.pallas_call(
        functools.partial(layer_kernel, n, [*inputs, *outputs, *scratch]),
        out_shape=tuple(outputs.values()),
        in_specs=[spec for _, spec in inputs.values()],
        out_specs=tuple(vmem for _ in outputs),
        scratch_shapes=list(scratch.values()),
        compiler_params=pltpu.CompilerParams(
            collective_id=0, has_side_effects=True, vmem_limit_bytes=VMEM_LIMIT
        ),
        name="layer",
    )(*[value for value, _ in inputs.values()])

    finals = [(n.rows, n.width, BF16), (n.rows, n.width, F32)]
    finals += [(s.shape[0], s.shape[1], F32) for s in shards] + [(8, HEAD_DIM, F32)]
    result, input_grad, oq, ok, ov, oo, og, ou, od, sums = pl.pallas_call(
        functools.partial(emit_kernel, n),
        out_shape=tuple(jax.ShapeDtypeStruct(f[:2], f[2]) for f in finals),
        in_specs=[vmem] * len(outputs),
        out_specs=tuple(vmem for _ in finals),
        name="emit",
    )(*landed)
    return (
        result[None],
        input_grad[None],
        oq,
        ok,
        ov,
        oo,
        sums[0, : n.each],
        sums[2, : n.few],
        sums[3, : n.few],
        sums[1, : n.each],
        og,
        ou,
        od,
    )


def emit_kernel(n, result, input_grad, attn_land, mlp_land, sums, *outs):
    outs[0][...] = result[...]
    outs[1][...] = input_grad[...]
    which = 2
    for land, widths in ((attn_land, n.cols[:4]), (mlp_land, n.cols[4:])):
        at = 0
        for width in widths:
            for j in range(n.ctx):
                outs[which][:, j * width : (j + 1) * width] = land[j, :, at : at + width].astype(
                    F32
                )
            at += width
            which += 1
    me = lax.axis_index("fsdp") * n.ctx + lax.axis_index("ctx")
    row, at = me * n.each // HEAD_DIM, lax.rem(me * n.each, HEAD_DIM)
    sums_out = outs[which]
    sums_out[...] = jnp.zeros_like(sums_out)
    for i, (line, lane) in enumerate(
        (
            (row, at),
            (n.lines + row, at),
            (2 * n.lines, me * n.few),
            (2 * n.lines + 1, me * n.few),
        )
    ):
        back = lax.rem(HEAD_DIM - lane, HEAD_DIM)
        sums_out[i : i + 1, :] = pltpu.roll(sums[pl.ds(line, 1), :], back, 1)


def fits(ctx, fsdp, shard_rows):
    per_tile = HEAD_DIM % (2 * shard_rows) == 0 and HEAD_DIM % (ctx * fsdp) == 0
    return per_tile and shard_rows % 16 == 0 and fsdp % 2 == 0 and KV_HEADS % ctx == 0


def solution(mesh):
    ctx, fsdp = mesh.shape["ctx"], mesh.shape["fsdp"]
    tokens = P("fsdp", "ctx", None)
    matrix = P(("fsdp", "ctx"), None)
    vector = P(("fsdp", "ctx"))
    def step(hidden_in, block_order, cotangent, q_weight, *rest):
        whole = fused if fits(ctx, fsdp, q_weight.shape[0]) else local
        return whole(ctx, fsdp, hidden_in, block_order, cotangent, q_weight, *rest)

    return jax.shard_map(
        step,
        mesh=mesh,
        in_specs=(tokens, P("fsdp", None), tokens)
        + (matrix,) * 4
        + (vector,) * 4
        + (matrix,) * 3,
        out_specs=(tokens,) * 2 + (matrix,) * 4 + (vector,) * 4 + (matrix,) * 3,
        check_vma=False,
    )
```

```python
import functools
import math
import types

import jax
import jax.numpy as jnp
from jax import lax
from jax.experimental import pallas as pl
from jax.experimental.pallas import tpu as pltpu
from jax.sharding import PartitionSpec as P

HEADS = 16
KV_HEADS = 8
HEAD_DIM = 128
EPSILON = 1e-06
FIRST_AXIS = (((0,), (0,)), ((), ()))
LAST_AXIS = (((1,), (1,)), ((), ()))
BF16 = jnp.bfloat16
F32 = jnp.float32
VMEM_LIMIT = 67043328
PARTS = 2
PIECES = 2


def mm(left, right, dims=(((1,), (0,)), ((), ()))):
    return lax.dot_general(left, right, dims, preferred_element_type=F32)


def rms(signal):
    return lax.rsqrt(jnp.mean(signal * signal, axis=-1, keepdims=True) + EPSILON)


def norm_back(signal, inverse_rms, gain_vec, upstream):
    unit_values = signal * inverse_rms
    scaled_up = upstream * gain_vec
    inner = scaled_up - unit_values * jnp.mean(scaled_up * unit_values, axis=-1, keepdims=True)
    return (inverse_rms * inner, upstream * unit_values)


def rope_tables(positions, head_width):
    exponent = jnp.arange(head_width // 2, dtype=F32) * (2.0 / head_width)
    inverse = jnp.exp(-exponent * math.log(1000000.0))
    angles = positions.astype(F32)[:, None] * inverse[None, :]
    angles = jnp.concatenate([angles, angles], axis=-1)
    return (jnp.cos(angles), jnp.sin(angles))


def rotate(signal, cosine, sine):
    half = signal.shape[-1] // 2
    turned = jnp.concatenate([-signal[..., half:], signal[..., :half]], axis=-1)
    return signal * cosine + turned * sine


def rotate_back(upstream, cosine, sine):
    half = upstream.shape[-1] // 2
    scaled_up = upstream * sine
    return upstream * cosine + jnp.concatenate(
        [scaled_up[..., half:], -scaled_up[..., :half]], axis=-1
    )


def gather_columns(ctx, shards):
    rows = shards[0].shape[0]
    cut = [s.reshape(rows, ctx, s.shape[1] // ctx).transpose(1, 0, 2) for s in shards]
    widths = [c.shape[2] for c in cut]
    both = jnp.concatenate(cut, axis=2)
    both = lax.all_to_all(both, "ctx", 0, 0, tiled=True)
    both = both.reshape(ctx * rows, -1)
    whole = lax.all_gather(both, "fsdp", axis=0, tiled=True)
    out, at = [], 0
    for width in widths:
        out.append(whole[:, at : at + width])
        at += width
    return out


def scatter_grads(ctx, fsdp, grads):
    rows = grads[0].shape[0] // (ctx * fsdp)
    widths = [g.shape[1] for g in grads]
    both = jnp.concatenate([g.astype(BF16) for g in grads], axis=1)
    both = lax.psum_scatter(both, "fsdp", scatter_dimension=0, tiled=True)
    both = lax.all_to_all(both.reshape(ctx, rows, -1), "ctx", 0, 0, tiled=True)
    out, at = [], 0
    for width in widths:
        piece = both[:, :, at : at + width]
        out.append(piece.transpose(1, 0, 2).reshape(rows, ctx * width).astype(F32))
        at += width
    return out


def ctx_gather(rows):
    return lax.all_gather(rows, "ctx", axis=0, tiled=True)


def ctx_scatter(partial):
    return lax.psum_scatter(partial.astype(BF16), "ctx", scatter_dimension=0, tiled=True).astype(
        F32
    )


def local(
    ctx,
    fsdp,
    hidden_in,
    block_order,
    cotangent,
    q_weight,
    k_weight,
    v_weight,
    o_weight,
    attn_gain,
    query_gain,
    key_gain,
    mlp_gain,
    gate_weight,
    up_weight,
    down_weight,
):
    inputs = hidden_in[0].astype(F32)
    row_count = inputs.shape[0]
    tokens = row_count * ctx
    slots = block_order.shape[1]
    block_len = tokens // slots
    heads, kv_heads = HEADS // ctx, KV_HEADS // ctx
    group = heads // kv_heads
    factor = 1.0 / math.sqrt(HEAD_DIM)
    positions = (
        block_order[0][:, None] * block_len + jnp.arange(block_len, dtype=jnp.int32)[None, :]
    ).reshape(-1)
    cosine, sine = rope_tables(positions, HEAD_DIM)
    cosine, sine = cosine[:, None, :], sine[:, None, :]

    both = ("fsdp", "ctx")
    norm_gain, qgain, kgain, mlp_norm_gain = (
        lax.all_gather(g, both, axis=0, tiled=True).astype(F32)
        for g in (attn_gain, query_gain, key_gain, mlp_gain)
    )
    norm_scale = rms(inputs)
    normed = ctx_gather((inputs * norm_scale * norm_gain).astype(BF16))
    upstream = ctx_gather(cotangent[0])
    q_full, k_full, v_full, o_full = gather_columns(ctx, (q_weight, k_weight, v_weight, o_weight))
    gate_full, up_full, down_full = gather_columns(ctx, (gate_weight, up_weight, down_weight))

    query_proj = mm(normed, q_full).reshape(tokens, heads, HEAD_DIM)
    key_proj = mm(normed, k_full).reshape(tokens, kv_heads, HEAD_DIM)
    value_low = mm(normed, v_full).astype(BF16).reshape(tokens, kv_heads, HEAD_DIM)
    query_scale, key_scale = rms(query_proj), rms(key_proj)
    query_low = (
        rotate(query_proj * query_scale * qgain, cosine, sine)
        .astype(BF16)
        .reshape(tokens, kv_heads, group, HEAD_DIM)
    )
    key_low = rotate(key_proj * key_scale * kgain, cosine, sine).astype(BF16)
    scores = jnp.einsum("rkgd,nkd->kgrn", query_low, key_low, preferred_element_type=F32) * factor
    allowed = positions[None, :] <= positions[:, None]
    weights_exp = jnp.where(allowed, jnp.exp(scores), 0.0)
    denominator = jnp.sum(weights_exp, axis=-1)
    weights_low = weights_exp.astype(BF16)
    numerator = jnp.einsum("kgrn,nkd->rkgd", weights_low, value_low, preferred_element_type=F32)
    denom_rows = jnp.transpose(denominator, (2, 0, 1))[..., None]
    attn_full = numerator / denom_rows
    attn_low = attn_full.astype(BF16).reshape(tokens, heads * HEAD_DIM)
    residual = inputs + ctx_scatter(mm(attn_low, o_full, LAST_AXIS))

    mix_scale = rms(residual)
    mixed = ctx_gather((residual * mix_scale * mlp_norm_gain).astype(BF16))
    gate_val = mm(mixed, gate_full)
    up_val = mm(mixed, up_full)
    sigmoid_gate = jax.nn.sigmoid(gate_val)
    swish_gate = gate_val * sigmoid_gate
    hidden_low = (swish_gate * up_val).astype(BF16)
    result = residual + ctx_scatter(mm(hidden_low, down_full, LAST_AXIS))
    hidden_grad = mm(upstream, down_full)
    gate_back = (
        hidden_grad * up_val * sigmoid_gate * (1.0 + gate_val * (1.0 - sigmoid_gate))
    ).astype(BF16)
    up_back = (hidden_grad * swish_gate).astype(BF16)
    mixed_grad = ctx_scatter(mm(gate_back, gate_full, LAST_AXIS) + mm(up_back, up_full, LAST_AXIS))
    resid_from_norm, mlp_gain_term = norm_back(residual, mix_scale, mlp_norm_gain, mixed_grad)
    residual_grad = cotangent[0].astype(F32) + resid_from_norm
    mlp_grads = scatter_grads(
        ctx,
        fsdp,
        (
            mm(mixed, gate_back, FIRST_AXIS),
            mm(mixed, up_back, FIRST_AXIS),
            mm(upstream, hidden_low, FIRST_AXIS),
        ),
    )
    resid_low = ctx_gather(residual_grad.astype(BF16))

    attn_grad = mm(resid_low, o_full).reshape(tokens, kv_heads, group, HEAD_DIM)
    share_low = (attn_grad / denom_rows).astype(BF16)
    denom_grad = jnp.transpose(jnp.sum(attn_grad * attn_full, axis=-1), (1, 2, 0)) / denominator
    weight_grad = jnp.einsum("rkgd,nkd->kgrn", share_low, value_low, preferred_element_type=F32)
    score_low = (weights_exp * (weight_grad - denom_grad[..., None])).astype(BF16)
    query_rot = (
        jnp.einsum("kgrn,nkd->rkgd", score_low, key_low, preferred_element_type=F32) * factor
    ).reshape(tokens, heads, HEAD_DIM)
    key_rot = (
        jnp.einsum("kgrn,rkgd->nkd", score_low, query_low, preferred_element_type=F32) * factor
    )
    value_back = (
        jnp.einsum("kgrn,rkgd->nkd", weights_low, share_low, preferred_element_type=F32)
        .reshape(tokens, kv_heads * HEAD_DIM)
        .astype(BF16)
    )
    query_grad, query_term = norm_back(
        query_proj, query_scale, qgain, rotate_back(query_rot, cosine, sine)
    )
    key_grad, key_term = norm_back(key_proj, key_scale, kgain, rotate_back(key_rot, cosine, sine))
    query_back = query_grad.reshape(tokens, heads * HEAD_DIM).astype(BF16)
    key_back = key_grad.reshape(tokens, kv_heads * HEAD_DIM).astype(BF16)
    normed_grad = ctx_scatter(
        mm(query_back, q_full, LAST_AXIS)
        + mm(key_back, k_full, LAST_AXIS)
        + mm(value_back, v_full, LAST_AXIS)
    )
    input_from_norm, attn_gain_term = norm_back(inputs, norm_scale, norm_gain, normed_grad)
    input_grad = residual_grad + input_from_norm
    attn_grads = scatter_grads(
        ctx,
        fsdp,
        (
            mm(normed, query_back, FIRST_AXIS),
            mm(normed, key_back, FIRST_AXIS),
            mm(normed, value_back, FIRST_AXIS),
            mm(resid_low, attn_low, FIRST_AXIS),
        ),
    )
    gains = (
        jnp.sum(attn_gain_term, axis=0),
        jnp.sum(query_term, axis=(0, 1)),
        jnp.sum(key_term, axis=(0, 1)),
        jnp.sum(mlp_gain_term, axis=0),
    )
    gains = [lax.psum_scatter(g, both, scatter_dimension=0, tiled=True) for g in gains]
    return (
        result.astype(BF16)[None],
        input_grad[None],
        *attn_grads,
        *gains,
        *mlp_grads,
    )


def rope_fwd(u, cosine, sine):
    return u * cosine + pltpu.roll(u, HEAD_DIM // 2, u.ndim - 1) * sine


def rope_bwd(du, cosine, sine):
    return du * cosine - pltpu.roll(du, HEAD_DIM // 2, du.ndim - 1) * sine


class Sizes:
    def __init__(self, ctx, fsdp, rows, shards):
        self.ctx, self.fsdp, self.rows = ctx, fsdp, rows
        self.chips = fsdp // 2
        self.shard = shards[0].shape[0]
        self.block = self.shard * ctx
        self.width = self.block * fsdp
        self.tokens = rows * ctx
        self.heads, self.kv = HEADS // ctx, KV_HEADS // ctx
        self.cols = [s.shape[1] // ctx for s in shards]
        self.attn_cols = sum(self.cols[:4])
        self.mlp_cols = sum(self.cols[4:])
        self.lines = self.width // HEAD_DIM
        self.gain_rows = 8 * ((2 * self.lines + 2 + 7) // 8)
        self.each, self.few = self.width // (ctx * fsdp), HEAD_DIM // (ctx * fsdp)


def scratch_of(n):
    bf, f32 = (lambda *s: pltpu.VMEM(s, BF16)), (lambda *s: pltpu.VMEM(s, F32))
    sem = lambda *s: pltpu.SemaphoreType.DMA(s)
    c, d, s, h, kv = n.ctx, n.width, n.tokens, n.heads, n.kv
    ff = n.cols[4]
    out = dict(
        wa=bf(d, n.attn_cols),
        wm=bf(d, n.mlp_cols),
        xb=bf(c, n.rows, d),
        gb=bf(c, n.rows, d),
        mb=bf(c, n.rows, d),
        rb=bf(c, n.rows, d),
        xn=bf(s, d),
        qp=f32(h, s, HEAD_DIM),
        kp=f32(kv, s, HEAD_DIM),
        qr=bf(h, s, HEAD_DIM),
        kr=bf(kv, s, HEAD_DIM),
        vv=bf(kv, s, HEAD_DIM),
        es=f32(h, s, s),
        af=f32(h, s, HEAD_DIM),
        at=bf(s, h * HEAD_DIM),
        da=f32(h, s, HEAD_DIM),
        dk=f32(kv, s, HEAD_DIM),
        dv=f32(kv, s, HEAD_DIM),
        ds=bf(s, s),
        eb=bf(s, s),
        wb=bf(s, HEAD_DIM),
        dqkv=bf(s, (h + 2 * kv) * HEAD_DIM),
        hid=bf(c, n.rows, ff),
        dgu=bf(c, n.rows, 2 * ff),
        ho=f32(n.rows, d),
        dh=f32(n.rows, d),
        gv=f32(2, 1, d),
        gp=f32(n.gain_rows, HEAD_DIM),
        cos=f32(s, HEAD_DIM),
        sin=f32(s, HEAD_DIM),
        posq=pltpu.VMEM((s, HEAD_DIM), jnp.int32),
        posk=pltpu.VMEM((1, s), jnp.int32),
        ga=bf(d, n.attn_cols),
        gm=bf(d, n.mlp_cols),
        ga_sib=bf(n.chips, n.block, n.attn_cols),
        gm_sib=bf(n.chips, n.block, n.mlp_cols),
        ga_in=bf(n.chips - 1, n.block, n.attn_cols),
        gm_in=bf(n.chips - 1, n.block, n.mlp_cols),
        ga_z=bf(n.block, n.attn_cols),
        gm_z=bf(n.block, n.mlp_cols),
        local_sem=sem(9),
    )
    for name in ("o", "y", "x2", "x1"):
        out["p_" + name] = bf(c, n.rows, d)
        out["l_" + name] = bf(c, n.rows, d)
        out["r_" + name] = bf(c, n.rows, d)
        out["sem_" + name] = sem(4, c, PARTS * PIECES)
    for name in ("xb", "gb", "mb", "rb"):
        out["sem_" + name] = sem(3, c, PARTS * PIECES)
    out["sem_wa"] = sem(2, c - 1, 4)
    out["sem_wm"] = sem(2, c - 1, 3)
    for name in ("pq", "po", "pm"):
        out["sem_" + name] = sem(4, n.chips)
    for name in ("gm", "go", "gq"):
        out["sem_" + name] = sem(4, n.chips)
        out["sem_z" + name] = sem(2, c)
    for name in ("g0", "g1"):
        out[name + "_in"] = f32(n.fsdp + c, n.gain_rows, HEAD_DIM)
        out[name + "_acc"] = f32(4, n.gain_rows, HEAD_DIM)
        out["sem_" + name] = sem(2, n.fsdp + c)
    return out


def layer_kernel(n, names, *refs):
    r = types.SimpleNamespace(**dict(zip(names, refs)))
    c, f = lax.axis_index("ctx"), lax.axis_index("fsdp")
    chip, core = f // 2, f % 2
    sibling = chip * 2 + 1 - core
    rows, d, block, shard = n.rows, n.width, n.block, n.shard
    sends = []

    def ahead(by):
        return lax.rem(c + by, n.ctx)

    def behind(by):
        return lax.rem(c + n.ctx - by, n.ctx)

    def chip_ahead(by):
        return lax.rem(chip + by, n.chips)

    def chip_behind(by):
        return lax.rem(chip + n.chips - by, n.chips)

    def remote(src, dst, send_sem, recv_sem, to_f=None, to_c=None):
        return pltpu.make_async_remote_copy(
            src_ref=src,
            dst_ref=dst,
            send_sem=send_sem,
            recv_sem=recv_sem,
            device_id={"fsdp": f if to_f is None else to_f, "ctx": c if to_c is None else to_c},
            device_id_type=pl.DeviceIdType.MESH,
        )

    def send(src, dst, send_sem, recv_sem, to_f=None, to_c=None):
        copy = remote(src, dst, send_sem, recv_sem, to_f, to_c)
        copy.start()
        sends.append(copy.wait_send)

    def arrived(dst, recv_sem):
        remote(dst, dst, recv_sem, recv_sem).wait_recv()

    def send_if(cond, src, dst, send_sem, recv_sem, to_c):
        copy = remote(src, dst, send_sem, recv_sem, None, to_c)
        pl.when(cond)(copy.start)
        sends.append(lambda: pl.when(cond)(copy.wait_send))

    barrier = pltpu.get_barrier_semaphore()

    def greet(to_f, to_c):
        pl.semaphore_signal(
            barrier,
            inc=1,
            device_id={"fsdp": to_f, "ctx": to_c},
            device_id_type=pl.DeviceIdType.MESH,
        )

    for by in range(1, n.ctx):
        greet(f, ahead(by))
    for by in range(1, n.fsdp):
        greet(lax.rem(f + by, n.fsdp), c)
    pl.semaphore_wait(barrier, n.ctx - 1 + n.fsdp - 1)

    right, left = jnp.minimum(c + 1, n.ctx - 1), jnp.maximum(c - 1, 0)
    part_rows, piece_rows = rows // PARTS, rows // (PARTS * PIECES)

    def pieces_of(k):
        return range(k * PIECES, (k + 1) * PIECES)

    def part_of(buf, j, i):
        return buf.at[j, pl.ds(i * piece_rows, piece_rows), :]

    def gather_start(src, buf, sem, k, to=None):
        for i in pieces_of(k):
            gather_piece(src, buf, sem, i, to)

    def gather_piece(src, buf, sem, i, to=None):
        piece = src.at[pl.ds(i * piece_rows, piece_rows), :]
        here = part_of(buf, c, i)
        up, down = c + 1 < n.ctx, c > 0
        if to == "between":
            up, down = c + 1 < n.ctx - 1, c > 1
        elif to == "ends":
            up, down = c + 1 == n.ctx - 1, c == 1
        send_if(up, piece, here, sem.at[0, 0, i], sem.at[2, c, i], right)
        send_if(down, piece, here, sem.at[1, 0, i], sem.at[2, c, i], left)

    def gather_relay(buf, sem, by, k, source=None):
        low, high = jnp.maximum(c - by, 0), jnp.minimum(c + by, n.ctx - 1)
        from_low, from_high = c - by >= 0, c + by < n.ctx
        if source == "end":
            from_low, from_high = c == by, c + by == n.ctx - 1
        elif source == "between":
            from_low, from_high = c > by, c + by < n.ctx - 1
        for i in pieces_of(k):
            piece, here = part_of(buf, low, i), sem.at[2, low, i]
            pl.when(from_low)(functools.partial(arrived, piece, here))
            send_if(from_low & (c + 1 < n.ctx), piece, piece, sem.at[0, by, i], here, right)
            piece, here = part_of(buf, high, i), sem.at[2, high, i]
            pl.when(from_high)(functools.partial(arrived, piece, here))
            send_if(from_high & (c > 0), piece, piece, sem.at[1, by, i], here, left)

    def rows_of(k):
        return slice(k * part_rows, (k + 1) * part_rows)

    def scatter_send(cond, part, there, sem, target, i, way, to_c):
        send_if(
            cond,
            part_of(part, target, i),
            part_of(there, target, i),
            sem.at[way, target, i],
            sem.at[2 + way, target, i],
            to_c,
        )

    def scatter_add(part, there, sem, target, i, way):
        arrived(part_of(there, target, i), sem.at[2 + way, target, i])
        span = slice(i * piece_rows, (i + 1) * piece_rows)
        part[target, span, :] = (
            part[target, span, :].astype(F32) + there[target, span, :].astype(F32)
        ).astype(BF16)

    def scatter_start(g, k):
        for step in range(n.ctx - 1):
            for i in pieces_of(k):
                scatter_send(c == n.ctx - 1, g.part, g.high, g.sem, step, i, 1, left)
                scatter_send(c == 0, g.part, g.low, g.sem, n.ctx - 1 - step, i, 0, right)

    def scatter_up(g, step, k, cond):
        target = n.ctx - 1 - step
        cond = cond & (c < target) & (c > 0)
        for i in pieces_of(k):
            pl.when(cond)(functools.partial(scatter_add, g.part, g.low, g.sem, target, i, 0))
            scatter_send(cond, g.part, g.low, g.sem, target, i, 0, right)

    def scatter_down(g, step, k, cond):
        cond = cond & (c > step) & (c + 1 < n.ctx)
        for i in pieces_of(k):
            pl.when(cond)(functools.partial(scatter_add, g.part, g.high, g.sem, step, i, 1))
            scatter_send(cond, g.part, g.high, g.sem, step, i, 1, left)

    def scatter_near(g, k):
        for step in range(n.ctx - 1):
            scatter_up(g, step, k, c < n.ctx // 2)
            scatter_down(g, step, k, c >= n.ctx // 2)

    def scatter_far(g, k):
        for step in range(n.ctx - 1):
            scatter_up(g, step, k, c >= n.ctx // 2)
            scatter_down(g, step, k, c < n.ctx // 2)

    def scatter_total(g, out, k):
        span = rows_of(k)
        out[span, :] = out[span, :] + g.part[c, span, :].astype(F32)

        @pl.when(c > 0)
        def _():
            for i in pieces_of(k):
                arrived(part_of(g.low, c, i), g.sem.at[2, c, i])
            out[span, :] = out[span, :] + g.low[c, span, :].astype(F32)

        @pl.when(c + 1 < n.ctx)
        def _():
            for i in pieces_of(k):
                arrived(part_of(g.high, c, i), g.sem.at[3, c, i])
            out[span, :] = out[span, :] + g.high[c, span, :].astype(F32)

    def block_of(buf, index, span):
        return buf.at[pl.ds(pl.multiple_of(index * block, block), block), pl.ds(*span)]

    def piece_of(buf, line, at, width):
        start = pl.multiple_of(f * block + line * shard, shard)
        return buf.at[pl.ds(start, shard), pl.ds(at, width)]

    def weights_send(shards, cols, buf, sem, now=None):
        for by in range(1, n.ctx):
            at = 0
            for i, (src, width) in enumerate(zip(shards, cols)):
                column = pl.multiple_of(ahead(by) * width, HEAD_DIM)
                copy = remote(
                    src.at[:, pl.ds(column, width)],
                    piece_of(buf, c, at, width),
                    sem.at[0, by - 1, i],
                    sem.at[1, by - 1, i],
                    None,
                    ahead(by),
                )
                at_end = (ahead(by) == 0) | (ahead(by) == n.ctx - 1)
                if now is None:
                    copy.start()
                else:
                    pl.when(at_end if now == "ends" else ~at_end)(copy.start)
                if now != "ends":
                    sends.append(copy.wait_send)
                at += width

    def weights_own(shards, cols, buf, first):
        at, out = 0, []
        for i, (src, width) in enumerate(zip(shards, cols)):
            column = pl.multiple_of(c * width, HEAD_DIM)
            copy = pltpu.make_async_copy(
                src.at[:, pl.ds(column, width)],
                piece_of(buf, c, at, width),
                r.local_sem.at[first + i],
            )
            copy.start()
            out.append(copy)
            at += width
        return out

    def weights_spread(own, cols, sem, g):
        for copy in own:
            copy.wait()
        for by in range(1, n.ctx):
            at = g.span[0]
            for i, width in enumerate(cols):
                arrived(piece_of(g.buf, behind(by), at, width), sem.at[1, by - 1, g.first + i])
                at += width
        mine = block_of(g.buf, f, g.span)
        for by in range(1, n.chips):
            send(mine, mine, g.sem.at[0, by], g.sem.at[1, by], chip_ahead(by) * 2 + core)
        send(mine, mine, g.sem.at[2, 0], g.sem.at[3, 0], sibling)

    def weights_forward(g):
        for by in range(1, n.chips):
            piece = block_of(g.buf, chip_behind(by) * 2 + core, g.span)
            arrived(piece, g.sem.at[1, by])
            send(piece, piece, g.sem.at[2, by], g.sem.at[3, by], sibling)

    def weights_wait(g):
        for by in range(n.chips):
            arrived(block_of(g.buf, chip_behind(by) * 2 + 1 - core, g.span), g.sem.at[3, by])

    def share_of(buf, index, span):
        return buf.at[pl.ds(pl.multiple_of(index * block, block), block), pl.ds(*span)]

    def grads_pair(g):
        for by in (*range(1, n.chips), 0):
            send(
                share_of(g.whole, chip_ahead(by) * 2 + 1 - core, g.span),
                g.pair.at[by, :, pl.ds(*g.span)],
                g.sem.at[0, by],
                g.sem.at[1, by],
                sibling,
            )

    def grads_plane(g):
        for by in range(1, n.chips):
            theirs = g.pair.at[by, :, pl.ds(*g.span)]
            arrived(theirs, g.sem.at[1, by])
            piece = share_of(g.whole, chip_ahead(by) * 2 + core, g.span)
            piece[...] = (piece[...].astype(F32) + theirs[...].astype(F32)).astype(BF16)
            send(
                piece,
                g.plane.at[by - 1, :, pl.ds(*g.span)],
                g.sem.at[2, by],
                g.sem.at[3, by],
                chip_ahead(by) * 2 + core,
            )

    def grads_line(g):
        theirs = g.pair.at[0, :, pl.ds(*g.span)]
        arrived(theirs, g.sem.at[1, 0])
        acc = share_of(g.whole, f, g.span)[...].astype(F32) + theirs[...].astype(F32)
        for by in range(1, n.chips):
            theirs = g.plane.at[by - 1, :, pl.ds(*g.span)]
            arrived(theirs, g.sem.at[3, by])
            acc = acc + theirs[...].astype(F32)
        g.total[:, pl.ds(*g.span)] = acc.astype(BF16)
        for by in range(1, n.ctx):
            start = pl.multiple_of(ahead(by) * shard, shard)
            send(
                g.total.at[pl.ds(start, shard), pl.ds(*g.span)],
                g.land.at[c, :, pl.ds(*g.span)],
                g.line_sem.at[0, by],
                g.line_sem.at[1, by],
                None,
                ahead(by),
            )
        start = pl.multiple_of(c * shard, shard)
        g.land[c, :, pl.ds(*g.span)] = g.total[pl.ds(start, shard), pl.ds(*g.span)]

    def grads_wait(g):
        for by in range(1, n.ctx):
            arrived(g.land.at[behind(by), :, pl.ds(*g.span)], g.line_sem.at[1, by])

    def small_peers(way):
        if way == "line":
            return [(n.fsdp + by, f, ahead(by)) for by in range(1, n.ctx)]
        return [(by, lax.rem(f + by, n.fsdp), c) for by in range(1, n.fsdp)]

    def small_send(src, incoming, sem, way):
        for slot, to_f, to_c in small_peers(way):
            send(src, incoming.at[slot], sem.at[0, slot], sem.at[1, slot], to_f, to_c)

    def small_sum(own, incoming, sem, way):
        total = own[...]
        for slot, _, _ in small_peers(way):
            arrived(incoming.at[slot], sem.at[1, slot])
            total = total + incoming[slot]
        return total

    def save_lines(first, line):
        for j in range(n.lines):
            row = slice(first + j, first + j + 1)
            r.g1_acc[3, row, :] += line[:, j * HEAD_DIM : (j + 1) * HEAD_DIM]

    attn_shards, mlp_shards = (r.wq, r.wk, r.wv, r.wo), (r.wg, r.wu, r.wd)
    attn_cols, mlp_cols = n.cols[:4], n.cols[4:]
    q_cols, k_cols, _, o_cols = attn_cols
    ff = mlp_cols[0]
    group = n.heads // n.kv
    factor = 1.0 / math.sqrt(HEAD_DIM)

    o_at = q_cols + 2 * k_cols
    attn_bufs = dict(whole=r.ga, pair=r.ga_sib, plane=r.ga_in, total=r.ga_z, land=r.ga_land)
    mlp_bufs = dict(whole=r.gm, pair=r.gm_sib, plane=r.gm_in, total=r.gm_z, land=r.gm_land)
    plane_q = types.SimpleNamespace(buf=r.wa, span=(0, o_at), first=0, sem=r.sem_pq)
    plane_o = types.SimpleNamespace(buf=r.wa, span=(o_at, o_cols), first=3, sem=r.sem_po)
    plane_m = types.SimpleNamespace(buf=r.wm, span=(0, n.mlp_cols), first=0, sem=r.sem_pm)
    group_m = types.SimpleNamespace(
        **mlp_bufs, span=(0, n.mlp_cols), sem=r.sem_gm, line_sem=r.sem_zgm
    )
    group_o = types.SimpleNamespace(
        **attn_bufs, span=(o_at, o_cols), sem=r.sem_go, line_sem=r.sem_zgo
    )
    group_q = types.SimpleNamespace(**attn_bufs, span=(0, o_at), sem=r.sem_gq, line_sem=r.sem_zgq)

    sum_o, sum_y, sum_x2, sum_x1 = (
        types.SimpleNamespace(part=part, low=low, high=high, sem=sem)
        for part, low, high, sem in (
            (r.p_o, r.l_o, r.r_o, r.sem_o),
            (r.p_y, r.l_y, r.r_y, r.sem_y),
            (r.p_x2, r.l_x2, r.r_x2, r.sem_x2),
            (r.p_x1, r.l_x1, r.r_x1, r.sem_x1),
        )
    )
    r.g1_acc[3] = jnp.zeros_like(r.g1_acc[3])

    me = f * n.ctx + c
    lane = lax.broadcasted_iota(jnp.int32, (1, HEAD_DIM), 1)

    def place(row, at, size, first):
        moved = pltpu.roll(r.gains[...], lax.rem(at + HEAD_DIM - first, HEAD_DIM), 1)
        r.gp[pl.ds(row, 1), :] = jnp.where((lane >= at) & (lane < at + size), moved, 0.0)

    r.gp[...] = jnp.zeros_like(r.gp)
    row, at = me * n.each // HEAD_DIM, lax.rem(me * n.each, HEAD_DIM)
    place(row, at, n.each, 0)
    place(n.lines + row, at, n.each, n.each)
    place(2 * n.lines, me * n.few, n.few, 2 * n.each)
    place(2 * n.lines + 1, me * n.few, n.few, 2 * n.each + n.few)
    small_send(r.gp, r.g0_in, r.sem_g0, "line")
    weights_send(attn_shards, attn_cols, r.wa, r.sem_wa)
    for k in range(PARTS):
        gather_start(r.hidden, r.xb, r.sem_xb, k)
    own_x = pltpu.make_async_copy(r.hidden, r.xb.at[c], r.local_sem.at[7])
    own_x.start()
    own_g = pltpu.make_async_copy(r.cot, r.gb.at[c], r.local_sem.at[8])
    own_g.start()
    own_attn = weights_own(attn_shards, attn_cols, r.wa, 0)
    own_mlp = weights_own(mlp_shards, mlp_cols, r.wm, 4)
    r.g0_acc[0] = small_sum(r.gp, r.g0_in, r.sem_g0, "line")
    small_send(r.g0_acc.at[0], r.g0_in, r.sem_g0, "plane")
    slots = r.order.shape[1]
    slot_len = n.tokens // slots
    exponent = (lane % (HEAD_DIM // 2)).astype(F32) * (2.0 / HEAD_DIM)
    inverse = jnp.exp(-exponent * math.log(1000000.0))
    sign = jnp.where(lane < HEAD_DIM // 2, -1.0, 1.0)
    for j in range(slots):
        first = r.order[0, j] * slot_len
        span = slice(j * slot_len, (j + 1) * slot_len)
        position = first + lax.broadcasted_iota(jnp.int32, (slot_len, HEAD_DIM), 0)
        r.posq[span, :] = position
        angle = position.astype(F32) * inverse
        r.cos[span, :] = jnp.cos(angle)
        r.sin[span, :] = jnp.sin(angle) * sign
    token = lax.broadcasted_iota(jnp.int32, (1, n.tokens), 1)
    posk = token % slot_len
    for j in range(slots):
        posk = posk + jnp.where(token // slot_len == j, r.order[0, j] * slot_len, 0)
    r.posk[...] = posk
    weights_spread(own_attn[:3], attn_cols[:3], r.sem_wa, plane_q)
    weights_spread(own_attn[3:], attn_cols[3:], r.sem_wa, plane_o)
    r.g0_acc[2] = small_sum(r.g0_acc.at[0], r.g0_in, r.sem_g0, "plane")
    for j in range(n.lines):
        r.gv[0, :, j * HEAD_DIM : (j + 1) * HEAD_DIM] = r.g0_acc[2, j : j + 1, :]
        r.gv[1, :, j * HEAD_DIM : (j + 1) * HEAD_DIM] = r.g0_acc[
            2, n.lines + j : n.lines + j + 1, :
        ]
    qgain = r.g0_acc[2, 2 * n.lines : 2 * n.lines + 1, :]
    kgain = r.g0_acc[2, 2 * n.lines + 1 : 2 * n.lines + 2, :]
    attn_gain, mlp_gain = r.gv[0], r.gv[1]
    for by in range(1, n.ctx):
        if by == n.ctx - 1:
            weights_send(mlp_shards, mlp_cols, r.wm, r.sem_wm, "between")
            for k in range(PARTS):
                gather_start(r.cot, r.gb, r.sem_gb, k, "between")
        for k in range(PARTS):
            gather_relay(r.xb, r.sem_xb, by, k)
    own_x.wait()
    own_g.wait()

    def norm_rows(j, carry):
        x = r.xb[j].astype(F32)
        start = pl.multiple_of(j * rows, rows)
        r.xn[pl.ds(start, rows), :] = (x * rms(x) * attn_gain).astype(BF16)
        return carry

    lax.fori_loop(0, n.ctx, norm_rows, 0)
    weights_forward(plane_q)
    weights_wait(plane_q)
    weights_send(mlp_shards, mlp_cols, r.wm, r.sem_wm, "ends")
    for k in range(PARTS):
        gather_start(r.cot, r.gb, r.sem_gb, k, "ends")

    cosine, sine = r.cos, r.sin
    tile = 2 * HEAD_DIM if n.kv % 2 == 0 else HEAD_DIM
    for at in range(0, q_cols + 2 * k_cols, tile):
        product = mm(r.xn[...], r.wa[:, at : at + tile])
        for part in range(tile // HEAD_DIM):
            head = at // HEAD_DIM + part
            u = product[:, part * HEAD_DIM : (part + 1) * HEAD_DIM]
            if head < n.heads:
                r.qp[head] = u
                r.qr[head] = rope_fwd(u * rms(u) * qgain, cosine[...], sine[...]).astype(BF16)
            elif head < n.heads + n.kv:
                r.kp[head - n.heads] = u
                r.kr[head - n.heads] = rope_fwd(u * rms(u) * kgain, cosine[...], sine[...]).astype(
                    BF16
                )
            else:
                r.vv[head - n.heads - n.kv] = u.astype(BF16)
    weights_forward(plane_o)
    half = n.tokens // 2

    def head_forward(h, carry):
        kv = h // group
        for q0 in (0, half):
            s = mm(r.qr[h, q0 : q0 + half, :], r.kr[kv], LAST_AXIS)
            allowed = r.posk[...] <= r.posq[q0 : q0 + half, 0:1]
            e = jnp.where(allowed, jnp.exp(s * factor), 0.0)
            r.es[h, q0 : q0 + half, :] = e
            total = jnp.sum(e, axis=-1, keepdims=True)
            a = mm(e.astype(BF16), r.vv[kv]) / total
            r.af[h, q0 : q0 + half, :] = a
            lane = pl.multiple_of(h * HEAD_DIM, HEAD_DIM)
            r.at[q0 : q0 + half, pl.ds(lane, HEAD_DIM)] = a.astype(BF16)
        return carry

    lax.fori_loop(0, n.heads, head_forward, 0)
    weights_wait(plane_o)

    def by_rows(left, right, out):
        step = 2 * HEAD_DIM
        for at in range(0, d, step):
            product = mm(left[...], right(slice(at, at + step)), LAST_AXIS)
            out[:, :, at : at + step] = product.astype(BF16).reshape(n.ctx, rows, step)

    by_rows(r.at, lambda span: r.wa[span, o_at:], r.p_o)
    for k in range(PARTS):
        scatter_start(sum_o, k)
    weights_spread(own_mlp, mlp_cols, r.sem_wm, plane_m)

    def residual(k):
        span = rows_of(k)
        r.ho[span, :] = r.xb[c, span, :].astype(F32)
        scatter_total(sum_o, r.ho, k)
        own = r.ho[span, :]
        r.mb[c, span, :] = (own * rms(own) * mlp_gain).astype(BF16)
        gather_start(r.mb.at[c], r.mb, r.sem_mb, k)

    gather_relay(r.gb, r.sem_gb, 1, 0)
    scatter_near(sum_o, 0)
    scatter_far(sum_o, 0)
    for by in range(2, n.ctx - 1):
        gather_relay(r.gb, r.sem_gb, by, 0)
    residual(0)
    scatter_near(sum_o, 1)
    gather_relay(r.mb, r.sem_mb, 1, 0, "between")
    scatter_far(sum_o, 1)
    residual(1)
    gather_relay(r.mb, r.sem_mb, 1, 0, "end")
    gather_relay(r.mb, r.sem_mb, 1, 1, "between")
    for by in range(2, n.ctx - 1):
        gather_relay(r.mb, r.sem_mb, by, 0)
    weights_forward(plane_m)
    gather_relay(r.mb, r.sem_mb, n.ctx - 1, 0)
    gather_relay(r.gb, r.sem_gb, n.ctx - 1, 0)
    weights_wait(plane_m)

    tile = 2 * HEAD_DIM if ff % (2 * HEAD_DIM) == 0 else HEAD_DIM
    span_rows = n.ctx * part_rows

    def mlp_part(k):
        span = rows_of(k)
        mixed = r.mb[:, span, :].reshape(span_rows, d)
        upstream = r.gb[:, span, :].reshape(span_rows, d)
        for at in range(0, ff, tile):
            gate = mm(mixed, r.wm[:, at : at + tile])
            up = mm(mixed, r.wm[:, ff + at : ff + at + tile])
            back = mm(upstream, r.wm[:, 2 * ff + at : 2 * ff + at + tile])
            sig = jax.nn.sigmoid(gate)
            swish = gate * sig
            shape = (n.ctx, part_rows, tile)
            r.hid[:, span, at : at + tile] = (swish * up).astype(BF16).reshape(shape)
            r.dgu[:, span, at : at + tile] = (
                (back * up * sig * (1.0 + gate * (1.0 - sig))).astype(BF16).reshape(shape)
            )
            r.dgu[:, span, ff + at : ff + at + tile] = (
                (back * swish).astype(BF16).reshape(shape)
            )
        both = r.dgu[:, span, :].reshape(span_rows, 2 * ff)
        for at in range(0, d, 2 * HEAD_DIM):
            product = mm(both, r.wm[at : at + 2 * HEAD_DIM, : 2 * ff], LAST_AXIS).astype(BF16)
            r.p_x2[:, span, at : at + 2 * HEAD_DIM] = product.reshape(
                n.ctx, part_rows, 2 * HEAD_DIM
            )
        scatter_start(sum_x2, k)

    def residual_back(k):
        span = rows_of(k)
        r.dh[span, :] = jnp.zeros((part_rows, d), F32)
        scatter_total(sum_x2, r.dh, k)
        own = r.ho[span, :]
        from_norm, term = norm_back(own, rms(own), mlp_gain, r.dh[span, :])
        save_lines(n.lines, jnp.sum(term, axis=0, keepdims=True))
        r.dh[span, :] = r.gb[c, span, :].astype(F32) + from_norm
        r.rb[c, span, :] = r.dh[span, :].astype(BF16)
        gather_start(r.rb.at[c], r.rb, r.sem_rb, k)

    mlp_part(0)
    gather_relay(r.mb, r.sem_mb, 1, 1, "end")
    gather_relay(r.gb, r.sem_gb, 1, 1)
    for by in range(2, n.ctx - 1):
        gather_relay(r.gb, r.sem_gb, by, 1)
        gather_relay(r.mb, r.sem_mb, by, 1)
    scatter_near(sum_x2, 0)
    scatter_far(sum_x2, 0)
    gather_relay(r.mb, r.sem_mb, n.ctx - 1, 1)
    gather_relay(r.gb, r.sem_gb, n.ctx - 1, 1)
    mlp_part(1)
    residual_back(0)
    hidden = r.hid[...].reshape(n.tokens, ff)
    by_rows(hidden, lambda span: r.wm[span, 2 * ff :], r.p_y)
    scatter_start(sum_y, 0)
    mixed = r.mb[...].reshape(n.tokens, d)
    upstream = r.gb[...].reshape(n.tokens, d)
    for at in range(0, 2 * ff, tile):
        part = r.dgu[:, :, at : at + tile].reshape(n.tokens, tile)
        r.gm[:, at : at + tile] = mm(mixed, part, FIRST_AXIS).astype(BF16)
    for at in range(0, ff, tile):
        part = r.hid[:, :, at : at + tile].reshape(n.tokens, tile)
        r.gm[:, 2 * ff + at : 2 * ff + at + tile] = mm(upstream, part, FIRST_AXIS).astype(BF16)
    grads_pair(group_m)
    scatter_near(sum_x2, 1)
    gather_relay(r.rb, r.sem_rb, 1, 0, "between")
    grads_plane(group_m)
    scatter_far(sum_x2, 1)
    gather_relay(r.rb, r.sem_rb, 1, 0, "end")
    for by in range(2, n.ctx - 1):
        gather_relay(r.rb, r.sem_rb, by, 0)
    residual_back(1)
    scatter_start(sum_y, 1)
    scatter_near(sum_y, 0)
    gather_relay(r.rb, r.sem_rb, 1, 1, "between")
    gather_relay(r.rb, r.sem_rb, 1, 1, "end")
    for by in range(2, n.ctx - 1):
        gather_relay(r.rb, r.sem_rb, by, 1)
    scatter_far(sum_y, 0)
    for k in range(PARTS):
        gather_relay(r.rb, r.sem_rb, n.ctx - 1, k)

    upstream = r.rb[...].reshape(n.tokens, d)
    for at in range(0, o_cols, HEAD_DIM):
        r.da[at // HEAD_DIM] = mm(upstream, r.wa[:, o_at + at : o_at + at + HEAD_DIM])
    grads_line(group_m)
    scatter_near(sum_y, 1)
    r.dk[...] = jnp.zeros_like(r.dk)
    r.dv[...] = jnp.zeros_like(r.dv)

    def head_backward(h, carry):
        kv = h // group
        for q0 in (0, half):
            span = slice(q0, q0 + half)
            e = r.es[h, span, :]
            total = jnp.sum(e, axis=-1, keepdims=True)
            da = r.da[h, span, :]
            w = (da / total).astype(BF16)
            dl = jnp.sum(da * r.af[h, span, :], axis=-1, keepdims=True) / total
            ds = (e * (mm(w, r.vv[kv], LAST_AXIS) - dl)).astype(BF16)
            r.ds[span, :] = ds
            r.eb[span, :] = e.astype(BF16)
            r.wb[span, :] = w
            r.da[h, span, :] = mm(ds, r.kr[kv])
        r.dk[kv] = r.dk[kv] + mm(r.ds[...], r.qr[h], FIRST_AXIS)
        r.dv[kv] = r.dv[kv] + mm(r.eb[...], r.wb[...], FIRST_AXIS)
        return carry

    lax.fori_loop(0, n.heads, head_backward, 0)

    def query_backward(h, term):
        u = r.qp[h]
        du, gain_term = norm_back(
            u, rms(u), qgain, rope_bwd(r.da[h] * factor, cosine[...], sine[...])
        )
        lane = pl.multiple_of(h * HEAD_DIM, HEAD_DIM)
        r.dqkv[:, pl.ds(lane, HEAD_DIM)] = du.astype(BF16)
        return term + jnp.sum(gain_term, axis=0, keepdims=True)

    q_term = lax.fori_loop(0, n.heads, query_backward, jnp.zeros((1, HEAD_DIM), F32))
    k_term = jnp.zeros((1, HEAD_DIM), F32)
    for kv in range(n.kv):
        u = r.kp[kv]
        du, gain_term = norm_back(
            u, rms(u), kgain, rope_bwd(r.dk[kv] * factor, cosine[...], sine[...])
        )
        at = q_cols + kv * HEAD_DIM
        r.dqkv[:, at : at + HEAD_DIM] = du.astype(BF16)
        at += k_cols
        r.dqkv[:, at : at + HEAD_DIM] = r.dv[kv].astype(BF16)
        k_term = k_term + jnp.sum(gain_term, axis=0, keepdims=True)
    by_rows(r.dqkv, lambda span: r.wa[span, :o_at], r.p_x1)
    for k in range(PARTS):
        scatter_start(sum_x1, k)
    for at in range(0, o_at, 2 * HEAD_DIM):
        r.ga[:, at : at + 2 * HEAD_DIM] = mm(
            r.xn[...], r.dqkv[:, at : at + 2 * HEAD_DIM], FIRST_AXIS
        ).astype(BF16)
    grads_pair(group_q)
    r.ga[:, o_at:] = mm(upstream, r.at[...], FIRST_AXIS).astype(BF16)
    grads_pair(group_o)
    grads_plane(group_q)
    grads_plane(group_o)
    scatter_near(sum_x1, 0)
    scatter_far(sum_y, 1)
    scatter_far(sum_x1, 0)
    scatter_near(sum_x1, 1)
    scatter_far(sum_x1, 1)
    grads_line(group_q)
    grads_line(group_o)
    for k in range(PARTS):
        scatter_total(sum_y, r.ho, k)
    r.out_hidden[...] = r.ho[...].astype(BF16)
    r.out_input[...] = jnp.zeros_like(r.out_input)
    for k in range(PARTS):
        scatter_total(sum_x1, r.out_input, k)
    x = r.xb[c].astype(F32)
    from_norm, term = norm_back(x, rms(x), attn_gain, r.out_input[...])
    save_lines(0, jnp.sum(term, axis=0, keepdims=True))
    r.out_input[...] = r.dh[...] + from_norm
    r.g1_acc[3, 2 * n.lines : 2 * n.lines + 1, :] = q_term
    r.g1_acc[3, 2 * n.lines + 1 : 2 * n.lines + 2, :] = k_term
    small_send(r.g1_acc.at[3], r.g1_in, r.sem_g1, "plane")
    r.g1_acc[1] = small_sum(r.g1_acc.at[3], r.g1_in, r.sem_g1, "plane")
    small_send(r.g1_acc.at[1], r.g1_in, r.sem_g1, "line")
    grads_wait(group_m)
    grads_wait(group_o)
    grads_wait(group_q)
    r.out_gains[...] = small_sum(r.g1_acc.at[1], r.g1_in, r.sem_g1, "line")
    for wait in sends:
        wait()


def fused(
    ctx,
    fsdp,
    hidden_in,
    block_order,
    cotangent,
    q_weight,
    k_weight,
    v_weight,
    o_weight,
    attn_gain,
    query_gain,
    key_gain,
    mlp_gain,
    gate_weight,
    up_weight,
    down_weight,
):
    shards = (q_weight, k_weight, v_weight, o_weight, gate_weight, up_weight, down_weight)
    n = Sizes(ctx, fsdp, hidden_in.shape[1], shards)
    gains = jnp.concatenate([attn_gain, mlp_gain, query_gain, key_gain]).astype(F32)
    gains = jnp.pad(gains, (0, HEAD_DIM - gains.shape[0])).reshape(1, HEAD_DIM)
    hbm, vmem = pl.BlockSpec(memory_space=pl.ANY), pl.BlockSpec(memory_space=pltpu.VMEM)
    inputs = dict(
        hidden=(hidden_in[0], hbm),
        cot=(cotangent[0], hbm),
        wq=(q_weight, hbm),
        wk=(k_weight, hbm),
        wv=(v_weight, hbm),
        wo=(o_weight, hbm),
        wg=(gate_weight, hbm),
        wu=(up_weight, hbm),
        wd=(down_weight, hbm),
        gains=(gains, vmem),
        order=(block_order, pl.BlockSpec(memory_space=pltpu.SMEM)),
    )
    outputs = dict(
        out_hidden=jax.ShapeDtypeStruct((n.rows, n.width), BF16),
        out_input=jax.ShapeDtypeStruct((n.rows, n.width), F32),
        ga_land=jax.ShapeDtypeStruct((ctx, n.shard, n.attn_cols), BF16),
        gm_land=jax.ShapeDtypeStruct((ctx, n.shard, n.mlp_cols), BF16),
        out_gains=jax.ShapeDtypeStruct((n.gain_rows, HEAD_DIM), F32),
    )
    scratch = scratch_of(n)
    landed = pl.pallas_call(
        functools.partial(layer_kernel, n, [*inputs, *outputs, *scratch]),
        out_shape=tuple(outputs.values()),
        in_specs=[spec for _, spec in inputs.values()],
        out_specs=tuple(vmem for _ in outputs),
        scratch_shapes=list(scratch.values()),
        compiler_params=pltpu.CompilerParams(
            collective_id=0, has_side_effects=True, vmem_limit_bytes=VMEM_LIMIT
        ),
        name="layer",
    )(*[value for value, _ in inputs.values()])

    finals = [(n.rows, n.width, BF16), (n.rows, n.width, F32)]
    finals += [(s.shape[0], s.shape[1], F32) for s in shards] + [(8, HEAD_DIM, F32)]
    result, input_grad, oq, ok, ov, oo, og, ou, od, sums = pl.pallas_call(
        functools.partial(emit_kernel, n),
        out_shape=tuple(jax.ShapeDtypeStruct(f[:2], f[2]) for f in finals),
        in_specs=[vmem] * len(outputs),
        out_specs=tuple(vmem for _ in finals),
        name="emit",
    )(*landed)
    return (
        result[None],
        input_grad[None],
        oq,
        ok,
        ov,
        oo,
        sums[0, : n.each],
        sums[2, : n.few],
        sums[3, : n.few],
        sums[1, : n.each],
        og,
        ou,
        od,
    )


def emit_kernel(n, result, input_grad, attn_land, mlp_land, sums, *outs):
    outs[0][...] = result[...]
    outs[1][...] = input_grad[...]
    which = 2
    for land, widths in ((attn_land, n.cols[:4]), (mlp_land, n.cols[4:])):
        at = 0
        for width in widths:
            for j in range(n.ctx):
                outs[which][:, j * width : (j + 1) * width] = land[j, :, at : at + width].astype(
                    F32
                )
            at += width
            which += 1
    me = lax.axis_index("fsdp") * n.ctx + lax.axis_index("ctx")
    row, at = me * n.each // HEAD_DIM, lax.rem(me * n.each, HEAD_DIM)
    sums_out = outs[which]
    sums_out[...] = jnp.zeros_like(sums_out)
    for i, (line, lane) in enumerate(
        (
            (row, at),
            (n.lines + row, at),
            (2 * n.lines, me * n.few),
            (2 * n.lines + 1, me * n.few),
        )
    ):
        back = lax.rem(HEAD_DIM - lane, HEAD_DIM)
        sums_out[i : i + 1, :] = pltpu.roll(sums[pl.ds(line, 1), :], back, 1)


def fits(ctx, fsdp, shard_rows):
    per_tile = HEAD_DIM % (2 * shard_rows) == 0 and HEAD_DIM % (ctx * fsdp) == 0
    return per_tile and shard_rows % 16 == 0 and fsdp % 2 == 0 and KV_HEADS % ctx == 0


def solution(mesh):
    ctx, fsdp = mesh.shape["ctx"], mesh.shape["fsdp"]
    tokens = P("fsdp", "ctx", None)
    matrix = P(("fsdp", "ctx"), None)
    vector = P(("fsdp", "ctx"))
    def step(hidden_in, block_order, cotangent, q_weight, *rest):
        whole = fused if fits(ctx, fsdp, q_weight.shape[0]) else local
        return whole(ctx, fsdp, hidden_in, block_order, cotangent, q_weight, *rest)

    return jax.shard_map(
        step,
        mesh=mesh,
        in_specs=(tokens, P("fsdp", None), tokens)
        + (matrix,) * 4
        + (vector,) * 4
        + (matrix,) * 3,
        out_specs=(tokens,) * 2 + (matrix,) * 4 + (vector,) * 4 + (matrix,) * 3,
        check_vma=False,
    )
```

```python
import functools
import math
import types

import jax
import jax.numpy as jnp
from jax import lax
from jax.experimental import pallas as pl
from jax.experimental.pallas import tpu as pltpu
from jax.sharding import PartitionSpec as P

HEADS = 16
KV_HEADS = 8
HEAD_DIM = 128
EPSILON = 1e-06
FIRST_AXIS = (((0,), (0,)), ((), ()))
LAST_AXIS = (((1,), (1,)), ((), ()))
BF16 = jnp.bfloat16
F32 = jnp.float32
VMEM_LIMIT = 67043328
PARTS = 2
PIECES = 2


def mm(left, right, dims=(((1,), (0,)), ((), ()))):
    return lax.dot_general(left, right, dims, preferred_element_type=F32)


def rms(signal):
    return lax.rsqrt(jnp.mean(signal * signal, axis=-1, keepdims=True) + EPSILON)


def norm_back(signal, inverse_rms, gain_vec, upstream):
    unit_values = signal * inverse_rms
    scaled_up = upstream * gain_vec
    inner = scaled_up - unit_values * jnp.mean(scaled_up * unit_values, axis=-1, keepdims=True)
    return (inverse_rms * inner, upstream * unit_values)


def rope_tables(positions, head_width):
    exponent = jnp.arange(head_width // 2, dtype=F32) * (2.0 / head_width)
    inverse = jnp.exp(-exponent * math.log(1000000.0))
    angles = positions.astype(F32)[:, None] * inverse[None, :]
    angles = jnp.concatenate([angles, angles], axis=-1)
    return (jnp.cos(angles), jnp.sin(angles))


def rotate(signal, cosine, sine):
    half = signal.shape[-1] // 2
    turned = jnp.concatenate([-signal[..., half:], signal[..., :half]], axis=-1)
    return signal * cosine + turned * sine


def rotate_back(upstream, cosine, sine):
    half = upstream.shape[-1] // 2
    scaled_up = upstream * sine
    return upstream * cosine + jnp.concatenate(
        [scaled_up[..., half:], -scaled_up[..., :half]], axis=-1
    )


def gather_columns(ctx, shards):
    rows = shards[0].shape[0]
    cut = [s.reshape(rows, ctx, s.shape[1] // ctx).transpose(1, 0, 2) for s in shards]
    widths = [c.shape[2] for c in cut]
    both = jnp.concatenate(cut, axis=2)
    both = lax.all_to_all(both, "ctx", 0, 0, tiled=True)
    both = both.reshape(ctx * rows, -1)
    whole = lax.all_gather(both, "fsdp", axis=0, tiled=True)
    out, at = [], 0
    for width in widths:
        out.append(whole[:, at : at + width])
        at += width
    return out


def scatter_grads(ctx, fsdp, grads):
    rows = grads[0].shape[0] // (ctx * fsdp)
    widths = [g.shape[1] for g in grads]
    both = jnp.concatenate([g.astype(BF16) for g in grads], axis=1)
    both = lax.psum_scatter(both, "fsdp", scatter_dimension=0, tiled=True)
    both = lax.all_to_all(both.reshape(ctx, rows, -1), "ctx", 0, 0, tiled=True)
    out, at = [], 0
    for width in widths:
        piece = both[:, :, at : at + width]
        out.append(piece.transpose(1, 0, 2).reshape(rows, ctx * width).astype(F32))
        at += width
    return out


def ctx_gather(rows):
    return lax.all_gather(rows, "ctx", axis=0, tiled=True)


def ctx_scatter(partial):
    return lax.psum_scatter(partial.astype(BF16), "ctx", scatter_dimension=0, tiled=True).astype(
        F32
    )


def local(
    ctx,
    fsdp,
    hidden_in,
    block_order,
    cotangent,
    q_weight,
    k_weight,
    v_weight,
    o_weight,
    attn_gain,
    query_gain,
    key_gain,
    mlp_gain,
    gate_weight,
    up_weight,
    down_weight,
):
    inputs = hidden_in[0].astype(F32)
    row_count = inputs.shape[0]
    tokens = row_count * ctx
    slots = block_order.shape[1]
    block_len = tokens // slots
    heads, kv_heads = HEADS // ctx, KV_HEADS // ctx
    group = heads // kv_heads
    factor = 1.0 / math.sqrt(HEAD_DIM)
    positions = (
        block_order[0][:, None] * block_len + jnp.arange(block_len, dtype=jnp.int32)[None, :]
    ).reshape(-1)
    cosine, sine = rope_tables(positions, HEAD_DIM)
    cosine, sine = cosine[:, None, :], sine[:, None, :]

    both = ("fsdp", "ctx")
    norm_gain, qgain, kgain, mlp_norm_gain = (
        lax.all_gather(g, both, axis=0, tiled=True).astype(F32)
        for g in (attn_gain, query_gain, key_gain, mlp_gain)
    )
    norm_scale = rms(inputs)
    normed = ctx_gather((inputs * norm_scale * norm_gain).astype(BF16))
    upstream = ctx_gather(cotangent[0])
    q_full, k_full, v_full, o_full = gather_columns(ctx, (q_weight, k_weight, v_weight, o_weight))
    gate_full, up_full, down_full = gather_columns(ctx, (gate_weight, up_weight, down_weight))

    query_proj = mm(normed, q_full).reshape(tokens, heads, HEAD_DIM)
    key_proj = mm(normed, k_full).reshape(tokens, kv_heads, HEAD_DIM)
    value_low = mm(normed, v_full).astype(BF16).reshape(tokens, kv_heads, HEAD_DIM)
    query_scale, key_scale = rms(query_proj), rms(key_proj)
    query_low = (
        rotate(query_proj * query_scale * qgain, cosine, sine)
        .astype(BF16)
        .reshape(tokens, kv_heads, group, HEAD_DIM)
    )
    key_low = rotate(key_proj * key_scale * kgain, cosine, sine).astype(BF16)
    scores = jnp.einsum("rkgd,nkd->kgrn", query_low, key_low, preferred_element_type=F32) * factor
    allowed = positions[None, :] <= positions[:, None]
    weights_exp = jnp.where(allowed, jnp.exp(scores), 0.0)
    denominator = jnp.sum(weights_exp, axis=-1)
    weights_low = weights_exp.astype(BF16)
    numerator = jnp.einsum("kgrn,nkd->rkgd", weights_low, value_low, preferred_element_type=F32)
    denom_rows = jnp.transpose(denominator, (2, 0, 1))[..., None]
    attn_full = numerator / denom_rows
    attn_low = attn_full.astype(BF16).reshape(tokens, heads * HEAD_DIM)
    residual = inputs + ctx_scatter(mm(attn_low, o_full, LAST_AXIS))

    mix_scale = rms(residual)
    mixed = ctx_gather((residual * mix_scale * mlp_norm_gain).astype(BF16))
    gate_val = mm(mixed, gate_full)
    up_val = mm(mixed, up_full)
    sigmoid_gate = jax.nn.sigmoid(gate_val)
    swish_gate = gate_val * sigmoid_gate
    hidden_low = (swish_gate * up_val).astype(BF16)
    result = residual + ctx_scatter(mm(hidden_low, down_full, LAST_AXIS))
    hidden_grad = mm(upstream, down_full)
    gate_back = (
        hidden_grad * up_val * sigmoid_gate * (1.0 + gate_val * (1.0 - sigmoid_gate))
    ).astype(BF16)
    up_back = (hidden_grad * swish_gate).astype(BF16)
    mixed_grad = ctx_scatter(mm(gate_back, gate_full, LAST_AXIS) + mm(up_back, up_full, LAST_AXIS))
    resid_from_norm, mlp_gain_term = norm_back(residual, mix_scale, mlp_norm_gain, mixed_grad)
    residual_grad = cotangent[0].astype(F32) + resid_from_norm
    mlp_grads = scatter_grads(
        ctx,
        fsdp,
        (
            mm(mixed, gate_back, FIRST_AXIS),
            mm(mixed, up_back, FIRST_AXIS),
            mm(upstream, hidden_low, FIRST_AXIS),
        ),
    )
    resid_low = ctx_gather(residual_grad.astype(BF16))

    attn_grad = mm(resid_low, o_full).reshape(tokens, kv_heads, group, HEAD_DIM)
    share_low = (attn_grad / denom_rows).astype(BF16)
    denom_grad = jnp.transpose(jnp.sum(attn_grad * attn_full, axis=-1), (1, 2, 0)) / denominator
    weight_grad = jnp.einsum("rkgd,nkd->kgrn", share_low, value_low, preferred_element_type=F32)
    score_low = (weights_exp * (weight_grad - denom_grad[..., None])).astype(BF16)
    query_rot = (
        jnp.einsum("kgrn,nkd->rkgd", score_low, key_low, preferred_element_type=F32) * factor
    ).reshape(tokens, heads, HEAD_DIM)
    key_rot = (
        jnp.einsum("kgrn,rkgd->nkd", score_low, query_low, preferred_element_type=F32) * factor
    )
    value_back = (
        jnp.einsum("kgrn,rkgd->nkd", weights_low, share_low, preferred_element_type=F32)
        .reshape(tokens, kv_heads * HEAD_DIM)
        .astype(BF16)
    )
    query_grad, query_term = norm_back(
        query_proj, query_scale, qgain, rotate_back(query_rot, cosine, sine)
    )
    key_grad, key_term = norm_back(key_proj, key_scale, kgain, rotate_back(key_rot, cosine, sine))
    query_back = query_grad.reshape(tokens, heads * HEAD_DIM).astype(BF16)
    key_back = key_grad.reshape(tokens, kv_heads * HEAD_DIM).astype(BF16)
    normed_grad = ctx_scatter(
        mm(query_back, q_full, LAST_AXIS)
        + mm(key_back, k_full, LAST_AXIS)
        + mm(value_back, v_full, LAST_AXIS)
    )
    input_from_norm, attn_gain_term = norm_back(inputs, norm_scale, norm_gain, normed_grad)
    input_grad = residual_grad + input_from_norm
    attn_grads = scatter_grads(
        ctx,
        fsdp,
        (
            mm(normed, query_back, FIRST_AXIS),
            mm(normed, key_back, FIRST_AXIS),
            mm(normed, value_back, FIRST_AXIS),
            mm(resid_low, attn_low, FIRST_AXIS),
        ),
    )
    gains = (
        jnp.sum(attn_gain_term, axis=0),
        jnp.sum(query_term, axis=(0, 1)),
        jnp.sum(key_term, axis=(0, 1)),
        jnp.sum(mlp_gain_term, axis=0),
    )
    gains = [lax.psum_scatter(g, both, scatter_dimension=0, tiled=True) for g in gains]
    return (
        result.astype(BF16)[None],
        input_grad[None],
        *attn_grads,
        *gains,
        *mlp_grads,
    )


def rope_fwd(u, cosine, sine):
    return u * cosine + pltpu.roll(u, HEAD_DIM // 2, u.ndim - 1) * sine


def rope_bwd(du, cosine, sine):
    return du * cosine - pltpu.roll(du, HEAD_DIM // 2, du.ndim - 1) * sine


class Sizes:
    def __init__(self, ctx, fsdp, rows, shards):
        self.ctx, self.fsdp, self.rows = ctx, fsdp, rows
        self.chips = fsdp // 2
        self.shard = shards[0].shape[0]
        self.block = self.shard * ctx
        self.width = self.block * fsdp
        self.tokens = rows * ctx
        self.heads, self.kv = HEADS // ctx, KV_HEADS // ctx
        self.cols = [s.shape[1] // ctx for s in shards]
        self.attn_cols = sum(self.cols[:4])
        self.mlp_cols = sum(self.cols[4:])
        self.lines = self.width // HEAD_DIM
        self.gain_rows = 8 * ((2 * self.lines + 2 + 7) // 8)
        self.each, self.few = self.width // (ctx * fsdp), HEAD_DIM // (ctx * fsdp)


def scratch_of(n):
    bf, f32 = (lambda *s: pltpu.VMEM(s, BF16)), (lambda *s: pltpu.VMEM(s, F32))
    sem = lambda *s: pltpu.SemaphoreType.DMA(s)
    c, d, s, h, kv = n.ctx, n.width, n.tokens, n.heads, n.kv
    ff = n.cols[4]
    out = dict(
        wa=bf(d, n.attn_cols),
        wm=bf(d, n.mlp_cols),
        xb=bf(c, n.rows, d),
        gb=bf(c, n.rows, d),
        mb=bf(c, n.rows, d),
        rb=bf(c, n.rows, d),
        xn=bf(s, d),
        qp=f32(h, s, HEAD_DIM),
        kp=f32(kv, s, HEAD_DIM),
        qr=bf(h, s, HEAD_DIM),
        kr=bf(kv, s, HEAD_DIM),
        vv=bf(kv, s, HEAD_DIM),
        es=f32(h, s, s),
        af=f32(h, s, HEAD_DIM),
        at=bf(s, h * HEAD_DIM),
        da=f32(h, s, HEAD_DIM),
        dk=f32(kv, s, HEAD_DIM),
        dv=f32(kv, s, HEAD_DIM),
        ds=bf(s, s),
        eb=bf(s, s),
        wb=bf(s, HEAD_DIM),
        dqkv=bf(s, (h + 2 * kv) * HEAD_DIM),
        hid=bf(c, n.rows, ff),
        dgu=bf(c, n.rows, 2 * ff),
        ho=f32(n.rows, d),
        dh=f32(n.rows, d),
        gv=f32(2, 1, d),
        gp=f32(n.gain_rows, HEAD_DIM),
        cos=f32(s, HEAD_DIM),
        sin=f32(s, HEAD_DIM),
        posq=pltpu.VMEM((s, HEAD_DIM), jnp.int32),
        posk=pltpu.VMEM((1, s), jnp.int32),
        ga=bf(d, n.attn_cols),
        gm=bf(d, n.mlp_cols),
        ga_sib=bf(n.chips, n.block, n.attn_cols),
        gm_sib=bf(n.chips, n.block, n.mlp_cols),
        ga_in=bf(n.chips - 1, n.block, n.attn_cols),
        gm_in=bf(n.chips - 1, n.block, n.mlp_cols),
        ga_z=bf(n.block, n.attn_cols),
        gm_z=bf(n.block, n.mlp_cols),
        local_sem=sem(9),
    )
    for name in ("o", "y", "x2", "x1"):
        out["p_" + name] = bf(c, n.rows, d)
        out["l_" + name] = bf(c, n.rows, d)
        out["r_" + name] = bf(c, n.rows, d)
        out["snd_" + name] = sem(2, c - 1)
        out["rcv_" + name] = sem(2, c - 1, PARTS * PIECES)
    for name in ("xb", "gb", "mb", "rb"):
        out["snd_" + name] = sem(2, c - 1)
        out["rcv_" + name] = sem(c, PARTS * PIECES)
    out["snd_w"] = sem(2, c - 1)
    out["rcv_w"] = sem(3, c - 1)
    for name in ("pq", "po", "pm"):
        out["sem_" + name] = sem(3 + n.chips)
    for name in ("gm", "go", "gq"):
        out["sem_" + name] = sem(5 + n.chips)
    for name in ("g0", "g1"):
        out[name + "_in"] = f32(n.fsdp + c, n.gain_rows, HEAD_DIM)
        out[name + "_acc"] = f32(4, n.gain_rows, HEAD_DIM)
        out["sem_" + name] = sem(4)
    return out


def layer_kernel(n, names, *refs):
    r = types.SimpleNamespace(**dict(zip(names, refs)))
    for name in ("o", "y", "x2", "x1", "xb", "gb", "mb", "rb"):
        setattr(r, "sem_" + name, (getattr(r, "snd_" + name), getattr(r, "rcv_" + name)))
    c, f = lax.axis_index("ctx"), lax.axis_index("fsdp")
    chip, core = f // 2, f % 2
    sibling = chip * 2 + 1 - core
    rows, d, block, shard = n.rows, n.width, n.block, n.shard
    sends = []

    def ahead(by):
        return lax.rem(c + by, n.ctx)

    def behind(by):
        return lax.rem(c + n.ctx - by, n.ctx)

    def chip_ahead(by):
        return lax.rem(chip + by, n.chips)

    def chip_behind(by):
        return lax.rem(chip + n.chips - by, n.chips)

    def remote(src, dst, send_sem, recv_sem, to_f=None, to_c=None):
        return pltpu.make_async_remote_copy(
            src_ref=src,
            dst_ref=dst,
            send_sem=send_sem,
            recv_sem=recv_sem,
            device_id={"fsdp": f if to_f is None else to_f, "ctx": c if to_c is None else to_c},
            device_id_type=pl.DeviceIdType.MESH,
        )

    def send(src, dst, send_sem, recv_sem, to_f=None, to_c=None):
        remote(src, dst, send_sem, recv_sem, to_f, to_c).start()

    def sent(like, send_sem, cond=None):
        wait = remote(like, like, send_sem, send_sem).wait_send
        sends.append(wait if cond is None else (lambda: pl.when(cond)(wait)))

    def arrived(dst, recv_sem):
        remote(dst, dst, recv_sem, recv_sem).wait_recv()

    def send_if(cond, src, dst, send_sem, recv_sem, to_c):
        pl.when(cond)(remote(src, dst, send_sem, recv_sem, None, to_c).start)

    barrier = pltpu.get_barrier_semaphore()

    def greet(to_f, to_c):
        pl.semaphore_signal(
            barrier,
            inc=1,
            device_id={"fsdp": to_f, "ctx": to_c},
            device_id_type=pl.DeviceIdType.MESH,
        )

    for by in range(1, n.ctx):
        greet(f, ahead(by))
    for by in range(1, n.fsdp):
        greet(lax.rem(f + by, n.fsdp), c)
    pl.semaphore_wait(barrier, n.ctx - 1 + n.fsdp - 1)

    right, left = jnp.minimum(c + 1, n.ctx - 1), jnp.maximum(c - 1, 0)
    part_rows, piece_rows = rows // PARTS, rows // (PARTS * PIECES)

    def pieces_of(k):
        return range(k * PIECES, (k + 1) * PIECES)

    def part_of(buf, j, i):
        return buf.at[j, pl.ds(i * piece_rows, piece_rows), :]

    def gather_start(src, buf, sem, k, to=None):
        for i in pieces_of(k):
            gather_piece(src, buf, sem, i, to)

    def gather_piece(src, buf, sem, i, to=None):
        piece = src.at[pl.ds(i * piece_rows, piece_rows), :]
        here = part_of(buf, c, i)
        up, down = c + 1 < n.ctx, c > 0
        if to == "between":
            up, down = c + 1 < n.ctx - 1, c > 1
        elif to == "ends":
            up, down = c + 1 == n.ctx - 1, c == 1
        send_if(up, piece, here, sem[0].at[0, 0], sem[1].at[c, i], right)
        send_if(down, piece, here, sem[0].at[1, 0], sem[1].at[c, i], left)

    def gather_relay(buf, sem, by, k, source=None):
        low, high = jnp.maximum(c - by, 0), jnp.minimum(c + by, n.ctx - 1)
        from_low, from_high = c - by >= 0, c + by < n.ctx
        if source == "end":
            from_low, from_high = c == by, c + by == n.ctx - 1
        elif source == "between":
            from_low, from_high = c > by, c + by < n.ctx - 1
        for i in pieces_of(k):
            piece, here = part_of(buf, low, i), sem[1].at[low, i]
            pl.when(from_low)(functools.partial(arrived, piece, here))
            send_if(from_low & (c + 1 < n.ctx), piece, piece, sem[0].at[0, by], here, right)
            piece, here = part_of(buf, high, i), sem[1].at[high, i]
            pl.when(from_high)(functools.partial(arrived, piece, here))
            send_if(from_high & (c > 0), piece, piece, sem[0].at[1, by], here, left)

    def gather_sent(buf, sem):
        for by in range(n.ctx - 1):
            sent(buf.at[0], sem[0].at[0, by], (c - by >= 0) & (c + 1 < n.ctx))
            sent(buf.at[0], sem[0].at[1, by], (c + by < n.ctx) & (c > 0))

    def rows_of(k):
        return slice(k * part_rows, (k + 1) * part_rows)

    def scatter_send(cond, part, there, sem, target, i, way, to_c):
        send_if(
            cond,
            part_of(part, target, i),
            part_of(there, target, i),
            sem[0].at[way, target - 1 + way],
            sem[1].at[way, target - 1 + way, i],
            to_c,
        )

    def scatter_add(part, there, sem, target, i, way):
        arrived(part_of(there, target, i), sem[1].at[way, target - 1 + way, i])
        span = slice(i * piece_rows, (i + 1) * piece_rows)
        part[target, span, :] = (
            part[target, span, :].astype(F32) + there[target, span, :].astype(F32)
        ).astype(BF16)

    def scatter_start(g, k):
        for step in range(n.ctx - 1):
            for i in pieces_of(k):
                scatter_send(c == n.ctx - 1, g.part, g.high, g.sem, step, i, 1, left)
                scatter_send(c == 0, g.part, g.low, g.sem, n.ctx - 1 - step, i, 0, right)

    def scatter_up(g, step, k, cond):
        target = n.ctx - 1 - step
        cond = cond & (c < target) & (c > 0)
        for i in pieces_of(k):
            pl.when(cond)(functools.partial(scatter_add, g.part, g.low, g.sem, target, i, 0))
            scatter_send(cond, g.part, g.low, g.sem, target, i, 0, right)

    def scatter_down(g, step, k, cond):
        cond = cond & (c > step) & (c + 1 < n.ctx)
        for i in pieces_of(k):
            pl.when(cond)(functools.partial(scatter_add, g.part, g.high, g.sem, step, i, 1))
            scatter_send(cond, g.part, g.high, g.sem, step, i, 1, left)

    def scatter_near(g, k):
        for step in range(n.ctx - 1):
            scatter_up(g, step, k, c < n.ctx // 2)
            scatter_down(g, step, k, c >= n.ctx // 2)

    def scatter_far(g, k):
        for step in range(n.ctx - 1):
            scatter_up(g, step, k, c >= n.ctx // 2)
            scatter_down(g, step, k, c < n.ctx // 2)

    def scatter_sent(g):
        for target in range(1, n.ctx):
            sent(g.part.at[0], g.sem[0].at[0, target - 1], c < target)
        for target in range(n.ctx - 1):
            sent(g.part.at[0], g.sem[0].at[1, target], c > target)

    def scatter_total(g, out, k):
        span = rows_of(k)
        out[span, :] = out[span, :] + g.part[c, span, :].astype(F32)

        @pl.when(c > 0)
        def _():
            for i in pieces_of(k):
                arrived(part_of(g.low, c, i), g.sem[1].at[0, jnp.maximum(c - 1, 0), i])
            out[span, :] = out[span, :] + g.low[c, span, :].astype(F32)

        @pl.when(c + 1 < n.ctx)
        def _():
            for i in pieces_of(k):
                arrived(part_of(g.high, c, i), g.sem[1].at[1, jnp.minimum(c, n.ctx - 2), i])
            out[span, :] = out[span, :] + g.high[c, span, :].astype(F32)

    def block_of(buf, index, span):
        return buf.at[pl.ds(pl.multiple_of(index * block, block), block), pl.ds(*span)]

    def blocks_of(buf, count, span):
        return buf.at[pl.ds(0, count * block), pl.ds(*span)]

    def piece_of(buf, line, at, width):
        start = pl.multiple_of(f * block + line * shard, shard)
        return buf.at[pl.ds(start, shard), pl.ds(at, width)]

    def weights_send(shards, cols, buf, send_sem, recv_sems, now=None):
        for by in range(1, n.ctx):
            at_end = (ahead(by) == 0) | (ahead(by) == n.ctx - 1)
            at = 0
            for src, width, recv_sem in zip(shards, cols, recv_sems):
                column = pl.multiple_of(ahead(by) * width, HEAD_DIM)
                copy = remote(
                    src.at[:, pl.ds(column, width)],
                    piece_of(buf, c, at, width),
                    send_sem.at[by - 1],
                    recv_sem.at[by - 1],
                    None,
                    ahead(by),
                )
                if now is None:
                    copy.start()
                else:
                    pl.when(at_end if now == "ends" else ~at_end)(copy.start)
                at += width

    def weights_sent(cols, buf, send_sem):
        for by in range(1, n.ctx):
            sent(piece_of(buf, c, 0, sum(cols)), send_sem.at[by - 1])

    def weights_own(shards, cols, buf, first):
        at, out = 0, []
        for i, (src, width) in enumerate(zip(shards, cols)):
            column = pl.multiple_of(c * width, HEAD_DIM)
            copy = pltpu.make_async_copy(
                src.at[:, pl.ds(column, width)],
                piece_of(buf, c, at, width),
                r.local_sem.at[first + i],
            )
            copy.start()
            out.append(copy)
            at += width
        return out

    def weights_spread(own, g):
        for copy in own:
            copy.wait()
        for by in range(1, n.ctx):
            arrived(piece_of(g.buf, behind(by), *g.span), g.line.at[by - 1])
        mine = block_of(g.buf, f, g.span)
        for by in range(1, n.chips):
            send(mine, mine, g.sem.at[0], g.sem.at[2 + by], chip_ahead(by) * 2 + core)
        send(mine, mine, g.sem.at[1], g.sem.at[2], sibling)

    def weights_forward(g):
        for by in range(1, n.chips):
            piece = block_of(g.buf, chip_behind(by) * 2 + core, g.span)
            arrived(piece, g.sem.at[2 + by])
            send(piece, piece, g.sem.at[1], g.sem.at[2], sibling)
        sent(blocks_of(g.buf, n.chips - 1, g.span), g.sem.at[0])
        sent(blocks_of(g.buf, n.chips, g.span), g.sem.at[1])

    def weights_wait(g):
        arrived(blocks_of(g.buf, n.chips, g.span), g.sem.at[2])

    def share_of(buf, index, span):
        return buf.at[pl.ds(pl.multiple_of(index * block, block), block), pl.ds(*span)]

    def grads_pair(g):
        for by in (*range(1, n.chips), 0):
            send(
                share_of(g.whole, chip_ahead(by) * 2 + 1 - core, g.span),
                g.pair.at[by, :, pl.ds(*g.span)],
                g.sem.at[0],
                g.sem.at[5 + by],
                sibling,
            )
        sent(g.pair.at[:, :, pl.ds(*g.span)], g.sem.at[0])

    def grads_plane(g):
        for by in range(1, n.chips):
            theirs = g.pair.at[by, :, pl.ds(*g.span)]
            arrived(theirs, g.sem.at[5 + by])
            piece = share_of(g.whole, chip_ahead(by) * 2 + core, g.span)
            piece[...] = (piece[...].astype(F32) + theirs[...].astype(F32)).astype(BF16)
            send(
                piece,
                g.plane.at[by - 1, :, pl.ds(*g.span)],
                g.sem.at[1],
                g.sem.at[2],
                chip_ahead(by) * 2 + core,
            )
        sent(g.plane.at[:, :, pl.ds(*g.span)], g.sem.at[1])

    def grads_line(g):
        theirs = g.pair.at[0, :, pl.ds(*g.span)]
        arrived(theirs, g.sem.at[5])
        acc = share_of(g.whole, f, g.span)[...].astype(F32) + theirs[...].astype(F32)
        arrived(g.plane.at[:, :, pl.ds(*g.span)], g.sem.at[2])
        for by in range(1, n.chips):
            acc = acc + g.plane[by - 1, :, pl.ds(*g.span)].astype(F32)
        g.total[:, pl.ds(*g.span)] = acc.astype(BF16)
        for by in range(1, n.ctx):
            start = pl.multiple_of(ahead(by) * shard, shard)
            send(
                g.total.at[pl.ds(start, shard), pl.ds(*g.span)],
                g.land.at[c, :, pl.ds(*g.span)],
                g.sem.at[3],
                g.sem.at[4],
                None,
                ahead(by),
            )
        sent(g.land.at[pl.ds(0, n.ctx - 1), :, pl.ds(*g.span)], g.sem.at[3])
        start = pl.multiple_of(c * shard, shard)
        g.land[c, :, pl.ds(*g.span)] = g.total[pl.ds(start, shard), pl.ds(*g.span)]

    def grads_wait(g):
        arrived(g.land.at[pl.ds(0, n.ctx - 1), :, pl.ds(*g.span)], g.sem.at[4])

    def small_peers(way):
        if way == "line":
            return [(n.fsdp + by - 1, f, ahead(by)) for by in range(1, n.ctx)]
        return [(by - 1, lax.rem(f + by, n.fsdp), c) for by in range(1, n.fsdp)]

    def small_span(incoming, way):
        first, count = (n.fsdp, n.ctx - 1) if way == "line" else (0, n.fsdp - 1)
        return incoming.at[pl.ds(first, count)]

    def small_send(src, incoming, sem, way):
        at = 2 * (way == "line")
        for slot, to_f, to_c in small_peers(way):
            send(src, incoming.at[slot], sem.at[at], sem.at[at + 1], to_f, to_c)
        sent(small_span(incoming, way), sem.at[at])

    def small_sum(own, incoming, sem, way):
        total = own[...]
        arrived(small_span(incoming, way), sem.at[2 * (way == "line") + 1])
        for slot, _, _ in small_peers(way):
            total = total + incoming[slot]
        return total

    def save_lines(first, line):
        for j in range(n.lines):
            row = slice(first + j, first + j + 1)
            r.g1_acc[3, row, :] += line[:, j * HEAD_DIM : (j + 1) * HEAD_DIM]

    attn_shards, mlp_shards = (r.wq, r.wk, r.wv, r.wo), (r.wg, r.wu, r.wd)
    attn_cols, mlp_cols = n.cols[:4], n.cols[4:]
    q_cols, k_cols, _, o_cols = attn_cols
    ff = mlp_cols[0]
    group = n.heads // n.kv
    factor = 1.0 / math.sqrt(HEAD_DIM)

    o_at = q_cols + 2 * k_cols
    attn_bufs = dict(whole=r.ga, pair=r.ga_sib, plane=r.ga_in, total=r.ga_z, land=r.ga_land)
    mlp_bufs = dict(whole=r.gm, pair=r.gm_sib, plane=r.gm_in, total=r.gm_z, land=r.gm_land)
    line_q, line_o, line_m = (r.rcv_w.at[i] for i in range(3))
    plane_q = types.SimpleNamespace(buf=r.wa, span=(0, o_at), line=line_q, sem=r.sem_pq)
    plane_o = types.SimpleNamespace(buf=r.wa, span=(o_at, o_cols), line=line_o, sem=r.sem_po)
    plane_m = types.SimpleNamespace(buf=r.wm, span=(0, n.mlp_cols), line=line_m, sem=r.sem_pm)
    to_attn = (r.wa, r.snd_w.at[0], (line_q, line_q, line_q, line_o))
    to_mlp = (r.wm, r.snd_w.at[1], (line_m, line_m, line_m))
    group_m = types.SimpleNamespace(
        **mlp_bufs, span=(0, n.mlp_cols), sem=r.sem_gm
    )
    group_o = types.SimpleNamespace(
        **attn_bufs, span=(o_at, o_cols), sem=r.sem_go
    )
    group_q = types.SimpleNamespace(**attn_bufs, span=(0, o_at), sem=r.sem_gq)

    sum_o, sum_y, sum_x2, sum_x1 = (
        types.SimpleNamespace(part=part, low=low, high=high, sem=sem)
        for part, low, high, sem in (
            (r.p_o, r.l_o, r.r_o, r.sem_o),
            (r.p_y, r.l_y, r.r_y, r.sem_y),
            (r.p_x2, r.l_x2, r.r_x2, r.sem_x2),
            (r.p_x1, r.l_x1, r.r_x1, r.sem_x1),
        )
    )
    r.g1_acc[3] = jnp.zeros_like(r.g1_acc[3])

    me = f * n.ctx + c
    lane = lax.broadcasted_iota(jnp.int32, (1, HEAD_DIM), 1)

    def place(row, at, size, first):
        moved = pltpu.roll(r.gains[...], lax.rem(at + HEAD_DIM - first, HEAD_DIM), 1)
        r.gp[pl.ds(row, 1), :] = jnp.where((lane >= at) & (lane < at + size), moved, 0.0)

    r.gp[...] = jnp.zeros_like(r.gp)
    row, at = me * n.each // HEAD_DIM, lax.rem(me * n.each, HEAD_DIM)
    place(row, at, n.each, 0)
    place(n.lines + row, at, n.each, n.each)
    place(2 * n.lines, me * n.few, n.few, 2 * n.each)
    place(2 * n.lines + 1, me * n.few, n.few, 2 * n.each + n.few)
    small_send(r.gp, r.g0_in, r.sem_g0, "line")
    weights_send(attn_shards, attn_cols, *to_attn)
    for k in range(PARTS):
        gather_start(r.hidden, r.xb, r.sem_xb, k)
    own_x = pltpu.make_async_copy(r.hidden, r.xb.at[c], r.local_sem.at[7])
    own_x.start()
    own_g = pltpu.make_async_copy(r.cot, r.gb.at[c], r.local_sem.at[8])
    own_g.start()
    own_attn = weights_own(attn_shards, attn_cols, r.wa, 0)
    own_mlp = weights_own(mlp_shards, mlp_cols, r.wm, 4)
    r.g0_acc[0] = small_sum(r.gp, r.g0_in, r.sem_g0, "line")
    small_send(r.g0_acc.at[0], r.g0_in, r.sem_g0, "plane")
    slots = r.order.shape[1]
    slot_len = n.tokens // slots
    exponent = (lane % (HEAD_DIM // 2)).astype(F32) * (2.0 / HEAD_DIM)
    inverse = jnp.exp(-exponent * math.log(1000000.0))
    sign = jnp.where(lane < HEAD_DIM // 2, -1.0, 1.0)
    for j in range(slots):
        first = r.order[0, j] * slot_len
        span = slice(j * slot_len, (j + 1) * slot_len)
        position = first + lax.broadcasted_iota(jnp.int32, (slot_len, HEAD_DIM), 0)
        r.posq[span, :] = position
        angle = position.astype(F32) * inverse
        r.cos[span, :] = jnp.cos(angle)
        r.sin[span, :] = jnp.sin(angle) * sign
    token = lax.broadcasted_iota(jnp.int32, (1, n.tokens), 1)
    posk = token % slot_len
    for j in range(slots):
        posk = posk + jnp.where(token // slot_len == j, r.order[0, j] * slot_len, 0)
    r.posk[...] = posk
    weights_spread(own_attn[:3], plane_q)
    weights_spread(own_attn[3:], plane_o)
    r.g0_acc[2] = small_sum(r.g0_acc.at[0], r.g0_in, r.sem_g0, "plane")
    for j in range(n.lines):
        r.gv[0, :, j * HEAD_DIM : (j + 1) * HEAD_DIM] = r.g0_acc[2, j : j + 1, :]
        r.gv[1, :, j * HEAD_DIM : (j + 1) * HEAD_DIM] = r.g0_acc[
            2, n.lines + j : n.lines + j + 1, :
        ]
    qgain = r.g0_acc[2, 2 * n.lines : 2 * n.lines + 1, :]
    kgain = r.g0_acc[2, 2 * n.lines + 1 : 2 * n.lines + 2, :]
    attn_gain, mlp_gain = r.gv[0], r.gv[1]
    for by in range(1, n.ctx):
        if by == n.ctx - 1:
            weights_send(mlp_shards, mlp_cols, *to_mlp, "between")
            for k in range(PARTS):
                gather_start(r.cot, r.gb, r.sem_gb, k, "between")
        for k in range(PARTS):
            gather_relay(r.xb, r.sem_xb, by, k)
    own_x.wait()
    own_g.wait()

    def norm_rows(j, carry):
        x = r.xb[j].astype(F32)
        start = pl.multiple_of(j * rows, rows)
        r.xn[pl.ds(start, rows), :] = (x * rms(x) * attn_gain).astype(BF16)
        return carry

    lax.fori_loop(0, n.ctx, norm_rows, 0)
    weights_forward(plane_q)
    weights_wait(plane_q)
    weights_send(mlp_shards, mlp_cols, *to_mlp, "ends")
    for k in range(PARTS):
        gather_start(r.cot, r.gb, r.sem_gb, k, "ends")

    cosine, sine = r.cos, r.sin
    tile = 2 * HEAD_DIM if n.kv % 2 == 0 else HEAD_DIM
    for at in range(0, q_cols + 2 * k_cols, tile):
        product = mm(r.xn[...], r.wa[:, at : at + tile])
        for part in range(tile // HEAD_DIM):
            head = at // HEAD_DIM + part
            u = product[:, part * HEAD_DIM : (part + 1) * HEAD_DIM]
            if head < n.heads:
                r.qp[head] = u
                r.qr[head] = rope_fwd(u * rms(u) * qgain, cosine[...], sine[...]).astype(BF16)
            elif head < n.heads + n.kv:
                r.kp[head - n.heads] = u
                r.kr[head - n.heads] = rope_fwd(u * rms(u) * kgain, cosine[...], sine[...]).astype(
                    BF16
                )
            else:
                r.vv[head - n.heads - n.kv] = u.astype(BF16)
    weights_forward(plane_o)
    half = n.tokens // 2

    def head_forward(h, carry):
        kv = h // group
        for q0 in (0, half):
            s = mm(r.qr[h, q0 : q0 + half, :], r.kr[kv], LAST_AXIS)
            allowed = r.posk[...] <= r.posq[q0 : q0 + half, 0:1]
            e = jnp.where(allowed, jnp.exp(s * factor), 0.0)
            r.es[h, q0 : q0 + half, :] = e
            total = jnp.sum(e, axis=-1, keepdims=True)
            a = mm(e.astype(BF16), r.vv[kv]) / total
            r.af[h, q0 : q0 + half, :] = a
            lane = pl.multiple_of(h * HEAD_DIM, HEAD_DIM)
            r.at[q0 : q0 + half, pl.ds(lane, HEAD_DIM)] = a.astype(BF16)
        return carry

    lax.fori_loop(0, n.heads, head_forward, 0)
    weights_wait(plane_o)

    def by_rows(left, right, out):
        step = 2 * HEAD_DIM
        for at in range(0, d, step):
            product = mm(left[...], right(slice(at, at + step)), LAST_AXIS)
            out[:, :, at : at + step] = product.astype(BF16).reshape(n.ctx, rows, step)

    by_rows(r.at, lambda span: r.wa[span, o_at:], r.p_o)
    for k in range(PARTS):
        scatter_start(sum_o, k)
    weights_spread(own_mlp, plane_m)

    def residual(k):
        span = rows_of(k)
        r.ho[span, :] = r.xb[c, span, :].astype(F32)
        scatter_total(sum_o, r.ho, k)
        own = r.ho[span, :]
        r.mb[c, span, :] = (own * rms(own) * mlp_gain).astype(BF16)
        gather_start(r.mb.at[c], r.mb, r.sem_mb, k)

    gather_relay(r.gb, r.sem_gb, 1, 0)
    scatter_near(sum_o, 0)
    scatter_far(sum_o, 0)
    for by in range(2, n.ctx - 1):
        gather_relay(r.gb, r.sem_gb, by, 0)
    residual(0)
    scatter_near(sum_o, 1)
    gather_relay(r.mb, r.sem_mb, 1, 0, "between")
    scatter_far(sum_o, 1)
    residual(1)
    gather_relay(r.mb, r.sem_mb, 1, 0, "end")
    gather_relay(r.mb, r.sem_mb, 1, 1, "between")
    for by in range(2, n.ctx - 1):
        gather_relay(r.mb, r.sem_mb, by, 0)
    weights_forward(plane_m)
    gather_relay(r.mb, r.sem_mb, n.ctx - 1, 0)
    gather_relay(r.gb, r.sem_gb, n.ctx - 1, 0)
    weights_wait(plane_m)

    tile = 2 * HEAD_DIM if ff % (2 * HEAD_DIM) == 0 else HEAD_DIM
    span_rows = n.ctx * part_rows

    def mlp_part(k):
        span = rows_of(k)
        mixed = r.mb[:, span, :].reshape(span_rows, d)
        upstream = r.gb[:, span, :].reshape(span_rows, d)
        for at in range(0, ff, tile):
            gate = mm(mixed, r.wm[:, at : at + tile])
            up = mm(mixed, r.wm[:, ff + at : ff + at + tile])
            back = mm(upstream, r.wm[:, 2 * ff + at : 2 * ff + at + tile])
            sig = jax.nn.sigmoid(gate)
            swish = gate * sig
            shape = (n.ctx, part_rows, tile)
            r.hid[:, span, at : at + tile] = (swish * up).astype(BF16).reshape(shape)
            r.dgu[:, span, at : at + tile] = (
                (back * up * sig * (1.0 + gate * (1.0 - sig))).astype(BF16).reshape(shape)
            )
            r.dgu[:, span, ff + at : ff + at + tile] = (
                (back * swish).astype(BF16).reshape(shape)
            )
        both = r.dgu[:, span, :].reshape(span_rows, 2 * ff)
        for at in range(0, d, 2 * HEAD_DIM):
            product = mm(both, r.wm[at : at + 2 * HEAD_DIM, : 2 * ff], LAST_AXIS).astype(BF16)
            r.p_x2[:, span, at : at + 2 * HEAD_DIM] = product.reshape(
                n.ctx, part_rows, 2 * HEAD_DIM
            )
        scatter_start(sum_x2, k)

    def residual_back(k):
        span = rows_of(k)
        r.dh[span, :] = jnp.zeros((part_rows, d), F32)
        scatter_total(sum_x2, r.dh, k)
        own = r.ho[span, :]
        from_norm, term = norm_back(own, rms(own), mlp_gain, r.dh[span, :])
        save_lines(n.lines, jnp.sum(term, axis=0, keepdims=True))
        r.dh[span, :] = r.gb[c, span, :].astype(F32) + from_norm
        r.rb[c, span, :] = r.dh[span, :].astype(BF16)
        gather_start(r.rb.at[c], r.rb, r.sem_rb, k)

    mlp_part(0)
    gather_relay(r.mb, r.sem_mb, 1, 1, "end")
    gather_relay(r.gb, r.sem_gb, 1, 1)
    for by in range(2, n.ctx - 1):
        gather_relay(r.gb, r.sem_gb, by, 1)
        gather_relay(r.mb, r.sem_mb, by, 1)
    scatter_near(sum_x2, 0)
    scatter_far(sum_x2, 0)
    gather_relay(r.mb, r.sem_mb, n.ctx - 1, 1)
    gather_relay(r.gb, r.sem_gb, n.ctx - 1, 1)
    mlp_part(1)
    residual_back(0)
    hidden = r.hid[...].reshape(n.tokens, ff)
    by_rows(hidden, lambda span: r.wm[span, 2 * ff :], r.p_y)
    scatter_start(sum_y, 0)
    mixed = r.mb[...].reshape(n.tokens, d)
    upstream = r.gb[...].reshape(n.tokens, d)
    for at in range(0, 2 * ff, tile):
        part = r.dgu[:, :, at : at + tile].reshape(n.tokens, tile)
        r.gm[:, at : at + tile] = mm(mixed, part, FIRST_AXIS).astype(BF16)
    for at in range(0, ff, tile):
        part = r.hid[:, :, at : at + tile].reshape(n.tokens, tile)
        r.gm[:, 2 * ff + at : 2 * ff + at + tile] = mm(upstream, part, FIRST_AXIS).astype(BF16)
    grads_pair(group_m)
    scatter_near(sum_x2, 1)
    gather_relay(r.rb, r.sem_rb, 1, 0, "between")
    grads_plane(group_m)
    scatter_far(sum_x2, 1)
    gather_relay(r.rb, r.sem_rb, 1, 0, "end")
    for by in range(2, n.ctx - 1):
        gather_relay(r.rb, r.sem_rb, by, 0)
    residual_back(1)
    scatter_start(sum_y, 1)
    scatter_near(sum_y, 0)
    gather_relay(r.rb, r.sem_rb, 1, 1, "between")
    gather_relay(r.rb, r.sem_rb, 1, 1, "end")
    for by in range(2, n.ctx - 1):
        gather_relay(r.rb, r.sem_rb, by, 1)
    scatter_far(sum_y, 0)
    for k in range(PARTS):
        gather_relay(r.rb, r.sem_rb, n.ctx - 1, k)

    upstream = r.rb[...].reshape(n.tokens, d)
    for at in range(0, o_cols, HEAD_DIM):
        r.da[at // HEAD_DIM] = mm(upstream, r.wa[:, o_at + at : o_at + at + HEAD_DIM])
    grads_line(group_m)
    scatter_near(sum_y, 1)
    r.dk[...] = jnp.zeros_like(r.dk)
    r.dv[...] = jnp.zeros_like(r.dv)

    def head_backward(h, carry):
        kv = h // group
        for q0 in (0, half):
            span = slice(q0, q0 + half)
            e = r.es[h, span, :]
            total = jnp.sum(e, axis=-1, keepdims=True)
            da = r.da[h, span, :]
            w = (da / total).astype(BF16)
            dl = jnp.sum(da * r.af[h, span, :], axis=-1, keepdims=True) / total
            ds = (e * (mm(w, r.vv[kv], LAST_AXIS) - dl)).astype(BF16)
            r.ds[span, :] = ds
            r.eb[span, :] = e.astype(BF16)
            r.wb[span, :] = w
            r.da[h, span, :] = mm(ds, r.kr[kv])
        r.dk[kv] = r.dk[kv] + mm(r.ds[...], r.qr[h], FIRST_AXIS)
        r.dv[kv] = r.dv[kv] + mm(r.eb[...], r.wb[...], FIRST_AXIS)
        return carry

    lax.fori_loop(0, n.heads, head_backward, 0)

    def query_backward(h, term):
        u = r.qp[h]
        du, gain_term = norm_back(
            u, rms(u), qgain, rope_bwd(r.da[h] * factor, cosine[...], sine[...])
        )
        lane = pl.multiple_of(h * HEAD_DIM, HEAD_DIM)
        r.dqkv[:, pl.ds(lane, HEAD_DIM)] = du.astype(BF16)
        return term + jnp.sum(gain_term, axis=0, keepdims=True)

    q_term = lax.fori_loop(0, n.heads, query_backward, jnp.zeros((1, HEAD_DIM), F32))
    k_term = jnp.zeros((1, HEAD_DIM), F32)
    for kv in range(n.kv):
        u = r.kp[kv]
        du, gain_term = norm_back(
            u, rms(u), kgain, rope_bwd(r.dk[kv] * factor, cosine[...], sine[...])
        )
        at = q_cols + kv * HEAD_DIM
        r.dqkv[:, at : at + HEAD_DIM] = du.astype(BF16)
        at += k_cols
        r.dqkv[:, at : at + HEAD_DIM] = r.dv[kv].astype(BF16)
        k_term = k_term + jnp.sum(gain_term, axis=0, keepdims=True)
    by_rows(r.dqkv, lambda span: r.wa[span, :o_at], r.p_x1)
    for k in range(PARTS):
        scatter_start(sum_x1, k)
    for at in range(0, o_at, 2 * HEAD_DIM):
        r.ga[:, at : at + 2 * HEAD_DIM] = mm(
            r.xn[...], r.dqkv[:, at : at + 2 * HEAD_DIM], FIRST_AXIS
        ).astype(BF16)
    grads_pair(group_q)
    r.ga[:, o_at:] = mm(upstream, r.at[...], FIRST_AXIS).astype(BF16)
    grads_pair(group_o)
    grads_plane(group_q)
    grads_plane(group_o)
    scatter_near(sum_x1, 0)
    scatter_far(sum_y, 1)
    scatter_far(sum_x1, 0)
    scatter_near(sum_x1, 1)
    scatter_far(sum_x1, 1)
    grads_line(group_q)
    grads_line(group_o)
    for k in range(PARTS):
        scatter_total(sum_y, r.ho, k)
    r.out_hidden[...] = r.ho[...].astype(BF16)
    r.out_input[...] = jnp.zeros_like(r.out_input)
    for k in range(PARTS):
        scatter_total(sum_x1, r.out_input, k)
    x = r.xb[c].astype(F32)
    from_norm, term = norm_back(x, rms(x), attn_gain, r.out_input[...])
    save_lines(0, jnp.sum(term, axis=0, keepdims=True))
    r.out_input[...] = r.dh[...] + from_norm
    r.g1_acc[3, 2 * n.lines : 2 * n.lines + 1, :] = q_term
    r.g1_acc[3, 2 * n.lines + 1 : 2 * n.lines + 2, :] = k_term
    small_send(r.g1_acc.at[3], r.g1_in, r.sem_g1, "plane")
    r.g1_acc[1] = small_sum(r.g1_acc.at[3], r.g1_in, r.sem_g1, "plane")
    small_send(r.g1_acc.at[1], r.g1_in, r.sem_g1, "line")
    grads_wait(group_m)
    grads_wait(group_o)
    grads_wait(group_q)
    r.out_gains[...] = small_sum(r.g1_acc.at[1], r.g1_in, r.sem_g1, "line")
    for buf, sem in ((r.xb, r.sem_xb), (r.gb, r.sem_gb), (r.mb, r.sem_mb), (r.rb, r.sem_rb)):
        gather_sent(buf, sem)
    for g in (sum_o, sum_y, sum_x2, sum_x1):
        scatter_sent(g)
    weights_sent(attn_cols, *to_attn[:2])
    weights_sent(mlp_cols, *to_mlp[:2])
    for wait in sends:
        wait()


def fused(
    ctx,
    fsdp,
    hidden_in,
    block_order,
    cotangent,
    q_weight,
    k_weight,
    v_weight,
    o_weight,
    attn_gain,
    query_gain,
    key_gain,
    mlp_gain,
    gate_weight,
    up_weight,
    down_weight,
):
    shards = (q_weight, k_weight, v_weight, o_weight, gate_weight, up_weight, down_weight)
    n = Sizes(ctx, fsdp, hidden_in.shape[1], shards)
    gains = jnp.concatenate([attn_gain, mlp_gain, query_gain, key_gain]).astype(F32)
    gains = jnp.pad(gains, (0, HEAD_DIM - gains.shape[0])).reshape(1, HEAD_DIM)
    hbm, vmem = pl.BlockSpec(memory_space=pl.ANY), pl.BlockSpec(memory_space=pltpu.VMEM)
    inputs = dict(
        hidden=(hidden_in[0], hbm),
        cot=(cotangent[0], hbm),
        wq=(q_weight, hbm),
        wk=(k_weight, hbm),
        wv=(v_weight, hbm),
        wo=(o_weight, hbm),
        wg=(gate_weight, hbm),
        wu=(up_weight, hbm),
        wd=(down_weight, hbm),
        gains=(gains, vmem),
        order=(block_order, pl.BlockSpec(memory_space=pltpu.SMEM)),
    )
    outputs = dict(
        out_hidden=jax.ShapeDtypeStruct((n.rows, n.width), BF16),
        out_input=jax.ShapeDtypeStruct((n.rows, n.width), F32),
        ga_land=jax.ShapeDtypeStruct((ctx, n.shard, n.attn_cols), BF16),
        gm_land=jax.ShapeDtypeStruct((ctx, n.shard, n.mlp_cols), BF16),
        out_gains=jax.ShapeDtypeStruct((n.gain_rows, HEAD_DIM), F32),
    )
    scratch = scratch_of(n)
    landed = pl.pallas_call(
        functools.partial(layer_kernel, n, [*inputs, *outputs, *scratch]),
        out_shape=tuple(outputs.values()),
        in_specs=[spec for _, spec in inputs.values()],
        out_specs=tuple(vmem for _ in outputs),
        scratch_shapes=list(scratch.values()),
        compiler_params=pltpu.CompilerParams(
            collective_id=0, has_side_effects=True, vmem_limit_bytes=VMEM_LIMIT
        ),
        name="layer",
    )(*[value for value, _ in inputs.values()])

    finals = [(n.rows, n.width, BF16), (n.rows, n.width, F32)]
    finals += [(s.shape[0], s.shape[1], F32) for s in shards] + [(8, HEAD_DIM, F32)]
    result, input_grad, oq, ok, ov, oo, og, ou, od, sums = pl.pallas_call(
        functools.partial(emit_kernel, n),
        out_shape=tuple(jax.ShapeDtypeStruct(f[:2], f[2]) for f in finals),
        in_specs=[vmem] * len(outputs),
        out_specs=tuple(vmem for _ in finals),
        name="emit",
    )(*landed)
    return (
        result[None],
        input_grad[None],
        oq,
        ok,
        ov,
        oo,
        sums[0, : n.each],
        sums[2, : n.few],
        sums[3, : n.few],
        sums[1, : n.each],
        og,
        ou,
        od,
    )


def emit_kernel(n, result, input_grad, attn_land, mlp_land, sums, *outs):
    outs[0][...] = result[...]
    outs[1][...] = input_grad[...]
    which = 2
    for land, widths in ((attn_land, n.cols[:4]), (mlp_land, n.cols[4:])):
        at = 0
        for width in widths:
            for j in range(n.ctx):
                outs[which][:, j * width : (j + 1) * width] = land[j, :, at : at + width].astype(
                    F32
                )
            at += width
            which += 1
    me = lax.axis_index("fsdp") * n.ctx + lax.axis_index("ctx")
    row, at = me * n.each // HEAD_DIM, lax.rem(me * n.each, HEAD_DIM)
    sums_out = outs[which]
    sums_out[...] = jnp.zeros_like(sums_out)
    for i, (line, lane) in enumerate(
        (
            (row, at),
            (n.lines + row, at),
            (2 * n.lines, me * n.few),
            (2 * n.lines + 1, me * n.few),
        )
    ):
        back = lax.rem(HEAD_DIM - lane, HEAD_DIM)
        sums_out[i : i + 1, :] = pltpu.roll(sums[pl.ds(line, 1), :], back, 1)


def fits(ctx, fsdp, shard_rows):
    per_tile = HEAD_DIM % (2 * shard_rows) == 0 and HEAD_DIM % (ctx * fsdp) == 0
    return per_tile and shard_rows % 16 == 0 and fsdp % 2 == 0 and KV_HEADS % ctx == 0


def solution(mesh):
    ctx, fsdp = mesh.shape["ctx"], mesh.shape["fsdp"]
    tokens = P("fsdp", "ctx", None)
    matrix = P(("fsdp", "ctx"), None)
    vector = P(("fsdp", "ctx"))
    def step(hidden_in, block_order, cotangent, q_weight, *rest):
        whole = fused if fits(ctx, fsdp, q_weight.shape[0]) else local
        return whole(ctx, fsdp, hidden_in, block_order, cotangent, q_weight, *rest)

    return jax.shard_map(
        step,
        mesh=mesh,
        in_specs=(tokens, P("fsdp", None), tokens)
        + (matrix,) * 4
        + (vector,) * 4
        + (matrix,) * 3,
        out_specs=(tokens,) * 2 + (matrix,) * 4 + (vector,) * 4 + (matrix,) * 3,
        check_vma=False,
    )
```

```python
import functools
import math
import types

import jax
import jax.numpy as jnp
from jax import lax
from jax.experimental import pallas as pl
from jax.experimental.pallas import tpu as pltpu
from jax.sharding import PartitionSpec as P

HEADS = 16
KV_HEADS = 8
HEAD_DIM = 128
EPSILON = 1e-06
FIRST_AXIS = (((0,), (0,)), ((), ()))
LAST_AXIS = (((1,), (1,)), ((), ()))
BF16 = jnp.bfloat16
F32 = jnp.float32
VMEM_LIMIT = 67043328
PARTS = 2
PIECES = 2


def mm(left, right, dims=(((1,), (0,)), ((), ()))):
    return lax.dot_general(left, right, dims, preferred_element_type=F32)


def rms(signal):
    return lax.rsqrt(jnp.mean(signal * signal, axis=-1, keepdims=True) + EPSILON)


def norm_back(signal, inverse_rms, gain_vec, upstream):
    unit_values = signal * inverse_rms
    scaled_up = upstream * gain_vec
    inner = scaled_up - unit_values * jnp.mean(scaled_up * unit_values, axis=-1, keepdims=True)
    return (inverse_rms * inner, upstream * unit_values)


def rope_tables(positions, head_width):
    exponent = jnp.arange(head_width // 2, dtype=F32) * (2.0 / head_width)
    inverse = jnp.exp(-exponent * math.log(1000000.0))
    angles = positions.astype(F32)[:, None] * inverse[None, :]
    angles = jnp.concatenate([angles, angles], axis=-1)
    return (jnp.cos(angles), jnp.sin(angles))


def rotate(signal, cosine, sine):
    half = signal.shape[-1] // 2
    turned = jnp.concatenate([-signal[..., half:], signal[..., :half]], axis=-1)
    return signal * cosine + turned * sine


def rotate_back(upstream, cosine, sine):
    half = upstream.shape[-1] // 2
    scaled_up = upstream * sine
    return upstream * cosine + jnp.concatenate(
        [scaled_up[..., half:], -scaled_up[..., :half]], axis=-1
    )


def gather_columns(ctx, shards):
    rows = shards[0].shape[0]
    cut = [s.reshape(rows, ctx, s.shape[1] // ctx).transpose(1, 0, 2) for s in shards]
    widths = [c.shape[2] for c in cut]
    both = jnp.concatenate(cut, axis=2)
    both = lax.all_to_all(both, "ctx", 0, 0, tiled=True)
    both = both.reshape(ctx * rows, -1)
    whole = lax.all_gather(both, "fsdp", axis=0, tiled=True)
    out, at = [], 0
    for width in widths:
        out.append(whole[:, at : at + width])
        at += width
    return out


def scatter_grads(ctx, fsdp, grads):
    rows = grads[0].shape[0] // (ctx * fsdp)
    widths = [g.shape[1] for g in grads]
    both = jnp.concatenate([g.astype(BF16) for g in grads], axis=1)
    both = lax.psum_scatter(both, "fsdp", scatter_dimension=0, tiled=True)
    both = lax.all_to_all(both.reshape(ctx, rows, -1), "ctx", 0, 0, tiled=True)
    out, at = [], 0
    for width in widths:
        piece = both[:, :, at : at + width]
        out.append(piece.transpose(1, 0, 2).reshape(rows, ctx * width).astype(F32))
        at += width
    return out


def ctx_gather(rows):
    return lax.all_gather(rows, "ctx", axis=0, tiled=True)


def ctx_scatter(partial):
    return lax.psum_scatter(partial.astype(BF16), "ctx", scatter_dimension=0, tiled=True).astype(
        F32
    )


def local(
    ctx,
    fsdp,
    hidden_in,
    block_order,
    cotangent,
    q_weight,
    k_weight,
    v_weight,
    o_weight,
    attn_gain,
    query_gain,
    key_gain,
    mlp_gain,
    gate_weight,
    up_weight,
    down_weight,
):
    inputs = hidden_in[0].astype(F32)
    row_count = inputs.shape[0]
    tokens = row_count * ctx
    slots = block_order.shape[1]
    block_len = tokens // slots
    heads, kv_heads = HEADS // ctx, KV_HEADS // ctx
    group = heads // kv_heads
    factor = 1.0 / math.sqrt(HEAD_DIM)
    positions = (
        block_order[0][:, None] * block_len + jnp.arange(block_len, dtype=jnp.int32)[None, :]
    ).reshape(-1)
    cosine, sine = rope_tables(positions, HEAD_DIM)
    cosine, sine = cosine[:, None, :], sine[:, None, :]

    both = ("fsdp", "ctx")
    norm_gain, qgain, kgain, mlp_norm_gain = (
        lax.all_gather(g, both, axis=0, tiled=True).astype(F32)
        for g in (attn_gain, query_gain, key_gain, mlp_gain)
    )
    norm_scale = rms(inputs)
    normed = ctx_gather((inputs * norm_scale * norm_gain).astype(BF16))
    upstream = ctx_gather(cotangent[0])
    q_full, k_full, v_full, o_full = gather_columns(ctx, (q_weight, k_weight, v_weight, o_weight))
    gate_full, up_full, down_full = gather_columns(ctx, (gate_weight, up_weight, down_weight))

    query_proj = mm(normed, q_full).reshape(tokens, heads, HEAD_DIM)
    key_proj = mm(normed, k_full).reshape(tokens, kv_heads, HEAD_DIM)
    value_low = mm(normed, v_full).astype(BF16).reshape(tokens, kv_heads, HEAD_DIM)
    query_scale, key_scale = rms(query_proj), rms(key_proj)
    query_low = (
        rotate(query_proj * query_scale * qgain, cosine, sine)
        .astype(BF16)
        .reshape(tokens, kv_heads, group, HEAD_DIM)
    )
    key_low = rotate(key_proj * key_scale * kgain, cosine, sine).astype(BF16)
    scores = jnp.einsum("rkgd,nkd->kgrn", query_low, key_low, preferred_element_type=F32) * factor
    allowed = positions[None, :] <= positions[:, None]
    weights_exp = jnp.where(allowed, jnp.exp(scores), 0.0)
    denominator = jnp.sum(weights_exp, axis=-1)
    weights_low = weights_exp.astype(BF16)
    numerator = jnp.einsum("kgrn,nkd->rkgd", weights_low, value_low, preferred_element_type=F32)
    denom_rows = jnp.transpose(denominator, (2, 0, 1))[..., None]
    attn_full = numerator / denom_rows
    attn_low = attn_full.astype(BF16).reshape(tokens, heads * HEAD_DIM)
    residual = inputs + ctx_scatter(mm(attn_low, o_full, LAST_AXIS))

    mix_scale = rms(residual)
    mixed = ctx_gather((residual * mix_scale * mlp_norm_gain).astype(BF16))
    gate_val = mm(mixed, gate_full)
    up_val = mm(mixed, up_full)
    sigmoid_gate = jax.nn.sigmoid(gate_val)
    swish_gate = gate_val * sigmoid_gate
    hidden_low = (swish_gate * up_val).astype(BF16)
    result = residual + ctx_scatter(mm(hidden_low, down_full, LAST_AXIS))
    hidden_grad = mm(upstream, down_full)
    gate_back = (
        hidden_grad * up_val * sigmoid_gate * (1.0 + gate_val * (1.0 - sigmoid_gate))
    ).astype(BF16)
    up_back = (hidden_grad * swish_gate).astype(BF16)
    mixed_grad = ctx_scatter(mm(gate_back, gate_full, LAST_AXIS) + mm(up_back, up_full, LAST_AXIS))
    resid_from_norm, mlp_gain_term = norm_back(residual, mix_scale, mlp_norm_gain, mixed_grad)
    residual_grad = cotangent[0].astype(F32) + resid_from_norm
    mlp_grads = scatter_grads(
        ctx,
        fsdp,
        (
            mm(mixed, gate_back, FIRST_AXIS),
            mm(mixed, up_back, FIRST_AXIS),
            mm(upstream, hidden_low, FIRST_AXIS),
        ),
    )
    resid_low = ctx_gather(residual_grad.astype(BF16))

    attn_grad = mm(resid_low, o_full).reshape(tokens, kv_heads, group, HEAD_DIM)
    share_low = (attn_grad / denom_rows).astype(BF16)
    denom_grad = jnp.transpose(jnp.sum(attn_grad * attn_full, axis=-1), (1, 2, 0)) / denominator
    weight_grad = jnp.einsum("rkgd,nkd->kgrn", share_low, value_low, preferred_element_type=F32)
    score_low = (weights_exp * (weight_grad - denom_grad[..., None])).astype(BF16)
    query_rot = (
        jnp.einsum("kgrn,nkd->rkgd", score_low, key_low, preferred_element_type=F32) * factor
    ).reshape(tokens, heads, HEAD_DIM)
    key_rot = (
        jnp.einsum("kgrn,rkgd->nkd", score_low, query_low, preferred_element_type=F32) * factor
    )
    value_back = (
        jnp.einsum("kgrn,rkgd->nkd", weights_low, share_low, preferred_element_type=F32)
        .reshape(tokens, kv_heads * HEAD_DIM)
        .astype(BF16)
    )
    query_grad, query_term = norm_back(
        query_proj, query_scale, qgain, rotate_back(query_rot, cosine, sine)
    )
    key_grad, key_term = norm_back(key_proj, key_scale, kgain, rotate_back(key_rot, cosine, sine))
    query_back = query_grad.reshape(tokens, heads * HEAD_DIM).astype(BF16)
    key_back = key_grad.reshape(tokens, kv_heads * HEAD_DIM).astype(BF16)
    normed_grad = ctx_scatter(
        mm(query_back, q_full, LAST_AXIS)
        + mm(key_back, k_full, LAST_AXIS)
        + mm(value_back, v_full, LAST_AXIS)
    )
    input_from_norm, attn_gain_term = norm_back(inputs, norm_scale, norm_gain, normed_grad)
    input_grad = residual_grad + input_from_norm
    attn_grads = scatter_grads(
        ctx,
        fsdp,
        (
            mm(normed, query_back, FIRST_AXIS),
            mm(normed, key_back, FIRST_AXIS),
            mm(normed, value_back, FIRST_AXIS),
            mm(resid_low, attn_low, FIRST_AXIS),
        ),
    )
    gains = (
        jnp.sum(attn_gain_term, axis=0),
        jnp.sum(query_term, axis=(0, 1)),
        jnp.sum(key_term, axis=(0, 1)),
        jnp.sum(mlp_gain_term, axis=0),
    )
    gains = [lax.psum_scatter(g, both, scatter_dimension=0, tiled=True) for g in gains]
    return (
        result.astype(BF16)[None],
        input_grad[None],
        *attn_grads,
        *gains,
        *mlp_grads,
    )


def rope_fwd(u, cosine, sine):
    return u * cosine + pltpu.roll(u, HEAD_DIM // 2, u.ndim - 1) * sine


def rope_bwd(du, cosine, sine):
    return du * cosine - pltpu.roll(du, HEAD_DIM // 2, du.ndim - 1) * sine


class Sizes:
    def __init__(self, ctx, fsdp, rows, shards):
        self.ctx, self.fsdp, self.rows = ctx, fsdp, rows
        self.chips = fsdp // 2
        self.shard = shards[0].shape[0]
        self.block = self.shard * ctx
        self.width = self.block * fsdp
        self.tokens = rows * ctx
        self.heads, self.kv = HEADS // ctx, KV_HEADS // ctx
        self.cols = [s.shape[1] // ctx for s in shards]
        self.attn_cols = sum(self.cols[:4])
        self.mlp_cols = sum(self.cols[4:])
        self.lines = self.width // HEAD_DIM
        self.gain_rows = 8 * ((2 * self.lines + 2 + 7) // 8)
        self.each, self.few = self.width // (ctx * fsdp), HEAD_DIM // (ctx * fsdp)


def scratch_of(n):
    bf, f32 = (lambda *s: pltpu.VMEM(s, BF16)), (lambda *s: pltpu.VMEM(s, F32))
    sem = lambda *s: pltpu.SemaphoreType.DMA(s)
    c, d, s, h, kv = n.ctx, n.width, n.tokens, n.heads, n.kv
    ff = n.cols[4]
    out = dict(
        wa=bf(d, n.attn_cols),
        wm=bf(d, n.mlp_cols),
        xb=bf(c, n.rows, d),
        gb=bf(c, n.rows, d),
        mb=bf(c, n.rows, d),
        rb=bf(c, n.rows, d),
        xn=bf(s, d),
        qp=f32(h, s, HEAD_DIM),
        kp=f32(kv, s, HEAD_DIM),
        qr=bf(h, s, HEAD_DIM),
        kr=bf(kv, s, HEAD_DIM),
        vv=bf(kv, s, HEAD_DIM),
        es=f32(h, s, s),
        af=f32(h, s, HEAD_DIM),
        at=bf(s, h * HEAD_DIM),
        da=f32(h, s, HEAD_DIM),
        dk=f32(kv, s, HEAD_DIM),
        dv=f32(kv, s, HEAD_DIM),
        ds=bf(s, s),
        eb=bf(s, s),
        wb=bf(s, HEAD_DIM),
        dqkv=bf(s, (h + 2 * kv) * HEAD_DIM),
        hid=bf(c, n.rows, ff),
        dgu=bf(c, n.rows, 2 * ff),
        ho=f32(n.rows, d),
        dh=f32(n.rows, d),
        gv=f32(2, 1, d),
        gp=f32(n.gain_rows, HEAD_DIM),
        cos=f32(s, HEAD_DIM),
        sin=f32(s, HEAD_DIM),
        posq=pltpu.VMEM((s, HEAD_DIM), jnp.int32),
        posk=pltpu.VMEM((1, s), jnp.int32),
        ga=bf(d, n.attn_cols),
        gm=bf(d, n.mlp_cols),
        ga_sib=bf(n.chips, n.block, n.attn_cols),
        gm_sib=bf(n.chips, n.block, n.mlp_cols),
        ga_in=bf(n.chips - 1, n.block, n.attn_cols),
        gm_in=bf(n.chips - 1, n.block, n.mlp_cols),
        ga_z=bf(n.block, n.attn_cols),
        gm_z=bf(n.block, n.mlp_cols),
        local_sem=sem(9),
    )
    for name in ("o", "y", "x2", "x1"):
        out["p_" + name] = bf(c, n.rows, d)
        out["l_" + name] = bf(c, n.rows, d)
        out["r_" + name] = bf(c, n.rows, d)
        out["snd_" + name] = sem(2, c - 1)
        out["rcv_" + name] = sem(2, c - 1, PARTS * PIECES)
    for name in ("xb", "gb", "mb", "rb"):
        out["snd_" + name] = sem(2, c - 1)
        out["rcv_" + name] = sem(c, PARTS * PIECES)
    out["snd_w"] = sem(2, c - 1)
    out["rcv_w"] = sem(3, c - 1)
    for name in ("pq", "po", "pm"):
        out["sem_" + name] = sem(3 + n.chips)
    for name in ("gm", "go", "gq"):
        out["sem_" + name] = sem(5 + n.chips)
    for name in ("g0", "g1"):
        out[name + "_in"] = f32(n.fsdp + c, n.gain_rows, HEAD_DIM)
        out[name + "_acc"] = f32(4, n.gain_rows, HEAD_DIM)
        out["sem_" + name] = sem(4)
    return out


def layer_kernel(n, names, *refs):
    r = types.SimpleNamespace(**dict(zip(names, refs)))
    for name in ("o", "y", "x2", "x1", "xb", "gb", "mb", "rb"):
        setattr(r, "sem_" + name, (getattr(r, "snd_" + name), getattr(r, "rcv_" + name)))
    c, f = lax.axis_index("ctx"), lax.axis_index("fsdp")
    chip, core = f // 2, f % 2
    sibling = chip * 2 + 1 - core
    rows, d, block, shard = n.rows, n.width, n.block, n.shard
    sends = []

    def ahead(by):
        return lax.rem(c + by, n.ctx)

    def behind(by):
        return lax.rem(c + n.ctx - by, n.ctx)

    def chip_ahead(by):
        return lax.rem(chip + by, n.chips)

    def chip_behind(by):
        return lax.rem(chip + n.chips - by, n.chips)

    def remote(src, dst, send_sem, recv_sem, to_f=None, to_c=None):
        return pltpu.make_async_remote_copy(
            src_ref=src,
            dst_ref=dst,
            send_sem=send_sem,
            recv_sem=recv_sem,
            device_id={"fsdp": f if to_f is None else to_f, "ctx": c if to_c is None else to_c},
            device_id_type=pl.DeviceIdType.MESH,
        )

    def send(src, dst, send_sem, recv_sem, to_f=None, to_c=None):
        remote(src, dst, send_sem, recv_sem, to_f, to_c).start()

    def sent(like, send_sem, cond=None):
        wait = remote(like, like, send_sem, send_sem).wait_send
        sends.append(wait if cond is None else (lambda: pl.when(cond)(wait)))

    def arrived(dst, recv_sem):
        remote(dst, dst, recv_sem, recv_sem).wait_recv()

    def send_if(cond, src, dst, send_sem, recv_sem, to_c):
        pl.when(cond)(remote(src, dst, send_sem, recv_sem, None, to_c).start)

    barrier = pltpu.get_barrier_semaphore()

    def greet(to_f, to_c):
        pl.semaphore_signal(
            barrier,
            inc=1,
            device_id={"fsdp": to_f, "ctx": to_c},
            device_id_type=pl.DeviceIdType.MESH,
        )

    for by in range(1, n.ctx):
        greet(f, ahead(by))
    for by in range(1, n.fsdp):
        greet(lax.rem(f + by, n.fsdp), c)
    pl.semaphore_wait(barrier, n.ctx - 1 + n.fsdp - 1)

    right, left = jnp.minimum(c + 1, n.ctx - 1), jnp.maximum(c - 1, 0)
    part_rows, piece_rows = rows // PARTS, rows // (PARTS * PIECES)

    def pieces_of(k):
        return range(k * PIECES, (k + 1) * PIECES)

    def part_of(buf, j, i):
        return buf.at[j, pl.ds(i * piece_rows, piece_rows), :]

    def gather_start(src, buf, sem, k, to=None):
        for i in pieces_of(k):
            gather_piece(src, buf, sem, i, to)

    def gather_piece(src, buf, sem, i, to=None):
        piece = src.at[pl.ds(i * piece_rows, piece_rows), :]
        here = part_of(buf, c, i)
        up, down = c + 1 < n.ctx, c > 0
        if to == "between":
            up, down = c + 1 < n.ctx - 1, c > 1
        elif to == "ends":
            up, down = c + 1 == n.ctx - 1, c == 1
        send_if(up, piece, here, sem[0].at[0, 0], sem[1].at[c, i], right)
        send_if(down, piece, here, sem[0].at[1, 0], sem[1].at[c, i], left)

    def gather_relay(buf, sem, by, k, source=None):
        low, high = jnp.maximum(c - by, 0), jnp.minimum(c + by, n.ctx - 1)
        from_low, from_high = c - by >= 0, c + by < n.ctx
        if source == "end":
            from_low, from_high = c == by, c + by == n.ctx - 1
        elif source == "between":
            from_low, from_high = c > by, c + by < n.ctx - 1
        for i in pieces_of(k):
            piece, here = part_of(buf, low, i), sem[1].at[low, i]
            pl.when(from_low)(functools.partial(arrived, piece, here))
            send_if(from_low & (c + 1 < n.ctx), piece, piece, sem[0].at[0, by], here, right)
            piece, here = part_of(buf, high, i), sem[1].at[high, i]
            pl.when(from_high)(functools.partial(arrived, piece, here))
            send_if(from_high & (c > 0), piece, piece, sem[0].at[1, by], here, left)

    def gather_sent(buf, sem):
        for by in range(n.ctx - 1):
            sent(buf.at[0], sem[0].at[0, by], (c - by >= 0) & (c + 1 < n.ctx))
            sent(buf.at[0], sem[0].at[1, by], (c + by < n.ctx) & (c > 0))

    def rows_of(k):
        return slice(k * part_rows, (k + 1) * part_rows)

    def scatter_send(cond, part, there, sem, target, i, way, to_c):
        send_if(
            cond,
            part_of(part, target, i),
            part_of(there, target, i),
            sem[0].at[way, target - 1 + way],
            sem[1].at[way, target - 1 + way, i],
            to_c,
        )

    def scatter_add(part, there, sem, target, i, way):
        arrived(part_of(there, target, i), sem[1].at[way, target - 1 + way, i])
        span = slice(i * piece_rows, (i + 1) * piece_rows)
        part[target, span, :] = (
            part[target, span, :].astype(F32) + there[target, span, :].astype(F32)
        ).astype(BF16)

    def scatter_start(g, k):
        for step in range(n.ctx - 1):
            for i in pieces_of(k):
                scatter_send(c == n.ctx - 1, g.part, g.high, g.sem, step, i, 1, left)
                scatter_send(c == 0, g.part, g.low, g.sem, n.ctx - 1 - step, i, 0, right)

    def scatter_up(g, step, k, cond):
        target = n.ctx - 1 - step
        cond = cond & (c < target) & (c > 0)
        for i in pieces_of(k):
            pl.when(cond)(functools.partial(scatter_add, g.part, g.low, g.sem, target, i, 0))
            scatter_send(cond, g.part, g.low, g.sem, target, i, 0, right)

    def scatter_down(g, step, k, cond):
        cond = cond & (c > step) & (c + 1 < n.ctx)
        for i in pieces_of(k):
            pl.when(cond)(functools.partial(scatter_add, g.part, g.high, g.sem, step, i, 1))
            scatter_send(cond, g.part, g.high, g.sem, step, i, 1, left)

    def scatter_near(g, k):
        for step in range(n.ctx - 1):
            scatter_up(g, step, k, c < n.ctx // 2)
            scatter_down(g, step, k, c >= n.ctx // 2)

    def scatter_far(g, k):
        for step in range(n.ctx - 1):
            scatter_up(g, step, k, c >= n.ctx // 2)
            scatter_down(g, step, k, c < n.ctx // 2)

    def scatter_sent(g):
        for target in range(1, n.ctx):
            sent(g.part.at[0], g.sem[0].at[0, target - 1], c < target)
        for target in range(n.ctx - 1):
            sent(g.part.at[0], g.sem[0].at[1, target], c > target)

    def scatter_total(g, out, k):
        span = rows_of(k)
        out[span, :] = out[span, :] + g.part[c, span, :].astype(F32)

        @pl.when(c > 0)
        def _():
            for i in pieces_of(k):
                arrived(part_of(g.low, c, i), g.sem[1].at[0, jnp.maximum(c - 1, 0), i])
            out[span, :] = out[span, :] + g.low[c, span, :].astype(F32)

        @pl.when(c + 1 < n.ctx)
        def _():
            for i in pieces_of(k):
                arrived(part_of(g.high, c, i), g.sem[1].at[1, jnp.minimum(c, n.ctx - 2), i])
            out[span, :] = out[span, :] + g.high[c, span, :].astype(F32)

    def block_of(buf, index, span):
        return buf.at[pl.ds(pl.multiple_of(index * block, block), block), pl.ds(*span)]

    def blocks_of(buf, count, span):
        return buf.at[pl.ds(0, count * block), pl.ds(*span)]

    def piece_of(buf, line, at, width):
        start = pl.multiple_of(f * block + line * shard, shard)
        return buf.at[pl.ds(start, shard), pl.ds(at, width)]

    def weights_send(shards, cols, buf, send_sem, recv_sems, now=None):
        for by in range(1, n.ctx):
            at_end = (ahead(by) == 0) | (ahead(by) == n.ctx - 1)
            at = 0
            for src, width, recv_sem in zip(shards, cols, recv_sems):
                column = pl.multiple_of(ahead(by) * width, HEAD_DIM)
                copy = remote(
                    src.at[:, pl.ds(column, width)],
                    piece_of(buf, c, at, width),
                    send_sem.at[by - 1],
                    recv_sem.at[by - 1],
                    None,
                    ahead(by),
                )
                if now is None:
                    copy.start()
                else:
                    pl.when(at_end if now == "ends" else ~at_end)(copy.start)
                at += width

    def weights_sent(cols, buf, send_sem):
        for by in range(1, n.ctx):
            sent(piece_of(buf, c, 0, sum(cols)), send_sem.at[by - 1])

    def weights_own(shards, cols, buf, first):
        at, out = 0, []
        for i, (src, width) in enumerate(zip(shards, cols)):
            column = pl.multiple_of(c * width, HEAD_DIM)
            copy = pltpu.make_async_copy(
                src.at[:, pl.ds(column, width)],
                piece_of(buf, c, at, width),
                r.local_sem.at[first + i],
            )
            copy.start()
            out.append(copy)
            at += width
        return out

    def weights_spread(own, g):
        for copy in own:
            copy.wait()
        for by in range(1, n.ctx):
            arrived(piece_of(g.buf, behind(by), *g.span), g.line.at[by - 1])
        mine = block_of(g.buf, f, g.span)
        for by in range(1, n.chips):
            send(mine, mine, g.sem.at[0], g.sem.at[2 + by], chip_ahead(by) * 2 + core)
        send(mine, mine, g.sem.at[1], g.sem.at[2], sibling)

    def weights_forward(g):
        for by in range(1, n.chips):
            piece = block_of(g.buf, chip_behind(by) * 2 + core, g.span)
            arrived(piece, g.sem.at[2 + by])
            send(piece, piece, g.sem.at[1], g.sem.at[2], sibling)
        sent(blocks_of(g.buf, n.chips - 1, g.span), g.sem.at[0])
        sent(blocks_of(g.buf, n.chips, g.span), g.sem.at[1])

    def weights_wait(g):
        arrived(blocks_of(g.buf, n.chips, g.span), g.sem.at[2])

    def share_of(buf, index, span):
        return buf.at[pl.ds(pl.multiple_of(index * block, block), block), pl.ds(*span)]

    def grads_pair(g):
        for by in (*range(1, n.chips), 0):
            send(
                share_of(g.whole, chip_ahead(by) * 2 + 1 - core, g.span),
                g.pair.at[by, :, pl.ds(*g.span)],
                g.sem.at[0],
                g.sem.at[5 + by],
                sibling,
            )
        sent(g.pair.at[:, :, pl.ds(*g.span)], g.sem.at[0])

    def grads_plane(g):
        for by in range(1, n.chips):
            theirs = g.pair.at[by, :, pl.ds(*g.span)]
            arrived(theirs, g.sem.at[5 + by])
            piece = share_of(g.whole, chip_ahead(by) * 2 + core, g.span)
            piece[...] = (piece[...].astype(F32) + theirs[...].astype(F32)).astype(BF16)
            send(
                piece,
                g.plane.at[by - 1, :, pl.ds(*g.span)],
                g.sem.at[1],
                g.sem.at[2],
                chip_ahead(by) * 2 + core,
            )
        sent(g.plane.at[:, :, pl.ds(*g.span)], g.sem.at[1])

    def grads_line(g):
        theirs = g.pair.at[0, :, pl.ds(*g.span)]
        arrived(theirs, g.sem.at[5])
        acc = share_of(g.whole, f, g.span)[...].astype(F32) + theirs[...].astype(F32)
        arrived(g.plane.at[:, :, pl.ds(*g.span)], g.sem.at[2])
        for by in range(1, n.chips):
            acc = acc + g.plane[by - 1, :, pl.ds(*g.span)].astype(F32)
        g.total[:, pl.ds(*g.span)] = acc.astype(BF16)
        for by in range(1, n.ctx):
            start = pl.multiple_of(ahead(by) * shard, shard)
            send(
                g.total.at[pl.ds(start, shard), pl.ds(*g.span)],
                g.land.at[c, :, pl.ds(*g.span)],
                g.sem.at[3],
                g.sem.at[4],
                None,
                ahead(by),
            )
        sent(g.land.at[pl.ds(0, n.ctx - 1), :, pl.ds(*g.span)], g.sem.at[3])
        start = pl.multiple_of(c * shard, shard)
        g.land[c, :, pl.ds(*g.span)] = g.total[pl.ds(start, shard), pl.ds(*g.span)]

    def grads_wait(g):
        arrived(g.land.at[pl.ds(0, n.ctx - 1), :, pl.ds(*g.span)], g.sem.at[4])

    def small_peers(way):
        if way == "line":
            return [(n.fsdp + by - 1, f, ahead(by)) for by in range(1, n.ctx)]
        return [(by - 1, lax.rem(f + by, n.fsdp), c) for by in range(1, n.fsdp)]

    def small_span(incoming, way):
        first, count = (n.fsdp, n.ctx - 1) if way == "line" else (0, n.fsdp - 1)
        return incoming.at[pl.ds(first, count)]

    def small_send(src, incoming, sem, way):
        at = 2 * (way == "line")
        for slot, to_f, to_c in small_peers(way):
            send(src, incoming.at[slot], sem.at[at], sem.at[at + 1], to_f, to_c)
        sent(small_span(incoming, way), sem.at[at])

    def small_sum(own, incoming, sem, way):
        total = own[...]
        arrived(small_span(incoming, way), sem.at[2 * (way == "line") + 1])
        for slot, _, _ in small_peers(way):
            total = total + incoming[slot]
        return total

    def save_lines(first, line):
        for j in range(n.lines):
            row = slice(first + j, first + j + 1)
            r.g1_acc[3, row, :] += line[:, j * HEAD_DIM : (j + 1) * HEAD_DIM]

    attn_shards, mlp_shards = (r.wq, r.wk, r.wv, r.wo), (r.wg, r.wu, r.wd)
    attn_cols, mlp_cols = n.cols[:4], n.cols[4:]
    q_cols, k_cols, _, o_cols = attn_cols
    ff = mlp_cols[0]
    group = n.heads // n.kv
    factor = 1.0 / math.sqrt(HEAD_DIM)

    o_at = q_cols + 2 * k_cols
    attn_bufs = dict(whole=r.ga, pair=r.ga_sib, plane=r.ga_in, total=r.ga_z, land=r.ga_land)
    mlp_bufs = dict(whole=r.gm, pair=r.gm_sib, plane=r.gm_in, total=r.gm_z, land=r.gm_land)
    line_q, line_o, line_m = (r.rcv_w.at[i] for i in range(3))
    plane_q = types.SimpleNamespace(buf=r.wa, span=(0, o_at), line=line_q, sem=r.sem_pq)
    plane_o = types.SimpleNamespace(buf=r.wa, span=(o_at, o_cols), line=line_o, sem=r.sem_po)
    plane_m = types.SimpleNamespace(buf=r.wm, span=(0, n.mlp_cols), line=line_m, sem=r.sem_pm)
    to_attn = (r.wa, r.snd_w.at[0], (line_q, line_q, line_q, line_o))
    to_mlp = (r.wm, r.snd_w.at[1], (line_m, line_m, line_m))
    group_m = types.SimpleNamespace(
        **mlp_bufs, span=(0, n.mlp_cols), sem=r.sem_gm
    )
    group_o = types.SimpleNamespace(
        **attn_bufs, span=(o_at, o_cols), sem=r.sem_go
    )
    group_q = types.SimpleNamespace(**attn_bufs, span=(0, o_at), sem=r.sem_gq)

    sum_o, sum_y, sum_x2, sum_x1 = (
        types.SimpleNamespace(part=part, low=low, high=high, sem=sem)
        for part, low, high, sem in (
            (r.p_o, r.l_o, r.r_o, r.sem_o),
            (r.p_y, r.l_y, r.r_y, r.sem_y),
            (r.p_x2, r.l_x2, r.r_x2, r.sem_x2),
            (r.p_x1, r.l_x1, r.r_x1, r.sem_x1),
        )
    )
    r.g1_acc[3] = jnp.zeros_like(r.g1_acc[3])

    me = f * n.ctx + c
    lane = lax.broadcasted_iota(jnp.int32, (1, HEAD_DIM), 1)

    def place(row, at, size, first):
        moved = pltpu.roll(r.gains[...], lax.rem(at + HEAD_DIM - first, HEAD_DIM), 1)
        r.gp[pl.ds(row, 1), :] = jnp.where((lane >= at) & (lane < at + size), moved, 0.0)

    r.gp[...] = jnp.zeros_like(r.gp)
    row, at = me * n.each // HEAD_DIM, lax.rem(me * n.each, HEAD_DIM)
    place(row, at, n.each, 0)
    place(n.lines + row, at, n.each, n.each)
    place(2 * n.lines, me * n.few, n.few, 2 * n.each)
    place(2 * n.lines + 1, me * n.few, n.few, 2 * n.each + n.few)
    small_send(r.gp, r.g0_in, r.sem_g0, "line")
    weights_send(attn_shards, attn_cols, *to_attn)
    for k in range(PARTS):
        gather_start(r.hidden, r.xb, r.sem_xb, k)
    own_x = pltpu.make_async_copy(r.hidden, r.xb.at[c], r.local_sem.at[7])
    own_x.start()
    own_g = pltpu.make_async_copy(r.cot, r.gb.at[c], r.local_sem.at[8])
    own_g.start()
    own_attn = weights_own(attn_shards, attn_cols, r.wa, 0)
    own_mlp = weights_own(mlp_shards, mlp_cols, r.wm, 4)
    r.g0_acc[0] = small_sum(r.gp, r.g0_in, r.sem_g0, "line")
    small_send(r.g0_acc.at[0], r.g0_in, r.sem_g0, "plane")
    slots = r.order.shape[1]
    slot_len = n.tokens // slots
    exponent = (lane % (HEAD_DIM // 2)).astype(F32) * (2.0 / HEAD_DIM)
    inverse = jnp.exp(-exponent * math.log(1000000.0))
    sign = jnp.where(lane < HEAD_DIM // 2, -1.0, 1.0)
    for j in range(slots):
        first = r.order[0, j] * slot_len
        span = slice(j * slot_len, (j + 1) * slot_len)
        position = first + lax.broadcasted_iota(jnp.int32, (slot_len, HEAD_DIM), 0)
        r.posq[span, :] = position
        angle = position.astype(F32) * inverse
        r.cos[span, :] = jnp.cos(angle)
        r.sin[span, :] = jnp.sin(angle) * sign
    token = lax.broadcasted_iota(jnp.int32, (1, n.tokens), 1)
    posk = token % slot_len
    for j in range(slots):
        posk = posk + jnp.where(token // slot_len == j, r.order[0, j] * slot_len, 0)
    r.posk[...] = posk
    weights_spread(own_attn[:3], plane_q)
    weights_spread(own_attn[3:], plane_o)
    r.g0_acc[2] = small_sum(r.g0_acc.at[0], r.g0_in, r.sem_g0, "plane")
    for j in range(n.lines):
        r.gv[0, :, j * HEAD_DIM : (j + 1) * HEAD_DIM] = r.g0_acc[2, j : j + 1, :]
        r.gv[1, :, j * HEAD_DIM : (j + 1) * HEAD_DIM] = r.g0_acc[
            2, n.lines + j : n.lines + j + 1, :
        ]
    qgain = r.g0_acc[2, 2 * n.lines : 2 * n.lines + 1, :]
    kgain = r.g0_acc[2, 2 * n.lines + 1 : 2 * n.lines + 2, :]
    attn_gain, mlp_gain = r.gv[0], r.gv[1]
    for by in range(1, n.ctx):
        if by == n.ctx - 1:
            weights_send(mlp_shards, mlp_cols, *to_mlp, "between")
            for k in range(PARTS):
                gather_start(r.cot, r.gb, r.sem_gb, k, "between")
        for k in range(PARTS):
            gather_relay(r.xb, r.sem_xb, by, k)
    own_x.wait()
    own_g.wait()

    def norm_rows(j, carry):
        x = r.xb[j].astype(F32)
        start = pl.multiple_of(j * rows, rows)
        r.xn[pl.ds(start, rows), :] = (x * rms(x) * attn_gain).astype(BF16)
        return carry

    lax.fori_loop(0, n.ctx, norm_rows, 0)
    weights_forward(plane_q)
    weights_wait(plane_q)
    weights_send(mlp_shards, mlp_cols, *to_mlp, "ends")
    for k in range(PARTS):
        gather_start(r.cot, r.gb, r.sem_gb, k, "ends")

    cosine, sine = r.cos, r.sin
    tile = 2 * HEAD_DIM if n.kv % 2 == 0 else HEAD_DIM
    for at in range(0, q_cols + 2 * k_cols, tile):
        product = mm(r.xn[...], r.wa[:, at : at + tile])
        for part in range(tile // HEAD_DIM):
            head = at // HEAD_DIM + part
            u = product[:, part * HEAD_DIM : (part + 1) * HEAD_DIM]
            if head < n.heads:
                r.qp[head] = u
                r.qr[head] = rope_fwd(u * rms(u) * qgain, cosine[...], sine[...]).astype(BF16)
            elif head < n.heads + n.kv:
                r.kp[head - n.heads] = u
                r.kr[head - n.heads] = rope_fwd(u * rms(u) * kgain, cosine[...], sine[...]).astype(
                    BF16
                )
            else:
                r.vv[head - n.heads - n.kv] = u.astype(BF16)
    weights_forward(plane_o)
    half = n.tokens // 2

    def head_forward(h, carry):
        kv = h // group
        for q0 in (0, half):
            s = mm(r.qr[h, q0 : q0 + half, :], r.kr[kv], LAST_AXIS)
            allowed = r.posk[...] <= r.posq[q0 : q0 + half, 0:1]
            e = jnp.where(allowed, jnp.exp(s * factor), 0.0)
            r.es[h, q0 : q0 + half, :] = e
            total = jnp.sum(e, axis=-1, keepdims=True)
            a = mm(e.astype(BF16), r.vv[kv]) / total
            r.af[h, q0 : q0 + half, :] = a
            lane = pl.multiple_of(h * HEAD_DIM, HEAD_DIM)
            r.at[q0 : q0 + half, pl.ds(lane, HEAD_DIM)] = a.astype(BF16)
        return carry

    lax.fori_loop(0, n.heads, head_forward, 0)
    weights_wait(plane_o)

    def by_rows(left, right, out):
        step = 2 * HEAD_DIM
        for at in range(0, d, step):
            product = mm(left[...], right(slice(at, at + step)), LAST_AXIS)
            out[:, :, at : at + step] = product.astype(BF16).reshape(n.ctx, rows, step)

    by_rows(r.at, lambda span: r.wa[span, o_at:], r.p_o)
    for k in range(PARTS):
        scatter_start(sum_o, k)
    weights_spread(own_mlp, plane_m)

    def residual(k):
        span = rows_of(k)
        r.ho[span, :] = r.xb[c, span, :].astype(F32)
        scatter_total(sum_o, r.ho, k)
        own = r.ho[span, :]
        r.mb[c, span, :] = (own * rms(own) * mlp_gain).astype(BF16)
        gather_start(r.mb.at[c], r.mb, r.sem_mb, k)

    gather_relay(r.gb, r.sem_gb, 1, 0)
    scatter_near(sum_o, 0)
    scatter_far(sum_o, 0)
    for by in range(2, n.ctx - 1):
        gather_relay(r.gb, r.sem_gb, by, 0)
    residual(0)
    scatter_near(sum_o, 1)
    gather_relay(r.mb, r.sem_mb, 1, 0, "between")
    scatter_far(sum_o, 1)
    residual(1)
    gather_relay(r.mb, r.sem_mb, 1, 0, "end")
    gather_relay(r.mb, r.sem_mb, 1, 1, "between")
    for by in range(2, n.ctx - 1):
        gather_relay(r.mb, r.sem_mb, by, 0)
    weights_forward(plane_m)
    gather_relay(r.mb, r.sem_mb, n.ctx - 1, 0)
    gather_relay(r.gb, r.sem_gb, n.ctx - 1, 0)
    weights_wait(plane_m)

    tile = 2 * HEAD_DIM if ff % (2 * HEAD_DIM) == 0 else HEAD_DIM
    span_rows = n.ctx * part_rows

    def mlp_part(k):
        span = rows_of(k)
        mixed = r.mb[:, span, :].reshape(span_rows, d)
        upstream = r.gb[:, span, :].reshape(span_rows, d)
        for at in range(0, ff, tile):
            gate = mm(mixed, r.wm[:, at : at + tile])
            up = mm(mixed, r.wm[:, ff + at : ff + at + tile])
            back = mm(upstream, r.wm[:, 2 * ff + at : 2 * ff + at + tile])
            sig = jax.nn.sigmoid(gate)
            swish = gate * sig
            shape = (n.ctx, part_rows, tile)
            r.hid[:, span, at : at + tile] = (swish * up).astype(BF16).reshape(shape)
            r.dgu[:, span, at : at + tile] = (
                (back * up * sig * (1.0 + gate * (1.0 - sig))).astype(BF16).reshape(shape)
            )
            r.dgu[:, span, ff + at : ff + at + tile] = (
                (back * swish).astype(BF16).reshape(shape)
            )
        both = r.dgu[:, span, :].reshape(span_rows, 2 * ff)
        for at in range(0, d, 2 * HEAD_DIM):
            product = mm(both, r.wm[at : at + 2 * HEAD_DIM, : 2 * ff], LAST_AXIS).astype(BF16)
            r.p_x2[:, span, at : at + 2 * HEAD_DIM] = product.reshape(
                n.ctx, part_rows, 2 * HEAD_DIM
            )
        scatter_start(sum_x2, k)

    def residual_back(k):
        span = rows_of(k)
        r.dh[span, :] = jnp.zeros((part_rows, d), F32)
        scatter_total(sum_x2, r.dh, k)
        own = r.ho[span, :]
        from_norm, term = norm_back(own, rms(own), mlp_gain, r.dh[span, :])
        save_lines(n.lines, jnp.sum(term, axis=0, keepdims=True))
        r.dh[span, :] = r.gb[c, span, :].astype(F32) + from_norm
        r.rb[c, span, :] = r.dh[span, :].astype(BF16)
        gather_start(r.rb.at[c], r.rb, r.sem_rb, k)

    mlp_part(0)
    gather_relay(r.mb, r.sem_mb, 1, 1, "end")
    gather_relay(r.gb, r.sem_gb, 1, 1)
    for by in range(2, n.ctx - 1):
        gather_relay(r.gb, r.sem_gb, by, 1)
        gather_relay(r.mb, r.sem_mb, by, 1)
    scatter_near(sum_x2, 0)
    scatter_far(sum_x2, 0)
    gather_relay(r.mb, r.sem_mb, n.ctx - 1, 1)
    gather_relay(r.gb, r.sem_gb, n.ctx - 1, 1)
    mlp_part(1)
    residual_back(0)
    hidden = r.hid[...].reshape(n.tokens, ff)
    by_rows(hidden, lambda span: r.wm[span, 2 * ff :], r.p_y)
    scatter_start(sum_y, 0)
    mixed = r.mb[...].reshape(n.tokens, d)
    upstream = r.gb[...].reshape(n.tokens, d)
    for at in range(0, 2 * ff, tile):
        part = r.dgu[:, :, at : at + tile].reshape(n.tokens, tile)
        r.gm[:, at : at + tile] = mm(mixed, part, FIRST_AXIS).astype(BF16)
    for at in range(0, ff, tile):
        part = r.hid[:, :, at : at + tile].reshape(n.tokens, tile)
        r.gm[:, 2 * ff + at : 2 * ff + at + tile] = mm(upstream, part, FIRST_AXIS).astype(BF16)
    grads_pair(group_m)
    scatter_near(sum_x2, 1)
    gather_relay(r.rb, r.sem_rb, 1, 0, "between")
    grads_plane(group_m)
    scatter_far(sum_x2, 1)
    gather_relay(r.rb, r.sem_rb, 1, 0, "end")
    for by in range(2, n.ctx - 1):
        gather_relay(r.rb, r.sem_rb, by, 0)
    residual_back(1)
    scatter_start(sum_y, 1)
    scatter_near(sum_y, 0)
    gather_relay(r.rb, r.sem_rb, 1, 1, "between")
    gather_relay(r.rb, r.sem_rb, 1, 1, "end")
    for by in range(2, n.ctx - 1):
        gather_relay(r.rb, r.sem_rb, by, 1)
    scatter_far(sum_y, 0)
    for k in range(PARTS):
        gather_relay(r.rb, r.sem_rb, n.ctx - 1, k)

    upstream = r.rb[...].reshape(n.tokens, d)
    for at in range(0, o_cols, HEAD_DIM):
        r.da[at // HEAD_DIM] = mm(upstream, r.wa[:, o_at + at : o_at + at + HEAD_DIM])
    grads_line(group_m)
    r.ga[:, o_at:] = mm(upstream, r.at[...], FIRST_AXIS).astype(BF16)
    grads_pair(group_o)
    scatter_near(sum_y, 1)
    r.dk[...] = jnp.zeros_like(r.dk)
    r.dv[...] = jnp.zeros_like(r.dv)

    def head_backward(h, carry):
        kv = h // group
        for q0 in (0, half):
            span = slice(q0, q0 + half)
            e = r.es[h, span, :]
            total = jnp.sum(e, axis=-1, keepdims=True)
            da = r.da[h, span, :]
            w = (da / total).astype(BF16)
            dl = jnp.sum(da * r.af[h, span, :], axis=-1, keepdims=True) / total
            ds = (e * (mm(w, r.vv[kv], LAST_AXIS) - dl)).astype(BF16)
            r.ds[span, :] = ds
            r.eb[span, :] = e.astype(BF16)
            r.wb[span, :] = w
            r.da[h, span, :] = mm(ds, r.kr[kv])
        r.dk[kv] = r.dk[kv] + mm(r.ds[...], r.qr[h], FIRST_AXIS)
        r.dv[kv] = r.dv[kv] + mm(r.eb[...], r.wb[...], FIRST_AXIS)
        return carry

    lax.fori_loop(0, n.heads, head_backward, 0)

    def query_backward(h, term):
        u = r.qp[h]
        du, gain_term = norm_back(
            u, rms(u), qgain, rope_bwd(r.da[h] * factor, cosine[...], sine[...])
        )
        lane = pl.multiple_of(h * HEAD_DIM, HEAD_DIM)
        r.dqkv[:, pl.ds(lane, HEAD_DIM)] = du.astype(BF16)
        return term + jnp.sum(gain_term, axis=0, keepdims=True)

    q_term = lax.fori_loop(0, n.heads, query_backward, jnp.zeros((1, HEAD_DIM), F32))
    grads_plane(group_o)
    k_term = jnp.zeros((1, HEAD_DIM), F32)
    for kv in range(n.kv):
        u = r.kp[kv]
        du, gain_term = norm_back(
            u, rms(u), kgain, rope_bwd(r.dk[kv] * factor, cosine[...], sine[...])
        )
        at = q_cols + kv * HEAD_DIM
        r.dqkv[:, at : at + HEAD_DIM] = du.astype(BF16)
        at += k_cols
        r.dqkv[:, at : at + HEAD_DIM] = r.dv[kv].astype(BF16)
        k_term = k_term + jnp.sum(gain_term, axis=0, keepdims=True)
    by_rows(r.dqkv, lambda span: r.wa[span, :o_at], r.p_x1)
    for k in range(PARTS):
        scatter_start(sum_x1, k)
    for at in range(0, o_at, 2 * HEAD_DIM):
        r.ga[:, at : at + 2 * HEAD_DIM] = mm(
            r.xn[...], r.dqkv[:, at : at + 2 * HEAD_DIM], FIRST_AXIS
        ).astype(BF16)
    grads_pair(group_q)
    for j in range(n.ctx):
        x = r.xb[j].astype(F32)
        share = r.p_x1[j].astype(F32) * (x * rms(x))
        save_lines(0, jnp.sum(share, axis=0, keepdims=True))
    r.g1_acc[3, 2 * n.lines : 2 * n.lines + 1, :] = q_term
    r.g1_acc[3, 2 * n.lines + 1 : 2 * n.lines + 2, :] = k_term
    small_send(r.g1_acc.at[3], r.g1_in, r.sem_g1, "plane")
    grads_plane(group_q)
    scatter_near(sum_x1, 0)
    scatter_far(sum_y, 1)
    scatter_far(sum_x1, 0)
    grads_line(group_o)
    r.g1_acc[1] = small_sum(r.g1_acc.at[3], r.g1_in, r.sem_g1, "plane")
    small_send(r.g1_acc.at[1], r.g1_in, r.sem_g1, "line")
    scatter_near(sum_x1, 1)
    grads_line(group_q)
    scatter_far(sum_x1, 1)
    for k in range(PARTS):
        scatter_total(sum_y, r.ho, k)
    r.out_hidden[...] = r.ho[...].astype(BF16)
    r.out_input[...] = jnp.zeros_like(r.out_input)
    for k in range(PARTS):
        scatter_total(sum_x1, r.out_input, k)
    x = r.xb[c].astype(F32)
    from_norm, _ = norm_back(x, rms(x), attn_gain, r.out_input[...])
    r.out_input[...] = r.dh[...] + from_norm
    grads_wait(group_m)
    grads_wait(group_o)
    grads_wait(group_q)
    r.out_gains[...] = small_sum(r.g1_acc.at[1], r.g1_in, r.sem_g1, "line")
    for buf, sem in ((r.xb, r.sem_xb), (r.gb, r.sem_gb), (r.mb, r.sem_mb), (r.rb, r.sem_rb)):
        gather_sent(buf, sem)
    for g in (sum_o, sum_y, sum_x2, sum_x1):
        scatter_sent(g)
    weights_sent(attn_cols, *to_attn[:2])
    weights_sent(mlp_cols, *to_mlp[:2])
    for wait in sends:
        wait()


def fused(
    ctx,
    fsdp,
    hidden_in,
    block_order,
    cotangent,
    q_weight,
    k_weight,
    v_weight,
    o_weight,
    attn_gain,
    query_gain,
    key_gain,
    mlp_gain,
    gate_weight,
    up_weight,
    down_weight,
):
    shards = (q_weight, k_weight, v_weight, o_weight, gate_weight, up_weight, down_weight)
    n = Sizes(ctx, fsdp, hidden_in.shape[1], shards)
    gains = jnp.concatenate([attn_gain, mlp_gain, query_gain, key_gain]).astype(F32)
    gains = jnp.pad(gains, (0, HEAD_DIM - gains.shape[0])).reshape(1, HEAD_DIM)
    hbm, vmem = pl.BlockSpec(memory_space=pl.ANY), pl.BlockSpec(memory_space=pltpu.VMEM)
    inputs = dict(
        hidden=(hidden_in[0], hbm),
        cot=(cotangent[0], hbm),
        wq=(q_weight, hbm),
        wk=(k_weight, hbm),
        wv=(v_weight, hbm),
        wo=(o_weight, hbm),
        wg=(gate_weight, hbm),
        wu=(up_weight, hbm),
        wd=(down_weight, hbm),
        gains=(gains, vmem),
        order=(block_order, pl.BlockSpec(memory_space=pltpu.SMEM)),
    )
    outputs = dict(
        out_hidden=jax.ShapeDtypeStruct((n.rows, n.width), BF16),
        out_input=jax.ShapeDtypeStruct((n.rows, n.width), F32),
        ga_land=jax.ShapeDtypeStruct((ctx, n.shard, n.attn_cols), BF16),
        gm_land=jax.ShapeDtypeStruct((ctx, n.shard, n.mlp_cols), BF16),
        out_gains=jax.ShapeDtypeStruct((n.gain_rows, HEAD_DIM), F32),
    )
    scratch = scratch_of(n)
    landed = pl.pallas_call(
        functools.partial(layer_kernel, n, [*inputs, *outputs, *scratch]),
        out_shape=tuple(outputs.values()),
        in_specs=[spec for _, spec in inputs.values()],
        out_specs=tuple(vmem for _ in outputs),
        scratch_shapes=list(scratch.values()),
        compiler_params=pltpu.CompilerParams(
            collective_id=0, has_side_effects=True, vmem_limit_bytes=VMEM_LIMIT
        ),
        name="layer",
    )(*[value for value, _ in inputs.values()])

    finals = [(n.rows, n.width, BF16), (n.rows, n.width, F32)]
    finals += [(*s.shape, F32) for s in shards]
    finals += [(1, size, F32) for size in (n.each, n.each, n.few, n.few)]
    result, input_grad, oq, ok, ov, oo, og, ou, od, *gains = pl.pallas_call(
        functools.partial(emit_kernel, n),
        out_shape=tuple(jax.ShapeDtypeStruct(f[:2], f[2]) for f in finals),
        in_specs=[vmem] * len(outputs),
        out_specs=tuple(vmem for _ in finals),
        name="emit",
    )(*landed)
    return (
        result[None],
        input_grad[None],
        oq,
        ok,
        ov,
        oo,
        gains[0].reshape(n.each),
        gains[2].reshape(n.few),
        gains[3].reshape(n.few),
        gains[1].reshape(n.each),
        og,
        ou,
        od,
    )


def emit_kernel(n, result, input_grad, attn_land, mlp_land, sums, *outs):
    outs[0][...] = result[...]
    outs[1][...] = input_grad[...]
    which = 2
    for land, widths in ((attn_land, n.cols[:4]), (mlp_land, n.cols[4:])):
        at = 0
        for width in widths:
            for j in range(n.ctx):
                outs[which][:, j * width : (j + 1) * width] = land[j, :, at : at + width].astype(
                    F32
                )
            at += width
            which += 1
    me = lax.axis_index("fsdp") * n.ctx + lax.axis_index("ctx")
    row, at = me * n.each // HEAD_DIM, lax.rem(me * n.each, HEAD_DIM)
    for out, (line, lane) in zip(
        outs[which:],
        (
            (row, at),
            (n.lines + row, at),
            (2 * n.lines, me * n.few),
            (2 * n.lines + 1, me * n.few),
        ),
    ):
        back = lax.rem(HEAD_DIM - lane, HEAD_DIM)
        out[...] = pltpu.roll(sums[pl.ds(line, 1), :], back, 1)[:, : out.shape[1]]


def fits(ctx, fsdp, shard_rows):
    per_tile = HEAD_DIM % (2 * shard_rows) == 0 and HEAD_DIM % (ctx * fsdp) == 0
    return per_tile and shard_rows % 16 == 0 and fsdp % 2 == 0 and KV_HEADS % ctx == 0


def solution(mesh):
    ctx, fsdp = mesh.shape["ctx"], mesh.shape["fsdp"]
    tokens = P("fsdp", "ctx", None)
    matrix = P(("fsdp", "ctx"), None)
    vector = P(("fsdp", "ctx"))
    def step(hidden_in, block_order, cotangent, q_weight, *rest):
        whole = fused if fits(ctx, fsdp, q_weight.shape[0]) else local
        return whole(ctx, fsdp, hidden_in, block_order, cotangent, q_weight, *rest)

    return jax.shard_map(
        step,
        mesh=mesh,
        in_specs=(tokens, P("fsdp", None), tokens)
        + (matrix,) * 4
        + (vector,) * 4
        + (matrix,) * 3,
        out_specs=(tokens,) * 2 + (matrix,) * 4 + (vector,) * 4 + (matrix,) * 3,
        check_vma=False,
    )
```

```python
import functools
import math
import types

import jax
import jax.numpy as jnp
from jax import lax
from jax.experimental import pallas as pl
from jax.experimental.pallas import tpu as pltpu
from jax.sharding import PartitionSpec as P

HEADS = 16
KV_HEADS = 8
HEAD_DIM = 128
EPSILON = 1e-06
FIRST_AXIS = (((0,), (0,)), ((), ()))
LAST_AXIS = (((1,), (1,)), ((), ()))
BF16 = jnp.bfloat16
F32 = jnp.float32
VMEM_LIMIT = 67043328
PARTS = 2
PIECES = 2


def mm(left, right, dims=(((1,), (0,)), ((), ()))):
    return lax.dot_general(left, right, dims, preferred_element_type=F32)


def rms(signal):
    return lax.rsqrt(jnp.mean(signal * signal, axis=-1, keepdims=True) + EPSILON)


def norm_back(signal, inverse_rms, gain_vec, upstream):
    unit_values = signal * inverse_rms
    scaled_up = upstream * gain_vec
    inner = scaled_up - unit_values * jnp.mean(scaled_up * unit_values, axis=-1, keepdims=True)
    return (inverse_rms * inner, upstream * unit_values)


def rope_tables(positions, head_width):
    exponent = jnp.arange(head_width // 2, dtype=F32) * (2.0 / head_width)
    inverse = jnp.exp(-exponent * math.log(1000000.0))
    angles = positions.astype(F32)[:, None] * inverse[None, :]
    angles = jnp.concatenate([angles, angles], axis=-1)
    return (jnp.cos(angles), jnp.sin(angles))


def rotate(signal, cosine, sine):
    half = signal.shape[-1] // 2
    turned = jnp.concatenate([-signal[..., half:], signal[..., :half]], axis=-1)
    return signal * cosine + turned * sine


def rotate_back(upstream, cosine, sine):
    half = upstream.shape[-1] // 2
    scaled_up = upstream * sine
    return upstream * cosine + jnp.concatenate(
        [scaled_up[..., half:], -scaled_up[..., :half]], axis=-1
    )


def gather_columns(ctx, shards):
    rows = shards[0].shape[0]
    cut = [s.reshape(rows, ctx, s.shape[1] // ctx).transpose(1, 0, 2) for s in shards]
    widths = [c.shape[2] for c in cut]
    both = jnp.concatenate(cut, axis=2)
    both = lax.all_to_all(both, "ctx", 0, 0, tiled=True)
    both = both.reshape(ctx * rows, -1)
    whole = lax.all_gather(both, "fsdp", axis=0, tiled=True)
    out, at = [], 0
    for width in widths:
        out.append(whole[:, at : at + width])
        at += width
    return out


def scatter_grads(ctx, fsdp, grads):
    rows = grads[0].shape[0] // (ctx * fsdp)
    widths = [g.shape[1] for g in grads]
    both = jnp.concatenate([g.astype(BF16) for g in grads], axis=1)
    both = lax.psum_scatter(both, "fsdp", scatter_dimension=0, tiled=True)
    both = lax.all_to_all(both.reshape(ctx, rows, -1), "ctx", 0, 0, tiled=True)
    out, at = [], 0
    for width in widths:
        piece = both[:, :, at : at + width]
        out.append(piece.transpose(1, 0, 2).reshape(rows, ctx * width).astype(F32))
        at += width
    return out


def ctx_gather(rows):
    return lax.all_gather(rows, "ctx", axis=0, tiled=True)


def ctx_scatter(partial):
    return lax.psum_scatter(partial.astype(BF16), "ctx", scatter_dimension=0, tiled=True).astype(
        F32
    )


def local(
    ctx,
    fsdp,
    hidden_in,
    block_order,
    cotangent,
    q_weight,
    k_weight,
    v_weight,
    o_weight,
    attn_gain,
    query_gain,
    key_gain,
    mlp_gain,
    gate_weight,
    up_weight,
    down_weight,
):
    inputs = hidden_in[0].astype(F32)
    row_count = inputs.shape[0]
    tokens = row_count * ctx
    slots = block_order.shape[1]
    block_len = tokens // slots
    heads, kv_heads = HEADS // ctx, KV_HEADS // ctx
    group = heads // kv_heads
    factor = 1.0 / math.sqrt(HEAD_DIM)
    positions = (
        block_order[0][:, None] * block_len + jnp.arange(block_len, dtype=jnp.int32)[None, :]
    ).reshape(-1)
    cosine, sine = rope_tables(positions, HEAD_DIM)
    cosine, sine = cosine[:, None, :], sine[:, None, :]

    both = ("fsdp", "ctx")
    norm_gain, qgain, kgain, mlp_norm_gain = (
        lax.all_gather(g, both, axis=0, tiled=True).astype(F32)
        for g in (attn_gain, query_gain, key_gain, mlp_gain)
    )
    norm_scale = rms(inputs)
    normed = ctx_gather((inputs * norm_scale * norm_gain).astype(BF16))
    upstream = ctx_gather(cotangent[0])
    q_full, k_full, v_full, o_full = gather_columns(ctx, (q_weight, k_weight, v_weight, o_weight))
    gate_full, up_full, down_full = gather_columns(ctx, (gate_weight, up_weight, down_weight))

    query_proj = mm(normed, q_full).reshape(tokens, heads, HEAD_DIM)
    key_proj = mm(normed, k_full).reshape(tokens, kv_heads, HEAD_DIM)
    value_low = mm(normed, v_full).astype(BF16).reshape(tokens, kv_heads, HEAD_DIM)
    query_scale, key_scale = rms(query_proj), rms(key_proj)
    query_low = (
        rotate(query_proj * query_scale * qgain, cosine, sine)
        .astype(BF16)
        .reshape(tokens, kv_heads, group, HEAD_DIM)
    )
    key_low = rotate(key_proj * key_scale * kgain, cosine, sine).astype(BF16)
    scores = jnp.einsum("rkgd,nkd->kgrn", query_low, key_low, preferred_element_type=F32) * factor
    allowed = positions[None, :] <= positions[:, None]
    weights_exp = jnp.where(allowed, jnp.exp(scores), 0.0)
    denominator = jnp.sum(weights_exp, axis=-1)
    weights_low = weights_exp.astype(BF16)
    numerator = jnp.einsum("kgrn,nkd->rkgd", weights_low, value_low, preferred_element_type=F32)
    denom_rows = jnp.transpose(denominator, (2, 0, 1))[..., None]
    attn_full = numerator / denom_rows
    attn_low = attn_full.astype(BF16).reshape(tokens, heads * HEAD_DIM)
    residual = inputs + ctx_scatter(mm(attn_low, o_full, LAST_AXIS))

    mix_scale = rms(residual)
    mixed = ctx_gather((residual * mix_scale * mlp_norm_gain).astype(BF16))
    gate_val = mm(mixed, gate_full)
    up_val = mm(mixed, up_full)
    sigmoid_gate = jax.nn.sigmoid(gate_val)
    swish_gate = gate_val * sigmoid_gate
    hidden_low = (swish_gate * up_val).astype(BF16)
    result = residual + ctx_scatter(mm(hidden_low, down_full, LAST_AXIS))
    hidden_grad = mm(upstream, down_full)
    gate_back = (
        hidden_grad * up_val * sigmoid_gate * (1.0 + gate_val * (1.0 - sigmoid_gate))
    ).astype(BF16)
    up_back = (hidden_grad * swish_gate).astype(BF16)
    mixed_grad = ctx_scatter(mm(gate_back, gate_full, LAST_AXIS) + mm(up_back, up_full, LAST_AXIS))
    resid_from_norm, mlp_gain_term = norm_back(residual, mix_scale, mlp_norm_gain, mixed_grad)
    residual_grad = cotangent[0].astype(F32) + resid_from_norm
    mlp_grads = scatter_grads(
        ctx,
        fsdp,
        (
            mm(mixed, gate_back, FIRST_AXIS),
            mm(mixed, up_back, FIRST_AXIS),
            mm(upstream, hidden_low, FIRST_AXIS),
        ),
    )
    resid_low = ctx_gather(residual_grad.astype(BF16))

    attn_grad = mm(resid_low, o_full).reshape(tokens, kv_heads, group, HEAD_DIM)
    share_low = (attn_grad / denom_rows).astype(BF16)
    denom_grad = jnp.transpose(jnp.sum(attn_grad * attn_full, axis=-1), (1, 2, 0)) / denominator
    weight_grad = jnp.einsum("rkgd,nkd->kgrn", share_low, value_low, preferred_element_type=F32)
    score_low = (weights_exp * (weight_grad - denom_grad[..., None])).astype(BF16)
    query_rot = (
        jnp.einsum("kgrn,nkd->rkgd", score_low, key_low, preferred_element_type=F32) * factor
    ).reshape(tokens, heads, HEAD_DIM)
    key_rot = (
        jnp.einsum("kgrn,rkgd->nkd", score_low, query_low, preferred_element_type=F32) * factor
    )
    value_back = (
        jnp.einsum("kgrn,rkgd->nkd", weights_low, share_low, preferred_element_type=F32)
        .reshape(tokens, kv_heads * HEAD_DIM)
        .astype(BF16)
    )
    query_grad, query_term = norm_back(
        query_proj, query_scale, qgain, rotate_back(query_rot, cosine, sine)
    )
    key_grad, key_term = norm_back(key_proj, key_scale, kgain, rotate_back(key_rot, cosine, sine))
    query_back = query_grad.reshape(tokens, heads * HEAD_DIM).astype(BF16)
    key_back = key_grad.reshape(tokens, kv_heads * HEAD_DIM).astype(BF16)
    normed_grad = ctx_scatter(
        mm(query_back, q_full, LAST_AXIS)
        + mm(key_back, k_full, LAST_AXIS)
        + mm(value_back, v_full, LAST_AXIS)
    )
    input_from_norm, attn_gain_term = norm_back(inputs, norm_scale, norm_gain, normed_grad)
    input_grad = residual_grad + input_from_norm
    attn_grads = scatter_grads(
        ctx,
        fsdp,
        (
            mm(normed, query_back, FIRST_AXIS),
            mm(normed, key_back, FIRST_AXIS),
            mm(normed, value_back, FIRST_AXIS),
            mm(resid_low, attn_low, FIRST_AXIS),
        ),
    )
    gains = (
        jnp.sum(attn_gain_term, axis=0),
        jnp.sum(query_term, axis=(0, 1)),
        jnp.sum(key_term, axis=(0, 1)),
        jnp.sum(mlp_gain_term, axis=0),
    )
    gains = [lax.psum_scatter(g, both, scatter_dimension=0, tiled=True) for g in gains]
    return (
        result.astype(BF16)[None],
        input_grad[None],
        *attn_grads,
        *gains,
        *mlp_grads,
    )


def rope_fwd(u, cosine, sine):
    return u * cosine + pltpu.roll(u, HEAD_DIM // 2, u.ndim - 1) * sine


def rope_bwd(du, cosine, sine):
    return du * cosine - pltpu.roll(du, HEAD_DIM // 2, du.ndim - 1) * sine


class Sizes:
    def __init__(self, ctx, fsdp, rows, shards):
        self.ctx, self.fsdp, self.rows = ctx, fsdp, rows
        self.chips = fsdp // 2
        self.shard = shards[0].shape[0]
        self.block = self.shard * ctx
        self.width = self.block * fsdp
        self.tokens = rows * ctx
        self.heads, self.kv = HEADS // ctx, KV_HEADS // ctx
        self.cols = [s.shape[1] // ctx for s in shards]
        self.attn_cols = sum(self.cols[:4])
        self.mlp_cols = sum(self.cols[4:])
        self.lines = self.width // HEAD_DIM
        self.gain_rows = 8 * ((2 * self.lines + 2 + 7) // 8)
        self.each, self.few = self.width // (ctx * fsdp), HEAD_DIM // (ctx * fsdp)


def scratch_of(n):
    bf, f32 = (lambda *s: pltpu.VMEM(s, BF16)), (lambda *s: pltpu.VMEM(s, F32))
    sem = lambda *s: pltpu.SemaphoreType.DMA(s)
    c, d, s, h, kv = n.ctx, n.width, n.tokens, n.heads, n.kv
    ff = n.cols[4]
    out = dict(
        wa=bf(d, n.attn_cols),
        wm=bf(d, n.mlp_cols),
        xb=bf(c, n.rows, d),
        gb=bf(c, n.rows, d),
        mb=bf(c, n.rows, d),
        rb=bf(c, n.rows, d),
        xn=bf(s, d),
        qp=f32(h, s, HEAD_DIM),
        kp=f32(kv, s, HEAD_DIM),
        qr=bf(h, s, HEAD_DIM),
        kr=bf(kv, s, HEAD_DIM),
        vv=bf(kv, s, HEAD_DIM),
        es=f32(h, s, s),
        af=f32(h, s, HEAD_DIM),
        at=bf(s, h * HEAD_DIM),
        da=f32(h, s, HEAD_DIM),
        dk=f32(kv, s, HEAD_DIM),
        dv=f32(kv, s, HEAD_DIM),
        ds=bf(s, s),
        eb=bf(s, s),
        wb=bf(s, HEAD_DIM),
        dqkv=bf(s, (h + 2 * kv) * HEAD_DIM),
        hid=bf(c, n.rows, ff),
        dgu=bf(c, n.rows, 2 * ff),
        ho=f32(n.rows, d),
        dh=f32(n.rows, d),
        gv=f32(2, 1, d),
        gp=f32(n.gain_rows, HEAD_DIM),
        cos=f32(s, HEAD_DIM),
        sin=f32(s, HEAD_DIM),
        posq=pltpu.VMEM((s, HEAD_DIM), jnp.int32),
        posk=pltpu.VMEM((1, s), jnp.int32),
        ga=bf(d, n.attn_cols),
        gm=bf(d, n.mlp_cols),
        ga_sib=bf(n.chips, n.block, n.attn_cols),
        gm_sib=bf(n.chips, n.block, n.mlp_cols),
        ga_in=bf(n.chips - 1, n.block, n.attn_cols),
        gm_in=bf(n.chips - 1, n.block, n.mlp_cols),
        ga_z=bf(n.block, n.attn_cols),
        gm_z=bf(n.block, n.mlp_cols),
        local_sem=sem(9),
    )
    for name in ("o", "y", "x2", "x1"):
        out["p_" + name] = bf(c, n.rows, d)
        out["l_" + name] = bf(c, n.rows, d)
        out["r_" + name] = bf(c, n.rows, d)
        out["snd_" + name] = sem(2, c - 1)
        out["rcv_" + name] = sem(2, c - 1, PARTS * PIECES)
    for name in ("xb", "gb", "mb", "rb"):
        out["snd_" + name] = sem(2, c - 1)
        out["rcv_" + name] = sem(c, PARTS * PIECES)
    out["snd_w"] = sem(2, c - 1)
    out["rcv_w"] = sem(3, c - 1)
    for name in ("pq", "po", "pm"):
        out["sem_" + name] = sem(3 + n.chips)
    for name in ("gm", "go", "gq"):
        out["sem_" + name] = sem(5 + n.chips)
    for name in ("g0", "g1"):
        out[name + "_in"] = f32(n.fsdp + c, n.gain_rows, HEAD_DIM)
        out[name + "_acc"] = f32(4, n.gain_rows, HEAD_DIM)
        out["sem_" + name] = sem(4)
    return out


def layer_kernel(n, names, *refs):
    r = types.SimpleNamespace(**dict(zip(names, refs)))
    for name in ("o", "y", "x2", "x1", "xb", "gb", "mb", "rb"):
        setattr(r, "sem_" + name, (getattr(r, "snd_" + name), getattr(r, "rcv_" + name)))
    c, f = lax.axis_index("ctx"), lax.axis_index("fsdp")
    chip, core = f // 2, f % 2
    sibling = chip * 2 + 1 - core
    rows, d, block, shard = n.rows, n.width, n.block, n.shard
    sends = []

    def ahead(by):
        return lax.rem(c + by, n.ctx)

    def behind(by):
        return lax.rem(c + n.ctx - by, n.ctx)

    def chip_ahead(by):
        return lax.rem(chip + by, n.chips)

    def chip_behind(by):
        return lax.rem(chip + n.chips - by, n.chips)

    def remote(src, dst, send_sem, recv_sem, to_f=None, to_c=None):
        return pltpu.make_async_remote_copy(
            src_ref=src,
            dst_ref=dst,
            send_sem=send_sem,
            recv_sem=recv_sem,
            device_id={"fsdp": f if to_f is None else to_f, "ctx": c if to_c is None else to_c},
            device_id_type=pl.DeviceIdType.MESH,
        )

    def send(src, dst, send_sem, recv_sem, to_f=None, to_c=None):
        remote(src, dst, send_sem, recv_sem, to_f, to_c).start()

    def sent(like, send_sem, cond=None):
        wait = remote(like, like, send_sem, send_sem).wait_send
        sends.append(wait if cond is None else (lambda: pl.when(cond)(wait)))

    def arrived(dst, recv_sem):
        remote(dst, dst, recv_sem, recv_sem).wait_recv()

    def send_if(cond, src, dst, send_sem, recv_sem, to_c):
        pl.when(cond)(remote(src, dst, send_sem, recv_sem, None, to_c).start)

    barrier = pltpu.get_barrier_semaphore()

    def greet(to_f, to_c):
        pl.semaphore_signal(
            barrier,
            inc=1,
            device_id={"fsdp": to_f, "ctx": to_c},
            device_id_type=pl.DeviceIdType.MESH,
        )

    for by in range(1, n.ctx):
        greet(f, ahead(by))
    for by in range(1, n.fsdp):
        greet(lax.rem(f + by, n.fsdp), c)
    pl.semaphore_wait(barrier, n.ctx - 1 + n.fsdp - 1)

    right, left = jnp.minimum(c + 1, n.ctx - 1), jnp.maximum(c - 1, 0)
    part_rows, piece_rows = rows // PARTS, rows // (PARTS * PIECES)

    def pieces_of(k):
        return range(k * PIECES, (k + 1) * PIECES)

    def part_of(buf, j, i):
        return buf.at[j, pl.ds(i * piece_rows, piece_rows), :]

    def gather_start(src, buf, sem, k, to=None):
        for i in pieces_of(k):
            gather_piece(src, buf, sem, i, to)

    def gather_piece(src, buf, sem, i, to=None):
        piece = src.at[pl.ds(i * piece_rows, piece_rows), :]
        here = part_of(buf, c, i)
        up, down = c + 1 < n.ctx, c > 0
        if to == "between":
            up, down = c + 1 < n.ctx - 1, c > 1
        elif to == "ends":
            up, down = c + 1 == n.ctx - 1, c == 1
        send_if(up, piece, here, sem[0].at[0, 0], sem[1].at[c, i], right)
        send_if(down, piece, here, sem[0].at[1, 0], sem[1].at[c, i], left)

    def gather_relay(buf, sem, by, k, source=None):
        low, high = jnp.maximum(c - by, 0), jnp.minimum(c + by, n.ctx - 1)
        from_low, from_high = c - by >= 0, c + by < n.ctx
        if source == "end":
            from_low, from_high = c == by, c + by == n.ctx - 1
        elif source == "between":
            from_low, from_high = c > by, c + by < n.ctx - 1
        for i in pieces_of(k):
            piece, here = part_of(buf, low, i), sem[1].at[low, i]
            pl.when(from_low)(functools.partial(arrived, piece, here))
            send_if(from_low & (c + 1 < n.ctx), piece, piece, sem[0].at[0, by], here, right)
            piece, here = part_of(buf, high, i), sem[1].at[high, i]
            pl.when(from_high)(functools.partial(arrived, piece, here))
            send_if(from_high & (c > 0), piece, piece, sem[0].at[1, by], here, left)

    def gather_sent(buf, sem):
        for by in range(n.ctx - 1):
            sent(buf.at[0], sem[0].at[0, by], (c - by >= 0) & (c + 1 < n.ctx))
            sent(buf.at[0], sem[0].at[1, by], (c + by < n.ctx) & (c > 0))

    def rows_of(k):
        return slice(k * part_rows, (k + 1) * part_rows)

    def scatter_send(cond, part, there, sem, target, i, way, to_c):
        send_if(
            cond,
            part_of(part, target, i),
            part_of(there, target, i),
            sem[0].at[way, target - 1 + way],
            sem[1].at[way, target - 1 + way, i],
            to_c,
        )

    def scatter_add(part, there, sem, target, i, way):
        arrived(part_of(there, target, i), sem[1].at[way, target - 1 + way, i])
        span = slice(i * piece_rows, (i + 1) * piece_rows)
        part[target, span, :] = (
            part[target, span, :].astype(F32) + there[target, span, :].astype(F32)
        ).astype(BF16)

    def scatter_start(g, k):
        for step in range(n.ctx - 1):
            for i in pieces_of(k):
                scatter_send(c == n.ctx - 1, g.part, g.high, g.sem, step, i, 1, left)
                scatter_send(c == 0, g.part, g.low, g.sem, n.ctx - 1 - step, i, 0, right)

    def scatter_up(g, step, k, cond):
        target = n.ctx - 1 - step
        cond = cond & (c < target) & (c > 0)
        for i in pieces_of(k):
            pl.when(cond)(functools.partial(scatter_add, g.part, g.low, g.sem, target, i, 0))
            scatter_send(cond, g.part, g.low, g.sem, target, i, 0, right)

    def scatter_down(g, step, k, cond):
        cond = cond & (c > step) & (c + 1 < n.ctx)
        for i in pieces_of(k):
            pl.when(cond)(functools.partial(scatter_add, g.part, g.high, g.sem, step, i, 1))
            scatter_send(cond, g.part, g.high, g.sem, step, i, 1, left)

    def scatter_near(g, k):
        for step in range(n.ctx - 1):
            scatter_up(g, step, k, c < n.ctx // 2)
            scatter_down(g, step, k, c >= n.ctx // 2)

    def scatter_far(g, k):
        for step in range(n.ctx - 1):
            scatter_up(g, step, k, c >= n.ctx // 2)
            scatter_down(g, step, k, c < n.ctx // 2)

    def scatter_sent(g):
        for target in range(1, n.ctx):
            sent(g.part.at[0], g.sem[0].at[0, target - 1], c < target)
        for target in range(n.ctx - 1):
            sent(g.part.at[0], g.sem[0].at[1, target], c > target)

    def scatter_total(g, out, k):
        span = rows_of(k)
        out[span, :] = out[span, :] + g.part[c, span, :].astype(F32)

        @pl.when(c > 0)
        def _():
            for i in pieces_of(k):
                arrived(part_of(g.low, c, i), g.sem[1].at[0, jnp.maximum(c - 1, 0), i])
            out[span, :] = out[span, :] + g.low[c, span, :].astype(F32)

        @pl.when(c + 1 < n.ctx)
        def _():
            for i in pieces_of(k):
                arrived(part_of(g.high, c, i), g.sem[1].at[1, jnp.minimum(c, n.ctx - 2), i])
            out[span, :] = out[span, :] + g.high[c, span, :].astype(F32)

    def block_of(buf, index, span):
        return buf.at[pl.ds(pl.multiple_of(index * block, block), block), pl.ds(*span)]

    def blocks_of(buf, count, span):
        return buf.at[pl.ds(0, count * block), pl.ds(*span)]

    def piece_of(buf, line, at, width):
        start = pl.multiple_of(f * block + line * shard, shard)
        return buf.at[pl.ds(start, shard), pl.ds(at, width)]

    def weights_send(shards, cols, buf, send_sem, recv_sems, now=None):
        for by in range(1, n.ctx):
            at_end = (ahead(by) == 0) | (ahead(by) == n.ctx - 1)
            at = 0
            for src, width, recv_sem in zip(shards, cols, recv_sems):
                column = pl.multiple_of(ahead(by) * width, HEAD_DIM)
                copy = remote(
                    src.at[:, pl.ds(column, width)],
                    piece_of(buf, c, at, width),
                    send_sem.at[by - 1],
                    recv_sem.at[by - 1],
                    None,
                    ahead(by),
                )
                if now is None:
                    copy.start()
                else:
                    pl.when(at_end if now == "ends" else ~at_end)(copy.start)
                at += width

    def weights_sent(cols, buf, send_sem):
        for by in range(1, n.ctx):
            sent(piece_of(buf, c, 0, sum(cols)), send_sem.at[by - 1])

    def weights_own(shards, cols, buf, first):
        at, out = 0, []
        for i, (src, width) in enumerate(zip(shards, cols)):
            column = pl.multiple_of(c * width, HEAD_DIM)
            copy = pltpu.make_async_copy(
                src.at[:, pl.ds(column, width)],
                piece_of(buf, c, at, width),
                r.local_sem.at[first + i],
            )
            copy.start()
            out.append(copy)
            at += width
        return out

    def weights_spread(own, g):
        for copy in own:
            copy.wait()
        for by in range(1, n.ctx):
            arrived(piece_of(g.buf, behind(by), *g.span), g.line.at[by - 1])
        mine = block_of(g.buf, f, g.span)
        for by in range(1, n.chips):
            send(mine, mine, g.sem.at[0], g.sem.at[2 + by], chip_ahead(by) * 2 + core)
        send(mine, mine, g.sem.at[1], g.sem.at[2], sibling)

    def weights_forward(g):
        for by in range(1, n.chips):
            piece = block_of(g.buf, chip_behind(by) * 2 + core, g.span)
            arrived(piece, g.sem.at[2 + by])
            send(piece, piece, g.sem.at[1], g.sem.at[2], sibling)
        sent(blocks_of(g.buf, n.chips - 1, g.span), g.sem.at[0])
        sent(blocks_of(g.buf, n.chips, g.span), g.sem.at[1])

    def weights_wait(g):
        arrived(blocks_of(g.buf, n.chips, g.span), g.sem.at[2])

    def share_of(buf, index, span):
        return buf.at[pl.ds(pl.multiple_of(index * block, block), block), pl.ds(*span)]

    def grads_pair(g):
        for by in (*range(1, n.chips), 0):
            send(
                share_of(g.whole, chip_ahead(by) * 2 + 1 - core, g.span),
                g.pair.at[by, :, pl.ds(*g.span)],
                g.sem.at[0],
                g.sem.at[5 + by],
                sibling,
            )
        sent(g.pair.at[:, :, pl.ds(*g.span)], g.sem.at[0])

    def grads_plane(g):
        for by in range(1, n.chips):
            theirs = g.pair.at[by, :, pl.ds(*g.span)]
            arrived(theirs, g.sem.at[5 + by])
            piece = share_of(g.whole, chip_ahead(by) * 2 + core, g.span)
            piece[...] = (piece[...].astype(F32) + theirs[...].astype(F32)).astype(BF16)
            send(
                piece,
                g.plane.at[by - 1, :, pl.ds(*g.span)],
                g.sem.at[1],
                g.sem.at[2],
                chip_ahead(by) * 2 + core,
            )
        sent(g.plane.at[:, :, pl.ds(*g.span)], g.sem.at[1])

    def grads_line(g):
        theirs = g.pair.at[0, :, pl.ds(*g.span)]
        arrived(theirs, g.sem.at[5])
        acc = share_of(g.whole, f, g.span)[...].astype(F32) + theirs[...].astype(F32)
        arrived(g.plane.at[:, :, pl.ds(*g.span)], g.sem.at[2])
        for by in range(1, n.chips):
            acc = acc + g.plane[by - 1, :, pl.ds(*g.span)].astype(F32)
        g.total[:, pl.ds(*g.span)] = acc.astype(BF16)
        for by in range(1, n.ctx):
            start = pl.multiple_of(ahead(by) * shard, shard)
            send(
                g.total.at[pl.ds(start, shard), pl.ds(*g.span)],
                g.land.at[c, :, pl.ds(*g.span)],
                g.sem.at[3],
                g.sem.at[4],
                None,
                ahead(by),
            )
        sent(g.land.at[pl.ds(0, n.ctx - 1), :, pl.ds(*g.span)], g.sem.at[3])
        start = pl.multiple_of(c * shard, shard)
        g.land[c, :, pl.ds(*g.span)] = g.total[pl.ds(start, shard), pl.ds(*g.span)]

    def grads_wait(g):
        arrived(g.land.at[pl.ds(0, n.ctx - 1), :, pl.ds(*g.span)], g.sem.at[4])

    def small_peers(way):
        if way == "line":
            return [(n.fsdp + by - 1, f, ahead(by)) for by in range(1, n.ctx)]
        return [(by - 1, lax.rem(f + by, n.fsdp), c) for by in range(1, n.fsdp)]

    def small_span(incoming, way):
        first, count = (n.fsdp, n.ctx - 1) if way == "line" else (0, n.fsdp - 1)
        return incoming.at[pl.ds(first, count)]

    def small_send(src, incoming, sem, way):
        at = 2 * (way == "line")
        for slot, to_f, to_c in small_peers(way):
            send(src, incoming.at[slot], sem.at[at], sem.at[at + 1], to_f, to_c)
        sent(small_span(incoming, way), sem.at[at])

    def small_sum(own, incoming, sem, way):
        total = own[...]
        arrived(small_span(incoming, way), sem.at[2 * (way == "line") + 1])
        for slot, _, _ in small_peers(way):
            total = total + incoming[slot]
        return total

    def save_lines(first, line):
        for j in range(n.lines):
            row = slice(first + j, first + j + 1)
            r.g1_acc[3, row, :] += line[:, j * HEAD_DIM : (j + 1) * HEAD_DIM]

    attn_shards, mlp_shards = (r.wq, r.wk, r.wv, r.wo), (r.wg, r.wu, r.wd)
    attn_cols, mlp_cols = n.cols[:4], n.cols[4:]
    q_cols, k_cols, _, o_cols = attn_cols
    ff = mlp_cols[0]
    group = n.heads // n.kv
    factor = 1.0 / math.sqrt(HEAD_DIM)

    o_at = q_cols + 2 * k_cols
    attn_bufs = dict(whole=r.ga, pair=r.ga_sib, plane=r.ga_in, total=r.ga_z, land=r.ga_land)
    mlp_bufs = dict(whole=r.gm, pair=r.gm_sib, plane=r.gm_in, total=r.gm_z, land=r.gm_land)
    line_q, line_o, line_m = (r.rcv_w.at[i] for i in range(3))
    plane_q = types.SimpleNamespace(buf=r.wa, span=(0, o_at), line=line_q, sem=r.sem_pq)
    plane_o = types.SimpleNamespace(buf=r.wa, span=(o_at, o_cols), line=line_o, sem=r.sem_po)
    plane_m = types.SimpleNamespace(buf=r.wm, span=(0, n.mlp_cols), line=line_m, sem=r.sem_pm)
    to_attn = (r.wa, r.snd_w.at[0], (line_q, line_q, line_q, line_o))
    to_mlp = (r.wm, r.snd_w.at[1], (line_m, line_m, line_m))
    group_m = types.SimpleNamespace(
        **mlp_bufs, span=(0, n.mlp_cols), sem=r.sem_gm
    )
    group_o = types.SimpleNamespace(
        **attn_bufs, span=(o_at, o_cols), sem=r.sem_go
    )
    group_q = types.SimpleNamespace(**attn_bufs, span=(0, o_at), sem=r.sem_gq)

    sum_o, sum_y, sum_x2, sum_x1 = (
        types.SimpleNamespace(part=part, low=low, high=high, sem=sem)
        for part, low, high, sem in (
            (r.p_o, r.l_o, r.r_o, r.sem_o),
            (r.p_y, r.l_y, r.r_y, r.sem_y),
            (r.p_x2, r.l_x2, r.r_x2, r.sem_x2),
            (r.p_x1, r.l_x1, r.r_x1, r.sem_x1),
        )
    )
    r.g1_acc[3] = jnp.zeros_like(r.g1_acc[3])

    me = f * n.ctx + c
    lane = lax.broadcasted_iota(jnp.int32, (1, HEAD_DIM), 1)

    def place(row, at, size, first):
        moved = pltpu.roll(r.gains[...], lax.rem(at + HEAD_DIM - first, HEAD_DIM), 1)
        r.gp[pl.ds(row, 1), :] = jnp.where((lane >= at) & (lane < at + size), moved, 0.0)

    r.gp[...] = jnp.zeros_like(r.gp)
    row, at = me * n.each // HEAD_DIM, lax.rem(me * n.each, HEAD_DIM)
    place(row, at, n.each, 0)
    place(n.lines + row, at, n.each, n.each)
    place(2 * n.lines, me * n.few, n.few, 2 * n.each)
    place(2 * n.lines + 1, me * n.few, n.few, 2 * n.each + n.few)
    small_send(r.gp, r.g0_in, r.sem_g0, "line")
    weights_send(attn_shards, attn_cols, *to_attn)
    for k in range(PARTS):
        gather_start(r.hidden, r.xb, r.sem_xb, k)
    own_x = pltpu.make_async_copy(r.hidden, r.xb.at[c], r.local_sem.at[7])
    own_x.start()
    own_g = pltpu.make_async_copy(r.cot, r.gb.at[c], r.local_sem.at[8])
    own_g.start()
    own_attn = weights_own(attn_shards, attn_cols, r.wa, 0)
    own_mlp = weights_own(mlp_shards, mlp_cols, r.wm, 4)
    r.g0_acc[0] = small_sum(r.gp, r.g0_in, r.sem_g0, "line")
    small_send(r.g0_acc.at[0], r.g0_in, r.sem_g0, "plane")
    slots = r.order.shape[1]
    slot_len = n.tokens // slots
    exponent = (lane % (HEAD_DIM // 2)).astype(F32) * (2.0 / HEAD_DIM)
    inverse = jnp.exp(-exponent * math.log(1000000.0))
    sign = jnp.where(lane < HEAD_DIM // 2, -1.0, 1.0)
    for j in range(slots):
        first = r.order[0, j] * slot_len
        span = slice(j * slot_len, (j + 1) * slot_len)
        position = first + lax.broadcasted_iota(jnp.int32, (slot_len, HEAD_DIM), 0)
        r.posq[span, :] = position
        angle = position.astype(F32) * inverse
        r.cos[span, :] = jnp.cos(angle)
        r.sin[span, :] = jnp.sin(angle) * sign
    token = lax.broadcasted_iota(jnp.int32, (1, n.tokens), 1)
    posk = token % slot_len
    for j in range(slots):
        posk = posk + jnp.where(token // slot_len == j, r.order[0, j] * slot_len, 0)
    r.posk[...] = posk
    weights_spread(own_attn[:3], plane_q)
    weights_spread(own_attn[3:], plane_o)
    r.g0_acc[2] = small_sum(r.g0_acc.at[0], r.g0_in, r.sem_g0, "plane")
    for j in range(n.lines):
        r.gv[0, :, j * HEAD_DIM : (j + 1) * HEAD_DIM] = r.g0_acc[2, j : j + 1, :]
        r.gv[1, :, j * HEAD_DIM : (j + 1) * HEAD_DIM] = r.g0_acc[
            2, n.lines + j : n.lines + j + 1, :
        ]
    qgain = r.g0_acc[2, 2 * n.lines : 2 * n.lines + 1, :]
    kgain = r.g0_acc[2, 2 * n.lines + 1 : 2 * n.lines + 2, :]
    attn_gain, mlp_gain = r.gv[0], r.gv[1]
    for by in range(1, n.ctx):
        if by == n.ctx - 1:
            weights_send(mlp_shards, mlp_cols, *to_mlp, "between")
            for k in range(PARTS):
                gather_start(r.cot, r.gb, r.sem_gb, k, "between")
        for k in range(PARTS):
            gather_relay(r.xb, r.sem_xb, by, k)
    own_x.wait()
    own_g.wait()

    def norm_rows(j, carry):
        x = r.xb[j].astype(F32)
        start = pl.multiple_of(j * rows, rows)
        r.xn[pl.ds(start, rows), :] = (x * rms(x) * attn_gain).astype(BF16)
        return carry

    lax.fori_loop(0, n.ctx, norm_rows, 0)
    weights_forward(plane_q)
    weights_wait(plane_q)
    weights_send(mlp_shards, mlp_cols, *to_mlp, "ends")
    for k in range(PARTS):
        gather_start(r.cot, r.gb, r.sem_gb, k, "ends")

    cosine, sine = r.cos, r.sin
    tile = 2 * HEAD_DIM if n.kv % 2 == 0 else HEAD_DIM
    for at in range(0, q_cols + 2 * k_cols, tile):
        product = mm(r.xn[...], r.wa[:, at : at + tile])
        for part in range(tile // HEAD_DIM):
            head = at // HEAD_DIM + part
            u = product[:, part * HEAD_DIM : (part + 1) * HEAD_DIM]
            if head < n.heads:
                r.qp[head] = u
                r.qr[head] = rope_fwd(u * rms(u) * qgain, cosine[...], sine[...]).astype(BF16)
            elif head < n.heads + n.kv:
                r.kp[head - n.heads] = u
                r.kr[head - n.heads] = rope_fwd(u * rms(u) * kgain, cosine[...], sine[...]).astype(
                    BF16
                )
            else:
                r.vv[head - n.heads - n.kv] = u.astype(BF16)
    weights_forward(plane_o)
    half = n.tokens // 2

    def head_forward(h, carry):
        kv = h // group
        for q0 in (0, half):
            s = mm(r.qr[h, q0 : q0 + half, :], r.kr[kv], LAST_AXIS)
            allowed = r.posk[...] <= r.posq[q0 : q0 + half, 0:1]
            e = jnp.where(allowed, jnp.exp(s * factor), 0.0)
            r.es[h, q0 : q0 + half, :] = e
            total = jnp.sum(e, axis=-1, keepdims=True)
            a = mm(e.astype(BF16), r.vv[kv]) / total
            r.af[h, q0 : q0 + half, :] = a
            lane = pl.multiple_of(h * HEAD_DIM, HEAD_DIM)
            r.at[q0 : q0 + half, pl.ds(lane, HEAD_DIM)] = a.astype(BF16)
        return carry

    lax.fori_loop(0, n.heads, head_forward, 0)
    weights_wait(plane_o)

    def by_rows(left, right, out):
        step = 2 * HEAD_DIM
        for at in range(0, d, step):
            product = mm(left[...], right(slice(at, at + step)), LAST_AXIS)
            out[:, :, at : at + step] = product.astype(BF16).reshape(n.ctx, rows, step)

    by_rows(r.at, lambda span: r.wa[span, o_at:], r.p_o)
    for k in range(PARTS):
        scatter_start(sum_o, k)
    weights_spread(own_mlp, plane_m)

    def residual(k):
        span = rows_of(k)
        r.ho[span, :] = r.xb[c, span, :].astype(F32)
        scatter_total(sum_o, r.ho, k)
        own = r.ho[span, :]
        r.mb[c, span, :] = (own * rms(own) * mlp_gain).astype(BF16)
        gather_start(r.mb.at[c], r.mb, r.sem_mb, k)

    gather_relay(r.gb, r.sem_gb, 1, 0)
    scatter_near(sum_o, 0)
    scatter_far(sum_o, 0)
    for by in range(2, n.ctx - 1):
        gather_relay(r.gb, r.sem_gb, by, 0)
    residual(0)
    scatter_near(sum_o, 1)
    gather_relay(r.mb, r.sem_mb, 1, 0, "between")
    scatter_far(sum_o, 1)
    residual(1)
    gather_relay(r.mb, r.sem_mb, 1, 0, "end")
    gather_relay(r.mb, r.sem_mb, 1, 1, "between")
    for by in range(2, n.ctx - 1):
        gather_relay(r.mb, r.sem_mb, by, 0)
    weights_forward(plane_m)
    gather_relay(r.mb, r.sem_mb, n.ctx - 1, 0)
    gather_relay(r.gb, r.sem_gb, n.ctx - 1, 0)
    weights_wait(plane_m)

    tile = 2 * HEAD_DIM if ff % (2 * HEAD_DIM) == 0 else HEAD_DIM
    span_rows = n.ctx * part_rows

    def mlp_part(k):
        span = rows_of(k)
        mixed = r.mb[:, span, :].reshape(span_rows, d)
        upstream = r.gb[:, span, :].reshape(span_rows, d)
        for at in range(0, ff, tile):
            gate = mm(mixed, r.wm[:, at : at + tile])
            up = mm(mixed, r.wm[:, ff + at : ff + at + tile])
            back = mm(upstream, r.wm[:, 2 * ff + at : 2 * ff + at + tile])
            sig = jax.nn.sigmoid(gate)
            swish = gate * sig
            shape = (n.ctx, part_rows, tile)
            r.hid[:, span, at : at + tile] = (swish * up).astype(BF16).reshape(shape)
            r.dgu[:, span, at : at + tile] = (
                (back * up * sig * (1.0 + gate * (1.0 - sig))).astype(BF16).reshape(shape)
            )
            r.dgu[:, span, ff + at : ff + at + tile] = (
                (back * swish).astype(BF16).reshape(shape)
            )
        both = r.dgu[:, span, :].reshape(span_rows, 2 * ff)
        for at in range(0, d, 2 * HEAD_DIM):
            product = mm(both, r.wm[at : at + 2 * HEAD_DIM, : 2 * ff], LAST_AXIS).astype(BF16)
            r.p_x2[:, span, at : at + 2 * HEAD_DIM] = product.reshape(
                n.ctx, part_rows, 2 * HEAD_DIM
            )
        scatter_start(sum_x2, k)

    def residual_back(k):
        span = rows_of(k)
        r.dh[span, :] = jnp.zeros((part_rows, d), F32)
        scatter_total(sum_x2, r.dh, k)
        own = r.ho[span, :]
        from_norm, term = norm_back(own, rms(own), mlp_gain, r.dh[span, :])
        save_lines(n.lines, jnp.sum(term, axis=0, keepdims=True))
        r.dh[span, :] = r.gb[c, span, :].astype(F32) + from_norm
        r.rb[c, span, :] = r.dh[span, :].astype(BF16)
        gather_start(r.rb.at[c], r.rb, r.sem_rb, k)

    gather_relay(r.mb, r.sem_mb, 1, 1, "end")
    gather_relay(r.gb, r.sem_gb, 1, 1)
    for by in range(2, n.ctx - 1):
        gather_relay(r.gb, r.sem_gb, by, 1)
        gather_relay(r.mb, r.sem_mb, by, 1)
    mlp_part(0)
    scatter_near(sum_x2, 0)
    scatter_far(sum_x2, 0)
    gather_relay(r.mb, r.sem_mb, n.ctx - 1, 1)
    gather_relay(r.gb, r.sem_gb, n.ctx - 1, 1)
    mlp_part(1)
    residual_back(0)
    hidden = r.hid[...].reshape(n.tokens, ff)
    by_rows(hidden, lambda span: r.wm[span, 2 * ff :], r.p_y)
    scatter_start(sum_y, 0)
    mixed = r.mb[...].reshape(n.tokens, d)
    upstream = r.gb[...].reshape(n.tokens, d)
    for at in range(0, 2 * ff, tile):
        part = r.dgu[:, :, at : at + tile].reshape(n.tokens, tile)
        r.gm[:, at : at + tile] = mm(mixed, part, FIRST_AXIS).astype(BF16)
    for at in range(0, ff, tile):
        part = r.hid[:, :, at : at + tile].reshape(n.tokens, tile)
        r.gm[:, 2 * ff + at : 2 * ff + at + tile] = mm(upstream, part, FIRST_AXIS).astype(BF16)
    grads_pair(group_m)
    scatter_near(sum_x2, 1)
    gather_relay(r.rb, r.sem_rb, 1, 0, "between")
    grads_plane(group_m)
    scatter_far(sum_x2, 1)
    gather_relay(r.rb, r.sem_rb, 1, 0, "end")
    for by in range(2, n.ctx - 1):
        gather_relay(r.rb, r.sem_rb, by, 0)
    residual_back(1)
    scatter_start(sum_y, 1)
    scatter_near(sum_y, 0)
    gather_relay(r.rb, r.sem_rb, 1, 1, "between")
    gather_relay(r.rb, r.sem_rb, 1, 1, "end")
    for by in range(2, n.ctx - 1):
        gather_relay(r.rb, r.sem_rb, by, 1)
    scatter_far(sum_y, 0)
    for k in range(PARTS):
        gather_relay(r.rb, r.sem_rb, n.ctx - 1, k)

    upstream = r.rb[...].reshape(n.tokens, d)
    for at in range(0, o_cols, HEAD_DIM):
        r.da[at // HEAD_DIM] = mm(upstream, r.wa[:, o_at + at : o_at + at + HEAD_DIM])
    r.ga[:, o_at:] = mm(upstream, r.at[...], FIRST_AXIS).astype(BF16)
    grads_pair(group_o)
    scatter_near(sum_y, 1)
    r.dk[...] = jnp.zeros_like(r.dk)
    r.dv[...] = jnp.zeros_like(r.dv)

    def head_backward(h, carry):
        kv = h // group
        for q0 in (0, half):
            span = slice(q0, q0 + half)
            e = r.es[h, span, :]
            total = jnp.sum(e, axis=-1, keepdims=True)
            da = r.da[h, span, :]
            w = (da / total).astype(BF16)
            dl = jnp.sum(da * r.af[h, span, :], axis=-1, keepdims=True) / total
            ds = (e * (mm(w, r.vv[kv], LAST_AXIS) - dl)).astype(BF16)
            r.ds[span, :] = ds
            r.eb[span, :] = e.astype(BF16)
            r.wb[span, :] = w
            r.da[h, span, :] = mm(ds, r.kr[kv])
        r.dk[kv] = r.dk[kv] + mm(r.ds[...], r.qr[h], FIRST_AXIS)
        r.dv[kv] = r.dv[kv] + mm(r.eb[...], r.wb[...], FIRST_AXIS)
        return carry

    lax.fori_loop(0, n.heads // 2, head_backward, 0)
    grads_line(group_m)
    lax.fori_loop(n.heads // 2, n.heads, head_backward, 0)

    def query_backward(h, term):
        u = r.qp[h]
        du, gain_term = norm_back(
            u, rms(u), qgain, rope_bwd(r.da[h] * factor, cosine[...], sine[...])
        )
        lane = pl.multiple_of(h * HEAD_DIM, HEAD_DIM)
        r.dqkv[:, pl.ds(lane, HEAD_DIM)] = du.astype(BF16)
        return term + jnp.sum(gain_term, axis=0, keepdims=True)

    q_term = lax.fori_loop(0, n.heads, query_backward, jnp.zeros((1, HEAD_DIM), F32))
    grads_plane(group_o)
    k_term = jnp.zeros((1, HEAD_DIM), F32)
    for kv in range(n.kv):
        u = r.kp[kv]
        du, gain_term = norm_back(
            u, rms(u), kgain, rope_bwd(r.dk[kv] * factor, cosine[...], sine[...])
        )
        at = q_cols + kv * HEAD_DIM
        r.dqkv[:, at : at + HEAD_DIM] = du.astype(BF16)
        at += k_cols
        r.dqkv[:, at : at + HEAD_DIM] = r.dv[kv].astype(BF16)
        k_term = k_term + jnp.sum(gain_term, axis=0, keepdims=True)
    by_rows(r.dqkv, lambda span: r.wa[span, :o_at], r.p_x1)
    for k in range(PARTS):
        scatter_start(sum_x1, k)
    for at in range(0, o_at, 2 * HEAD_DIM):
        r.ga[:, at : at + 2 * HEAD_DIM] = mm(
            r.xn[...], r.dqkv[:, at : at + 2 * HEAD_DIM], FIRST_AXIS
        ).astype(BF16)
    grads_pair(group_q)
    for j in range(n.ctx):
        x = r.xb[j].astype(F32)
        share = r.p_x1[j].astype(F32) * (x * rms(x))
        save_lines(0, jnp.sum(share, axis=0, keepdims=True))
    r.g1_acc[3, 2 * n.lines : 2 * n.lines + 1, :] = q_term
    r.g1_acc[3, 2 * n.lines + 1 : 2 * n.lines + 2, :] = k_term
    small_send(r.g1_acc.at[3], r.g1_in, r.sem_g1, "plane")
    grads_plane(group_q)
    scatter_near(sum_x1, 0)
    scatter_far(sum_y, 1)
    scatter_far(sum_x1, 0)
    grads_line(group_o)
    r.g1_acc[1] = small_sum(r.g1_acc.at[3], r.g1_in, r.sem_g1, "plane")
    small_send(r.g1_acc.at[1], r.g1_in, r.sem_g1, "line")
    scatter_near(sum_x1, 1)
    grads_line(group_q)
    scatter_far(sum_x1, 1)
    for k in range(PARTS):
        scatter_total(sum_y, r.ho, k)
    r.out_hidden[...] = r.ho[...].astype(BF16)
    r.out_input[...] = jnp.zeros_like(r.out_input)
    for k in range(PARTS):
        scatter_total(sum_x1, r.out_input, k)
    x = r.xb[c].astype(F32)
    from_norm, _ = norm_back(x, rms(x), attn_gain, r.out_input[...])
    r.out_input[...] = r.dh[...] + from_norm
    grads_wait(group_m)
    grads_wait(group_o)
    grads_wait(group_q)
    r.out_gains[...] = small_sum(r.g1_acc.at[1], r.g1_in, r.sem_g1, "line")
    for buf, sem in ((r.xb, r.sem_xb), (r.gb, r.sem_gb), (r.mb, r.sem_mb), (r.rb, r.sem_rb)):
        gather_sent(buf, sem)
    for g in (sum_o, sum_y, sum_x2, sum_x1):
        scatter_sent(g)
    weights_sent(attn_cols, *to_attn[:2])
    weights_sent(mlp_cols, *to_mlp[:2])
    for wait in sends:
        wait()


def fused(
    ctx,
    fsdp,
    hidden_in,
    block_order,
    cotangent,
    q_weight,
    k_weight,
    v_weight,
    o_weight,
    attn_gain,
    query_gain,
    key_gain,
    mlp_gain,
    gate_weight,
    up_weight,
    down_weight,
):
    shards = (q_weight, k_weight, v_weight, o_weight, gate_weight, up_weight, down_weight)
    n = Sizes(ctx, fsdp, hidden_in.shape[1], shards)
    gains = jnp.concatenate([attn_gain, mlp_gain, query_gain, key_gain]).astype(F32)
    gains = jnp.pad(gains, (0, HEAD_DIM - gains.shape[0])).reshape(1, HEAD_DIM)
    hbm, vmem = pl.BlockSpec(memory_space=pl.ANY), pl.BlockSpec(memory_space=pltpu.VMEM)
    inputs = dict(
        hidden=(hidden_in[0], hbm),
        cot=(cotangent[0], hbm),
        wq=(q_weight, hbm),
        wk=(k_weight, hbm),
        wv=(v_weight, hbm),
        wo=(o_weight, hbm),
        wg=(gate_weight, hbm),
        wu=(up_weight, hbm),
        wd=(down_weight, hbm),
        gains=(gains, vmem),
        order=(block_order, pl.BlockSpec(memory_space=pltpu.SMEM)),
    )
    outputs = dict(
        out_hidden=jax.ShapeDtypeStruct((n.rows, n.width), BF16),
        out_input=jax.ShapeDtypeStruct((n.rows, n.width), F32),
        ga_land=jax.ShapeDtypeStruct((ctx, n.shard, n.attn_cols), BF16),
        gm_land=jax.ShapeDtypeStruct((ctx, n.shard, n.mlp_cols), BF16),
        out_gains=jax.ShapeDtypeStruct((n.gain_rows, HEAD_DIM), F32),
    )
    scratch = scratch_of(n)
    landed = pl.pallas_call(
        functools.partial(layer_kernel, n, [*inputs, *outputs, *scratch]),
        out_shape=tuple(outputs.values()),
        in_specs=[spec for _, spec in inputs.values()],
        out_specs=tuple(vmem for _ in outputs),
        scratch_shapes=list(scratch.values()),
        compiler_params=pltpu.CompilerParams(
            collective_id=0, has_side_effects=True, vmem_limit_bytes=VMEM_LIMIT
        ),
        name="layer",
    )(*[value for value, _ in inputs.values()])

    finals = [(n.rows, n.width, BF16), (n.rows, n.width, F32)]
    finals += [(*s.shape, F32) for s in shards]
    finals += [(1, size, F32) for size in (n.each, n.each, n.few, n.few)]
    result, input_grad, oq, ok, ov, oo, og, ou, od, *gains = pl.pallas_call(
        functools.partial(emit_kernel, n),
        out_shape=tuple(jax.ShapeDtypeStruct(f[:2], f[2]) for f in finals),
        in_specs=[vmem] * len(outputs),
        out_specs=tuple(vmem for _ in finals),
        name="emit",
    )(*landed)
    return (
        result[None],
        input_grad[None],
        oq,
        ok,
        ov,
        oo,
        gains[0].reshape(n.each),
        gains[2].reshape(n.few),
        gains[3].reshape(n.few),
        gains[1].reshape(n.each),
        og,
        ou,
        od,
    )


def emit_kernel(n, result, input_grad, attn_land, mlp_land, sums, *outs):
    outs[0][...] = result[...]
    outs[1][...] = input_grad[...]
    which = 2
    for land, widths in ((attn_land, n.cols[:4]), (mlp_land, n.cols[4:])):
        at = 0
        for width in widths:
            for j in range(n.ctx):
                outs[which][:, j * width : (j + 1) * width] = land[j, :, at : at + width].astype(
                    F32
                )
            at += width
            which += 1
    me = lax.axis_index("fsdp") * n.ctx + lax.axis_index("ctx")
    row, at = me * n.each // HEAD_DIM, lax.rem(me * n.each, HEAD_DIM)
    for out, (line, lane) in zip(
        outs[which:],
        (
            (row, at),
            (n.lines + row, at),
            (2 * n.lines, me * n.few),
            (2 * n.lines + 1, me * n.few),
        ),
    ):
        back = lax.rem(HEAD_DIM - lane, HEAD_DIM)
        out[...] = pltpu.roll(sums[pl.ds(line, 1), :], back, 1)[:, : out.shape[1]]


def fits(ctx, fsdp, shard_rows):
    per_tile = HEAD_DIM % (2 * shard_rows) == 0 and HEAD_DIM % (ctx * fsdp) == 0
    return per_tile and shard_rows % 16 == 0 and fsdp % 2 == 0 and KV_HEADS % ctx == 0


def solution(mesh):
    ctx, fsdp = mesh.shape["ctx"], mesh.shape["fsdp"]
    tokens = P("fsdp", "ctx", None)
    matrix = P(("fsdp", "ctx"), None)
    vector = P(("fsdp", "ctx"))
    def step(hidden_in, block_order, cotangent, q_weight, *rest):
        whole = fused if fits(ctx, fsdp, q_weight.shape[0]) else local
        return whole(ctx, fsdp, hidden_in, block_order, cotangent, q_weight, *rest)

    return jax.shard_map(
        step,
        mesh=mesh,
        in_specs=(tokens, P("fsdp", None), tokens)
        + (matrix,) * 4
        + (vector,) * 4
        + (matrix,) * 3,
        out_specs=(tokens,) * 2 + (matrix,) * 4 + (vector,) * 4 + (matrix,) * 3,
        check_vma=False,
    )
```

```python
import functools
import math
import types

import jax
import jax.numpy as jnp
from jax import lax
from jax.experimental import pallas as pl
from jax.experimental.pallas import tpu as pltpu
from jax.sharding import PartitionSpec as P

HEADS = 16
KV_HEADS = 8
HEAD_DIM = 128
EPSILON = 1e-06
FIRST_AXIS = (((0,), (0,)), ((), ()))
LAST_AXIS = (((1,), (1,)), ((), ()))
BF16 = jnp.bfloat16
F32 = jnp.float32
VMEM_LIMIT = 67043328
PARTS = 2
PIECES = 2


def mm(left, right, dims=(((1,), (0,)), ((), ()))):
    return lax.dot_general(left, right, dims, preferred_element_type=F32)


def rms(signal):
    return lax.rsqrt(jnp.mean(signal * signal, axis=-1, keepdims=True) + EPSILON)


def norm_back(signal, inverse_rms, gain_vec, upstream):
    unit_values = signal * inverse_rms
    scaled_up = upstream * gain_vec
    inner = scaled_up - unit_values * jnp.mean(scaled_up * unit_values, axis=-1, keepdims=True)
    return (inverse_rms * inner, upstream * unit_values)


def rope_tables(positions, head_width):
    exponent = jnp.arange(head_width // 2, dtype=F32) * (2.0 / head_width)
    inverse = jnp.exp(-exponent * math.log(1000000.0))
    angles = positions.astype(F32)[:, None] * inverse[None, :]
    angles = jnp.concatenate([angles, angles], axis=-1)
    return (jnp.cos(angles), jnp.sin(angles))


def rotate(signal, cosine, sine):
    half = signal.shape[-1] // 2
    turned = jnp.concatenate([-signal[..., half:], signal[..., :half]], axis=-1)
    return signal * cosine + turned * sine


def rotate_back(upstream, cosine, sine):
    half = upstream.shape[-1] // 2
    scaled_up = upstream * sine
    return upstream * cosine + jnp.concatenate(
        [scaled_up[..., half:], -scaled_up[..., :half]], axis=-1
    )


def gather_columns(ctx, shards):
    rows = shards[0].shape[0]
    cut = [s.reshape(rows, ctx, s.shape[1] // ctx).transpose(1, 0, 2) for s in shards]
    widths = [c.shape[2] for c in cut]
    both = jnp.concatenate(cut, axis=2)
    both = lax.all_to_all(both, "ctx", 0, 0, tiled=True)
    both = both.reshape(ctx * rows, -1)
    whole = lax.all_gather(both, "fsdp", axis=0, tiled=True)
    out, at = [], 0
    for width in widths:
        out.append(whole[:, at : at + width])
        at += width
    return out


def scatter_grads(ctx, fsdp, grads):
    rows = grads[0].shape[0] // (ctx * fsdp)
    widths = [g.shape[1] for g in grads]
    both = jnp.concatenate([g.astype(BF16) for g in grads], axis=1)
    both = lax.psum_scatter(both, "fsdp", scatter_dimension=0, tiled=True)
    both = lax.all_to_all(both.reshape(ctx, rows, -1), "ctx", 0, 0, tiled=True)
    out, at = [], 0
    for width in widths:
        piece = both[:, :, at : at + width]
        out.append(piece.transpose(1, 0, 2).reshape(rows, ctx * width).astype(F32))
        at += width
    return out


def ctx_gather(rows):
    return lax.all_gather(rows, "ctx", axis=0, tiled=True)


def ctx_scatter(partial):
    return lax.psum_scatter(partial.astype(BF16), "ctx", scatter_dimension=0, tiled=True).astype(
        F32
    )


def local(
    ctx,
    fsdp,
    hidden_in,
    block_order,
    cotangent,
    q_weight,
    k_weight,
    v_weight,
    o_weight,
    attn_gain,
    query_gain,
    key_gain,
    mlp_gain,
    gate_weight,
    up_weight,
    down_weight,
):
    inputs = hidden_in[0].astype(F32)
    row_count = inputs.shape[0]
    tokens = row_count * ctx
    slots = block_order.shape[1]
    block_len = tokens // slots
    heads, kv_heads = HEADS // ctx, KV_HEADS // ctx
    group = heads // kv_heads
    factor = 1.0 / math.sqrt(HEAD_DIM)
    positions = (
        block_order[0][:, None] * block_len + jnp.arange(block_len, dtype=jnp.int32)[None, :]
    ).reshape(-1)
    cosine, sine = rope_tables(positions, HEAD_DIM)
    cosine, sine = cosine[:, None, :], sine[:, None, :]

    both = ("fsdp", "ctx")
    norm_gain, qgain, kgain, mlp_norm_gain = (
        lax.all_gather(g, both, axis=0, tiled=True).astype(F32)
        for g in (attn_gain, query_gain, key_gain, mlp_gain)
    )
    norm_scale = rms(inputs)
    normed = ctx_gather((inputs * norm_scale * norm_gain).astype(BF16))
    upstream = ctx_gather(cotangent[0])
    q_full, k_full, v_full, o_full = gather_columns(ctx, (q_weight, k_weight, v_weight, o_weight))
    gate_full, up_full, down_full = gather_columns(ctx, (gate_weight, up_weight, down_weight))

    query_proj = mm(normed, q_full).reshape(tokens, heads, HEAD_DIM)
    key_proj = mm(normed, k_full).reshape(tokens, kv_heads, HEAD_DIM)
    value_low = mm(normed, v_full).astype(BF16).reshape(tokens, kv_heads, HEAD_DIM)
    query_scale, key_scale = rms(query_proj), rms(key_proj)
    query_low = (
        rotate(query_proj * query_scale * qgain, cosine, sine)
        .astype(BF16)
        .reshape(tokens, kv_heads, group, HEAD_DIM)
    )
    key_low = rotate(key_proj * key_scale * kgain, cosine, sine).astype(BF16)
    scores = jnp.einsum("rkgd,nkd->kgrn", query_low, key_low, preferred_element_type=F32) * factor
    allowed = positions[None, :] <= positions[:, None]
    weights_exp = jnp.where(allowed, jnp.exp(scores), 0.0)
    denominator = jnp.sum(weights_exp, axis=-1)
    weights_low = weights_exp.astype(BF16)
    numerator = jnp.einsum("kgrn,nkd->rkgd", weights_low, value_low, preferred_element_type=F32)
    denom_rows = jnp.transpose(denominator, (2, 0, 1))[..., None]
    attn_full = numerator / denom_rows
    attn_low = attn_full.astype(BF16).reshape(tokens, heads * HEAD_DIM)
    residual = inputs + ctx_scatter(mm(attn_low, o_full, LAST_AXIS))

    mix_scale = rms(residual)
    mixed = ctx_gather((residual * mix_scale * mlp_norm_gain).astype(BF16))
    gate_val = mm(mixed, gate_full)
    up_val = mm(mixed, up_full)
    sigmoid_gate = jax.nn.sigmoid(gate_val)
    swish_gate = gate_val * sigmoid_gate
    hidden_low = (swish_gate * up_val).astype(BF16)
    result = residual + ctx_scatter(mm(hidden_low, down_full, LAST_AXIS))
    hidden_grad = mm(upstream, down_full)
    gate_back = (
        hidden_grad * up_val * sigmoid_gate * (1.0 + gate_val * (1.0 - sigmoid_gate))
    ).astype(BF16)
    up_back = (hidden_grad * swish_gate).astype(BF16)
    mixed_grad = ctx_scatter(mm(gate_back, gate_full, LAST_AXIS) + mm(up_back, up_full, LAST_AXIS))
    resid_from_norm, mlp_gain_term = norm_back(residual, mix_scale, mlp_norm_gain, mixed_grad)
    residual_grad = cotangent[0].astype(F32) + resid_from_norm
    mlp_grads = scatter_grads(
        ctx,
        fsdp,
        (
            mm(mixed, gate_back, FIRST_AXIS),
            mm(mixed, up_back, FIRST_AXIS),
            mm(upstream, hidden_low, FIRST_AXIS),
        ),
    )
    resid_low = ctx_gather(residual_grad.astype(BF16))

    attn_grad = mm(resid_low, o_full).reshape(tokens, kv_heads, group, HEAD_DIM)
    share_low = (attn_grad / denom_rows).astype(BF16)
    denom_grad = jnp.transpose(jnp.sum(attn_grad * attn_full, axis=-1), (1, 2, 0)) / denominator
    weight_grad = jnp.einsum("rkgd,nkd->kgrn", share_low, value_low, preferred_element_type=F32)
    score_low = (weights_exp * (weight_grad - denom_grad[..., None])).astype(BF16)
    query_rot = (
        jnp.einsum("kgrn,nkd->rkgd", score_low, key_low, preferred_element_type=F32) * factor
    ).reshape(tokens, heads, HEAD_DIM)
    key_rot = (
        jnp.einsum("kgrn,rkgd->nkd", score_low, query_low, preferred_element_type=F32) * factor
    )
    value_back = (
        jnp.einsum("kgrn,rkgd->nkd", weights_low, share_low, preferred_element_type=F32)
        .reshape(tokens, kv_heads * HEAD_DIM)
        .astype(BF16)
    )
    query_grad, query_term = norm_back(
        query_proj, query_scale, qgain, rotate_back(query_rot, cosine, sine)
    )
    key_grad, key_term = norm_back(key_proj, key_scale, kgain, rotate_back(key_rot, cosine, sine))
    query_back = query_grad.reshape(tokens, heads * HEAD_DIM).astype(BF16)
    key_back = key_grad.reshape(tokens, kv_heads * HEAD_DIM).astype(BF16)
    normed_grad = ctx_scatter(
        mm(query_back, q_full, LAST_AXIS)
        + mm(key_back, k_full, LAST_AXIS)
        + mm(value_back, v_full, LAST_AXIS)
    )
    input_from_norm, attn_gain_term = norm_back(inputs, norm_scale, norm_gain, normed_grad)
    input_grad = residual_grad + input_from_norm
    attn_grads = scatter_grads(
        ctx,
        fsdp,
        (
            mm(normed, query_back, FIRST_AXIS),
            mm(normed, key_back, FIRST_AXIS),
            mm(normed, value_back, FIRST_AXIS),
            mm(resid_low, attn_low, FIRST_AXIS),
        ),
    )
    gains = (
        jnp.sum(attn_gain_term, axis=0),
        jnp.sum(query_term, axis=(0, 1)),
        jnp.sum(key_term, axis=(0, 1)),
        jnp.sum(mlp_gain_term, axis=0),
    )
    gains = [lax.psum_scatter(g, both, scatter_dimension=0, tiled=True) for g in gains]
    return (
        result.astype(BF16)[None],
        input_grad[None],
        *attn_grads,
        *gains,
        *mlp_grads,
    )


def rope_fwd(u, cosine, sine):
    return u * cosine + pltpu.roll(u, HEAD_DIM // 2, u.ndim - 1) * sine


def rope_bwd(du, cosine, sine):
    return du * cosine - pltpu.roll(du, HEAD_DIM // 2, du.ndim - 1) * sine


class Sizes:
    def __init__(self, ctx, fsdp, rows, shards):
        self.ctx, self.fsdp, self.rows = ctx, fsdp, rows
        self.chips = fsdp // 2
        self.shard = shards[0].shape[0]
        self.block = self.shard * ctx
        self.width = self.block * fsdp
        self.tokens = rows * ctx
        self.heads, self.kv = HEADS // ctx, KV_HEADS // ctx
        self.cols = [s.shape[1] // ctx for s in shards]
        self.attn_cols = sum(self.cols[:4])
        self.mlp_cols = sum(self.cols[4:])
        self.lines = self.width // HEAD_DIM
        self.gain_rows = 8 * ((2 * self.lines + 2 + 7) // 8)
        self.each, self.few = self.width // (ctx * fsdp), HEAD_DIM // (ctx * fsdp)


def scratch_of(n):
    bf, f32 = (lambda *s: pltpu.VMEM(s, BF16)), (lambda *s: pltpu.VMEM(s, F32))
    sem = lambda *s: pltpu.SemaphoreType.DMA(s)
    c, d, s, h, kv = n.ctx, n.width, n.tokens, n.heads, n.kv
    ff = n.cols[4]
    out = dict(
        wa=bf(d, n.attn_cols),
        wm=bf(d, n.mlp_cols),
        xb=bf(c, n.rows, d),
        gb=bf(c, n.rows, d),
        mb=bf(c, n.rows, d),
        rb=bf(c, n.rows, d),
        xn=bf(s, d),
        qp=f32(h, s, HEAD_DIM),
        kp=f32(kv, s, HEAD_DIM),
        qr=bf(h, s, HEAD_DIM),
        kr=bf(kv, s, HEAD_DIM),
        vv=bf(kv, s, HEAD_DIM),
        es=f32(h, s, s),
        af=f32(h, s, HEAD_DIM),
        at=bf(s, h * HEAD_DIM),
        da=f32(h, s, HEAD_DIM),
        dk=f32(kv, s, HEAD_DIM),
        dv=f32(kv, s, HEAD_DIM),
        ds=bf(s, s),
        eb=bf(s, s),
        wb=bf(s, HEAD_DIM),
        dqkv=bf(s, (h + 2 * kv) * HEAD_DIM),
        hid=bf(c, n.rows, ff),
        dgu=bf(c, n.rows, 2 * ff),
        ho=f32(n.rows, d),
        dh=f32(n.rows, d),
        gv=f32(2, 1, d),
        gp=f32(n.gain_rows, HEAD_DIM),
        cos=f32(s, HEAD_DIM),
        sin=f32(s, HEAD_DIM),
        posq=pltpu.VMEM((s, HEAD_DIM), jnp.int32),
        posk=pltpu.VMEM((1, s), jnp.int32),
        ga=bf(d, n.attn_cols),
        gm=bf(d, n.mlp_cols),
        ga_sib=bf(n.chips, n.block, n.attn_cols),
        gm_sib=bf(n.chips, n.block, n.mlp_cols),
        ga_in=bf(n.chips - 1, n.block, n.attn_cols),
        gm_in=bf(n.chips - 1, n.block, n.mlp_cols),
        ga_z=bf(n.block, n.attn_cols),
        gm_z=bf(n.block, n.mlp_cols),
        local_sem=sem(9),
    )
    for name in ("o", "y", "x2", "x1"):
        out["p_" + name] = bf(c, n.rows, d)
        out["l_" + name] = bf(c, n.rows, d)
        out["r_" + name] = bf(c, n.rows, d)
        out["snd_" + name] = sem(2, c - 1)
        out["rcv_" + name] = sem(2, c - 1, PARTS * PIECES)
    for name in ("xb", "gb", "mb", "rb"):
        out["snd_" + name] = sem(2, c - 1)
        out["rcv_" + name] = sem(c, PARTS * PIECES)
    out["snd_w"] = sem(2, c - 1)
    out["rcv_w"] = sem(3, c - 1)
    for name in ("pq", "po", "pm"):
        out["sem_" + name] = sem(3 + n.chips)
    for name in ("gm", "go", "gq"):
        out["sem_" + name] = sem(5 + n.chips)
    for name in ("g0", "g1"):
        out[name + "_in"] = f32(n.fsdp + c, n.gain_rows, HEAD_DIM)
        out[name + "_acc"] = f32(4, n.gain_rows, HEAD_DIM)
        out["sem_" + name] = sem(4)
    return out


def layer_kernel(n, names, *refs):
    r = types.SimpleNamespace(**dict(zip(names, refs)))
    for name in ("o", "y", "x2", "x1", "xb", "gb", "mb", "rb"):
        setattr(r, "sem_" + name, (getattr(r, "snd_" + name), getattr(r, "rcv_" + name)))
    c, f = lax.axis_index("ctx"), lax.axis_index("fsdp")
    chip, core = f // 2, f % 2
    sibling = chip * 2 + 1 - core
    rows, d, block, shard = n.rows, n.width, n.block, n.shard
    sends = []

    def ahead(by):
        return lax.rem(c + by, n.ctx)

    def behind(by):
        return lax.rem(c + n.ctx - by, n.ctx)

    def chip_ahead(by):
        return lax.rem(chip + by, n.chips)

    def chip_behind(by):
        return lax.rem(chip + n.chips - by, n.chips)

    def remote(src, dst, send_sem, recv_sem, to_f=None, to_c=None):
        return pltpu.make_async_remote_copy(
            src_ref=src,
            dst_ref=dst,
            send_sem=send_sem,
            recv_sem=recv_sem,
            device_id={"fsdp": f if to_f is None else to_f, "ctx": c if to_c is None else to_c},
            device_id_type=pl.DeviceIdType.MESH,
        )

    def send(src, dst, send_sem, recv_sem, to_f=None, to_c=None):
        remote(src, dst, send_sem, recv_sem, to_f, to_c).start()

    def sent(like, send_sem, cond=None):
        wait = remote(like, like, send_sem, send_sem).wait_send
        sends.append(wait if cond is None else (lambda: pl.when(cond)(wait)))

    def arrived(dst, recv_sem):
        remote(dst, dst, recv_sem, recv_sem).wait_recv()

    def send_if(cond, src, dst, send_sem, recv_sem, to_c):
        pl.when(cond)(remote(src, dst, send_sem, recv_sem, None, to_c).start)

    barrier = pltpu.get_barrier_semaphore()

    def greet(to_f, to_c):
        pl.semaphore_signal(
            barrier,
            inc=1,
            device_id={"fsdp": to_f, "ctx": to_c},
            device_id_type=pl.DeviceIdType.MESH,
        )

    for by in range(1, n.ctx):
        greet(f, ahead(by))
    for by in range(1, n.fsdp):
        greet(lax.rem(f + by, n.fsdp), c)
    pl.semaphore_wait(barrier, n.ctx - 1 + n.fsdp - 1)

    right, left = jnp.minimum(c + 1, n.ctx - 1), jnp.maximum(c - 1, 0)
    part_rows, piece_rows = rows // PARTS, rows // (PARTS * PIECES)

    def pieces_of(k):
        return range(k * PIECES, (k + 1) * PIECES)

    def part_of(buf, j, i):
        return buf.at[j, pl.ds(i * piece_rows, piece_rows), :]

    def gather_start(src, buf, sem, k, to=None):
        for i in pieces_of(k):
            gather_piece(src, buf, sem, i, to)

    def gather_piece(src, buf, sem, i, to=None):
        piece = src.at[pl.ds(i * piece_rows, piece_rows), :]
        here = part_of(buf, c, i)
        up, down = c + 1 < n.ctx, c > 0
        if to == "between":
            up, down = c + 1 < n.ctx - 1, c > 1
        elif to == "ends":
            up, down = c + 1 == n.ctx - 1, c == 1
        send_if(up, piece, here, sem[0].at[0, 0], sem[1].at[c, i], right)
        send_if(down, piece, here, sem[0].at[1, 0], sem[1].at[c, i], left)

    def gather_relay(buf, sem, by, k, source=None):
        low, high = jnp.maximum(c - by, 0), jnp.minimum(c + by, n.ctx - 1)
        from_low, from_high = c - by >= 0, c + by < n.ctx
        if source == "end":
            from_low, from_high = c == by, c + by == n.ctx - 1
        elif source == "between":
            from_low, from_high = c > by, c + by < n.ctx - 1
        for i in pieces_of(k):
            piece, here = part_of(buf, low, i), sem[1].at[low, i]
            pl.when(from_low)(functools.partial(arrived, piece, here))
            send_if(from_low & (c + 1 < n.ctx), piece, piece, sem[0].at[0, by], here, right)
            piece, here = part_of(buf, high, i), sem[1].at[high, i]
            pl.when(from_high)(functools.partial(arrived, piece, here))
            send_if(from_high & (c > 0), piece, piece, sem[0].at[1, by], here, left)

    def gather_sent(buf, sem):
        for by in range(n.ctx - 1):
            sent(buf.at[0], sem[0].at[0, by], (c - by >= 0) & (c + 1 < n.ctx))
            sent(buf.at[0], sem[0].at[1, by], (c + by < n.ctx) & (c > 0))

    def rows_of(k):
        return slice(k * part_rows, (k + 1) * part_rows)

    def scatter_send(cond, part, there, sem, target, i, way, to_c):
        send_if(
            cond,
            part_of(part, target, i),
            part_of(there, target, i),
            sem[0].at[way, target - 1 + way],
            sem[1].at[way, target - 1 + way, i],
            to_c,
        )

    def scatter_add(part, there, sem, target, i, way):
        arrived(part_of(there, target, i), sem[1].at[way, target - 1 + way, i])
        span = slice(i * piece_rows, (i + 1) * piece_rows)
        part[target, span, :] = (
            part[target, span, :].astype(F32) + there[target, span, :].astype(F32)
        ).astype(BF16)

    def scatter_start(g, k):
        for step in range(n.ctx - 1):
            for i in pieces_of(k):
                scatter_send(c == n.ctx - 1, g.part, g.high, g.sem, step, i, 1, left)
                scatter_send(c == 0, g.part, g.low, g.sem, n.ctx - 1 - step, i, 0, right)

    def scatter_up(g, step, k, cond):
        target = n.ctx - 1 - step
        cond = cond & (c < target) & (c > 0)
        for i in pieces_of(k):
            pl.when(cond)(functools.partial(scatter_add, g.part, g.low, g.sem, target, i, 0))
            scatter_send(cond, g.part, g.low, g.sem, target, i, 0, right)

    def scatter_down(g, step, k, cond):
        cond = cond & (c > step) & (c + 1 < n.ctx)
        for i in pieces_of(k):
            pl.when(cond)(functools.partial(scatter_add, g.part, g.high, g.sem, step, i, 1))
            scatter_send(cond, g.part, g.high, g.sem, step, i, 1, left)

    def scatter_near(g, k):
        for step in range(n.ctx - 1):
            scatter_up(g, step, k, c < n.ctx // 2)
            scatter_down(g, step, k, c >= n.ctx // 2)

    def scatter_far(g, k):
        for step in range(n.ctx - 1):
            scatter_up(g, step, k, c >= n.ctx // 2)
            scatter_down(g, step, k, c < n.ctx // 2)

    def scatter_sent(g):
        for target in range(1, n.ctx):
            sent(g.part.at[0], g.sem[0].at[0, target - 1], c < target)
        for target in range(n.ctx - 1):
            sent(g.part.at[0], g.sem[0].at[1, target], c > target)

    def scatter_total(g, out, k):
        span = rows_of(k)
        out[span, :] = out[span, :] + g.part[c, span, :].astype(F32)

        @pl.when(c > 0)
        def _():
            for i in pieces_of(k):
                arrived(part_of(g.low, c, i), g.sem[1].at[0, jnp.maximum(c - 1, 0), i])
            out[span, :] = out[span, :] + g.low[c, span, :].astype(F32)

        @pl.when(c + 1 < n.ctx)
        def _():
            for i in pieces_of(k):
                arrived(part_of(g.high, c, i), g.sem[1].at[1, jnp.minimum(c, n.ctx - 2), i])
            out[span, :] = out[span, :] + g.high[c, span, :].astype(F32)

    def block_of(buf, index, span):
        return buf.at[pl.ds(pl.multiple_of(index * block, block), block), pl.ds(*span)]

    def blocks_of(buf, count, span):
        return buf.at[pl.ds(0, count * block), pl.ds(*span)]

    def piece_of(buf, line, at, width):
        start = pl.multiple_of(f * block + line * shard, shard)
        return buf.at[pl.ds(start, shard), pl.ds(at, width)]

    def weights_send(shards, cols, buf, send_sem, recv_sems, now=None):
        for by in range(1, n.ctx):
            at_end = (ahead(by) == 0) | (ahead(by) == n.ctx - 1)
            at = 0
            for src, width, recv_sem in zip(shards, cols, recv_sems):
                column = pl.multiple_of(ahead(by) * width, HEAD_DIM)
                copy = remote(
                    src.at[:, pl.ds(column, width)],
                    piece_of(buf, c, at, width),
                    send_sem.at[by - 1],
                    recv_sem.at[by - 1],
                    None,
                    ahead(by),
                )
                if now is None:
                    copy.start()
                else:
                    pl.when(at_end if now == "ends" else ~at_end)(copy.start)
                at += width

    def weights_sent(cols, buf, send_sem):
        for by in range(1, n.ctx):
            sent(piece_of(buf, c, 0, sum(cols)), send_sem.at[by - 1])

    def weights_own(shards, cols, buf, first):
        at, out = 0, []
        for i, (src, width) in enumerate(zip(shards, cols)):
            column = pl.multiple_of(c * width, HEAD_DIM)
            copy = pltpu.make_async_copy(
                src.at[:, pl.ds(column, width)],
                piece_of(buf, c, at, width),
                r.local_sem.at[first + i],
            )
            copy.start()
            out.append(copy)
            at += width
        return out

    def weights_spread(own, g):
        for copy in own:
            copy.wait()
        for by in range(1, n.ctx):
            arrived(piece_of(g.buf, behind(by), *g.span), g.line.at[by - 1])
        mine = block_of(g.buf, f, g.span)
        for by in range(1, n.chips):
            send(mine, mine, g.sem.at[0], g.sem.at[2 + by], chip_ahead(by) * 2 + core)
        send(mine, mine, g.sem.at[1], g.sem.at[2], sibling)

    def weights_forward(g):
        for by in range(1, n.chips):
            piece = block_of(g.buf, chip_behind(by) * 2 + core, g.span)
            arrived(piece, g.sem.at[2 + by])
            send(piece, piece, g.sem.at[1], g.sem.at[2], sibling)
        sent(blocks_of(g.buf, n.chips - 1, g.span), g.sem.at[0])
        sent(blocks_of(g.buf, n.chips, g.span), g.sem.at[1])

    def weights_wait(g):
        arrived(blocks_of(g.buf, n.chips, g.span), g.sem.at[2])

    def share_of(buf, index, span):
        return buf.at[pl.ds(pl.multiple_of(index * block, block), block), pl.ds(*span)]

    def grads_pair(g):
        for by in (*range(1, n.chips), 0):
            send(
                share_of(g.whole, chip_ahead(by) * 2 + 1 - core, g.span),
                g.pair.at[by, :, pl.ds(*g.span)],
                g.sem.at[0],
                g.sem.at[5 + by],
                sibling,
            )
        sent(g.pair.at[:, :, pl.ds(*g.span)], g.sem.at[0])

    def grads_plane(g):
        for by in range(1, n.chips):
            theirs = g.pair.at[by, :, pl.ds(*g.span)]
            arrived(theirs, g.sem.at[5 + by])
            piece = share_of(g.whole, chip_ahead(by) * 2 + core, g.span)
            piece[...] = (piece[...].astype(F32) + theirs[...].astype(F32)).astype(BF16)
            send(
                piece,
                g.plane.at[by - 1, :, pl.ds(*g.span)],
                g.sem.at[1],
                g.sem.at[2],
                chip_ahead(by) * 2 + core,
            )
        sent(g.plane.at[:, :, pl.ds(*g.span)], g.sem.at[1])

    def grads_line(g):
        theirs = g.pair.at[0, :, pl.ds(*g.span)]
        arrived(theirs, g.sem.at[5])
        acc = share_of(g.whole, f, g.span)[...].astype(F32) + theirs[...].astype(F32)
        arrived(g.plane.at[:, :, pl.ds(*g.span)], g.sem.at[2])
        for by in range(1, n.chips):
            acc = acc + g.plane[by - 1, :, pl.ds(*g.span)].astype(F32)
        g.total[:, pl.ds(*g.span)] = acc.astype(BF16)
        for by in range(1, n.ctx):
            start = pl.multiple_of(ahead(by) * shard, shard)
            send(
                g.total.at[pl.ds(start, shard), pl.ds(*g.span)],
                g.land.at[c, :, pl.ds(*g.span)],
                g.sem.at[3],
                g.sem.at[4],
                None,
                ahead(by),
            )
        sent(g.land.at[pl.ds(0, n.ctx - 1), :, pl.ds(*g.span)], g.sem.at[3])
        start = pl.multiple_of(c * shard, shard)
        g.land[c, :, pl.ds(*g.span)] = g.total[pl.ds(start, shard), pl.ds(*g.span)]

    def grads_wait(g):
        arrived(g.land.at[pl.ds(0, n.ctx - 1), :, pl.ds(*g.span)], g.sem.at[4])

    def small_peers(way):
        if way == "line":
            return [(n.fsdp + by - 1, f, ahead(by)) for by in range(1, n.ctx)]
        return [(by - 1, lax.rem(f + by, n.fsdp), c) for by in range(1, n.fsdp)]

    def small_span(incoming, way):
        first, count = (n.fsdp, n.ctx - 1) if way == "line" else (0, n.fsdp - 1)
        return incoming.at[pl.ds(first, count)]

    def small_send(src, incoming, sem, way):
        at = 2 * (way == "line")
        for slot, to_f, to_c in small_peers(way):
            send(src, incoming.at[slot], sem.at[at], sem.at[at + 1], to_f, to_c)
        sent(small_span(incoming, way), sem.at[at])

    def small_sum(own, incoming, sem, way):
        total = own[...]
        arrived(small_span(incoming, way), sem.at[2 * (way == "line") + 1])
        for slot, _, _ in small_peers(way):
            total = total + incoming[slot]
        return total

    def save_lines(first, line):
        for j in range(n.lines):
            row = slice(first + j, first + j + 1)
            r.g1_acc[3, row, :] += line[:, j * HEAD_DIM : (j + 1) * HEAD_DIM]

    attn_shards, mlp_shards = (r.wq, r.wk, r.wv, r.wo), (r.wg, r.wu, r.wd)
    attn_cols, mlp_cols = n.cols[:4], n.cols[4:]
    q_cols, k_cols, _, o_cols = attn_cols
    ff = mlp_cols[0]
    group = n.heads // n.kv
    factor = 1.0 / math.sqrt(HEAD_DIM)

    o_at = q_cols + 2 * k_cols
    attn_bufs = dict(whole=r.ga, pair=r.ga_sib, plane=r.ga_in, total=r.ga_z, land=r.ga_land)
    mlp_bufs = dict(whole=r.gm, pair=r.gm_sib, plane=r.gm_in, total=r.gm_z, land=r.gm_land)
    line_q, line_o, line_m = (r.rcv_w.at[i] for i in range(3))
    plane_q = types.SimpleNamespace(buf=r.wa, span=(0, o_at), line=line_q, sem=r.sem_pq)
    plane_o = types.SimpleNamespace(buf=r.wa, span=(o_at, o_cols), line=line_o, sem=r.sem_po)
    plane_m = types.SimpleNamespace(buf=r.wm, span=(0, n.mlp_cols), line=line_m, sem=r.sem_pm)
    to_attn = (r.wa, r.snd_w.at[0], (line_q, line_q, line_q, line_o))
    to_mlp = (r.wm, r.snd_w.at[1], (line_m, line_m, line_m))
    group_m = types.SimpleNamespace(
        **mlp_bufs, span=(0, n.mlp_cols), sem=r.sem_gm
    )
    group_o = types.SimpleNamespace(
        **attn_bufs, span=(o_at, o_cols), sem=r.sem_go
    )
    group_q = types.SimpleNamespace(**attn_bufs, span=(0, o_at), sem=r.sem_gq)

    sum_o, sum_y, sum_x2, sum_x1 = (
        types.SimpleNamespace(part=part, low=low, high=high, sem=sem)
        for part, low, high, sem in (
            (r.p_o, r.l_o, r.r_o, r.sem_o),
            (r.p_y, r.l_y, r.r_y, r.sem_y),
            (r.p_x2, r.l_x2, r.r_x2, r.sem_x2),
            (r.p_x1, r.l_x1, r.r_x1, r.sem_x1),
        )
    )
    r.g1_acc[3] = jnp.zeros_like(r.g1_acc[3])

    me = f * n.ctx + c
    lane = lax.broadcasted_iota(jnp.int32, (1, HEAD_DIM), 1)

    def place(row, at, size, first):
        moved = pltpu.roll(r.gains[...], lax.rem(at + HEAD_DIM - first, HEAD_DIM), 1)
        r.gp[pl.ds(row, 1), :] = jnp.where((lane >= at) & (lane < at + size), moved, 0.0)

    r.gp[...] = jnp.zeros_like(r.gp)
    row, at = me * n.each // HEAD_DIM, lax.rem(me * n.each, HEAD_DIM)
    place(row, at, n.each, 0)
    place(n.lines + row, at, n.each, n.each)
    place(2 * n.lines, me * n.few, n.few, 2 * n.each)
    place(2 * n.lines + 1, me * n.few, n.few, 2 * n.each + n.few)
    small_send(r.gp, r.g0_in, r.sem_g0, "line")
    weights_send(attn_shards, attn_cols, *to_attn)
    for k in range(PARTS):
        gather_start(r.hidden, r.xb, r.sem_xb, k)
    own_x = pltpu.make_async_copy(r.hidden, r.xb.at[c], r.local_sem.at[7])
    own_x.start()
    own_g = pltpu.make_async_copy(r.cot, r.gb.at[c], r.local_sem.at[8])
    own_g.start()
    own_attn = weights_own(attn_shards, attn_cols, r.wa, 0)
    own_mlp = weights_own(mlp_shards, mlp_cols, r.wm, 4)
    r.g0_acc[0] = small_sum(r.gp, r.g0_in, r.sem_g0, "line")
    small_send(r.g0_acc.at[0], r.g0_in, r.sem_g0, "plane")
    slots = r.order.shape[1]
    slot_len = n.tokens // slots
    exponent = (lane % (HEAD_DIM // 2)).astype(F32) * (2.0 / HEAD_DIM)
    inverse = jnp.exp(-exponent * math.log(1000000.0))
    sign = jnp.where(lane < HEAD_DIM // 2, -1.0, 1.0)
    for j in range(slots):
        first = r.order[0, j] * slot_len
        span = slice(j * slot_len, (j + 1) * slot_len)
        position = first + lax.broadcasted_iota(jnp.int32, (slot_len, HEAD_DIM), 0)
        r.posq[span, :] = position
        angle = position.astype(F32) * inverse
        r.cos[span, :] = jnp.cos(angle)
        r.sin[span, :] = jnp.sin(angle) * sign
    token = lax.broadcasted_iota(jnp.int32, (1, n.tokens), 1)
    posk = token % slot_len
    for j in range(slots):
        posk = posk + jnp.where(token // slot_len == j, r.order[0, j] * slot_len, 0)
    r.posk[...] = posk
    weights_spread(own_attn[:3], plane_q)
    weights_spread(own_attn[3:], plane_o)
    r.g0_acc[2] = small_sum(r.g0_acc.at[0], r.g0_in, r.sem_g0, "plane")
    for j in range(n.lines):
        r.gv[0, :, j * HEAD_DIM : (j + 1) * HEAD_DIM] = r.g0_acc[2, j : j + 1, :]
        r.gv[1, :, j * HEAD_DIM : (j + 1) * HEAD_DIM] = r.g0_acc[
            2, n.lines + j : n.lines + j + 1, :
        ]
    qgain = r.g0_acc[2, 2 * n.lines : 2 * n.lines + 1, :]
    kgain = r.g0_acc[2, 2 * n.lines + 1 : 2 * n.lines + 2, :]
    attn_gain, mlp_gain = r.gv[0], r.gv[1]
    for by in range(1, n.ctx):
        if by == n.ctx - 1:
            weights_send(mlp_shards, mlp_cols, *to_mlp, "between")
            for k in range(PARTS):
                gather_start(r.cot, r.gb, r.sem_gb, k, "between")
        for k in range(PARTS):
            gather_relay(r.xb, r.sem_xb, by, k)
    own_x.wait()
    own_g.wait()

    def norm_rows(j, carry):
        x = r.xb[j].astype(F32)
        start = pl.multiple_of(j * rows, rows)
        r.xn[pl.ds(start, rows), :] = (x * rms(x) * attn_gain).astype(BF16)
        return carry

    lax.fori_loop(0, n.ctx, norm_rows, 0)
    weights_forward(plane_q)
    weights_wait(plane_q)
    weights_send(mlp_shards, mlp_cols, *to_mlp, "ends")
    for k in range(PARTS):
        gather_start(r.cot, r.gb, r.sem_gb, k, "ends")

    cosine, sine = r.cos, r.sin
    tile = 2 * HEAD_DIM if n.kv % 2 == 0 else HEAD_DIM
    for at in range(0, q_cols + 2 * k_cols, tile):
        product = mm(r.xn[...], r.wa[:, at : at + tile])
        for part in range(tile // HEAD_DIM):
            head = at // HEAD_DIM + part
            u = product[:, part * HEAD_DIM : (part + 1) * HEAD_DIM]
            if head < n.heads:
                r.qp[head] = u
                r.qr[head] = rope_fwd(u * rms(u) * qgain, cosine[...], sine[...]).astype(BF16)
            elif head < n.heads + n.kv:
                r.kp[head - n.heads] = u
                r.kr[head - n.heads] = rope_fwd(u * rms(u) * kgain, cosine[...], sine[...]).astype(
                    BF16
                )
            else:
                r.vv[head - n.heads - n.kv] = u.astype(BF16)
    weights_forward(plane_o)
    half = n.tokens // 2

    def head_forward(h, carry):
        kv = h // group
        for q0 in (0, half):
            s = mm(r.qr[h, q0 : q0 + half, :], r.kr[kv], LAST_AXIS)
            allowed = r.posk[...] <= r.posq[q0 : q0 + half, 0:1]
            e = jnp.where(allowed, jnp.exp(s * factor), 0.0)
            r.es[h, q0 : q0 + half, :] = e
            total = jnp.sum(e, axis=-1, keepdims=True)
            a = mm(e.astype(BF16), r.vv[kv]) / total
            r.af[h, q0 : q0 + half, :] = a
            lane = pl.multiple_of(h * HEAD_DIM, HEAD_DIM)
            r.at[q0 : q0 + half, pl.ds(lane, HEAD_DIM)] = a.astype(BF16)
        return carry

    lax.fori_loop(0, n.heads, head_forward, 0)
    weights_wait(plane_o)

    def by_rows(left, right, out):
        step = 2 * HEAD_DIM
        for at in range(0, d, step):
            product = mm(left[...], right(slice(at, at + step)), LAST_AXIS)
            out[:, :, at : at + step] = product.astype(BF16).reshape(n.ctx, rows, step)

    by_rows(r.at, lambda span: r.wa[span, o_at:], r.p_o)
    for k in range(PARTS):
        scatter_start(sum_o, k)
    weights_spread(own_mlp, plane_m)

    def residual(k):
        span = rows_of(k)
        r.ho[span, :] = r.xb[c, span, :].astype(F32)
        scatter_total(sum_o, r.ho, k)
        own = r.ho[span, :]
        r.mb[c, span, :] = (own * rms(own) * mlp_gain).astype(BF16)
        gather_start(r.mb.at[c], r.mb, r.sem_mb, k)

    gather_relay(r.gb, r.sem_gb, 1, 0)
    scatter_near(sum_o, 0)
    scatter_far(sum_o, 0)
    for by in range(2, n.ctx - 1):
        gather_relay(r.gb, r.sem_gb, by, 0)
    residual(0)
    scatter_near(sum_o, 1)
    gather_relay(r.mb, r.sem_mb, 1, 0, "between")
    scatter_far(sum_o, 1)
    residual(1)
    gather_relay(r.mb, r.sem_mb, 1, 0, "end")
    gather_relay(r.mb, r.sem_mb, 1, 1, "between")
    for by in range(2, n.ctx - 1):
        gather_relay(r.mb, r.sem_mb, by, 0)
    weights_forward(plane_m)
    gather_relay(r.mb, r.sem_mb, n.ctx - 1, 0)
    gather_relay(r.gb, r.sem_gb, n.ctx - 1, 0)
    weights_wait(plane_m)

    tile = 2 * HEAD_DIM if ff % (2 * HEAD_DIM) == 0 else HEAD_DIM
    span_rows = n.ctx * part_rows

    def mlp_part(k):
        span = rows_of(k)
        mixed = r.mb[:, span, :].reshape(span_rows, d)
        upstream = r.gb[:, span, :].reshape(span_rows, d)
        for at in range(0, ff, tile):
            gate = mm(mixed, r.wm[:, at : at + tile])
            up = mm(mixed, r.wm[:, ff + at : ff + at + tile])
            back = mm(upstream, r.wm[:, 2 * ff + at : 2 * ff + at + tile])
            sig = jax.nn.sigmoid(gate)
            swish = gate * sig
            shape = (n.ctx, part_rows, tile)
            r.hid[:, span, at : at + tile] = (swish * up).astype(BF16).reshape(shape)
            r.dgu[:, span, at : at + tile] = (
                (back * up * sig * (1.0 + gate * (1.0 - sig))).astype(BF16).reshape(shape)
            )
            r.dgu[:, span, ff + at : ff + at + tile] = (
                (back * swish).astype(BF16).reshape(shape)
            )
        both = r.dgu[:, span, :].reshape(span_rows, 2 * ff)
        for at in range(0, d, 2 * HEAD_DIM):
            product = mm(both, r.wm[at : at + 2 * HEAD_DIM, : 2 * ff], LAST_AXIS).astype(BF16)
            r.p_x2[:, span, at : at + 2 * HEAD_DIM] = product.reshape(
                n.ctx, part_rows, 2 * HEAD_DIM
            )
        scatter_start(sum_x2, k)

    def residual_back(k):
        span = rows_of(k)
        r.dh[span, :] = jnp.zeros((part_rows, d), F32)
        scatter_total(sum_x2, r.dh, k)
        own = r.ho[span, :]
        from_norm, term = norm_back(own, rms(own), mlp_gain, r.dh[span, :])
        save_lines(n.lines, jnp.sum(term, axis=0, keepdims=True))
        r.dh[span, :] = r.gb[c, span, :].astype(F32) + from_norm
        r.rb[c, span, :] = r.dh[span, :].astype(BF16)
        gather_start(r.rb.at[c], r.rb, r.sem_rb, k)

    gather_relay(r.mb, r.sem_mb, 1, 1, "end")
    gather_relay(r.gb, r.sem_gb, 1, 1)
    for by in range(2, n.ctx - 1):
        gather_relay(r.gb, r.sem_gb, by, 1)
        gather_relay(r.mb, r.sem_mb, by, 1)
    mlp_part(0)
    scatter_near(sum_x2, 0)
    scatter_far(sum_x2, 0)
    gather_relay(r.mb, r.sem_mb, n.ctx - 1, 1)
    gather_relay(r.gb, r.sem_gb, n.ctx - 1, 1)
    mlp_part(1)
    residual_back(0)
    hidden = r.hid[...].reshape(n.tokens, ff)
    by_rows(hidden, lambda span: r.wm[span, 2 * ff :], r.p_y)
    scatter_start(sum_y, 0)
    mixed = r.mb[...].reshape(n.tokens, d)
    upstream = r.gb[...].reshape(n.tokens, d)
    for at in range(0, 2 * ff, tile):
        part = r.dgu[:, :, at : at + tile].reshape(n.tokens, tile)
        r.gm[:, at : at + tile] = mm(mixed, part, FIRST_AXIS).astype(BF16)
    for at in range(0, ff, tile):
        part = r.hid[:, :, at : at + tile].reshape(n.tokens, tile)
        r.gm[:, 2 * ff + at : 2 * ff + at + tile] = mm(upstream, part, FIRST_AXIS).astype(BF16)
    grads_pair(group_m)
    scatter_near(sum_x2, 1)
    gather_relay(r.rb, r.sem_rb, 1, 0, "between")
    grads_plane(group_m)
    scatter_far(sum_x2, 1)
    gather_relay(r.rb, r.sem_rb, 1, 0, "end")
    for by in range(2, n.ctx - 1):
        gather_relay(r.rb, r.sem_rb, by, 0)
    residual_back(1)
    scatter_start(sum_y, 1)
    scatter_near(sum_y, 0)
    gather_relay(r.rb, r.sem_rb, 1, 1, "between")
    gather_relay(r.rb, r.sem_rb, 1, 1, "end")
    for by in range(2, n.ctx - 1):
        gather_relay(r.rb, r.sem_rb, by, 1)
    scatter_far(sum_y, 0)
    for k in range(PARTS):
        gather_relay(r.rb, r.sem_rb, n.ctx - 1, k)

    upstream = r.rb[...].reshape(n.tokens, d)
    for at in range(0, o_cols, HEAD_DIM):
        r.da[at // HEAD_DIM] = mm(upstream, r.wa[:, o_at + at : o_at + at + HEAD_DIM])
    r.ga[:, o_at:] = mm(upstream, r.at[...], FIRST_AXIS).astype(BF16)
    grads_pair(group_o)
    scatter_near(sum_y, 1)
    r.dk[...] = jnp.zeros_like(r.dk)
    r.dv[...] = jnp.zeros_like(r.dv)

    def head_backward(h, carry):
        kv = h // group
        for q0 in (0, half):
            span = slice(q0, q0 + half)
            e = r.es[h, span, :]
            total = jnp.sum(e, axis=-1, keepdims=True)
            da = r.da[h, span, :]
            w = (da / total).astype(BF16)
            dl = jnp.sum(da * r.af[h, span, :], axis=-1, keepdims=True) / total
            ds = (e * (mm(w, r.vv[kv], LAST_AXIS) - dl)).astype(BF16)
            r.ds[span, :] = ds
            r.eb[span, :] = e.astype(BF16)
            r.wb[span, :] = w
            r.da[h, span, :] = mm(ds, r.kr[kv])
        r.dk[kv] = r.dk[kv] + mm(r.ds[...], r.qr[h], FIRST_AXIS)
        r.dv[kv] = r.dv[kv] + mm(r.eb[...], r.wb[...], FIRST_AXIS)
        return carry

    lax.fori_loop(0, n.heads // 2, head_backward, 0)
    grads_line(group_m)
    lax.fori_loop(n.heads // 2, n.heads, head_backward, 0)

    def query_backward(h, term):
        u = r.qp[h]
        du, gain_term = norm_back(
            u, rms(u), qgain, rope_bwd(r.da[h] * factor, cosine[...], sine[...])
        )
        lane = pl.multiple_of(h * HEAD_DIM, HEAD_DIM)
        r.dqkv[:, pl.ds(lane, HEAD_DIM)] = du.astype(BF16)
        return term + jnp.sum(gain_term, axis=0, keepdims=True)

    q_term = lax.fori_loop(0, n.heads, query_backward, jnp.zeros((1, HEAD_DIM), F32))
    grads_plane(group_o)
    k_term = jnp.zeros((1, HEAD_DIM), F32)
    for kv in range(n.kv):
        u = r.kp[kv]
        du, gain_term = norm_back(
            u, rms(u), kgain, rope_bwd(r.dk[kv] * factor, cosine[...], sine[...])
        )
        at = q_cols + kv * HEAD_DIM
        r.dqkv[:, at : at + HEAD_DIM] = du.astype(BF16)
        at += k_cols
        r.dqkv[:, at : at + HEAD_DIM] = r.dv[kv].astype(BF16)
        k_term = k_term + jnp.sum(gain_term, axis=0, keepdims=True)
    by_rows(r.dqkv, lambda span: r.wa[span, :o_at], r.p_x1)
    for k in range(PARTS):
        scatter_start(sum_x1, k)
    for at in range(0, o_at, 2 * HEAD_DIM):
        r.ga[:, at : at + 2 * HEAD_DIM] = mm(
            r.xn[...], r.dqkv[:, at : at + 2 * HEAD_DIM], FIRST_AXIS
        ).astype(BF16)
    grads_pair(group_q)
    for j in range(n.ctx):
        x = r.xb[j].astype(F32)
        share = r.p_x1[j].astype(F32) * (x * rms(x))
        save_lines(0, jnp.sum(share, axis=0, keepdims=True))
    r.g1_acc[3, 2 * n.lines : 2 * n.lines + 1, :] = q_term
    r.g1_acc[3, 2 * n.lines + 1 : 2 * n.lines + 2, :] = k_term
    small_send(r.g1_acc.at[3], r.g1_in, r.sem_g1, "plane")
    grads_plane(group_q)
    scatter_near(sum_x1, 0)
    scatter_far(sum_y, 1)
    scatter_far(sum_x1, 0)
    grads_line(group_o)
    r.g1_acc[1] = small_sum(r.g1_acc.at[3], r.g1_in, r.sem_g1, "plane")
    small_send(r.g1_acc.at[1], r.g1_in, r.sem_g1, "line")
    scatter_near(sum_x1, 1)
    grads_line(group_q)
    scatter_far(sum_x1, 1)
    for k in range(PARTS):
        scatter_total(sum_y, r.ho, k)
    r.out_hidden[...] = r.ho[...].astype(BF16)
    r.out_input[...] = jnp.zeros_like(r.out_input)
    for k in range(PARTS):
        scatter_total(sum_x1, r.out_input, k)
    x = r.xb[c].astype(F32)
    from_norm, _ = norm_back(x, rms(x), attn_gain, r.out_input[...])
    r.out_input[...] = r.dh[...] + from_norm
    grads_wait(group_m)
    grads_wait(group_o)
    grads_wait(group_q)
    r.out_gains[...] = small_sum(r.g1_acc.at[1], r.g1_in, r.sem_g1, "line")
    for buf, sem in ((r.xb, r.sem_xb), (r.gb, r.sem_gb), (r.mb, r.sem_mb), (r.rb, r.sem_rb)):
        gather_sent(buf, sem)
    for g in (sum_o, sum_y, sum_x2, sum_x1):
        scatter_sent(g)
    weights_sent(attn_cols, *to_attn[:2])
    weights_sent(mlp_cols, *to_mlp[:2])
    for wait in sends:
        wait()


def fused(
    ctx,
    fsdp,
    hidden_in,
    block_order,
    cotangent,
    q_weight,
    k_weight,
    v_weight,
    o_weight,
    attn_gain,
    query_gain,
    key_gain,
    mlp_gain,
    gate_weight,
    up_weight,
    down_weight,
):
    shards = (q_weight, k_weight, v_weight, o_weight, gate_weight, up_weight, down_weight)
    n = Sizes(ctx, fsdp, hidden_in.shape[1], shards)
    gains = jnp.concatenate([attn_gain, mlp_gain, query_gain, key_gain]).astype(F32)
    gains = jnp.pad(gains, (0, HEAD_DIM - gains.shape[0])).reshape(1, HEAD_DIM)
    hbm, vmem = pl.BlockSpec(memory_space=pl.ANY), pl.BlockSpec(memory_space=pltpu.VMEM)
    inputs = dict(
        hidden=(hidden_in[0], hbm),
        cot=(cotangent[0], hbm),
        wq=(q_weight, hbm),
        wk=(k_weight, hbm),
        wv=(v_weight, hbm),
        wo=(o_weight, hbm),
        wg=(gate_weight, hbm),
        wu=(up_weight, hbm),
        wd=(down_weight, hbm),
        gains=(gains, vmem),
        order=(block_order, pl.BlockSpec(memory_space=pltpu.SMEM)),
    )
    outputs = dict(
        out_hidden=jax.ShapeDtypeStruct((n.rows, n.width), BF16),
        out_input=jax.ShapeDtypeStruct((n.rows, n.width), F32),
        ga_land=jax.ShapeDtypeStruct((ctx, n.shard, n.attn_cols), BF16),
        gm_land=jax.ShapeDtypeStruct((ctx, n.shard, n.mlp_cols), BF16),
        out_gains=jax.ShapeDtypeStruct((n.gain_rows, HEAD_DIM), F32),
    )
    scratch = scratch_of(n)
    landed = pl.pallas_call(
        functools.partial(layer_kernel, n, [*inputs, *outputs, *scratch]),
        out_shape=tuple(outputs.values()),
        in_specs=[spec for _, spec in inputs.values()],
        out_specs=tuple(vmem for _ in outputs),
        scratch_shapes=list(scratch.values()),
        compiler_params=pltpu.CompilerParams(
            collective_id=0, has_side_effects=True, vmem_limit_bytes=VMEM_LIMIT
        ),
        name="layer",
    )(*[value for value, _ in inputs.values()])

    finals = [(n.rows, n.width, BF16), (n.rows, n.width, F32)]
    finals += [(*s.shape, F32) for s in shards]
    finals += [(1, size, F32) for size in (n.each, n.each, n.few, n.few)]
    result, input_grad, oq, ok, ov, oo, og, ou, od, *gains = pl.pallas_call(
        functools.partial(emit_kernel, n),
        out_shape=tuple(jax.ShapeDtypeStruct(f[:2], f[2]) for f in finals),
        in_specs=[hbm] * (len(outputs) - 1) + [vmem],
        out_specs=tuple(hbm if i < 2 + len(shards) else vmem for i in range(len(finals))),
        scratch_shapes=[
            *(pltpu.VMEM(a.shape, a.dtype) for a in landed[:-1]),
            *(pltpu.VMEM(a.shape, F32) for a in shards),
            pltpu.SemaphoreType.DMA((len(outputs) - 1,)),
            pltpu.SemaphoreType.DMA((2 + len(shards),)),
        ],
        name="emit",
    )(*landed)
    return (
        result[None],
        input_grad[None],
        oq,
        ok,
        ov,
        oo,
        gains[0].reshape(n.each),
        gains[2].reshape(n.few),
        gains[3].reshape(n.few),
        gains[1].reshape(n.each),
        og,
        ou,
        od,
    )


def emit_kernel(n, *refs):
    sources, sums, outs = refs[:4], refs[4], refs[5:18]
    held, wide, in_sem, out_sem = refs[18:22], refs[22:29], refs[29], refs[30]
    loads = [pltpu.make_async_copy(sources[i], held[i], in_sem.at[i]) for i in range(4)]
    stores = []

    def store(src, i):
        copy = pltpu.make_async_copy(src, outs[i], out_sem.at[i])
        copy.start()
        stores.append(copy)

    for i in (3, 2, 1, 0):
        loads[i].start()
    which = 2
    for i, widths, first in ((3, n.cols[4:], 6), (2, n.cols[:4], 2)):
        loads[i].wait()
        land, at, which = held[i], 0, first
        for width in widths:
            out = wide[which - 2]
            for j in range(n.ctx):
                out[:, j * width : (j + 1) * width] = land[j, :, at : at + width].astype(F32)
            store(out, which)
            at += width
            which += 1
    for i in (1, 0):
        loads[i].wait()
        store(held[i], i)
    which = 9
    me = lax.axis_index("fsdp") * n.ctx + lax.axis_index("ctx")
    row, at = me * n.each // HEAD_DIM, lax.rem(me * n.each, HEAD_DIM)
    for out, (line, lane) in zip(
        outs[which:],
        (
            (row, at),
            (n.lines + row, at),
            (2 * n.lines, me * n.few),
            (2 * n.lines + 1, me * n.few),
        ),
    ):
        back = lax.rem(HEAD_DIM - lane, HEAD_DIM)
        out[...] = pltpu.roll(sums[pl.ds(line, 1), :], back, 1)[:, : out.shape[1]]
    for copy in stores:
        copy.wait()


def fits(ctx, fsdp, shard_rows):
    per_tile = HEAD_DIM % (2 * shard_rows) == 0 and HEAD_DIM % (ctx * fsdp) == 0
    return per_tile and shard_rows % 16 == 0 and fsdp % 2 == 0 and KV_HEADS % ctx == 0


def solution(mesh):
    ctx, fsdp = mesh.shape["ctx"], mesh.shape["fsdp"]
    tokens = P("fsdp", "ctx", None)
    matrix = P(("fsdp", "ctx"), None)
    vector = P(("fsdp", "ctx"))
    def step(hidden_in, block_order, cotangent, q_weight, *rest):
        whole = fused if fits(ctx, fsdp, q_weight.shape[0]) else local
        return whole(ctx, fsdp, hidden_in, block_order, cotangent, q_weight, *rest)

    return jax.shard_map(
        step,
        mesh=mesh,
        in_specs=(tokens, P("fsdp", None), tokens)
        + (matrix,) * 4
        + (vector,) * 4
        + (matrix,) * 3,
        out_specs=(tokens,) * 2 + (matrix,) * 4 + (vector,) * 4 + (matrix,) * 3,
        check_vma=False,
    )
```
